32 devices in a mesh: section: 2 (over x), batch: 16 (over z, y, core).
Axes of the slice: x: 2, y: 2, z: 4, core: 2. Of those that a mesh axis runs over, the one named last changes fastest.
Arguments:
- hidden_in: bfloat16 [8192, 1024], P('batch', 'section'), may hold values from -6 to 6
- cotangent: bfloat16 [8192, 1024], P('batch', 'section'), may hold values from -6 to 6
- lengths: int32 [32], P('batch'), may hold values from 30 to 256, as said below
- norm_gain: bfloat16 [2, 1024], P('section', 'batch'), may hold values from 0.099609375 to 1.8984375
- norm_offset: bfloat16 [2, 1024], P('section', 'batch'), may hold values from -1.5 to 1.5
- joint_weight: bfloat16 [2, 1024, 3072], P('section', 'batch'), may hold values from -0.1875 to 0.1875
- output_weight: bfloat16 [2, 1024, 1024], P('section', 'batch'), may hold values from -1.5 to 1.5
- expand_weight: bfloat16 [2, 1024, 4096], P('section', 'batch'), may hold values from -0.1875 to 0.1875
- inner_bias: bfloat16 [2, 4096], P('section', 'batch'), may hold values from -1.5 to 1.5
- contract_weight: bfloat16 [2, 4096, 1024], P('section', 'batch'), may hold values from -0.09375 to 0.09375
- outer_bias: bfloat16 [2, 1024], P('section', 'batch'), may hold values from -1.5 to 1.5
Outputs:
- hidden_out: bfloat16 [8192, 1024], P('batch', 'section')
- input_grad: bfloat16 [8192, 1024], P('batch', 'section')
- gain_grad: float32 [2, 1024], P('section')
- offset_grad: float32 [2, 1024], P('section')
- joint_grad: float32 [2, 1024, 3072], P('section')
- output_grad: float32 [2, 1024, 1024], P('section')
- expand_grad: float32 [2, 1024, 4096], P('section')
- inner_grad: float32 [2, 4096], P('section')
- contract_grad: float32 [2, 4096, 1024], P('section')
- outer_grad: float32 [2, 1024], P('section')
The draws below stay inside these ranges and needn't reach their ends.
Inputs may be any that keep to these rules, and one draw needn't show every extreme that they name: `lengths`: among the 2 proteins of every index of batch, one, which one drawn from the seed, is exactly 256 long.
All inputs are finite; a program needn't handle non-finite values.
Results may differ from the reference program's by a relative error of at most 0.017.
Values may be sent and summed in bfloat16 or wider, within the bound.
A program may use at most 256 MiB of HBM per device.

```python
import jax
import jax.numpy as jnp
from jax import lax

D = 1024
HEADS = 16
HEAD_DIM = 64
ROT = 32
FF = 4096
SLOT = 256
MIN_LEN = 30
SEQ_DEV = 2
TOK_DEV = 512
SEQS = 32
TOKENS = 8192


def draw_lengths(key, part):
    groups = SEQS // SEQ_DEV
    spread = jax.random.randint(jax.random.fold_in(key, 11), (groups, SEQ_DEV), MIN_LEN, SLOT + 1)
    picked = jax.random.randint(jax.random.fold_in(key, 12), (groups, 1), 0, SEQ_DEV)
    columns = jnp.arange(SEQ_DEV)[None, :]
    return jnp.where(columns == picked, SLOT, spread).reshape(SEQS).astype(jnp.int32)


def block_scale(own_key, shape, pieces, low, top_value):
    def one(position, parts):
        steps = jax.random.uniform(jax.random.fold_in(jax.random.fold_in(own_key, 6), position), (parts,), jnp.float32, low / len(pieces), top_value / len(pieces))
        return jnp.repeat(jnp.exp(steps), shape[position] // parts).reshape((-1,) + (1,) * (len(shape) - position - 1))

    factor_of = one(*pieces[0])
    for cut in pieces[1:]:
        factor_of = factor_of * one(*cut)
    return factor_of


def centred(key, extent, scale, reach, shards=(), dtype=jnp.bfloat16):
    entries = jax.random.normal(key, extent, jnp.float32) * scale
    if len(shards) > 0:
        entries = block_scale(key, extent, shards, -0.22, 0.18) * entries
    return jnp.clip(entries, min=-reach, max=reach).astype(dtype)


def setup_inputs(seed: int = 0) -> dict:
    key_list = jax.random.split(jax.random.key(seed), 12)
    hidden_in = centred(key_list[0], (TOKENS, D), 1.0, 6.0, ((0, 16), (1, 2)))
    cotangent = centred(key_list[1], (TOKENS, D), 1.0, 6.0, ((0, 16), (1, 2)))
    lengths = draw_lengths(jax.random.fold_in(key_list[11], 71), 0)
    norm_gain = jnp.clip(1.0 + 0.18 * jax.random.normal(key_list[3], (2, D), jnp.float32), 0.099609375, 1.8984375).astype(jnp.bfloat16)
    norm_offset = centred(key_list[4], (2, D), 0.3, 1.5, ((0, 2), (1, 16)))
    joint_weight = centred(key_list[5], (2, D, 3 * D), D ** -0.5, 0.1875, ((0, 2), (1, 16)))
    output_weight = centred(key_list[6], (2, D, D), (D // 64) ** -0.5, 1.5, ((0, 2), (1, 16)))
    expand_weight = centred(key_list[7], (2, D, FF), D ** -0.5, 0.1875, ((0, 2), (1, 16)))
    inner_bias = centred(key_list[8], (2, FF), 0.3, 1.5, ((0, 2), (1, 16)))
    contract_weight = centred(key_list[9], (2, FF, D), FF ** -0.5, 0.09375, ((0, 2), (1, 16)))
    outer_bias = centred(key_list[10], (2, D), 0.3, 1.5, ((0, 2), (1, 16)))
    return {"hidden_in": hidden_in, "cotangent": cotangent, "lengths": lengths, "norm_gain": norm_gain, "norm_offset": norm_offset, "joint_weight": joint_weight, "output_weight": output_weight, "expand_weight": expand_weight, "inner_bias": inner_bias, "contract_weight": contract_weight, "outer_bias": outer_bias}


@jax.custom_vjp
def low(v):
    return lax.optimization_barrier(v.astype(jnp.bfloat16)).astype(jnp.float32)

@jax.custom_vjp
def low_back(v):
    return v

def low_keep(v):
    return (low(v), None)

def low_pass(kept, grad):
    return (grad,)

def back_keep(v):
    return (v, None)

def back_low(kept, grad):
    return (low(grad),)
low.defvjp(low_keep, low_pass)
low_back.defvjp(back_keep, back_low)
norm_epsilon = 1e-05
rotary_base = 10000.0
masked_score = -1e+30

def matmul(left, right):
    return jnp.dot(left, right, precision=lax.Precision.HIGHEST, preferred_element_type=jnp.float32)

def rotary_tables():
    positions = jnp.arange(SLOT).astype(jnp.float32)
    exponent = jnp.arange(ROT // 2).astype(jnp.float32) * (2.0 / ROT)
    angles = positions[:, None] * (rotary_base ** (-exponent))[None, :]
    return (jnp.cos(angles)[:, None, :], jnp.sin(angles)[:, None, :])

def rotate(tensor, cosine, sine):
    turned = tensor[..., :ROT].reshape(tensor.shape[:-1] + (ROT // 2, 2))
    even_part = turned[..., 0]
    odd_part = turned[..., 1]
    paired = jnp.stack([even_part * cosine - odd_part * sine, odd_part * cosine + even_part * sine], axis=-1)
    return jnp.concatenate([paired.reshape(tensor.shape[:-1] + (ROT,)), tensor[..., ROT:]], axis=-1)

def attend_one(inputs):
    projected, length = inputs
    cosine, sine = rotary_tables()
    heads = projected.reshape(SLOT, 3, HEADS, HEAD_DIM)
    queries = low(rotate(heads[:, 0], cosine, sine))
    keys = low(rotate(heads[:, 1], cosine, sine))
    values = low(heads[:, 2])
    scores = jnp.einsum('qhd,khd->hqk', queries, keys, precision=lax.Precision.HIGHEST)
    scores = low_back(scores * HEAD_DIM ** (-0.5))
    positions = jnp.arange(SLOT)
    allowed = (positions[None, :] <= positions[:, None]) & (positions[None, :] < length)
    scores = jnp.where(allowed[None], scores, masked_score)
    attention = low(jax.nn.softmax(scores, axis=-1))
    mixture = jnp.einsum('hqk,khd->qhd', attention, values, precision=lax.Precision.HIGHEST)
    return mixture.reshape(SLOT, HEADS * HEAD_DIM)

def residual_block(stream, parameters, group_lengths):
    gain, offset, joint, output, expand, inner, contract, outer = parameters
    average = lax.optimization_barrier(jnp.mean(stream, axis=-1, keepdims=True))
    centered = stream - average
    variance = lax.optimization_barrier(jnp.mean(centered * centered, axis=-1, keepdims=True))
    normed = low(centered * lax.rsqrt(variance + norm_epsilon) * gain + offset)
    projected = low_back(matmul(normed, joint))
    per_sequence = projected.reshape(-1, SLOT, 3 * HEADS * HEAD_DIM)
    mixture = lax.map(jax.checkpoint(attend_one), (per_sequence, group_lengths))
    mixture = low_back(low(mixture.reshape(stream.shape)))
    hidden_pre = low_back(matmul(normed, expand) + inner)
    activated = low(jax.nn.gelu(hidden_pre, approximate=True))
    return stream + matmul(mixture, output) + matmul(activated, contract) + outer

def two_layers(stream, layer_one, layer_two, group_lengths):
    middle = residual_block(stream, layer_one, group_lengths)
    middle = low_back(low(middle))
    return residual_block(middle, layer_two, group_lengths)

def stack_add(running, one_part, two_part):
    return running + jnp.stack([one_part, two_part])

def reference(hidden_in, cotangent, lengths, norm_gain, norm_offset, joint_weight, output_weight, expand_weight, inner_bias, contract_weight, outer_bias):
    parameters = tuple((member.astype(jnp.float32) for member in (norm_gain, norm_offset, joint_weight, output_weight, expand_weight, inner_bias, contract_weight, outer_bias)))
    first_params = tuple((member[0] for member in parameters))
    second_params = tuple((member[1] for member in parameters))
    groups = TOKENS // TOK_DEV
    positions = jnp.arange(SLOT)
    valid = (positions[None, :] < lengths[:, None]).astype(jnp.float32).reshape(groups, TOK_DEV, 1)
    streams = hidden_in.astype(jnp.float32).reshape(groups, TOK_DEV, D)
    tangents = cotangent.astype(jnp.float32).reshape(groups, TOK_DEV, D) * valid
    group_lengths = lengths.reshape(groups, SEQ_DEV)

    def accumulate(running, inputs):
        stream, tangent, lengths_here = inputs

        def forward(start, layer_one, layer_two):
            return two_layers(start, layer_one, layer_two, lengths_here)
        result, pullback = jax.vjp(forward, stream, first_params, second_params)
        stream_grad, one_grad, two_grad = pullback(tangent)
        running = jax.tree.map(stack_add, running, one_grad, two_grad)
        return (running, (result.astype(jnp.bfloat16), stream_grad.astype(jnp.bfloat16)))
    initial = tuple((jnp.zeros_like(member) for member in parameters))
    grads, (outputs, stream_grads) = lax.scan(accumulate, initial, (streams, tangents, group_lengths))
    return (outputs.reshape(TOKENS, D), stream_grads.reshape(TOKENS, D), grads[0], grads[1], grads[2], grads[3], grads[4], grads[5], grads[6], grads[7])
```

```python
from functools import partial

import jax
import jax.numpy as jnp
from jax import lax
from jax.experimental import pallas as pl
from jax.experimental.pallas import tpu as pltpu
from jax.sharding import PartitionSpec as P

HEADS = 16
HEAD_DIM = 64
ROT = 32
SLOT = 256
MICRO = 2
SMALL_ROWS = 16
LANES = 128
MESH = pl.DeviceIdType.MESH
ANY = pl.BlockSpec(memory_space=pl.ANY)


class Place:
    def __init__(self):
        index = lax.axis_index("batch")
        self.levels = lax.axis_size("batch") // 4
        self.z, self.y, self.c = index // 4, index // 2 % 2, index % 2

    def at(self, z=None, y=None, c=None):
        z = self.z if z is None else z
        y = self.y if y is None else y
        c = self.c if c is None else c
        return z * 4 + y * 2 + c


def remote(source, target, send, receive, index):
    return pltpu.make_async_remote_copy(
        source, target, send, receive, device_id={"batch": index}, device_id_type=MESH
    )


def greet(here, with_section):
    barrier = pltpu.get_barrier_semaphore()

    def signal(**who):
        pl.semaphore_signal(barrier, inc=1, device_id=who, device_id_type=MESH)

    signal(batch=here.at(y=1 - here.y))
    signal(batch=here.at(c=1 - here.c))
    pl.when(here.z > 0)(lambda: signal(batch=here.at(z=here.z - 1)))
    pl.when(here.z < here.levels - 1)(lambda: signal(batch=here.at(z=here.z + 1)))
    waits = 2
    if with_section:
        signal(section=1 - lax.axis_index("section"))
        waits = 3
    below = jnp.minimum(here.z, 1)
    above = jnp.minimum(here.levels - 1 - here.z, 1)
    pl.semaphore_wait(barrier, waits + below + above)


def spread_semaphores(pieces, levels):
    dma = pltpu.SemaphoreType.DMA
    return [
        dma((pieces,)),
        dma((pieces, levels, 2)),
        dma((pieces, levels)),
        dma((pieces, levels)),
        dma((pieces, levels)),
        dma((pieces, levels, 2)),
        dma((pieces, levels, 2)),
    ]


class Spread:
    def __init__(self, here, owns, outs, semaphores):
        self.here, self.owns, self.outs = here, owns, outs
        (self.keep, self.zs, self.zr, self.ys, self.yr, self.cs, self.cr) = semaphores

    def block(self, p, z, y, c):
        rows = self.outs[p].shape[0] // (4 * self.here.levels)
        start = pl.multiple_of((z * 4 + y * 2 + c) * rows, rows)
        return self.outs[p].at[pl.ds(start, rows), :]

    def along(self, p, z, source, way):
        here = self.here
        target = self.block(p, z, here.y, here.c)
        step = 1 if way == 0 else -1
        return remote(
            source, target, self.zs.at[p, z, way], self.zr.at[p, z], here.at(z=here.z + step)
        )

    def across(self, p, z, source):
        here = self.here
        target = self.block(p, z, here.y, here.c)
        return remote(source, target, self.ys.at[p, z], self.yr.at[p, z], here.at(y=1 - here.y))

    def beside(self, p, z, y, source):
        here = self.here
        target = self.block(p, z, y, here.c)
        return remote(
            source, target, self.cs.at[p, z, y], self.cr.at[p, z, y], here.at(c=1 - here.c)
        )

    def begin(self, p):
        here = self.here
        own, last = self.owns[p], here.levels - 1
        pl.when(here.z < last)(lambda: self.along(p, here.z, own, 0).start())
        pl.when(here.z > 0)(lambda: self.along(p, here.z, own, 1).start())
        self.across(p, here.z, own).start()
        self.beside(p, here.z, here.y, own).start()
        pltpu.make_async_copy(
            own, self.block(p, here.z, here.y, here.c), self.keep.at[p]
        ).start()

    def from_z(self, p, z, way):
        here = self.here
        block = self.block(p, z, here.y, here.c)
        self.along(p, z, block, way).wait_recv()
        more = here.z < here.levels - 1 if way == 0 else here.z > 0
        pl.when(more)(lambda: self.along(p, z, block, way).start())
        self.across(p, z, block).start()
        self.beside(p, z, here.y, block).start()

    def from_y(self, p, z):
        here = self.here
        block = self.block(p, z, 1 - here.y, here.c)
        self.across(p, z, block).wait_recv()
        self.beside(p, z, 1 - here.y, block).start()

    def middle(self):
        here, last = self.here, self.here.levels - 1
        count = len(self.outs)

        def y_events(distance):
            @pl.when(here.z - distance >= 0)
            def _():
                for p in range(count):
                    self.from_y(p, here.z - distance)

            @pl.when((here.z + distance <= last) & (distance > 0))
            def _():
                for p in range(count):
                    self.from_y(p, here.z + distance)

        def step(distance, carry):
            @pl.when(here.z - distance >= 0)
            def _():
                for p in range(count):
                    self.from_z(p, here.z - distance, 0)

            @pl.when(here.z + distance <= last)
            def _():
                for p in range(count):
                    self.from_z(p, here.z + distance, 1)

            y_events(distance - 1)
            return carry

        lax.fori_loop(1, here.levels, step, 0)
        y_events(here.levels - 1)

    def finish(self):
        here, last = self.here, self.here.levels - 1

        def level(z, carry):
            for p in range(len(self.outs)):
                own = self.block(p, z, here.y, here.c)
                for y in range(2):
                    self.beside(p, z, y, own).wait_send()
                    self.beside(p, z, y, own).wait_recv()
                self.across(p, z, own).wait_send()
                pl.when((z <= here.z) & (here.z < last))(
                    lambda p=p, own=own: self.along(p, z, own, 0).wait_send()
                )
                pl.when((z >= here.z) & (here.z > 0))(
                    lambda p=p, own=own: self.along(p, z, own, 1).wait_send()
                )
            return carry

        lax.fori_loop(0, here.levels, level, 0)
        for p in range(len(self.outs)):
            block = self.block(p, here.z, here.y, here.c)
            pltpu.make_async_copy(block, block, self.keep.at[p]).wait()


def gather_kernel(pieces, *refs):
    owns, halves = refs[:pieces], refs[pieces : pieces + 2]
    outs, wholes = refs[pieces + 2 : 2 * pieces + 2], refs[2 * pieces + 2 : 2 * pieces + 4]
    half_send, half_receive, half_keep = refs[2 * pieces + 4 : 2 * pieces + 7]
    here = Place()
    section = lax.axis_index("section")
    greet(here, True)
    spread = Spread(here, owns, outs, refs[2 * pieces + 7 :])
    for p in range(pieces):
        spread.begin(p)
    moves = []
    for i, (half, whole) in enumerate(zip(halves, wholes)):
        width = half.shape[1]
        mine = whole.at[:, pl.ds(pl.multiple_of(section * width, width), width)]
        send = pltpu.make_async_remote_copy(
            half,
            mine,
            half_send.at[i],
            half_receive.at[i],
            device_id={"section": 1 - section},
            device_id_type=MESH,
        )
        keep = pltpu.make_async_copy(half, mine, half_keep.at[i])
        send.start()
        keep.start()
        moves.append((send, keep))
    spread.middle()
    spread.finish()
    for send, keep in moves:
        send.wait()
        keep.wait()


def gather_all(owns, halves, number):
    levels = lax.axis_size("batch") // 4
    pieces = len(owns)
    shapes = [
        jax.ShapeDtypeStruct((own.shape[0] * 4 * levels, own.shape[1]), own.dtype) for own in owns
    ] + [jax.ShapeDtypeStruct((half.shape[0], half.shape[1] * 2), half.dtype) for half in halves]
    dma = pltpu.SemaphoreType.DMA
    results = pl.pallas_call(
        partial(gather_kernel, pieces),
        out_shape=shapes,
        in_specs=[ANY] * (pieces + 2),
        out_specs=[ANY] * (pieces + 2),
        scratch_shapes=[dma((2,)), dma((2,)), dma((2,))] + spread_semaphores(pieces, levels),
        compiler_params=pltpu.CompilerParams(collective_id=number, has_side_effects=True),
        name="gather_weights",
    )(*owns, *halves)
    return results[:pieces], results[pieces:]


def add_rows(target, other):
    rows = target.shape[0]
    step = min(rows, 16)

    def body(i, carry):
        at = pl.ds(pl.multiple_of(i * step, step), step)
        total = target[at, :].astype(jnp.float32) + other[at, :].astype(jnp.float32)
        target[at, :] = total.astype(target.dtype)
        return carry

    lax.fori_loop(0, rows // step, body, 0)


class Reduce:
    def __init__(self, here, partials, mine, beside, across, along, semaphores):
        self.here, self.partials = here, partials
        self.mine, self.sib, self.yb, self.zb = mine, beside, across, along
        (self.ls, self.cs, self.cr, self.ys, self.yr, self.zs, self.zr) = semaphores

    def block(self, p, z, y, c):
        rows = self.partials[p].shape[0] // (4 * self.here.levels)
        start = pl.multiple_of((z * 4 + y * 2 + c) * rows, rows)
        return self.partials[p].at[pl.ds(start, rows), :]

    def load(self, p, z, y):
        return pltpu.make_async_copy(
            self.block(p, z, y, self.here.c), self.mine[p].at[z, y], self.ls.at[p, z, y]
        )

    def to_core(self, p, z, y):
        here = self.here
        return remote(
            self.block(p, z, y, 1 - here.c),
            self.sib[p].at[z, y],
            self.cs.at[p, z, y],
            self.cr.at[p, z, y],
            here.at(c=1 - here.c),
        )

    def to_y(self, p, z):
        here = self.here
        return remote(
            self.mine[p].at[z, 1 - here.y],
            self.yb[p].at[z],
            self.ys.at[p, z],
            self.yr.at[p, z],
            here.at(y=1 - here.y),
        )

    def to_z(self, p, z, way):
        here = self.here
        return remote(
            self.mine[p].at[z, here.y],
            self.zb[p].at[way, z],
            self.zs.at[p, z],
            self.zr.at[p, way, z],
            here.at(z=here.z + (1 if way == 0 else -1)),
        )

    def begin(self, p, z):
        for y in range(2):
            self.to_core(p, z, y).start()
            self.load(p, z, y).start()

    def cores(self, p, z):
        here = self.here
        for y in range(2):
            self.to_core(p, z, y).wait_recv()
            self.load(p, z, y).wait()
            add_rows(self.mine[p].at[z, y], self.sib[p].at[z, y])
        self.to_y(p, z).start()

    def rows(self, p, z):
        self.to_y(p, z).wait_recv()
        add_rows(self.mine[p].at[z, self.here.y], self.yb[p].at[z])

    def arrive(self, p, z, way):
        self.to_z(p, z, way).wait_recv()
        add_rows(self.mine[p].at[z, self.here.y], self.zb[p].at[way, z])

    def both(self, distance, action):
        here, last = self.here, self.here.levels - 1

        @pl.when(here.z + distance <= last)
        def _():
            for p in range(len(self.partials)):
                action(p, here.z + distance, 0)

        @pl.when(here.z - distance >= 0)
        def _():
            for p in range(len(self.partials)):
                action(p, here.z - distance, 1)

    def pass_on(self, p, z, way):
        here, last = self.here, self.here.levels - 1
        self.rows(p, z)
        pl.when(here.z > 0 if way == 0 else here.z < last)(lambda: self.arrive(p, z, way))
        self.to_z(p, z, way).start()

    def run(self):
        here, last = self.here, self.here.levels - 1
        count = len(self.partials)

        def start(i, carry):
            self.both(last - i, lambda p, z, way: self.begin(p, z))
            return carry

        lax.fori_loop(0, last, start, 0)
        for p in range(count):
            self.begin(p, here.z)

        def step(i, carry):
            distance = last - i
            self.both(distance, lambda p, z, way: self.cores(p, z))
            pl.when(i > 0)(lambda: self.both(distance + 1, self.pass_on))
            return carry

        lax.fori_loop(0, last, step, 0)
        for p in range(count):
            self.cores(p, here.z)
        self.both(1, self.pass_on)

    def own(self, p):
        here, last = self.here, self.here.levels - 1
        self.rows(p, here.z)
        pl.when(here.z > 0)(lambda: self.arrive(p, here.z, 0))
        pl.when(here.z < last)(lambda: self.arrive(p, here.z, 1))
        return self.mine[p].at[here.z, here.y]

    def finish(self):
        here = self.here

        def level(z, carry):
            for p in range(len(self.partials)):
                for y in range(2):
                    self.to_core(p, z, y).wait_send()
                self.to_y(p, z).wait_send()
                pl.when(z > here.z)(lambda p=p: self.to_z(p, z, 0).wait_send())
                pl.when(z < here.z)(lambda p=p: self.to_z(p, z, 1).wait_send())
            return carry

        lax.fori_loop(0, here.levels, level, 0)


def reduce_kernel(pieces, *refs):
    partials, outs, rest = refs[:pieces], refs[pieces : 2 * pieces], refs[2 * pieces :]
    mine, beside, across, along = (rest[i * pieces : (i + 1) * pieces] for i in range(4))
    rest = rest[4 * pieces :]
    here = Place()
    greet(here, False)
    reduce = Reduce(here, partials, mine, beside, across, along, rest[:7])
    reduce.run()
    owns = [mine[p].at[here.z, here.y] for p in range(pieces)]
    spread = Spread(here, owns, outs, rest[7:])
    for p in range(pieces):
        reduce.own(p)
        spread.begin(p)
    spread.middle()
    reduce.finish()
    spread.finish()


def reduce_all(partials, number):
    levels = lax.axis_size("batch") // 4
    pieces = len(partials)
    blocks = [(partial.shape[0] // (4 * levels), partial.shape[1]) for partial in partials]
    dma = pltpu.SemaphoreType.DMA
    scratch = []
    for lead in ((levels, 2), (levels, 2), (levels,), (2, levels)):
        scratch += [pltpu.VMEM(lead + block, jnp.bfloat16) for block in blocks]
    scratch += [
        dma((pieces, levels, 2)),
        dma((pieces, levels, 2)),
        dma((pieces, levels, 2)),
        dma((pieces, levels)),
        dma((pieces, levels)),
        dma((pieces, levels)),
        dma((pieces, 2, levels)),
    ] + spread_semaphores(pieces, levels)
    return pl.pallas_call(
        partial(reduce_kernel, pieces),
        out_shape=[jax.ShapeDtypeStruct(part.shape, jnp.bfloat16) for part in partials],
        in_specs=[ANY] * pieces,
        out_specs=[ANY] * pieces,
        scratch_shapes=scratch,
        compiler_params=pltpu.CompilerParams(
            collective_id=number, has_side_effects=True, vmem_limit_bytes=60 * 2**20
        ),
        name="reduce_gradients",
    )(*partials)


norm_epsilon = 1e-05
rotary_base = 10000.0
masked_score = -1e30


def shifted(value, axis, steps):
    count = lax.axis_size(axis)
    initial, last = (max(0, -steps), min(count, count - steps))
    return lax.ppermute(value, axis, [(source, source + steps) for source in range(initial, last)])


def partner(value, axis, bit):
    mask = 2**bit
    pairs = [(source, source ^ mask) for source in range(lax.axis_size(axis))]
    return lax.ppermute(value, axis, pairs)


def pack_small(members):
    flat = jnp.concatenate([member.astype(jnp.float32) for member in members], axis=1)
    flat = jnp.pad(flat, ((0, 0), (0, SMALL_ROWS * LANES - flat.shape[1])))
    return flat.reshape(-1, LANES).astype(jnp.bfloat16)


def unpack_small(packed, widths, devices):
    flat = packed.reshape(devices, -1)
    members, start = [], 0
    for width in widths:
        members.append(flat[:, start : start + width].reshape(-1))
        start += width
    return members


def partial_product(left, right):
    return jnp.dot(left.T, right, preferred_element_type=jnp.float32).astype(jnp.bfloat16)


def rotary_tables():
    positions = jnp.arange(SLOT).astype(jnp.float32)
    exponent = jnp.arange(ROT // 2).astype(jnp.float32) * (2.0 / ROT)
    angles = positions[:, None] * (rotary_base ** (-exponent))[None, :]
    return (jnp.cos(angles)[:, None, :], jnp.sin(angles)[:, None, :])


def rotate(tensor, cosine, sine):
    turned = tensor[..., :ROT].reshape(tensor.shape[:-1] + (ROT // 2, 2))
    even_part = turned[..., 0]
    odd_part = turned[..., 1]
    paired = jnp.stack(
        [even_part * cosine - odd_part * sine, odd_part * cosine + even_part * sine], axis=-1
    )
    return jnp.concatenate([paired.reshape(tensor.shape[:-1] + (ROT,)), tensor[..., ROT:]], axis=-1)


def gelu_tanh(values):
    return jax.nn.gelu(values, approximate=True)


def allowed_keys(lengths_now):
    positions = jnp.arange(SLOT)
    causal = positions[None, :] <= positions[:, None]
    inside = positions[None, None, :] < lengths_now[:, None, None]
    return (causal[None] & inside)[:, None]


def attention_weights(queries, keys, allowed):
    scores = jnp.einsum(
        "sqhd,skhd->shqk", queries, keys, preferred_element_type=jnp.float32
    ) * HEAD_DIM ** (-0.5)
    scores = jnp.where(allowed, scores, masked_score)
    return jax.nn.softmax(scores, axis=-1)


def layer_forward(stream, weights, tables, allowed):
    gain, offset, joint, output, expand, inner, contract, outer = weights
    cosine, sine = tables
    average = jnp.mean(stream, axis=-1, keepdims=True)
    centered = stream - average
    variance = jnp.mean(centered * centered, axis=-1, keepdims=True)
    inverse = lax.rsqrt(variance + norm_epsilon)
    standard = centered * inverse
    normed = (standard * gain.astype(jnp.float32) + offset.astype(jnp.float32)).astype(jnp.bfloat16)
    projected = jnp.dot(normed, joint, preferred_element_type=jnp.float32)
    heads = projected.reshape(-1, SLOT, 3, HEADS, HEAD_DIM)
    queries = rotate(heads[:, :, 0], cosine, sine).astype(jnp.bfloat16)
    keys = rotate(heads[:, :, 1], cosine, sine).astype(jnp.bfloat16)
    values = heads[:, :, 2].astype(jnp.bfloat16)
    attention = attention_weights(queries, keys, allowed).astype(jnp.bfloat16)
    mixture = jnp.einsum("shqk,skhd->sqhd", attention, values, preferred_element_type=jnp.float32)
    mixture = mixture.reshape(stream.shape).astype(jnp.bfloat16)
    hidden_pre = jnp.dot(normed, expand, preferred_element_type=jnp.float32) + inner.astype(
        jnp.float32
    )
    activated = gelu_tanh(hidden_pre).astype(jnp.bfloat16)
    result = stream + jnp.dot(mixture, output, preferred_element_type=jnp.float32)
    result = (
        result
        + jnp.dot(activated, contract, preferred_element_type=jnp.float32)
        + outer.astype(jnp.float32)
    )
    return (
        result,
        (standard, inverse, normed, queries, keys, values, mixture, hidden_pre, activated),
    )


def layer_backward(upstream, stored, weights, tables, allowed):
    gain, offset, joint, output, expand, inner, contract, outer = weights
    cosine, sine = tables
    standard, inverse, normed, queries, keys, values, mixture, hidden_pre, activated = stored
    upstream_low = upstream.astype(jnp.bfloat16)
    outer_grad = jnp.sum(upstream, axis=0)
    activated_grad = jnp.dot(upstream_low, contract.T, preferred_element_type=jnp.float32)
    pullback = jax.vjp(gelu_tanh, hidden_pre)[1]
    pre_grad = pullback(activated_grad)[0].astype(jnp.bfloat16)
    inner_grad = jnp.sum(pre_grad.astype(jnp.float32), axis=0)
    mixture_grad = jnp.dot(upstream_low, output.T, preferred_element_type=jnp.float32)
    mixture_grad = mixture_grad.astype(jnp.bfloat16).reshape(values.shape)
    attention = attention_weights(queries, keys, allowed)
    value_grad = jnp.einsum(
        "shqk,sqhd->skhd",
        attention.astype(jnp.bfloat16),
        mixture_grad,
        preferred_element_type=jnp.float32,
    )
    weight_grad = jnp.einsum(
        "sqhd,skhd->shqk", mixture_grad, values, preferred_element_type=jnp.float32
    )
    score_grad = attention * (
        weight_grad - jnp.sum(attention * weight_grad, axis=-1, keepdims=True)
    )
    score_grad = score_grad.astype(jnp.bfloat16)
    scaling = HEAD_DIM ** (-0.5)
    query_grad = (
        jnp.einsum("shqk,skhd->sqhd", score_grad, keys, preferred_element_type=jnp.float32)
        * scaling
    )
    key_grad = (
        jnp.einsum("shqk,sqhd->skhd", score_grad, queries, preferred_element_type=jnp.float32)
        * scaling
    )
    query_grad = rotate(query_grad, cosine, -sine)
    key_grad = rotate(key_grad, cosine, -sine)
    joint_part = (
        jnp.stack([query_grad, key_grad, value_grad], axis=2)
        .reshape(upstream.shape[0], -1)
        .astype(jnp.bfloat16)
    )
    normed_grad = jnp.dot(joint_part, joint.T, preferred_element_type=jnp.float32)
    normed_grad = normed_grad + jnp.dot(pre_grad, expand.T, preferred_element_type=jnp.float32)
    gain_grad = jnp.sum(normed_grad * standard, axis=0)
    offset_grad = jnp.sum(normed_grad, axis=0)
    scaled_grad = normed_grad * gain.astype(jnp.float32)
    centered_grad = scaled_grad - jnp.mean(scaled_grad, axis=-1, keepdims=True)
    centered_grad = centered_grad - standard * jnp.mean(
        scaled_grad * standard, axis=-1, keepdims=True
    )
    stream_grad = upstream + inverse * centered_grad
    return (
        stream_grad,
        (gain_grad, offset_grad, outer_grad, inner_grad),
        (normed, mixture, activated, upstream_low, pre_grad, joint_part),
    )


def select_section(is_first, early_tree, later_tree):
    return jax.tree.map(partial(jnp.where, is_first), early_tree, later_tree)


def local(
    hidden_in,
    cotangent,
    lengths,
    norm_gain,
    norm_offset,
    joint_weight,
    output_weight,
    expand_weight,
    inner_bias,
    contract_weight,
    outer_bias,
):
    section_index = lax.axis_index("section")
    is_first = section_index == 0
    small_own = pack_small((norm_gain, norm_offset, outer_bias, inner_bias))
    (joint_all, output_all, expand_all, contract_all, small_all), (whole_in, whole_cotangent) = (
        gather_all(
            [joint_weight[0], output_weight[0], expand_weight[0], contract_weight[0], small_own],
            [hidden_in, cotangent],
            1,
        )
    )
    devices = lax.axis_size("batch")
    gain, offset, outer, inner = unpack_small(
        small_all,
        [member.shape[1] for member in (norm_gain, norm_offset, outer_bias, inner_bias)],
        devices,
    )
    weights = (gain, offset, joint_all, output_all, expand_all, inner, contract_all, outer)
    tables = rotary_tables()
    block_rows = whole_in.shape[0] // MICRO
    width = whole_in.shape[1]
    positions = jnp.arange(SLOT)
    valid = (positions[None, :] < lengths[:, None]).astype(jnp.float32).reshape(-1, 1)
    block_lengths = lengths.reshape(MICRO, -1)
    incoming = jnp.zeros((block_rows, width), jnp.bfloat16)
    memory = []
    finished = []
    for moment in range(MICRO + 1):
        first_block = min(moment, MICRO - 1)
        second_block = max(moment - 1, 0)
        block_in = jnp.where(
            is_first, whole_in[first_block * block_rows : (first_block + 1) * block_rows], incoming
        )
        lengths_now = jnp.where(is_first, block_lengths[first_block], block_lengths[second_block])
        result, stored = layer_forward(
            block_in.astype(jnp.float32), weights, tables, allowed_keys(lengths_now)
        )
        result_low = result.astype(jnp.bfloat16)
        if moment >= 1:
            finished.append(result_low)
        if moment < MICRO:
            incoming = shifted(result_low, "section", 1)
        memory.append((stored, lengths_now))
    returning = jnp.zeros((block_rows, width), jnp.bfloat16)
    sums, factors = [], []
    upstream_done = []
    for moment in range(MICRO + 1):
        later_block = min(moment, MICRO - 1)
        active = 1.0 if moment < MICRO else 0.0
        row_start = later_block * block_rows
        from_loss = (
            whole_cotangent[row_start : row_start + block_rows].astype(jnp.float32)
            * valid[row_start : row_start + block_rows]
            * active
        )
        upstream = jnp.where(is_first, returning.astype(jnp.float32), from_loss)
        picked = select_section(
            is_first, memory[max(moment - 1, 0)], memory[min(moment + 1, MICRO)]
        )
        saved_part, lengths_now = picked
        allowed = allowed_keys(lengths_now)
        stored = saved_part
        stream_grad, small, pairs = layer_backward(upstream, stored, weights, tables, allowed)
        sums.append(small)
        factors.append(pairs)
        grad_low = stream_grad.astype(jnp.bfloat16)
        if moment >= 1:
            upstream_done.append(grad_low)
        if moment < MICRO:
            returning = shifted(grad_low, "section", -1)
    normed, mixture, activated, upstream, pre_grad, joint_part = [
        jnp.concatenate(
            [
                jnp.where(is_first, factors[block + 1][i], factors[block][i])
                for block in range(MICRO)
            ]
        )
        for i in range(6)
    ]
    small = [
        sum(jnp.where(is_first, sums[block + 1][i], sums[block][i]) for block in range(MICRO))
        for i in range(4)
    ]
    partials = [
        partial_product(normed, joint_part),
        partial_product(mixture, upstream),
        partial_product(normed, pre_grad),
        partial_product(activated, upstream),
        pack_small([member.reshape(devices, -1) for member in small]),
    ]
    joint_sum, output_sum, expand_sum, contract_sum, small_sum = [
        member.astype(jnp.float32) for member in reduce_all(partials, 2)
    ]
    gain_sum, offset_sum, outer_sum, inner_sum = unpack_small(
        small_sum, [member.shape[0] // devices for member in small], devices
    )
    whole_grads = [
        member[None]
        for member in (
            gain_sum,
            offset_sum,
            joint_sum,
            output_sum,
            expand_sum,
            inner_sum,
            contract_sum,
            outer_sum,
        )
    ]
    final_out = jnp.concatenate(finished, axis=0)
    final_grad = jnp.concatenate(upstream_done, axis=0)
    half_width = width // lax.axis_size("section")
    outgoing = jnp.where(is_first, final_grad[:, half_width:], final_out[:, :half_width])
    arrived = partner(outgoing, "section", 0)
    hidden_out = jnp.where(is_first, arrived, final_out[:, half_width:])
    input_grad = jnp.where(is_first, final_grad[:, :half_width], arrived)
    return (
        hidden_out,
        input_grad,
        whole_grads[0],
        whole_grads[1],
        whole_grads[2],
        whole_grads[3],
        whole_grads[4],
        whole_grads[5],
        whole_grads[6],
        whole_grads[7],
    )


def solution(mesh):
    return jax.shard_map(
        local,
        mesh=mesh,
        in_specs=(
            P("batch", "section"),
            P("batch", "section"),
            P("batch"),
            P("section", "batch"),
            P("section", "batch"),
            P("section", "batch", None),
            P("section", "batch", None),
            P("section", "batch", None),
            P("section", "batch"),
            P("section", "batch", None),
            P("section", "batch"),
        ),
        out_specs=(
            P("batch", "section"),
            P("batch", "section"),
            P("section", None),
            P("section", None),
            P("section", None, None),
            P("section", None, None),
            P("section", None, None),
            P("section", None),
            P("section", None, None),
            P("section", None),
        ),
        check_vma=False,
    )
```

```python
from functools import partial

import jax
import jax.numpy as jnp
import numpy as np
from jax import lax
from jax.experimental import pallas as pl
from jax.experimental.pallas import tpu as pltpu
from jax.sharding import PartitionSpec as P

HEADS = 16
HEAD_DIM = 64
ROT = 32
SLOT = 256
MICRO = 2
SMALL_ROWS = 16
LANES = 128
ROW_STEP = 32
FF_STEP = 1024
JOINT_STEP = 512
GELU_SCALE = (2.0 / np.pi) ** 0.5
GELU_CUBE = 0.044715
norm_epsilon = 1e-05
rotary_base = 10000.0
masked_score = -1e30
MESH = pl.DeviceIdType.MESH
ANY = pl.BlockSpec(memory_space=pl.ANY)


class Place:
    def __init__(self):
        index = lax.axis_index("batch")
        self.levels = lax.axis_size("batch") // 4
        self.z, self.y, self.c = index // 4, index // 2 % 2, index % 2

    def at(self, z=None, y=None, c=None):
        z = self.z if z is None else z
        y = self.y if y is None else y
        c = self.c if c is None else c
        return z * 4 + y * 2 + c


def remote(source, target, send, receive, index):
    return pltpu.make_async_remote_copy(
        source, target, send, receive, device_id={"batch": index}, device_id_type=MESH
    )


def greet(here, with_section):
    barrier = pltpu.get_barrier_semaphore()

    def signal(**who):
        pl.semaphore_signal(barrier, inc=1, device_id=who, device_id_type=MESH)

    signal(batch=here.at(y=1 - here.y))
    signal(batch=here.at(c=1 - here.c))
    pl.when(here.z > 0)(lambda: signal(batch=here.at(z=here.z - 1)))
    pl.when(here.z < here.levels - 1)(lambda: signal(batch=here.at(z=here.z + 1)))
    waits = 2
    if with_section:
        signal(section=1 - lax.axis_index("section"))
        waits = 3
    below = jnp.minimum(here.z, 1)
    above = jnp.minimum(here.levels - 1 - here.z, 1)
    pl.semaphore_wait(barrier, waits + below + above)


def spread_semaphores(pieces, levels):
    dma = pltpu.SemaphoreType.DMA
    return [
        dma((pieces,)),
        dma((pieces, levels, 2)),
        dma((pieces, levels)),
        dma((pieces, levels)),
        dma((pieces, levels)),
        dma((pieces, levels, 2)),
        dma((pieces, levels, 2)),
    ]


class Spread:
    def __init__(self, here, owns, outs, semaphores):
        self.here, self.owns, self.outs = here, owns, outs
        (self.keep, self.zs, self.zr, self.ys, self.yr, self.cs, self.cr) = semaphores

    def block(self, p, z, y, c):
        rows = self.outs[p].shape[0] // (4 * self.here.levels)
        start = pl.multiple_of((z * 4 + y * 2 + c) * rows, rows)
        return self.outs[p].at[pl.ds(start, rows), :]

    def along(self, p, z, source, way):
        here = self.here
        target = self.block(p, z, here.y, here.c)
        step = 1 if way == 0 else -1
        return remote(
            source, target, self.zs.at[p, z, way], self.zr.at[p, z], here.at(z=here.z + step)
        )

    def across(self, p, z, source):
        here = self.here
        target = self.block(p, z, here.y, here.c)
        return remote(source, target, self.ys.at[p, z], self.yr.at[p, z], here.at(y=1 - here.y))

    def beside(self, p, z, y, source):
        here = self.here
        target = self.block(p, z, y, here.c)
        return remote(
            source, target, self.cs.at[p, z, y], self.cr.at[p, z, y], here.at(c=1 - here.c)
        )

    def begin(self, p):
        here = self.here
        own, last = self.owns[p], here.levels - 1
        pl.when(here.z < last)(lambda: self.along(p, here.z, own, 0).start())
        pl.when(here.z > 0)(lambda: self.along(p, here.z, own, 1).start())
        self.across(p, here.z, own).start()
        self.beside(p, here.z, here.y, own).start()
        pltpu.make_async_copy(
            own, self.block(p, here.z, here.y, here.c), self.keep.at[p]
        ).start()

    def from_z(self, p, z, way):
        here = self.here
        block = self.block(p, z, here.y, here.c)
        self.along(p, z, block, way).wait_recv()
        more = here.z < here.levels - 1 if way == 0 else here.z > 0
        pl.when(more)(lambda: self.along(p, z, block, way).start())
        self.across(p, z, block).start()
        self.beside(p, z, here.y, block).start()

    def from_y(self, p, z):
        here = self.here
        block = self.block(p, z, 1 - here.y, here.c)
        self.across(p, z, block).wait_recv()
        self.beside(p, z, 1 - here.y, block).start()

    def middle(self):
        here, last = self.here, self.here.levels - 1
        count = len(self.outs)

        def y_events(distance):
            @pl.when(here.z - distance >= 0)
            def _():
                for p in range(count):
                    self.from_y(p, here.z - distance)

            @pl.when((here.z + distance <= last) & (distance > 0))
            def _():
                for p in range(count):
                    self.from_y(p, here.z + distance)

        def step(distance, carry):
            @pl.when(here.z - distance >= 0)
            def _():
                for p in range(count):
                    self.from_z(p, here.z - distance, 0)

            @pl.when(here.z + distance <= last)
            def _():
                for p in range(count):
                    self.from_z(p, here.z + distance, 1)

            y_events(distance - 1)
            return carry

        lax.fori_loop(1, here.levels, step, 0)
        y_events(here.levels - 1)

    def finish(self):
        here, last = self.here, self.here.levels - 1

        def level(z, carry):
            for p in range(len(self.outs)):
                own = self.block(p, z, here.y, here.c)
                for y in range(2):
                    self.beside(p, z, y, own).wait_send()
                    self.beside(p, z, y, own).wait_recv()
                self.across(p, z, own).wait_send()
                pl.when((z <= here.z) & (here.z < last))(
                    lambda p=p, own=own: self.along(p, z, own, 0).wait_send()
                )
                pl.when((z >= here.z) & (here.z > 0))(
                    lambda p=p, own=own: self.along(p, z, own, 1).wait_send()
                )
            return carry

        lax.fori_loop(0, here.levels, level, 0)
        for p in range(len(self.outs)):
            block = self.block(p, here.z, here.y, here.c)
            pltpu.make_async_copy(block, block, self.keep.at[p]).wait()


def gather_kernel(pieces, *refs):
    owns, halves = refs[:pieces], refs[pieces : pieces + 2]
    outs, wholes = refs[pieces + 2 : 2 * pieces + 2], refs[2 * pieces + 2 : 2 * pieces + 4]
    half_send, half_receive, half_keep = refs[2 * pieces + 4 : 2 * pieces + 7]
    here = Place()
    section = lax.axis_index("section")
    greet(here, True)
    spread = Spread(here, owns, outs, refs[2 * pieces + 7 :])
    for p in range(pieces):
        spread.begin(p)
    moves = []
    for i, (half, whole) in enumerate(zip(halves, wholes)):
        width = half.shape[1]
        mine = whole.at[:, pl.ds(pl.multiple_of(section * width, width), width)]
        send = pltpu.make_async_remote_copy(
            half,
            mine,
            half_send.at[i],
            half_receive.at[i],
            device_id={"section": 1 - section},
            device_id_type=MESH,
        )
        keep = pltpu.make_async_copy(half, mine, half_keep.at[i])
        send.start()
        keep.start()
        moves.append((send, keep))
    spread.middle()
    spread.finish()
    for send, keep in moves:
        send.wait()
        keep.wait()


def gather_all(owns, halves, number):
    levels = lax.axis_size("batch") // 4
    pieces = len(owns)
    shapes = [
        jax.ShapeDtypeStruct((own.shape[0] * 4 * levels, own.shape[1]), own.dtype) for own in owns
    ] + [jax.ShapeDtypeStruct((half.shape[0], half.shape[1] * 2), half.dtype) for half in halves]
    dma = pltpu.SemaphoreType.DMA
    results = pl.pallas_call(
        partial(gather_kernel, pieces),
        out_shape=shapes,
        in_specs=[ANY] * (pieces + 2),
        out_specs=[ANY] * (pieces + 2),
        scratch_shapes=[dma((2,)), dma((2,)), dma((2,))] + spread_semaphores(pieces, levels),
        compiler_params=pltpu.CompilerParams(collective_id=number, has_side_effects=True),
        name="gather_weights",
    )(*owns, *halves)
    return results[:pieces], results[pieces:]


def add_rows(target, other):
    rows = target.shape[0]
    step = min(rows, 16)

    def body(i, carry):
        at = pl.ds(pl.multiple_of(i * step, step), step)
        total = target[at, :].astype(jnp.float32) + other[at, :].astype(jnp.float32)
        target[at, :] = total.astype(target.dtype)
        return carry

    lax.fori_loop(0, rows // step, body, 0)


class Reduce:
    def __init__(self, here, partials, mine, beside, across, along, semaphores):
        self.here, self.partials = here, partials
        self.mine, self.sib, self.yb, self.zb = mine, beside, across, along
        (self.ls, self.cs, self.cr, self.ys, self.yr, self.zs, self.zr) = semaphores

    def block(self, p, z, y, c):
        rows = self.partials[p].shape[0] // (4 * self.here.levels)
        start = pl.multiple_of((z * 4 + y * 2 + c) * rows, rows)
        return self.partials[p].at[pl.ds(start, rows), :]

    def load(self, p, z, y):
        return pltpu.make_async_copy(
            self.block(p, z, y, self.here.c), self.mine[p].at[z, y], self.ls.at[p, z, y]
        )

    def to_core(self, p, z, y):
        here = self.here
        return remote(
            self.block(p, z, y, 1 - here.c),
            self.sib[p].at[z, y],
            self.cs.at[p, z, y],
            self.cr.at[p, z, y],
            here.at(c=1 - here.c),
        )

    def to_y(self, p, z):
        here = self.here
        return remote(
            self.mine[p].at[z, 1 - here.y],
            self.yb[p].at[z],
            self.ys.at[p, z],
            self.yr.at[p, z],
            here.at(y=1 - here.y),
        )

    def to_z(self, p, z, way):
        here = self.here
        return remote(
            self.mine[p].at[z, here.y],
            self.zb[p].at[way, z],
            self.zs.at[p, z],
            self.zr.at[p, way, z],
            here.at(z=here.z + (1 if way == 0 else -1)),
        )

    def begin(self, p, z):
        for y in range(2):
            self.to_core(p, z, y).start()
            self.load(p, z, y).start()

    def cores(self, p, z):
        here = self.here
        for y in range(2):
            self.to_core(p, z, y).wait_recv()
            self.load(p, z, y).wait()
            add_rows(self.mine[p].at[z, y], self.sib[p].at[z, y])
        self.to_y(p, z).start()

    def rows(self, p, z):
        self.to_y(p, z).wait_recv()
        add_rows(self.mine[p].at[z, self.here.y], self.yb[p].at[z])

    def arrive(self, p, z, way):
        self.to_z(p, z, way).wait_recv()
        add_rows(self.mine[p].at[z, self.here.y], self.zb[p].at[way, z])

    def both(self, distance, action):
        here, last = self.here, self.here.levels - 1

        @pl.when(here.z + distance <= last)
        def _():
            for p in range(len(self.partials)):
                action(p, here.z + distance, 0)

        @pl.when(here.z - distance >= 0)
        def _():
            for p in range(len(self.partials)):
                action(p, here.z - distance, 1)

    def pass_on(self, p, z, way):
        here, last = self.here, self.here.levels - 1
        self.rows(p, z)
        pl.when(here.z > 0 if way == 0 else here.z < last)(lambda: self.arrive(p, z, way))
        self.to_z(p, z, way).start()

    def run(self):
        here, last = self.here, self.here.levels - 1
        count = len(self.partials)

        def start(i, carry):
            self.both(last - i, lambda p, z, way: self.begin(p, z))
            return carry

        lax.fori_loop(0, last, start, 0)
        for p in range(count):
            self.begin(p, here.z)

        def step(i, carry):
            distance = last - i
            self.both(distance, lambda p, z, way: self.cores(p, z))
            pl.when(i > 0)(lambda: self.both(distance + 1, self.pass_on))
            return carry

        lax.fori_loop(0, last, step, 0)
        for p in range(count):
            self.cores(p, here.z)
        self.both(1, self.pass_on)

    def own(self, p):
        here, last = self.here, self.here.levels - 1
        self.rows(p, here.z)
        pl.when(here.z > 0)(lambda: self.arrive(p, here.z, 0))
        pl.when(here.z < last)(lambda: self.arrive(p, here.z, 1))
        return self.mine[p].at[here.z, here.y]

    def finish(self):
        here = self.here

        def level(z, carry):
            for p in range(len(self.partials)):
                for y in range(2):
                    self.to_core(p, z, y).wait_send()
                self.to_y(p, z).wait_send()
                pl.when(z > here.z)(lambda p=p: self.to_z(p, z, 0).wait_send())
                pl.when(z < here.z)(lambda p=p: self.to_z(p, z, 1).wait_send())
            return carry

        lax.fori_loop(0, here.levels, level, 0)


def reduce_kernel(pieces, *refs):
    partials, outs, rest = refs[:pieces], refs[pieces : 2 * pieces], refs[2 * pieces :]
    mine, beside, across, along = (rest[i * pieces : (i + 1) * pieces] for i in range(4))
    rest = rest[4 * pieces :]
    here = Place()
    greet(here, False)
    reduce = Reduce(here, partials, mine, beside, across, along, rest[:7])
    reduce.run()
    owns = [mine[p].at[here.z, here.y] for p in range(pieces)]
    spread = Spread(here, owns, outs, rest[7:])
    for p in range(pieces):
        reduce.own(p)
        spread.begin(p)
    spread.middle()
    reduce.finish()
    spread.finish()


def reduce_all(partials, number):
    levels = lax.axis_size("batch") // 4
    pieces = len(partials)
    blocks = [(partial.shape[0] // (4 * levels), partial.shape[1]) for partial in partials]
    dma = pltpu.SemaphoreType.DMA
    scratch = []
    for lead in ((levels, 2), (levels, 2), (levels,), (2, levels)):
        scratch += [pltpu.VMEM(lead + block, jnp.bfloat16) for block in blocks]
    scratch += [
        dma((pieces, levels, 2)),
        dma((pieces, levels, 2)),
        dma((pieces, levels, 2)),
        dma((pieces, levels)),
        dma((pieces, levels)),
        dma((pieces, levels)),
        dma((pieces, 2, levels)),
    ] + spread_semaphores(pieces, levels)
    return pl.pallas_call(
        partial(reduce_kernel, pieces),
        out_shape=[jax.ShapeDtypeStruct(part.shape, jnp.bfloat16) for part in partials],
        in_specs=[ANY] * pieces,
        out_specs=[ANY] * pieces,
        scratch_shapes=scratch,
        compiler_params=pltpu.CompilerParams(
            collective_id=number, has_side_effects=True, vmem_limit_bytes=60 * 2**20
        ),
        name="reduce_gradients",
    )(*partials)


def rotary_rows():
    positions = np.arange(SLOT, dtype=np.float64)[:, None]
    lane = np.arange(2 * HEAD_DIM)[None, :] % HEAD_DIM
    angles = positions * rotary_base ** (-(lane // 2 * 2.0) / ROT)
    turned = lane < ROT
    cosine = np.where(turned, np.cos(angles), 1.0)
    sine = np.where(turned, np.sin(angles), 0.0)
    even = np.where(lane % 2 == 0, sine, 0.0)
    odd = np.where(lane % 2 == 1, sine, 0.0)
    return np.stack([cosine, even, odd]).astype(np.float32)


def turn(pair, tables, back):
    lanes = pair.shape[1]
    following = pltpu.roll(pair, lanes - 1, 1)
    preceding = pltpu.roll(pair, 1, 1)
    side = following * tables[1] - preceding * tables[2]
    return pair * tables[0] + (side if back else -side)


def product(left, right, left_axis=1, right_axis=0):
    return lax.dot_general(
        left, right, (((left_axis,), (right_axis,)), ((), ())), preferred_element_type=jnp.float32
    )


def statistics(rows):
    average = jnp.mean(rows, axis=-1, keepdims=True)
    centered = rows - average
    variance = jnp.mean(centered * centered, axis=-1, keepdims=True)
    inverse = lax.rsqrt(variance + norm_epsilon)
    return centered * inverse, inverse


def low_lanes(width):
    return lax.broadcasted_iota(jnp.int32, (1, width), 1) < HEAD_DIM


def pair_lanes(index):
    return pl.ds(pl.multiple_of(index * 2 * HEAD_DIM, 2 * HEAD_DIM), 2 * HEAD_DIM)


def rows_at(index, step):
    return pl.ds(pl.multiple_of(index * step, step), step)


def forward_block(m, length, loads, refs):
    (x, normed, qkv, attention, mixture, active, slope, total, result) = refs["state"]
    joint, output, expand, contract = refs["weights"]
    gain, offset, outer, inner = refs["vectors"]
    tables = refs["tables"]
    width = x.shape[2]

    def norm(i, carry):
        at = rows_at(i, ROW_STEP)
        standard, _ = statistics(x[m, at, :].astype(jnp.float32))
        normed[m, at, :] = (standard * gain[...] + offset[...]).astype(jnp.bfloat16)
        return carry

    lax.fori_loop(0, SLOT // ROW_STEP, norm, 0)
    loads(0)
    for part in range(3):
        scale = HEAD_DIM**-0.5 if part == 0 else 1.0
        total[...] = product(normed[m], joint[:, part * width : (part + 1) * width])
        if part == 2:
            qkv[m, :, 2 * width :] = total[...].astype(jnp.bfloat16)
        else:

            def rotary(i, carry, part=part, scale=scale):
                pair = turn(total[:, pair_lanes(i)], tables, False)
                at = pair_lanes(i + part * (width // (2 * HEAD_DIM)))
                qkv[m, :, at] = pair.astype(jnp.bfloat16) * jnp.bfloat16(scale)
                return carry

            lax.fori_loop(0, width // (2 * HEAD_DIM), rotary, 0)

    query = lax.broadcasted_iota(jnp.int32, (SLOT, SLOT), 0)
    key = lax.broadcasted_iota(jnp.int32, (SLOT, SLOT), 1)
    allowed = (key <= query) & (key < length)
    pairs = width // (2 * HEAD_DIM)
    low = low_lanes(2 * HEAD_DIM)

    def heads(i, carry):
        queries, keys = qkv[m, :, pair_lanes(i)], qkv[m, :, pair_lanes(i + pairs)]
        values = qkv[m, :, pair_lanes(i + 2 * pairs)]
        mixed = []
        for half in range(2):
            own = jnp.where(low == (half == 0), queries, jnp.zeros_like(queries))
            scores = jnp.where(allowed, product(own, keys, 1, 1), masked_score)
            raised = jnp.exp(scores - jnp.max(scores, axis=-1, keepdims=True))
            share = raised / jnp.sum(raised, axis=-1, keepdims=True)
            share = share.astype(jnp.bfloat16)
            attention[m, 2 * i + half] = share
            mixed.append(product(share, values))
        mixture[m, :, pair_lanes(i)] = jnp.where(low, mixed[0], mixed[1]).astype(jnp.bfloat16)
        return carry

    lax.fori_loop(0, pairs, heads, 0)
    loads(1)
    total[...] = x[m].astype(jnp.float32) + outer[...] + product(mixture[m], output[...])
    loads(2)
    loads(3)

    def hidden(i, carry):
        at = rows_at(i, FF_STEP)
        pre = product(normed[m], expand[:, at]) + inner[:, at]
        square = pre * pre
        bend = jnp.tanh(GELU_SCALE * (pre + GELU_CUBE * (square * pre)))
        lifted = 0.5 * (1.0 + bend)
        slant = (0.5 * GELU_SCALE) * (1.0 + (3.0 * GELU_CUBE) * square)
        slope[m, :, at] = (lifted + pre * (1.0 - bend * bend) * slant).astype(jnp.bfloat16)
        activated = (pre * lifted).astype(jnp.bfloat16)
        active[m, :, at] = activated
        total[...] += product(activated, contract[at, :])
        return carry

    lax.fori_loop(0, slope.shape[2] // FF_STEP, hidden, 0)
    result[m] = total[...].astype(jnp.bfloat16)


def backward_block(m, refs):
    (x, _, qkv, attention, _, _, slope, total, result) = refs["state"]
    joint, output, expand, contract = refs["weights"]
    gain, offset, outer, inner = refs["vectors"]
    upstream, mixture_grad = refs["gradients"]
    gain_sum, offset_sum, outer_sum, inner_sum = refs["sums"]
    tables = refs["tables"]
    width = x.shape[2]
    outer_sum[...] += jnp.sum(upstream[m].astype(jnp.float32), axis=0, keepdims=True)
    mixture_grad[...] = product(upstream[m], output[...], 1, 1).astype(jnp.bfloat16)
    total[...] = jnp.zeros_like(total)

    def hidden(i, carry):
        at = rows_at(i, FF_STEP)
        active_grad = product(upstream[m], contract[at, :], 1, 1)
        pre_grad = (active_grad * slope[m, :, at].astype(jnp.float32)).astype(jnp.bfloat16)
        slope[m, :, at] = pre_grad
        inner_sum[:, at] += jnp.sum(pre_grad.astype(jnp.float32), axis=0, keepdims=True)
        total[...] += product(pre_grad, expand[:, at], 1, 1)
        return carry

    lax.fori_loop(0, slope.shape[2] // FF_STEP, hidden, 0)
    pairs = width // (2 * HEAD_DIM)
    low = low_lanes(2 * HEAD_DIM)

    def heads(i, carry):
        queries, keys = qkv[m, :, pair_lanes(i)], qkv[m, :, pair_lanes(i + pairs)]
        values = qkv[m, :, pair_lanes(i + 2 * pairs)]
        mixed_grad = mixture_grad[:, pair_lanes(i)]
        query_grads, key_grads, value_grads = [], [], []
        for half in range(2):
            share = attention[m, 2 * i + half]
            own = jnp.where(low == (half == 0), mixed_grad, jnp.zeros_like(mixed_grad))
            value_grads.append(product(share, mixed_grad, 0, 0))
            share_grad = product(own, values, 1, 1)
            weight = share.astype(jnp.float32)
            weighted = weight * share_grad
            score_grad = weighted - weight * jnp.sum(weighted, axis=-1, keepdims=True)
            score_grad = score_grad.astype(jnp.bfloat16)
            query_grads.append(product(score_grad, keys))
            key_grads.append(product(score_grad, queries, 0, 0))
        query_grad = jnp.where(low, query_grads[0], query_grads[1]) * HEAD_DIM**-0.5
        key_grad = jnp.where(low, key_grads[0], key_grads[1])
        value_grad = jnp.where(low, value_grads[0], value_grads[1])
        qkv[m, :, pair_lanes(i)] = turn(query_grad, tables, True).astype(jnp.bfloat16)
        qkv[m, :, pair_lanes(i + pairs)] = turn(key_grad, tables, True).astype(jnp.bfloat16)
        qkv[m, :, pair_lanes(i + 2 * pairs)] = value_grad.astype(jnp.bfloat16)
        return carry

    lax.fori_loop(0, pairs, heads, 0)

    def project(i, carry):
        at = rows_at(i, JOINT_STEP)
        total[:, at] += product(qkv[m], joint[at, :], 1, 1)
        return carry

    lax.fori_loop(0, width // JOINT_STEP, project, 0)

    def norm(i, carry):
        at = rows_at(i, ROW_STEP)
        standard, inverse = statistics(x[m, at, :].astype(jnp.float32))
        normed_grad = total[at, :]
        gain_sum[...] += jnp.sum(normed_grad * standard, axis=0, keepdims=True)
        offset_sum[...] += jnp.sum(normed_grad, axis=0, keepdims=True)
        scaled = normed_grad * gain[...]
        inner_mean = jnp.mean(scaled, axis=-1, keepdims=True)
        along = jnp.mean(scaled * standard, axis=-1, keepdims=True)
        change = inverse * (scaled - inner_mean - standard * along)
        result[m, at, :] = (upstream[m, at, :].astype(jnp.float32) + change).astype(jnp.bfloat16)
        return carry

    lax.fori_loop(0, SLOT // ROW_STEP, norm, 0)


BLOCK_OUTPUTS = 12


def blocks_kernel(*refs):
    lengths, whole_in, cotangent, tables_in, gain, offset, outer, inner = refs[:8]
    weight_sources = refs[8:12]
    outs = refs[12:24]
    weights = refs[24:28]
    x, normed, qkv, attention, mixture, active, slope, total, result = refs[28:37]
    upstream, mixture_grad, tables = refs[37:40]
    weight_sem, in_sem, hand_send, hand_receive, half_send, half_receive, half_keep, out_sem = refs[
        40:48
    ]
    hidden_out, input_grad = outs[:2]
    factor_outs, sums = outs[2:8], outs[8:12]
    section = lax.axis_index("section")
    partner = {"section": 1 - section}
    barrier = pltpu.get_barrier_semaphore()
    pl.semaphore_signal(barrier, inc=1, device_id=partner, device_id_type=MESH)
    pl.semaphore_wait(barrier, 1)
    half = hidden_out.shape[1]

    def loading(i):
        return pltpu.make_async_copy(weight_sources[i], weights[i], weight_sem.at[i])

    def taking(source, target, m):
        return pltpu.make_async_copy(source.at[rows_at(m, SLOT), :], target.at[m], in_sem.at[m])

    def handing(target, m):
        return pltpu.make_async_remote_copy(
            result.at[m],
            target.at[m],
            hand_send.at[m],
            hand_receive.at[m],
            device_id=partner,
            device_id_type=MESH,
        )

    def away(target, start, m):
        return pltpu.make_async_remote_copy(
            result.at[m, :, pl.ds(start, half)],
            target.at[rows_at(m, SLOT), :],
            half_send.at[m],
            half_receive.at[m],
            device_id=partner,
            device_id_type=MESH,
        )

    def kept(target, start, m):
        return pltpu.make_async_copy(
            result.at[m, :, pl.ds(start, half)], target.at[rows_at(m, SLOT), :], half_keep.at[m]
        )

    def giving(i, source, m):
        return pltpu.make_async_copy(
            source.at[m], factor_outs[i].at[rows_at(m, SLOT), :], out_sem.at[i, m]
        )

    pltpu.make_async_copy(tables_in, tables, weight_sem.at[4]).start()
    for m in range(MICRO):
        pl.when(section == 0)(lambda m=m: taking(whole_in, x, m).start())
        pl.when(section == 1)(lambda m=m: taking(cotangent, upstream, m).start())
    for i in range(4):
        loading(i).start()
    for total_sum in sums:
        total_sum[...] = jnp.zeros_like(total_sum)
    pltpu.make_async_copy(tables_in, tables, weight_sem.at[4]).wait()
    shared = {
        "state": (x, normed, qkv, attention, mixture, active, slope, total, result),
        "weights": weights,
        "vectors": (gain, offset, outer, inner),
        "tables": tables,
        "gradients": (upstream, mixture_grad),
        "sums": sums,
    }

    def forward(m, carry):
        pl.when(section == 0)(lambda: taking(whole_in, x, m).wait())
        pl.when(section == 1)(lambda: handing(x, m).wait_recv())
        forward_block(
            m, lengths[m], lambda i: pl.when(m == 0)(lambda: loading(i).wait()), shared
        )

        @pl.when(section == 0)
        def _():
            handing(x, m).start()

        @pl.when(section == 1)
        def _():
            away(hidden_out, 0, m).start()
            kept(hidden_out, half, m).start()

        for i, source in enumerate((normed, mixture, active)):
            giving(i, source, m).start()
        return carry

    lax.fori_loop(0, MICRO, forward, 0)

    def backward(m, carry):
        @pl.when(section == 0)
        def _():
            handing(x, m).wait_send()
            handing(upstream, m).wait_recv()

        @pl.when(section == 1)
        def _():
            away(hidden_out, 0, m).wait_send()
            kept(hidden_out, half, m).wait()
            taking(cotangent, upstream, m).wait()
            row = lax.broadcasted_iota(jnp.int32, (SLOT, 1), 0)
            inside = (row < lengths[m]).astype(jnp.float32)
            masked = upstream[m].astype(jnp.float32) * inside
            upstream[m] = masked.astype(jnp.bfloat16)

        backward_block(m, shared)

        @pl.when(section == 1)
        def _():
            handing(upstream, m).start()

        @pl.when(section == 0)
        def _():
            away(input_grad, half, m).start()
            kept(input_grad, 0, m).start()

        for i, source in enumerate((qkv, slope, upstream)):
            giving(3 + i, source, m).start()
        return carry

    lax.fori_loop(0, MICRO, backward, 0)

    def last(m, carry):
        @pl.when(section == 0)
        def _():
            away(input_grad, half, m).wait_send()
            kept(input_grad, 0, m).wait()
            away(hidden_out, 0, m).wait_recv()

        @pl.when(section == 1)
        def _():
            handing(upstream, m).wait_send()
            away(input_grad, half, m).wait_recv()

        for i, source in enumerate((normed, mixture, active, qkv, slope, upstream)):
            giving(i, source, m).wait()
        return carry

    lax.fori_loop(0, MICRO, last, 0)


def run_blocks(lengths, whole_in, cotangent, vectors, weights, number):
    tokens, width = whole_in.shape
    wide = weights[2].shape[1]
    half = width // lax.axis_size("section")
    low, full = jnp.bfloat16, jnp.float32
    shape = jax.ShapeDtypeStruct
    vmem = pltpu.VMEM
    dma = pltpu.SemaphoreType.DMA
    inside = pl.BlockSpec(memory_space=vmem)
    outputs = [shape((tokens, half), low)] * 2
    outputs += [shape((tokens, n), low) for n in (width, width, wide, 3 * width, wide, width)]
    outputs += [shape((1, n), full) for n in (width, width, width, wide)]
    scratch = [vmem(weight.shape, low) for weight in weights]
    scratch += [
        vmem((MICRO, SLOT, width), low),
        vmem((MICRO, SLOT, width), low),
        vmem((MICRO, SLOT, 3 * width), low),
        vmem((MICRO, HEADS, SLOT, SLOT), low),
        vmem((MICRO, SLOT, width), low),
        vmem((MICRO, SLOT, wide), low),
        vmem((MICRO, SLOT, wide), low),
        vmem((SLOT, width), full),
        vmem((MICRO, SLOT, width), low),
        vmem((MICRO, SLOT, width), low),
        vmem((SLOT, width), low),
        vmem((3, SLOT, 2 * HEAD_DIM), full),
        dma((5,)),
        dma((MICRO,)),
        dma((MICRO,)),
        dma((MICRO,)),
        dma((MICRO,)),
        dma((MICRO,)),
        dma((MICRO,)),
        dma((6, MICRO)),
    ]
    vectors = [vector.astype(full).reshape(1, -1) for vector in vectors]
    return pl.pallas_call(
        blocks_kernel,
        out_shape=outputs,
        in_specs=[pl.BlockSpec(memory_space=pltpu.SMEM), ANY, ANY, ANY] + [inside] * 4 + [ANY] * 4,
        out_specs=[ANY] * 8 + [inside] * 4,
        scratch_shapes=scratch,
        compiler_params=pltpu.CompilerParams(
            collective_id=number, has_side_effects=True, vmem_limit_bytes=60 * 2**20
        ),
        name="two_blocks",
    )(lengths, whole_in, cotangent, jnp.asarray(rotary_rows()), *vectors, *weights)


def pack_small(members):
    flat = jnp.concatenate([member.astype(jnp.float32) for member in members], axis=1)
    flat = jnp.pad(flat, ((0, 0), (0, SMALL_ROWS * LANES - flat.shape[1])))
    return flat.reshape(-1, LANES).astype(jnp.bfloat16)


def unpack_small(packed, widths, devices):
    flat = packed.reshape(devices, -1)
    members, start = [], 0
    for width in widths:
        members.append(flat[:, start : start + width].reshape(-1))
        start += width
    return members


def partial_product(left, right):
    return jnp.dot(left.T, right, preferred_element_type=jnp.float32).astype(jnp.bfloat16)


def local(
    hidden_in,
    cotangent,
    lengths,
    norm_gain,
    norm_offset,
    joint_weight,
    output_weight,
    expand_weight,
    inner_bias,
    contract_weight,
    outer_bias,
):
    devices = lax.axis_size("batch")
    vectors_own = (norm_gain, norm_offset, outer_bias, inner_bias)
    (*weights, small_all), (whole_in, whole_cotangent) = gather_all(
        [
            joint_weight[0],
            output_weight[0],
            expand_weight[0],
            contract_weight[0],
            pack_small(vectors_own),
        ],
        [hidden_in, cotangent],
        1,
    )
    vectors = unpack_small(small_all, [member.shape[1] for member in vectors_own], devices)
    results = run_blocks(lengths, whole_in, whole_cotangent, vectors, weights, 2)
    hidden_out, input_grad = results[:2]
    normed, mixture, activated, joint_part, pre_grad, upstream = results[2:8]
    small = results[8:]
    partials = [
        partial_product(normed, joint_part),
        partial_product(mixture, upstream),
        partial_product(normed, pre_grad),
        partial_product(activated, upstream),
        pack_small([member.reshape(devices, -1) for member in small]),
    ]
    joint_sum, output_sum, expand_sum, contract_sum, small_sum = [
        member.astype(jnp.float32) for member in reduce_all(partials, 3)
    ]
    gain_sum, offset_sum, outer_sum, inner_sum = unpack_small(
        small_sum, [member.shape[1] // devices for member in small], devices
    )
    return (
        hidden_out,
        input_grad,
        gain_sum[None],
        offset_sum[None],
        joint_sum[None],
        output_sum[None],
        expand_sum[None],
        inner_sum[None],
        contract_sum[None],
        outer_sum[None],
    )


def solution(mesh):
    return jax.shard_map(
        local,
        mesh=mesh,
        in_specs=(
            P("batch", "section"),
            P("batch", "section"),
            P("batch"),
            P("section", "batch"),
            P("section", "batch"),
            P("section", "batch", None),
            P("section", "batch", None),
            P("section", "batch", None),
            P("section", "batch"),
            P("section", "batch", None),
            P("section", "batch"),
        ),
        out_specs=(
            P("batch", "section"),
            P("batch", "section"),
            P("section", None),
            P("section", None),
            P("section", None, None),
            P("section", None, None),
            P("section", None, None),
            P("section", None),
            P("section", None, None),
            P("section", None),
        ),
        check_vma=False,
    )
```

```python
from functools import partial

import jax
import jax.numpy as jnp
import numpy as np
from jax import lax
from jax.experimental import pallas as pl
from jax.experimental.pallas import tpu as pltpu
from jax.sharding import PartitionSpec as P

HEADS = 16
HEAD_DIM = 64
ROT = 32
SLOT = 256
MICRO = 2
SMALL_ROWS = 16
LANES = 128
ROW_STEP = 256
FF_STEP = 4096
JOINT_STEP = 1024
GELU_SCALE = (2.0 / np.pi) ** 0.5
GELU_CUBE = 0.044715
norm_epsilon = 1e-05
rotary_base = 10000.0
masked_score = -1e30
MESH = pl.DeviceIdType.MESH
ANY = pl.BlockSpec(memory_space=pl.ANY)


class Place:
    def __init__(self):
        index = lax.axis_index("batch")
        self.levels = lax.axis_size("batch") // 4
        self.z, self.y, self.c = index // 4, index // 2 % 2, index % 2

    def at(self, z=None, y=None, c=None):
        z = self.z if z is None else z
        y = self.y if y is None else y
        c = self.c if c is None else c
        return z * 4 + y * 2 + c


def remote(source, target, send, receive, index):
    return pltpu.make_async_remote_copy(
        source, target, send, receive, device_id={"batch": index}, device_id_type=MESH
    )


def greet(here, with_section):
    barrier = pltpu.get_barrier_semaphore()

    def signal(**who):
        pl.semaphore_signal(barrier, inc=1, device_id=who, device_id_type=MESH)

    signal(batch=here.at(y=1 - here.y))
    signal(batch=here.at(c=1 - here.c))
    pl.when(here.z > 0)(lambda: signal(batch=here.at(z=here.z - 1)))
    pl.when(here.z < here.levels - 1)(lambda: signal(batch=here.at(z=here.z + 1)))
    waits = 2
    if with_section:
        signal(section=1 - lax.axis_index("section"))
        waits = 3
    below = jnp.minimum(here.z, 1)
    above = jnp.minimum(here.levels - 1 - here.z, 1)
    pl.semaphore_wait(barrier, waits + below + above)


def spread_semaphores(pieces, levels):
    dma = pltpu.SemaphoreType.DMA
    return [
        dma((pieces,)),
        dma((pieces, levels, 2)),
        dma((pieces, levels)),
        dma((pieces, levels)),
        dma((pieces, levels)),
        dma((pieces, levels, 2)),
        dma((pieces, levels, 2)),
    ]


class Spread:
    def __init__(self, here, owns, outs, semaphores):
        self.here, self.owns, self.outs = here, owns, outs
        (self.keep, self.zs, self.zr, self.ys, self.yr, self.cs, self.cr) = semaphores

    def block(self, p, z, y, c):
        rows = self.outs[p].shape[0] // (4 * self.here.levels)
        start = pl.multiple_of((z * 4 + y * 2 + c) * rows, rows)
        return self.outs[p].at[pl.ds(start, rows), :]

    def along(self, p, z, source, way):
        here = self.here
        target = self.block(p, z, here.y, here.c)
        step = 1 if way == 0 else -1
        return remote(
            source, target, self.zs.at[p, z, way], self.zr.at[p, z], here.at(z=here.z + step)
        )

    def across(self, p, z, source):
        here = self.here
        target = self.block(p, z, here.y, here.c)
        return remote(source, target, self.ys.at[p, z], self.yr.at[p, z], here.at(y=1 - here.y))

    def beside(self, p, z, y, source):
        here = self.here
        target = self.block(p, z, y, here.c)
        return remote(
            source, target, self.cs.at[p, z, y], self.cr.at[p, z, y], here.at(c=1 - here.c)
        )

    def begin(self, p):
        here = self.here
        own, last = self.owns[p], here.levels - 1
        pl.when(here.z < last)(lambda: self.along(p, here.z, own, 0).start())
        pl.when(here.z > 0)(lambda: self.along(p, here.z, own, 1).start())
        self.across(p, here.z, own).start()
        self.beside(p, here.z, here.y, own).start()
        pltpu.make_async_copy(
            own, self.block(p, here.z, here.y, here.c), self.keep.at[p]
        ).start()

    def from_z(self, p, z, way):
        here = self.here
        block = self.block(p, z, here.y, here.c)
        self.along(p, z, block, way).wait_recv()
        more = here.z < here.levels - 1 if way == 0 else here.z > 0
        pl.when(more)(lambda: self.along(p, z, block, way).start())
        self.across(p, z, block).start()
        self.beside(p, z, here.y, block).start()

    def from_y(self, p, z):
        here = self.here
        block = self.block(p, z, 1 - here.y, here.c)
        self.across(p, z, block).wait_recv()
        self.beside(p, z, 1 - here.y, block).start()

    def middle(self):
        here, last = self.here, self.here.levels - 1
        count = len(self.outs)

        def y_events(distance):
            @pl.when(here.z - distance >= 0)
            def _():
                for p in range(count):
                    self.from_y(p, here.z - distance)

            @pl.when((here.z + distance <= last) & (distance > 0))
            def _():
                for p in range(count):
                    self.from_y(p, here.z + distance)

        def step(distance, carry):
            @pl.when(here.z - distance >= 0)
            def _():
                for p in range(count):
                    self.from_z(p, here.z - distance, 0)

            @pl.when(here.z + distance <= last)
            def _():
                for p in range(count):
                    self.from_z(p, here.z + distance, 1)

            y_events(distance - 1)
            return carry

        lax.fori_loop(1, here.levels, step, 0)
        y_events(here.levels - 1)

    def finish(self):
        here, last = self.here, self.here.levels - 1

        def level(z, carry):
            for p in range(len(self.outs)):
                own = self.block(p, z, here.y, here.c)
                for y in range(2):
                    self.beside(p, z, y, own).wait_send()
                    self.beside(p, z, y, own).wait_recv()
                self.across(p, z, own).wait_send()
                pl.when((z <= here.z) & (here.z < last))(
                    lambda p=p, own=own: self.along(p, z, own, 0).wait_send()
                )
                pl.when((z >= here.z) & (here.z > 0))(
                    lambda p=p, own=own: self.along(p, z, own, 1).wait_send()
                )
            return carry

        lax.fori_loop(0, here.levels, level, 0)
        for p in range(len(self.outs)):
            block = self.block(p, here.z, here.y, here.c)
            pltpu.make_async_copy(block, block, self.keep.at[p]).wait()


def gather_kernel(pieces, *refs):
    owns, halves = refs[:pieces], refs[pieces : pieces + 2]
    outs, wholes = refs[pieces + 2 : 2 * pieces + 2], refs[2 * pieces + 2 : 2 * pieces + 4]
    half_send, half_receive, half_keep = refs[2 * pieces + 4 : 2 * pieces + 7]
    here = Place()
    section = lax.axis_index("section")
    greet(here, True)
    spread = Spread(here, owns, outs, refs[2 * pieces + 7 :])
    for p in range(pieces):
        spread.begin(p)
    moves = []
    for i, (half, whole) in enumerate(zip(halves, wholes)):
        width = half.shape[1]
        mine = whole.at[:, pl.ds(pl.multiple_of(section * width, width), width)]
        send = pltpu.make_async_remote_copy(
            half,
            mine,
            half_send.at[i],
            half_receive.at[i],
            device_id={"section": 1 - section},
            device_id_type=MESH,
        )
        keep = pltpu.make_async_copy(half, mine, half_keep.at[i])
        send.start()
        keep.start()
        moves.append((send, keep))
    spread.middle()
    spread.finish()
    for send, keep in moves:
        send.wait()
        keep.wait()


def gather_all(owns, halves, number):
    levels = lax.axis_size("batch") // 4
    pieces = len(owns)
    shapes = [
        jax.ShapeDtypeStruct((own.shape[0] * 4 * levels, own.shape[1]), own.dtype) for own in owns
    ] + [jax.ShapeDtypeStruct((half.shape[0], half.shape[1] * 2), half.dtype) for half in halves]
    dma = pltpu.SemaphoreType.DMA
    results = pl.pallas_call(
        partial(gather_kernel, pieces),
        out_shape=shapes,
        in_specs=[ANY] * (pieces + 2),
        out_specs=[ANY] * (pieces + 2),
        scratch_shapes=[dma((2,)), dma((2,)), dma((2,))] + spread_semaphores(pieces, levels),
        compiler_params=pltpu.CompilerParams(collective_id=number, has_side_effects=True),
        name="gather_weights",
    )(*owns, *halves)
    return results[:pieces], results[pieces:]


def add_rows(target, other):
    rows = target.shape[0]
    step = min(rows, 16)

    def body(i, carry):
        at = pl.ds(pl.multiple_of(i * step, step), step)
        total = target[at, :].astype(jnp.float32) + other[at, :].astype(jnp.float32)
        target[at, :] = total.astype(target.dtype)
        return carry

    lax.fori_loop(0, rows // step, body, 0)


class Reduce:
    def __init__(self, here, partials, mine, beside, across, along, semaphores):
        self.here, self.partials = here, partials
        self.mine, self.sib, self.yb, self.zb = mine, beside, across, along
        (self.ls, self.cs, self.cr, self.ys, self.yr, self.zs, self.zr) = semaphores

    def block(self, p, z, y, c):
        rows = self.partials[p].shape[0] // (4 * self.here.levels)
        start = pl.multiple_of((z * 4 + y * 2 + c) * rows, rows)
        return self.partials[p].at[pl.ds(start, rows), :]

    def load(self, p, z, y):
        return pltpu.make_async_copy(
            self.block(p, z, y, self.here.c), self.mine[p].at[z, y], self.ls.at[p, z, y]
        )

    def to_core(self, p, z, y):
        here = self.here
        return remote(
            self.block(p, z, y, 1 - here.c),
            self.sib[p].at[z, y],
            self.cs.at[p, z, y],
            self.cr.at[p, z, y],
            here.at(c=1 - here.c),
        )

    def to_y(self, p, z):
        here = self.here
        return remote(
            self.mine[p].at[z, 1 - here.y],
            self.yb[p].at[z],
            self.ys.at[p, z],
            self.yr.at[p, z],
            here.at(y=1 - here.y),
        )

    def to_z(self, p, z, way):
        here = self.here
        return remote(
            self.mine[p].at[z, here.y],
            self.zb[p].at[way, z],
            self.zs.at[p, z],
            self.zr.at[p, way, z],
            here.at(z=here.z + (1 if way == 0 else -1)),
        )

    def begin(self, p, z):
        for y in range(2):
            self.to_core(p, z, y).start()
            self.load(p, z, y).start()

    def cores(self, p, z):
        here = self.here
        for y in range(2):
            self.to_core(p, z, y).wait_recv()
            self.load(p, z, y).wait()
            add_rows(self.mine[p].at[z, y], self.sib[p].at[z, y])
        self.to_y(p, z).start()

    def rows(self, p, z):
        self.to_y(p, z).wait_recv()
        add_rows(self.mine[p].at[z, self.here.y], self.yb[p].at[z])

    def arrive(self, p, z, way):
        self.to_z(p, z, way).wait_recv()
        add_rows(self.mine[p].at[z, self.here.y], self.zb[p].at[way, z])

    def both(self, distance, action):
        here, last = self.here, self.here.levels - 1

        @pl.when(here.z + distance <= last)
        def _():
            for p in range(len(self.partials)):
                action(p, here.z + distance, 0)

        @pl.when(here.z - distance >= 0)
        def _():
            for p in range(len(self.partials)):
                action(p, here.z - distance, 1)

    def pass_on(self, p, z, way):
        here, last = self.here, self.here.levels - 1
        self.rows(p, z)
        pl.when(here.z > 0 if way == 0 else here.z < last)(lambda: self.arrive(p, z, way))
        self.to_z(p, z, way).start()

    def run(self):
        here, last = self.here, self.here.levels - 1
        count = len(self.partials)

        def start(i, carry):
            self.both(last - i, lambda p, z, way: self.begin(p, z))
            return carry

        lax.fori_loop(0, last, start, 0)
        for p in range(count):
            self.begin(p, here.z)

        def step(i, carry):
            distance = last - i
            self.both(distance, lambda p, z, way: self.cores(p, z))
            pl.when(i > 0)(lambda: self.both(distance + 1, self.pass_on))
            return carry

        lax.fori_loop(0, last, step, 0)
        for p in range(count):
            self.cores(p, here.z)
        self.both(1, self.pass_on)

    def own(self, p):
        here, last = self.here, self.here.levels - 1
        self.rows(p, here.z)
        pl.when(here.z > 0)(lambda: self.arrive(p, here.z, 0))
        pl.when(here.z < last)(lambda: self.arrive(p, here.z, 1))
        return self.mine[p].at[here.z, here.y]

    def finish(self):
        here = self.here

        def level(z, carry):
            for p in range(len(self.partials)):
                for y in range(2):
                    self.to_core(p, z, y).wait_send()
                self.to_y(p, z).wait_send()
                pl.when(z > here.z)(lambda p=p: self.to_z(p, z, 0).wait_send())
                pl.when(z < here.z)(lambda p=p: self.to_z(p, z, 1).wait_send())
            return carry

        lax.fori_loop(0, here.levels, level, 0)


def reduce_kernel(pieces, *refs):
    partials, outs, rest = refs[:pieces], refs[pieces : 2 * pieces], refs[2 * pieces :]
    mine, beside, across, along = (rest[i * pieces : (i + 1) * pieces] for i in range(4))
    rest = rest[4 * pieces :]
    here = Place()
    greet(here, False)
    reduce = Reduce(here, partials, mine, beside, across, along, rest[:7])
    reduce.run()
    owns = [mine[p].at[here.z, here.y] for p in range(pieces)]
    spread = Spread(here, owns, outs, rest[7:])
    for p in range(pieces):
        reduce.own(p)
        spread.begin(p)
    spread.middle()
    reduce.finish()
    spread.finish()


def reduce_all(partials, number):
    levels = lax.axis_size("batch") // 4
    pieces = len(partials)
    blocks = [(partial.shape[0] // (4 * levels), partial.shape[1]) for partial in partials]
    dma = pltpu.SemaphoreType.DMA
    scratch = []
    for lead in ((levels, 2), (levels, 2), (levels,), (2, levels)):
        scratch += [pltpu.VMEM(lead + block, jnp.bfloat16) for block in blocks]
    scratch += [
        dma((pieces, levels, 2)),
        dma((pieces, levels, 2)),
        dma((pieces, levels, 2)),
        dma((pieces, levels)),
        dma((pieces, levels)),
        dma((pieces, levels)),
        dma((pieces, 2, levels)),
    ] + spread_semaphores(pieces, levels)
    return pl.pallas_call(
        partial(reduce_kernel, pieces),
        out_shape=[jax.ShapeDtypeStruct(part.shape, jnp.bfloat16) for part in partials],
        in_specs=[ANY] * pieces,
        out_specs=[ANY] * pieces,
        scratch_shapes=scratch,
        compiler_params=pltpu.CompilerParams(
            collective_id=number, has_side_effects=True, vmem_limit_bytes=60 * 2**20
        ),
        name="reduce_gradients",
    )(*partials)


def rotary_rows():
    positions = np.arange(SLOT, dtype=np.float64)[:, None]
    lane = np.arange(2 * HEAD_DIM)[None, :] % HEAD_DIM
    angles = positions * rotary_base ** (-(lane // 2 * 2.0) / ROT)
    turned = lane < ROT
    cosine = np.where(turned, np.cos(angles), 1.0)
    sine = np.where(turned, np.sin(angles), 0.0)
    even = np.where(lane % 2 == 0, sine, 0.0)
    odd = np.where(lane % 2 == 1, sine, 0.0)
    return np.stack([cosine, even, odd]).astype(np.float32)


def turn(pair, tables, back):
    lanes = pair.shape[1]
    following = pltpu.roll(pair, lanes - 1, 1)
    preceding = pltpu.roll(pair, 1, 1)
    side = following * tables[1] - preceding * tables[2]
    return pair * tables[0] + (side if back else -side)


def product(left, right, left_axis=1, right_axis=0):
    return lax.dot_general(
        left, right, (((left_axis,), (right_axis,)), ((), ())), preferred_element_type=jnp.float32
    )


def statistics(rows):
    average = jnp.mean(rows, axis=-1, keepdims=True)
    centered = rows - average
    variance = jnp.mean(centered * centered, axis=-1, keepdims=True)
    inverse = lax.rsqrt(variance + norm_epsilon)
    return centered * inverse, inverse


def low_lanes(width):
    return lax.broadcasted_iota(jnp.int32, (1, width), 1) < HEAD_DIM


def pair_lanes(index):
    return pl.ds(pl.multiple_of(index * 2 * HEAD_DIM, 2 * HEAD_DIM), 2 * HEAD_DIM)


def rows_at(index, step):
    return pl.ds(pl.multiple_of(index * step, step), step)


def forward_block(m, length, loads, refs):
    (x, normed, qkv, attention, mixture, active, slope, total, result) = refs["state"]
    joint, output, expand, contract = refs["weights"]
    gain, offset, outer, inner = refs["vectors"]
    tables = refs["tables"]
    width = x.shape[2]

    def norm(i, carry):
        at = rows_at(i, ROW_STEP)
        standard, _ = statistics(x[m, at, :].astype(jnp.float32))
        normed[m, at, :] = (standard * gain[...] + offset[...]).astype(jnp.bfloat16)
        return carry

    lax.fori_loop(0, SLOT // ROW_STEP, norm, 0)
    loads(0)
    for part in range(3):
        scale = HEAD_DIM**-0.5 if part == 0 else 1.0
        total[...] = product(normed[m], joint[:, part * width : (part + 1) * width])
        if part == 2:
            qkv[m, :, 2 * width :] = total[...].astype(jnp.bfloat16)
        else:

            def rotary(i, carry, part=part, scale=scale):
                pair = turn(total[:, pair_lanes(i)], tables, False)
                at = pair_lanes(i + part * (width // (2 * HEAD_DIM)))
                qkv[m, :, at] = pair.astype(jnp.bfloat16) * jnp.bfloat16(scale)
                return carry

            lax.fori_loop(0, width // (2 * HEAD_DIM), rotary, 0)

    query = lax.broadcasted_iota(jnp.int32, (SLOT, SLOT), 0)
    key = lax.broadcasted_iota(jnp.int32, (SLOT, SLOT), 1)
    allowed = (key <= query) & (key < length)
    pairs = width // (2 * HEAD_DIM)
    low = low_lanes(2 * HEAD_DIM)

    def heads(i, carry):
        queries, keys = qkv[m, :, pair_lanes(i)], qkv[m, :, pair_lanes(i + pairs)]
        values = qkv[m, :, pair_lanes(i + 2 * pairs)]
        mixed = []
        for half in range(2):
            own = jnp.where(low == (half == 0), queries, jnp.zeros_like(queries))
            scores = jnp.where(allowed, product(own, keys, 1, 1), masked_score)
            raised = jnp.exp(scores - jnp.max(scores, axis=-1, keepdims=True))
            share = raised * (1.0 / jnp.sum(raised, axis=-1, keepdims=True))
            share = share.astype(jnp.bfloat16)
            attention[m, 2 * i + half] = share
            mixed.append(product(share, values))
        mixture[m, :, pair_lanes(i)] = jnp.where(low, mixed[0], mixed[1]).astype(jnp.bfloat16)
        return carry

    lax.fori_loop(0, pairs, heads, 0, unroll=8)
    loads(1)
    total[...] = x[m].astype(jnp.float32) + outer[...] + product(mixture[m], output[...])
    loads(2)
    loads(3)

    def hidden(i, carry):
        at = rows_at(i, FF_STEP)
        pre = product(normed[m], expand[:, at]) + inner[:, at]
        square = pre * pre
        bend = jnp.tanh(GELU_SCALE * (pre + GELU_CUBE * (square * pre)))
        lifted = 0.5 * (1.0 + bend)
        slant = (0.5 * GELU_SCALE) * (1.0 + (3.0 * GELU_CUBE) * square)
        slope[m, :, at] = (lifted + pre * (1.0 - bend * bend) * slant).astype(jnp.bfloat16)
        activated = (pre * lifted).astype(jnp.bfloat16)
        active[m, :, at] = activated
        total[...] += product(activated, contract[at, :])
        return carry

    lax.fori_loop(0, slope.shape[2] // FF_STEP, hidden, 0)
    result[m] = total[...].astype(jnp.bfloat16)


def backward_block(m, refs):
    (x, _, qkv, attention, _, _, slope, total, result) = refs["state"]
    joint, output, expand, contract = refs["weights"]
    gain, offset, outer, inner = refs["vectors"]
    upstream, mixture_grad = refs["gradients"]
    gain_sum, offset_sum, outer_sum, inner_sum = refs["sums"]
    tables = refs["tables"]
    width = x.shape[2]
    outer_sum[...] += jnp.sum(upstream[m].astype(jnp.float32), axis=0, keepdims=True)
    mixture_grad[...] = product(upstream[m], output[...], 1, 1).astype(jnp.bfloat16)
    total[...] = jnp.zeros_like(total)

    def hidden(i, carry):
        at = rows_at(i, FF_STEP)
        active_grad = product(upstream[m], contract[at, :], 1, 1)
        pre_grad = (active_grad * slope[m, :, at].astype(jnp.float32)).astype(jnp.bfloat16)
        slope[m, :, at] = pre_grad
        inner_sum[:, at] += jnp.sum(pre_grad.astype(jnp.float32), axis=0, keepdims=True)
        total[...] += product(pre_grad, expand[:, at], 1, 1)
        return carry

    lax.fori_loop(0, slope.shape[2] // FF_STEP, hidden, 0)
    pairs = width // (2 * HEAD_DIM)
    low = low_lanes(2 * HEAD_DIM)

    def heads(i, carry):
        queries, keys = qkv[m, :, pair_lanes(i)], qkv[m, :, pair_lanes(i + pairs)]
        values = qkv[m, :, pair_lanes(i + 2 * pairs)]
        mixed_grad = mixture_grad[:, pair_lanes(i)]
        query_grads, key_grads, value_grads = [], [], []
        for half in range(2):
            share = attention[m, 2 * i + half]
            own = jnp.where(low == (half == 0), mixed_grad, jnp.zeros_like(mixed_grad))
            value_grads.append(product(share, mixed_grad, 0, 0))
            share_grad = product(own, values, 1, 1)
            weight = share.astype(jnp.float32)
            weighted = weight * share_grad
            score_grad = weighted - weight * jnp.sum(weighted, axis=-1, keepdims=True)
            score_grad = score_grad.astype(jnp.bfloat16)
            query_grads.append(product(score_grad, keys))
            key_grads.append(product(score_grad, queries, 0, 0))
        query_grad = jnp.where(low, query_grads[0], query_grads[1]) * HEAD_DIM**-0.5
        key_grad = jnp.where(low, key_grads[0], key_grads[1])
        value_grad = jnp.where(low, value_grads[0], value_grads[1])
        qkv[m, :, pair_lanes(i)] = turn(query_grad, tables, True).astype(jnp.bfloat16)
        qkv[m, :, pair_lanes(i + pairs)] = turn(key_grad, tables, True).astype(jnp.bfloat16)
        qkv[m, :, pair_lanes(i + 2 * pairs)] = value_grad.astype(jnp.bfloat16)
        return carry

    lax.fori_loop(0, pairs, heads, 0, unroll=2)

    def project(i, carry):
        at = rows_at(i, JOINT_STEP)
        total[:, at] += product(qkv[m], joint[at, :], 1, 1)
        return carry

    lax.fori_loop(0, width // JOINT_STEP, project, 0)

    def norm(i, carry):
        at = rows_at(i, ROW_STEP)
        standard, inverse = statistics(x[m, at, :].astype(jnp.float32))
        normed_grad = total[at, :]
        gain_sum[...] += jnp.sum(normed_grad * standard, axis=0, keepdims=True)
        offset_sum[...] += jnp.sum(normed_grad, axis=0, keepdims=True)
        scaled = normed_grad * gain[...]
        inner_mean = jnp.mean(scaled, axis=-1, keepdims=True)
        along = jnp.mean(scaled * standard, axis=-1, keepdims=True)
        change = inverse * (scaled - inner_mean - standard * along)
        result[m, at, :] = (upstream[m, at, :].astype(jnp.float32) + change).astype(jnp.bfloat16)
        return carry

    lax.fori_loop(0, SLOT // ROW_STEP, norm, 0)


BLOCK_OUTPUTS = 12


def blocks_kernel(*refs):
    lengths, whole_in, cotangent, tables_in, gain, offset, outer, inner = refs[:8]
    weight_sources = refs[8:12]
    outs = refs[12:24]
    weights = refs[24:28]
    x, normed, qkv, attention, mixture, active, slope, total, result = refs[28:37]
    upstream, mixture_grad, tables = refs[37:40]
    weight_sem, in_sem, hand_send, hand_receive, half_send, half_receive, half_keep, out_sem = refs[
        40:48
    ]
    hidden_out, input_grad = outs[:2]
    factor_outs, sums = outs[2:8], outs[8:12]
    section = lax.axis_index("section")
    partner = {"section": 1 - section}
    barrier = pltpu.get_barrier_semaphore()
    pl.semaphore_signal(barrier, inc=1, device_id=partner, device_id_type=MESH)
    pl.semaphore_wait(barrier, 1)
    half = hidden_out.shape[1]

    def loading(i):
        return pltpu.make_async_copy(weight_sources[i], weights[i], weight_sem.at[i])

    def taking(source, target, m):
        return pltpu.make_async_copy(source.at[rows_at(m, SLOT), :], target.at[m], in_sem.at[m])

    def handing(target, m):
        return pltpu.make_async_remote_copy(
            result.at[m],
            target.at[m],
            hand_send.at[m],
            hand_receive.at[m],
            device_id=partner,
            device_id_type=MESH,
        )

    def away(target, start, m):
        return pltpu.make_async_remote_copy(
            result.at[m, :, pl.ds(start, half)],
            target.at[rows_at(m, SLOT), :],
            half_send.at[m],
            half_receive.at[m],
            device_id=partner,
            device_id_type=MESH,
        )

    def kept(target, start, m):
        return pltpu.make_async_copy(
            result.at[m, :, pl.ds(start, half)], target.at[rows_at(m, SLOT), :], half_keep.at[m]
        )

    def giving(i, source, m):
        return pltpu.make_async_copy(
            source.at[m], factor_outs[i].at[rows_at(m, SLOT), :], out_sem.at[i, m]
        )

    pltpu.make_async_copy(tables_in, tables, weight_sem.at[4]).start()
    for m in range(MICRO):
        pl.when(section == 0)(lambda m=m: taking(whole_in, x, m).start())
        pl.when(section == 1)(lambda m=m: taking(cotangent, upstream, m).start())
    for i in range(4):
        loading(i).start()
    for total_sum in sums:
        total_sum[...] = jnp.zeros_like(total_sum)
    pltpu.make_async_copy(tables_in, tables, weight_sem.at[4]).wait()
    shared = {
        "state": (x, normed, qkv, attention, mixture, active, slope, total, result),
        "weights": weights,
        "vectors": (gain, offset, outer, inner),
        "tables": tables,
        "gradients": (upstream, mixture_grad),
        "sums": sums,
    }

    def forward(m, carry):
        pl.when(section == 0)(lambda: taking(whole_in, x, m).wait())
        pl.when(section == 1)(lambda: handing(x, m).wait_recv())
        forward_block(
            m, lengths[m], lambda i: pl.when(m == 0)(lambda: loading(i).wait()), shared
        )

        @pl.when(section == 0)
        def _():
            handing(x, m).start()

        @pl.when(section == 1)
        def _():
            away(hidden_out, 0, m).start()
            kept(hidden_out, half, m).start()

        for i, source in enumerate((normed, mixture, active)):
            giving(i, source, m).start()
        return carry

    lax.fori_loop(0, MICRO, forward, 0)

    def backward(m, carry):
        @pl.when(section == 0)
        def _():
            handing(x, m).wait_send()
            handing(upstream, m).wait_recv()

        @pl.when(section == 1)
        def _():
            away(hidden_out, 0, m).wait_send()
            kept(hidden_out, half, m).wait()
            taking(cotangent, upstream, m).wait()
            row = lax.broadcasted_iota(jnp.int32, (SLOT, 1), 0)
            inside = (row < lengths[m]).astype(jnp.float32)
            masked = upstream[m].astype(jnp.float32) * inside
            upstream[m] = masked.astype(jnp.bfloat16)

        backward_block(m, shared)

        @pl.when(section == 1)
        def _():
            handing(upstream, m).start()

        @pl.when(section == 0)
        def _():
            away(input_grad, half, m).start()
            kept(input_grad, 0, m).start()

        for i, source in enumerate((qkv, slope, upstream)):
            giving(3 + i, source, m).start()
        return carry

    lax.fori_loop(0, MICRO, backward, 0)

    def last(m, carry):
        @pl.when(section == 0)
        def _():
            away(input_grad, half, m).wait_send()
            kept(input_grad, 0, m).wait()
            away(hidden_out, 0, m).wait_recv()

        @pl.when(section == 1)
        def _():
            handing(upstream, m).wait_send()
            away(input_grad, half, m).wait_recv()

        for i, source in enumerate((normed, mixture, active, qkv, slope, upstream)):
            giving(i, source, m).wait()
        return carry

    lax.fori_loop(0, MICRO, last, 0)


def run_blocks(lengths, whole_in, cotangent, vectors, weights, number):
    tokens, width = whole_in.shape
    wide = weights[2].shape[1]
    half = width // lax.axis_size("section")
    low, full = jnp.bfloat16, jnp.float32
    shape = jax.ShapeDtypeStruct
    vmem = pltpu.VMEM
    dma = pltpu.SemaphoreType.DMA
    inside = pl.BlockSpec(memory_space=vmem)
    outputs = [shape((tokens, half), low)] * 2
    outputs += [shape((tokens, n), low) for n in (width, width, wide, 3 * width, wide, width)]
    outputs += [shape((1, n), full) for n in (width, width, width, wide)]
    scratch = [vmem(weight.shape, low) for weight in weights]
    scratch += [
        vmem((MICRO, SLOT, width), low),
        vmem((MICRO, SLOT, width), low),
        vmem((MICRO, SLOT, 3 * width), low),
        vmem((MICRO, HEADS, SLOT, SLOT), low),
        vmem((MICRO, SLOT, width), low),
        vmem((MICRO, SLOT, wide), low),
        vmem((MICRO, SLOT, wide), low),
        vmem((SLOT, width), full),
        vmem((MICRO, SLOT, width), low),
        vmem((MICRO, SLOT, width), low),
        vmem((SLOT, width), low),
        vmem((3, SLOT, 2 * HEAD_DIM), full),
        dma((5,)),
        dma((MICRO,)),
        dma((MICRO,)),
        dma((MICRO,)),
        dma((MICRO,)),
        dma((MICRO,)),
        dma((MICRO,)),
        dma((6, MICRO)),
    ]
    vectors = [vector.astype(full).reshape(1, -1) for vector in vectors]
    return pl.pallas_call(
        blocks_kernel,
        out_shape=outputs,
        in_specs=[pl.BlockSpec(memory_space=pltpu.SMEM), ANY, ANY, ANY] + [inside] * 4 + [ANY] * 4,
        out_specs=[ANY] * 8 + [inside] * 4,
        scratch_shapes=scratch,
        compiler_params=pltpu.CompilerParams(
            collective_id=number, has_side_effects=True, vmem_limit_bytes=60 * 2**20
        ),
        name="two_blocks",
    )(lengths, whole_in, cotangent, jnp.asarray(rotary_rows()), *vectors, *weights)


def pack_small(members):
    flat = jnp.concatenate([member.astype(jnp.float32) for member in members], axis=1)
    flat = jnp.pad(flat, ((0, 0), (0, SMALL_ROWS * LANES - flat.shape[1])))
    return flat.reshape(-1, LANES).astype(jnp.bfloat16)


def unpack_small(packed, widths, devices):
    flat = packed.reshape(devices, -1)
    members, start = [], 0
    for width in widths:
        members.append(flat[:, start : start + width].reshape(-1))
        start += width
    return members


def partial_product(left, right):
    return jnp.dot(left.T, right, preferred_element_type=jnp.float32).astype(jnp.bfloat16)


def local(
    hidden_in,
    cotangent,
    lengths,
    norm_gain,
    norm_offset,
    joint_weight,
    output_weight,
    expand_weight,
    inner_bias,
    contract_weight,
    outer_bias,
):
    devices = lax.axis_size("batch")
    vectors_own = (norm_gain, norm_offset, outer_bias, inner_bias)
    (*weights, small_all), (whole_in, whole_cotangent) = gather_all(
        [
            joint_weight[0],
            output_weight[0],
            expand_weight[0],
            contract_weight[0],
            pack_small(vectors_own),
        ],
        [hidden_in, cotangent],
        1,
    )
    vectors = unpack_small(small_all, [member.shape[1] for member in vectors_own], devices)
    results = run_blocks(lengths, whole_in, whole_cotangent, vectors, weights, 2)
    hidden_out, input_grad = results[:2]
    normed, mixture, activated, joint_part, pre_grad, upstream = results[2:8]
    small = results[8:]
    partials = [
        partial_product(normed, joint_part),
        partial_product(mixture, upstream),
        partial_product(normed, pre_grad),
        partial_product(activated, upstream),
        pack_small([member.reshape(devices, -1) for member in small]),
    ]
    joint_sum, output_sum, expand_sum, contract_sum, small_sum = [
        member.astype(jnp.float32) for member in reduce_all(partials, 3)
    ]
    gain_sum, offset_sum, outer_sum, inner_sum = unpack_small(
        small_sum, [member.shape[1] // devices for member in small], devices
    )
    return (
        hidden_out,
        input_grad,
        gain_sum[None],
        offset_sum[None],
        joint_sum[None],
        output_sum[None],
        expand_sum[None],
        inner_sum[None],
        contract_sum[None],
        outer_sum[None],
    )


def solution(mesh):
    return jax.shard_map(
        local,
        mesh=mesh,
        in_specs=(
            P("batch", "section"),
            P("batch", "section"),
            P("batch"),
            P("section", "batch"),
            P("section", "batch"),
            P("section", "batch", None),
            P("section", "batch", None),
            P("section", "batch", None),
            P("section", "batch"),
            P("section", "batch", None),
            P("section", "batch"),
        ),
        out_specs=(
            P("batch", "section"),
            P("batch", "section"),
            P("section", None),
            P("section", None),
            P("section", None, None),
            P("section", None, None),
            P("section", None, None),
            P("section", None),
            P("section", None, None),
            P("section", None),
        ),
        check_vma=False,
    )
```

```python
from functools import partial

import jax
import jax.numpy as jnp
import numpy as np
from jax import lax
from jax.experimental import pallas as pl
from jax.experimental.pallas import tpu as pltpu
from jax.sharding import PartitionSpec as P

HEADS = 16
HEAD_DIM = 64
ROT = 32
SLOT = 256
MICRO = 2
SMALL_ROWS = 16
LANES = 128
ROW_STEP = 256
FF_STEP = 4096
JOINT_STEP = 1024
GELU_SCALE = (2.0 / np.pi) ** 0.5
GELU_CUBE = 0.044715
norm_epsilon = 1e-05
rotary_base = 10000.0
masked_score = -1e30
MESH = pl.DeviceIdType.MESH
ANY = pl.BlockSpec(memory_space=pl.ANY)


class Place:
    def __init__(self):
        index = lax.axis_index("batch")
        self.levels = lax.axis_size("batch") // 4
        self.last = self.levels - 1
        self.z, self.y, self.c = index // 4, index // 2 % 2, index % 2

    def at(self, z=None, y=None, c=None):
        z = self.z if z is None else z
        y = self.y if y is None else y
        c = self.c if c is None else c
        return z * 4 + y * 2 + c


class Piece:
    def __init__(self, array, offset, rows, columns, direct):
        self.array, self.offset, self.rows, self.columns = array, offset, rows, columns
        self.direct = direct

    def sides(self, y):
        return (y,) if self.direct else (y, 1 - y)


def pieces_of(blocks):
    joint, output, expand, contract, small = blocks
    cut = contract[0] // 4
    return [
        Piece(1, 0, *output, False),
        Piece(3, 0, cut, contract[1], False),
        Piece(0, 0, *joint, True),
        Piece(2, 0, *expand, True),
        Piece(3, cut, contract[0] - cut, contract[1], True),
        Piece(4, 0, *small, True),
    ]


def remote(source, target, send, receive, index):
    return pltpu.make_async_remote_copy(
        source, target, send, receive, device_id={"batch": index}, device_id_type=MESH
    )


def greet(here, with_section):
    barrier = pltpu.get_barrier_semaphore()

    def signal(**who):
        pl.semaphore_signal(barrier, inc=1, device_id=who, device_id_type=MESH)

    signal(batch=here.at(y=1 - here.y))
    signal(batch=here.at(c=1 - here.c))
    pl.when(here.z > 0)(lambda: signal(batch=here.at(z=here.z - 1)))
    pl.when(here.z < here.last)(lambda: signal(batch=here.at(z=here.z + 1)))
    waits = 2
    if with_section:
        signal(section=1 - lax.axis_index("section"))
        waits = 3
    below = jnp.minimum(here.z, 1)
    above = jnp.minimum(here.last - here.z, 1)
    pl.semaphore_wait(barrier, waits + below + above)


def spread_semaphores(count, levels):
    dma = pltpu.SemaphoreType.DMA
    return [
        dma((count,)),
        dma((count, levels, 2, 2)),
        dma((count, levels, 2)),
        dma((count, levels)),
        dma((count, levels)),
        dma((count, levels, 2)),
        dma((count, levels, 2)),
    ]


class Spread:
    def __init__(self, here, pieces, owns, outs, semaphores):
        self.here, self.pieces, self.owns, self.outs = here, pieces, owns, outs
        (self.keep, self.zs, self.zr, self.ys, self.yr, self.cs, self.cr) = semaphores

    def block(self, p, z, y, c):
        piece = self.pieces[p]
        out = self.outs[piece.array]
        rows = out.shape[0] // (4 * self.here.levels)
        start = (z * 4 + y * 2 + c) * rows + piece.offset
        return out.at[pl.ds(pl.multiple_of(start, 8), piece.rows), :]

    def along(self, p, z, y, source, way):
        here = self.here
        return remote(
            source,
            self.block(p, z, y, here.c),
            self.zs.at[p, z, y, way],
            self.zr.at[p, z, y],
            here.at(z=here.z + (1 if way == 0 else -1)),
        )

    def across(self, p, z, source):
        here = self.here
        target = self.block(p, z, here.y, here.c)
        return remote(source, target, self.ys.at[p, z], self.yr.at[p, z], here.at(y=1 - here.y))

    def beside(self, p, z, y, source):
        here = self.here
        target = self.block(p, z, y, here.c)
        return remote(
            source, target, self.cs.at[p, z, y], self.cr.at[p, z, y], here.at(c=1 - here.c)
        )

    def both_ways(self, p, y, source):
        here = self.here
        pl.when(here.z < here.last)(lambda: self.along(p, here.z, y, source, 0).start())
        pl.when(here.z > 0)(lambda: self.along(p, here.z, y, source, 1).start())

    def begin(self, p):
        here, own = self.here, self.owns[p]
        self.across(p, here.z, own).start()
        self.both_ways(p, here.y, own)
        self.beside(p, here.z, here.y, own).start()
        target = self.block(p, here.z, here.y, here.c)
        pltpu.make_async_copy(own, target, self.keep.at[p]).start()

    def from_z(self, p, z, y, way):
        here = self.here
        block = self.block(p, z, y, here.c)
        self.along(p, z, y, block, way).wait_recv()
        more = here.z < here.last if way == 0 else here.z > 0
        pl.when(more)(lambda: self.along(p, z, y, block, way).start())
        if self.pieces[p].direct:
            self.across(p, z, block).start()
        self.beside(p, z, y, block).start()

    def from_y(self, p, z):
        here = self.here
        block = self.block(p, z, 1 - here.y, here.c)
        self.across(p, z, block).wait_recv()
        if not self.pieces[p].direct:
            self.both_ways(p, 1 - here.y, block)
        self.beside(p, z, 1 - here.y, block).start()

    def swap(self):
        for p, piece in enumerate(self.pieces):
            if not piece.direct:
                self.from_y(p, self.here.z)

    def z_events(self, z, way):
        here = self.here
        for p in range(len(self.pieces)):
            self.from_z(p, z, here.y, way)
        for p, piece in enumerate(self.pieces):
            if not piece.direct:
                self.from_z(p, z, 1 - here.y, way)

    def y_events(self, z):
        for p, piece in enumerate(self.pieces):
            if piece.direct:
                self.from_y(p, z)

    def middle(self):
        here = self.here

        def y_pair(distance):
            pl.when(here.z - distance >= 0)(lambda: self.y_events(here.z - distance))
            pl.when((here.z + distance <= here.last) & (distance > 0))(
                lambda: self.y_events(here.z + distance)
            )

        def step(distance, carry):
            pl.when(here.z - distance >= 0)(lambda: self.z_events(here.z - distance, 0))
            pl.when(here.z + distance <= here.last)(lambda: self.z_events(here.z + distance, 1))
            y_pair(distance - 1)
            return carry

        lax.fori_loop(1, here.levels, step, 0)
        y_pair(here.last)

    def finish(self):
        here = self.here

        def level(z, carry):
            for p, piece in enumerate(self.pieces):
                own = self.block(p, z, here.y, here.c)
                for y in range(2):
                    self.beside(p, z, y, own).wait_send()
                    self.beside(p, z, y, own).wait_recv()
                crossed = z >= 0 if piece.direct else z == here.z
                pl.when(crossed)(lambda p=p, own=own: self.across(p, z, own).wait_send())
                for y in piece.sides(here.y):
                    pl.when((z <= here.z) & (here.z < here.last))(
                        lambda p=p, y=y, own=own: self.along(p, z, y, own, 0).wait_send()
                    )
                    pl.when((z >= here.z) & (here.z > 0))(
                        lambda p=p, y=y, own=own: self.along(p, z, y, own, 1).wait_send()
                    )
            return carry

        lax.fori_loop(0, here.levels, level, 0)
        for p in range(len(self.pieces)):
            block = self.block(p, here.z, here.y, here.c)
            pltpu.make_async_copy(block, block, self.keep.at[p]).wait()


def gather_kernel(pieces, *refs):
    sources, halves, outs, wholes = refs[:5], refs[5:7], refs[7:12], refs[12:14]
    half_send, half_receive, half_keep = refs[14:17]
    here = Place()
    section = lax.axis_index("section")
    greet(here, True)
    owns = [sources[piece.array].at[pl.ds(piece.offset, piece.rows), :] for piece in pieces]
    spread = Spread(here, pieces, owns, outs, refs[17:])
    for p in range(len(pieces)):
        spread.begin(p)
    moves = []
    for i, (half, whole) in enumerate(zip(halves, wholes)):
        width = half.shape[1]
        mine = whole.at[:, pl.ds(pl.multiple_of(section * width, width), width)]
        send = pltpu.make_async_remote_copy(
            half,
            mine,
            half_send.at[i],
            half_receive.at[i],
            device_id={"section": 1 - section},
            device_id_type=MESH,
        )
        keep = pltpu.make_async_copy(half, mine, half_keep.at[i])
        send.start()
        keep.start()
        moves.append((send, keep))
    spread.swap()
    spread.middle()
    spread.finish()
    for send, keep in moves:
        send.wait()
        keep.wait()


def gather_all(owns, halves, number):
    levels = lax.axis_size("batch") // 4
    pieces = pieces_of([own.shape for own in owns])
    shapes = [
        jax.ShapeDtypeStruct((own.shape[0] * 4 * levels, own.shape[1]), own.dtype) for own in owns
    ] + [jax.ShapeDtypeStruct((half.shape[0], half.shape[1] * 2), half.dtype) for half in halves]
    dma = pltpu.SemaphoreType.DMA
    results = pl.pallas_call(
        partial(gather_kernel, pieces),
        out_shape=shapes,
        in_specs=[ANY] * 7,
        out_specs=[ANY] * 7,
        scratch_shapes=[dma((2,)), dma((2,)), dma((2,))] + spread_semaphores(len(pieces), levels),
        compiler_params=pltpu.CompilerParams(collective_id=number, has_side_effects=True),
        name="gather_weights",
    )(*owns, *halves)
    return results[:5], results[5:]


def add_rows(target, other):
    rows = target.shape[0]
    step = min(rows, 16)

    def body(i, carry):
        at = pl.ds(pl.multiple_of(i * step, step), step)
        total = target[at, :].astype(jnp.float32) + other[at, :].astype(jnp.float32)
        target[at, :] = total.astype(target.dtype)
        return carry

    lax.fori_loop(0, rows // step, body, 0)


FACTORS = ((0, 3), (1, 5), (0, 4), (2, 5))
MAKE_ORDER = (1, 3, 0, 2, 4)
COLUMN_STEP = 1024


class Reduce:
    def __init__(self, here, pieces, factors, small, product_rows, buffers, semaphores):
        self.here, self.pieces, self.factors, self.small = here, pieces, factors, small
        self.made = product_rows
        self.mine, self.sent, self.sib, self.yb, self.zb = buffers
        (self.load, self.cs, self.cr, self.ys, self.yr, self.zs, self.zr, self.credit) = semaphores

    def level(self, i):
        here = self.here
        above, below = here.last - here.z, here.z
        lead = jnp.maximum(above, below) - jnp.minimum(above, below)
        single = jnp.where(above > below, here.last - i, i)
        later = i - lead
        distance = jnp.minimum(above, below) - later // 2
        paired = jnp.where(later % 2 == 0, here.z + distance, here.z - distance)
        return jnp.where(i < lead, single, paired)

    def to_core(self, p, slot, y):
        here = self.here
        return remote(
            self.sent[p].at[slot, y],
            self.sib[p].at[slot, y],
            self.cs.at[p, slot, y],
            self.cr.at[p, slot, y],
            here.at(c=1 - here.c),
        )

    def to_y(self, p, z):
        here = self.here
        return remote(
            self.mine[p].at[z, 1 - here.y],
            self.yb[p].at[z if self.pieces[p].direct else 0],
            self.ys.at[p, z],
            self.yr.at[p, z],
            here.at(y=1 - here.y),
        )

    def slot(self, z, at_z, way):
        if way == 0:
            return z
        return jnp.where(z == at_z, self.here.levels, z)

    def to_z(self, p, z, y, way):
        here = self.here
        step = 1 if way == 0 else -1
        slot = self.slot(z, here.z + step, way)
        side = 0 if self.pieces[p].direct else y
        return remote(
            self.mine[p].at[z, y],
            self.zb[p].at[slot, side],
            self.zs.at[p, z, side],
            self.zr.at[p, slot, side],
            here.at(z=here.z + step),
        )

    def arrive(self, p, z, y, way):
        here = self.here
        slot = self.slot(z, here.z, way)
        side = 0 if self.pieces[p].direct else y
        block = self.zb[p].at[slot, side]
        remote(
            block, block, self.zs.at[p, z, side], self.zr.at[p, slot, side], here.at(y=1 - here.y)
        ).wait_recv()
        add_rows(self.mine[p].at[z, y], block)

    def store(self, array, z, slot, y, own, value, column):
        at = pl.ds(column, value.shape[1])
        for p, piece in enumerate(self.pieces):
            if piece.array == array:
                target = self.mine[p].at[z, y] if own else self.sent[p].at[slot, y]
                rows = value[piece.offset : piece.offset + piece.rows]
                target[:, at] = rows.astype(jnp.bfloat16)

    def make(self, array, z, slot):
        here = self.here
        rows = sum(piece.rows for piece in self.pieces if piece.array == array)
        cores = ((False, 1 - here.c), (True, here.c))
        if array == 4:
            for own, c in cores:
                for y in range(2):
                    at = pl.multiple_of((z * 4 + y * 2 + c) * rows, 16)
                    self.store(array, z, slot, y, own, self.small[pl.ds(at, rows), :], 0)
            return
        left, right = (self.factors[i] for i in FACTORS[array])
        columns = right.shape[1]
        tiles = range(0, columns, COLUMN_STEP)
        if rows % 128 == 0:
            for own, c in cores:
                for y in range(2):
                    at = pl.multiple_of((z * 4 + y * 2 + c) * rows, 128)
                    turned = left[:, pl.ds(at, rows)].T
                    for tile in tiles:
                        value = product(turned, right[:, tile : tile + COLUMN_STEP])
                        self.store(array, z, slot, y, own, value, tile)
            return
        span = max(4 * rows, 128)
        start = z * 4 * rows // span * span
        turned = left[:, pl.ds(pl.multiple_of(start, 128), span)].T
        for tile in tiles:
            self.made[:span, :] = product(turned, right[:, tile : tile + COLUMN_STEP])
            for own, c in cores:
                for y in range(2):
                    at = pl.multiple_of((z * 4 + y * 2 + c) * rows - start, 8)
                    self.store(array, z, slot, y, own, self.made[pl.ds(at, rows), :], tile)

    def of(self, array):
        return [p for p, piece in enumerate(self.pieces) if piece.array == array]

    def build(self, i, waits):
        here = self.here
        z, slot = self.level(i), i % 2

        @pl.when(i >= 2)
        def _():
            for p in range(len(self.pieces)):
                for y in range(2):
                    self.to_core(p, slot, y).wait_send()
            pl.semaphore_wait(self.credit, 1)

        def add(array):
            for p in self.of(array):
                for y in range(2):
                    self.to_core(p, slot, y).wait_recv()
                    add_rows(self.mine[p].at[z, y], self.sib[p].at[slot, y])
                if self.pieces[p].direct:
                    self.to_y(p, z).start()

        for step, array in enumerate(MAKE_ORDER):
            waits(i, array)
            self.make(array, z, slot)
            for p in self.of(array):
                for y in range(2):
                    self.to_core(p, slot, y).start()
            if step > 0:
                add(MAKE_ORDER[step - 1])
        add(MAKE_ORDER[-1])

        @pl.when(i < here.levels - 2)
        def _():
            other = {"batch": here.at(c=1 - here.c)}
            pl.semaphore_signal(self.credit, inc=1, device_id=other, device_id_type=MESH)

    def rows(self, p, z):
        self.to_y(p, z).wait_recv()
        source = self.yb[p].at[z if self.pieces[p].direct else 0]
        add_rows(self.mine[p].at[z, self.here.y], source)

    def pass_on(self, z):
        here = self.here

        def hop(way):
            further = here.z > 0 if way == 0 else here.z < here.last
            for direct in (False, True):
                for p, piece in enumerate(self.pieces):
                    if piece.direct != direct:
                        continue
                    if direct:
                        self.rows(p, z)
                    for y in piece.sides(here.y):
                        pl.when(further)(lambda p=p, y=y: self.arrive(p, z, y, way))
                        self.to_z(p, z, y, way).start()

        pl.when(z > here.z)(lambda: hop(0))
        pl.when(z < here.z)(lambda: hop(1))

    def run(self, waits):
        here = self.here

        def step(i, carry):
            self.build(i, waits)
            pl.when(i > 0)(lambda: self.pass_on(self.level(i - 1)))
            return carry

        lax.fori_loop(0, here.levels, step, 0)

    def settle(self, p):
        here = self.here
        for y in self.pieces[p].sides(here.y):
            pl.when(here.z > 0)(lambda y=y: self.arrive(p, here.z, y, 0))
            pl.when(here.z < here.last)(lambda y=y: self.arrive(p, here.z, y, 1))

    def finish(self):
        here = self.here
        for slot in range(min(2, here.levels)):
            for p in range(len(self.pieces)):
                for y in range(2):
                    self.to_core(p, slot, y).wait_send()

        def level(z, carry):
            for p, piece in enumerate(self.pieces):
                crossed = z >= 0 if piece.direct else z == here.z
                pl.when(crossed)(lambda p=p: self.to_y(p, z).wait_send())
                for y in piece.sides(here.y):
                    pl.when(z > here.z)(lambda p=p, y=y: self.to_z(p, z, y, 0).wait_send())
                    pl.when(z < here.z)(lambda p=p, y=y: self.to_z(p, z, y, 1).wait_send())
            return carry

        lax.fori_loop(0, here.levels, level, 0)


def reduce_kernel(pieces, *refs):
    count = len(pieces)
    sources, outs, rest = refs[:7], refs[7:12], refs[12:]
    factors, small, made = rest[:6], rest[6], rest[7]
    rest = rest[8:]
    buffers = [rest[i * count : (i + 1) * count] for i in range(5)]
    rest = rest[5 * count :]
    here = Place()
    loads = [
        pltpu.make_async_copy(source, target, rest[0].at[i])
        for i, (source, target) in enumerate(zip(sources, [*factors, small]))
    ]
    order = (1, 5, 2, 0, 3, 4, 6)
    for i in order:
        loads[i].start()
    greet(here, False)
    reduce = Reduce(here, pieces, factors, small, made, buffers, rest[:8])
    needs = {1: (1, 5), 3: (2,), 0: (0, 3), 2: (4,), 4: (6,)}

    def waits(i, array):
        @pl.when(i == 0)
        def _():
            for k in needs[array]:
                loads[k].wait()

    reduce.run(waits)
    owns = [buffers[0][p].at[here.z, here.y] for p in range(count)]
    spread = Spread(here, pieces, owns, outs, rest[8:])
    turned = [p for p in range(count) if not pieces[p].direct]
    for p in turned:
        reduce.settle(p)
        reduce.to_y(p, here.z).start()
    for p in range(count):
        if pieces[p].direct:
            reduce.rows(p, here.z)
            reduce.settle(p)
            spread.begin(p)
    for p in turned:
        reduce.rows(p, here.z)
        spread.begin(p)
    spread.swap()
    spread.middle()
    reduce.finish()
    spread.finish()


def reduce_all(factors, small, shapes, number):
    levels = lax.axis_size("batch") // 4
    shapes = [*shapes, small.shape]
    pieces = pieces_of([(rows // (4 * levels), columns) for rows, columns in shapes])
    count = len(pieces)
    dma = pltpu.SemaphoreType.DMA
    low = jnp.bfloat16
    scratch = [pltpu.VMEM(factor.shape, low) for factor in factors]
    scratch += [pltpu.VMEM(small.shape, low), pltpu.VMEM((256, COLUMN_STEP), jnp.float32)]
    blocks = [(piece.rows, piece.columns) for piece in pieces]
    scratch += [pltpu.VMEM((levels, 2) + block, low) for block in blocks]
    scratch += [pltpu.VMEM((2, 2) + block, low) for block in blocks] * 2
    scratch += [
        pltpu.VMEM((levels if piece.direct else 1,) + block, low)
        for piece, block in zip(pieces, blocks)
    ]
    scratch += [
        pltpu.VMEM((levels + 1, 1 if piece.direct else 2) + block, low)
        for piece, block in zip(pieces, blocks)
    ]
    scratch += [
        dma((7,)),
        dma((count, 2, 2)),
        dma((count, 2, 2)),
        dma((count, levels)),
        dma((count, levels)),
        dma((count, levels, 2)),
        dma((count, levels + 1, 2)),
        pltpu.SemaphoreType.REGULAR,
    ] + spread_semaphores(count, levels)
    return pl.pallas_call(
        partial(reduce_kernel, pieces),
        out_shape=[jax.ShapeDtypeStruct(shape, low) for shape in shapes],
        in_specs=[ANY] * 7,
        out_specs=[ANY] * 5,
        scratch_shapes=scratch,
        compiler_params=pltpu.CompilerParams(
            collective_id=number, has_side_effects=True, vmem_limit_bytes=60 * 2**20
        ),
        name="reduce_gradients",
    )(*factors, small)


def rotary_rows():
    positions = np.arange(SLOT, dtype=np.float64)[:, None]
    lane = np.arange(2 * HEAD_DIM)[None, :] % HEAD_DIM
    angles = positions * rotary_base ** (-(lane // 2 * 2.0) / ROT)
    turned = lane < ROT
    cosine = np.where(turned, np.cos(angles), 1.0)
    sine = np.where(turned, np.sin(angles), 0.0)
    even = np.where(lane % 2 == 0, sine, 0.0)
    odd = np.where(lane % 2 == 1, sine, 0.0)
    return np.stack([cosine, even, odd]).astype(np.float32)


def turn(pair, tables, back):
    lanes = pair.shape[1]
    following = pltpu.roll(pair, lanes - 1, 1)
    preceding = pltpu.roll(pair, 1, 1)
    side = following * tables[1] - preceding * tables[2]
    return pair * tables[0] + (side if back else -side)


def product(left, right, left_axis=1, right_axis=0):
    return lax.dot_general(
        left, right, (((left_axis,), (right_axis,)), ((), ())), preferred_element_type=jnp.float32
    )


def statistics(rows):
    average = jnp.mean(rows, axis=-1, keepdims=True)
    centered = rows - average
    variance = jnp.mean(centered * centered, axis=-1, keepdims=True)
    inverse = lax.rsqrt(variance + norm_epsilon)
    return centered * inverse, inverse


def low_lanes(width):
    return lax.broadcasted_iota(jnp.int32, (1, width), 1) < HEAD_DIM


def pair_lanes(index):
    return pl.ds(pl.multiple_of(index * 2 * HEAD_DIM, 2 * HEAD_DIM), 2 * HEAD_DIM)


def rows_at(index, step):
    return pl.ds(pl.multiple_of(index * step, step), step)


def forward_block(m, length, loads, refs):
    (x, normed, qkv, attention, mixture, active, slope, total, result) = refs["state"]
    joint, output, expand, contract = refs["weights"]
    gain, offset, outer, inner = refs["vectors"]
    tables = refs["tables"]
    width = x.shape[2]

    def norm(i, carry):
        at = rows_at(i, ROW_STEP)
        standard, _ = statistics(x[m, at, :].astype(jnp.float32))
        normed[m, at, :] = (standard * gain[...] + offset[...]).astype(jnp.bfloat16)
        return carry

    lax.fori_loop(0, SLOT // ROW_STEP, norm, 0)
    loads(0)
    for part in range(3):
        scale = HEAD_DIM**-0.5 if part == 0 else 1.0
        total[...] = product(normed[m], joint[:, part * width : (part + 1) * width])
        if part == 2:
            qkv[m, :, 2 * width :] = total[...].astype(jnp.bfloat16)
        else:

            def rotary(i, carry, part=part, scale=scale):
                pair = turn(total[:, pair_lanes(i)], tables, False)
                at = pair_lanes(i + part * (width // (2 * HEAD_DIM)))
                qkv[m, :, at] = pair.astype(jnp.bfloat16) * jnp.bfloat16(scale)
                return carry

            lax.fori_loop(0, width // (2 * HEAD_DIM), rotary, 0)

    query = lax.broadcasted_iota(jnp.int32, (SLOT, SLOT), 0)
    key = lax.broadcasted_iota(jnp.int32, (SLOT, SLOT), 1)
    allowed = (key <= query) & (key < length)
    pairs = width // (2 * HEAD_DIM)
    low = low_lanes(2 * HEAD_DIM)

    def heads(i, carry):
        queries, keys = qkv[m, :, pair_lanes(i)], qkv[m, :, pair_lanes(i + pairs)]
        values = qkv[m, :, pair_lanes(i + 2 * pairs)]
        mixed = []
        for half in range(2):
            own = jnp.where(low == (half == 0), queries, jnp.zeros_like(queries))
            scores = jnp.where(allowed, product(own, keys, 1, 1), masked_score)
            raised = jnp.exp(scores - jnp.max(scores, axis=-1, keepdims=True))
            share = raised * (1.0 / jnp.sum(raised, axis=-1, keepdims=True))
            share = share.astype(jnp.bfloat16)
            attention[m, 2 * i + half] = share
            mixed.append(product(share, values))
        mixture[m, :, pair_lanes(i)] = jnp.where(low, mixed[0], mixed[1]).astype(jnp.bfloat16)
        return carry

    lax.fori_loop(0, pairs, heads, 0, unroll=8)
    loads(1)
    total[...] = x[m].astype(jnp.float32) + outer[...] + product(mixture[m], output[...])
    loads(2)
    loads(3)

    def hidden(i, carry):
        at = rows_at(i, FF_STEP)
        pre = product(normed[m], expand[:, at]) + inner[:, at]
        square = pre * pre
        bend = jnp.tanh(GELU_SCALE * (pre + GELU_CUBE * (square * pre)))
        lifted = 0.5 * (1.0 + bend)
        slant = (0.5 * GELU_SCALE) * (1.0 + (3.0 * GELU_CUBE) * square)
        slope[m, :, at] = (lifted + pre * (1.0 - bend * bend) * slant).astype(jnp.bfloat16)
        activated = (pre * lifted).astype(jnp.bfloat16)
        active[m, :, at] = activated
        total[...] += product(activated, contract[at, :])
        return carry

    lax.fori_loop(0, slope.shape[2] // FF_STEP, hidden, 0)
    result[m] = total[...].astype(jnp.bfloat16)


def backward_block(m, refs):
    (x, _, qkv, attention, _, _, slope, total, result) = refs["state"]
    joint, output, expand, contract = refs["weights"]
    gain, offset, outer, inner = refs["vectors"]
    upstream, mixture_grad = refs["gradients"]
    gain_sum, offset_sum, outer_sum, inner_sum = refs["sums"]
    tables = refs["tables"]
    width = x.shape[2]
    outer_sum[...] += jnp.sum(upstream[m].astype(jnp.float32), axis=0, keepdims=True)
    mixture_grad[...] = product(upstream[m], output[...], 1, 1).astype(jnp.bfloat16)
    total[...] = jnp.zeros_like(total)

    def hidden(i, carry):
        at = rows_at(i, FF_STEP)
        active_grad = product(upstream[m], contract[at, :], 1, 1)
        pre_grad = (active_grad * slope[m, :, at].astype(jnp.float32)).astype(jnp.bfloat16)
        slope[m, :, at] = pre_grad
        inner_sum[:, at] += jnp.sum(pre_grad.astype(jnp.float32), axis=0, keepdims=True)
        total[...] += product(pre_grad, expand[:, at], 1, 1)
        return carry

    lax.fori_loop(0, slope.shape[2] // FF_STEP, hidden, 0)
    pairs = width // (2 * HEAD_DIM)
    low = low_lanes(2 * HEAD_DIM)

    def heads(i, carry):
        queries, keys = qkv[m, :, pair_lanes(i)], qkv[m, :, pair_lanes(i + pairs)]
        values = qkv[m, :, pair_lanes(i + 2 * pairs)]
        mixed_grad = mixture_grad[:, pair_lanes(i)]
        query_grads, key_grads, value_grads = [], [], []
        for half in range(2):
            share = attention[m, 2 * i + half]
            own = jnp.where(low == (half == 0), mixed_grad, jnp.zeros_like(mixed_grad))
            value_grads.append(product(share, mixed_grad, 0, 0))
            share_grad = product(own, values, 1, 1)
            weight = share.astype(jnp.float32)
            weighted = weight * share_grad
            score_grad = weighted - weight * jnp.sum(weighted, axis=-1, keepdims=True)
            score_grad = score_grad.astype(jnp.bfloat16)
            query_grads.append(product(score_grad, keys))
            key_grads.append(product(score_grad, queries, 0, 0))
        query_grad = jnp.where(low, query_grads[0], query_grads[1]) * HEAD_DIM**-0.5
        key_grad = jnp.where(low, key_grads[0], key_grads[1])
        value_grad = jnp.where(low, value_grads[0], value_grads[1])
        qkv[m, :, pair_lanes(i)] = turn(query_grad, tables, True).astype(jnp.bfloat16)
        qkv[m, :, pair_lanes(i + pairs)] = turn(key_grad, tables, True).astype(jnp.bfloat16)
        qkv[m, :, pair_lanes(i + 2 * pairs)] = value_grad.astype(jnp.bfloat16)
        return carry

    lax.fori_loop(0, pairs, heads, 0, unroll=2)

    def project(i, carry):
        at = rows_at(i, JOINT_STEP)
        total[:, at] += product(qkv[m], joint[at, :], 1, 1)
        return carry

    lax.fori_loop(0, width // JOINT_STEP, project, 0)

    def norm(i, carry):
        at = rows_at(i, ROW_STEP)
        standard, inverse = statistics(x[m, at, :].astype(jnp.float32))
        normed_grad = total[at, :]
        gain_sum[...] += jnp.sum(normed_grad * standard, axis=0, keepdims=True)
        offset_sum[...] += jnp.sum(normed_grad, axis=0, keepdims=True)
        scaled = normed_grad * gain[...]
        inner_mean = jnp.mean(scaled, axis=-1, keepdims=True)
        along = jnp.mean(scaled * standard, axis=-1, keepdims=True)
        change = inverse * (scaled - inner_mean - standard * along)
        result[m, at, :] = (upstream[m, at, :].astype(jnp.float32) + change).astype(jnp.bfloat16)
        return carry

    lax.fori_loop(0, SLOT // ROW_STEP, norm, 0)


BLOCK_OUTPUTS = 12


def blocks_kernel(*refs):
    lengths, whole_in, cotangent, tables_in, gain, offset, outer, inner = refs[:8]
    weight_sources = refs[8:12]
    outs = refs[12:24]
    weights = refs[24:28]
    x, normed, qkv, attention, mixture, active, slope, total, result = refs[28:37]
    upstream, mixture_grad, tables = refs[37:40]
    weight_sem, in_sem, hand_send, hand_receive, half_send, half_receive, half_keep, out_sem = refs[
        40:48
    ]
    hidden_out, input_grad = outs[:2]
    factor_outs, sums = outs[2:8], outs[8:12]
    section = lax.axis_index("section")
    partner = {"section": 1 - section}
    barrier = pltpu.get_barrier_semaphore()
    pl.semaphore_signal(barrier, inc=1, device_id=partner, device_id_type=MESH)
    pl.semaphore_wait(barrier, 1)
    half = hidden_out.shape[1]

    def loading(i):
        return pltpu.make_async_copy(weight_sources[i], weights[i], weight_sem.at[i])

    def taking(source, target, m):
        return pltpu.make_async_copy(source.at[rows_at(m, SLOT), :], target.at[m], in_sem.at[m])

    def handing(target, m):
        return pltpu.make_async_remote_copy(
            result.at[m],
            target.at[m],
            hand_send.at[m],
            hand_receive.at[m],
            device_id=partner,
            device_id_type=MESH,
        )

    def away(target, start, m):
        return pltpu.make_async_remote_copy(
            result.at[m, :, pl.ds(start, half)],
            target.at[rows_at(m, SLOT), :],
            half_send.at[m],
            half_receive.at[m],
            device_id=partner,
            device_id_type=MESH,
        )

    def kept(target, start, m):
        return pltpu.make_async_copy(
            result.at[m, :, pl.ds(start, half)], target.at[rows_at(m, SLOT), :], half_keep.at[m]
        )

    def giving(i, source, m):
        return pltpu.make_async_copy(
            source.at[m], factor_outs[i].at[rows_at(m, SLOT), :], out_sem.at[i, m]
        )

    pltpu.make_async_copy(tables_in, tables, weight_sem.at[4]).start()
    for m in range(MICRO):
        pl.when(section == 0)(lambda m=m: taking(whole_in, x, m).start())
        pl.when(section == 1)(lambda m=m: taking(cotangent, upstream, m).start())
    for i in range(4):
        loading(i).start()
    for total_sum in sums:
        total_sum[...] = jnp.zeros_like(total_sum)
    pltpu.make_async_copy(tables_in, tables, weight_sem.at[4]).wait()
    shared = {
        "state": (x, normed, qkv, attention, mixture, active, slope, total, result),
        "weights": weights,
        "vectors": (gain, offset, outer, inner),
        "tables": tables,
        "gradients": (upstream, mixture_grad),
        "sums": sums,
    }

    def forward(m, carry):
        pl.when(section == 0)(lambda: taking(whole_in, x, m).wait())
        pl.when(section == 1)(lambda: handing(x, m).wait_recv())
        forward_block(
            m, lengths[m], lambda i: pl.when(m == 0)(lambda: loading(i).wait()), shared
        )

        @pl.when(section == 0)
        def _():
            handing(x, m).start()

        @pl.when(section == 1)
        def _():
            away(hidden_out, 0, m).start()
            kept(hidden_out, half, m).start()

        for i, source in enumerate((normed, mixture, active)):
            giving(i, source, m).start()
        return carry

    lax.fori_loop(0, MICRO, forward, 0)

    def backward(m, carry):
        @pl.when(section == 0)
        def _():
            handing(x, m).wait_send()
            handing(upstream, m).wait_recv()

        @pl.when(section == 1)
        def _():
            away(hidden_out, 0, m).wait_send()
            kept(hidden_out, half, m).wait()
            taking(cotangent, upstream, m).wait()
            row = lax.broadcasted_iota(jnp.int32, (SLOT, 1), 0)
            inside = (row < lengths[m]).astype(jnp.float32)
            masked = upstream[m].astype(jnp.float32) * inside
            upstream[m] = masked.astype(jnp.bfloat16)

        backward_block(m, shared)

        @pl.when(section == 1)
        def _():
            handing(upstream, m).start()

        @pl.when(section == 0)
        def _():
            away(input_grad, half, m).start()
            kept(input_grad, 0, m).start()

        for i, source in enumerate((qkv, slope, upstream)):
            giving(3 + i, source, m).start()
        return carry

    lax.fori_loop(0, MICRO, backward, 0)

    def last(m, carry):
        @pl.when(section == 0)
        def _():
            away(input_grad, half, m).wait_send()
            kept(input_grad, 0, m).wait()
            away(hidden_out, 0, m).wait_recv()

        @pl.when(section == 1)
        def _():
            handing(upstream, m).wait_send()
            away(input_grad, half, m).wait_recv()

        for i, source in enumerate((normed, mixture, active, qkv, slope, upstream)):
            giving(i, source, m).wait()
        return carry

    lax.fori_loop(0, MICRO, last, 0)


def run_blocks(lengths, whole_in, cotangent, vectors, weights, number):
    tokens, width = whole_in.shape
    wide = weights[2].shape[1]
    half = width // lax.axis_size("section")
    low, full = jnp.bfloat16, jnp.float32
    shape = jax.ShapeDtypeStruct
    vmem = pltpu.VMEM
    dma = pltpu.SemaphoreType.DMA
    inside = pl.BlockSpec(memory_space=vmem)
    outputs = [shape((tokens, half), low)] * 2
    outputs += [shape((tokens, n), low) for n in (width, width, wide, 3 * width, wide, width)]
    outputs += [shape((1, n), full) for n in (width, width, width, wide)]
    scratch = [vmem(weight.shape, low) for weight in weights]
    scratch += [
        vmem((MICRO, SLOT, width), low),
        vmem((MICRO, SLOT, width), low),
        vmem((MICRO, SLOT, 3 * width), low),
        vmem((MICRO, HEADS, SLOT, SLOT), low),
        vmem((MICRO, SLOT, width), low),
        vmem((MICRO, SLOT, wide), low),
        vmem((MICRO, SLOT, wide), low),
        vmem((SLOT, width), full),
        vmem((MICRO, SLOT, width), low),
        vmem((MICRO, SLOT, width), low),
        vmem((SLOT, width), low),
        vmem((3, SLOT, 2 * HEAD_DIM), full),
        dma((5,)),
        dma((MICRO,)),
        dma((MICRO,)),
        dma((MICRO,)),
        dma((MICRO,)),
        dma((MICRO,)),
        dma((MICRO,)),
        dma((6, MICRO)),
    ]
    vectors = [vector.astype(full).reshape(1, -1) for vector in vectors]
    return pl.pallas_call(
        blocks_kernel,
        out_shape=outputs,
        in_specs=[pl.BlockSpec(memory_space=pltpu.SMEM), ANY, ANY, ANY] + [inside] * 4 + [ANY] * 4,
        out_specs=[ANY] * 8 + [inside] * 4,
        scratch_shapes=scratch,
        compiler_params=pltpu.CompilerParams(
            collective_id=number, has_side_effects=True, vmem_limit_bytes=60 * 2**20
        ),
        name="two_blocks",
    )(lengths, whole_in, cotangent, jnp.asarray(rotary_rows()), *vectors, *weights)


def pack_small(members):
    flat = jnp.concatenate([member.astype(jnp.float32) for member in members], axis=1)
    flat = jnp.pad(flat, ((0, 0), (0, SMALL_ROWS * LANES - flat.shape[1])))
    return flat.reshape(-1, LANES).astype(jnp.bfloat16)


def unpack_small(packed, widths, devices):
    flat = packed.reshape(devices, -1)
    members, start = [], 0
    for width in widths:
        members.append(flat[:, start : start + width].reshape(-1))
        start += width
    return members


def local(
    hidden_in,
    cotangent,
    lengths,
    norm_gain,
    norm_offset,
    joint_weight,
    output_weight,
    expand_weight,
    inner_bias,
    contract_weight,
    outer_bias,
):
    devices = lax.axis_size("batch")
    vectors_own = (norm_gain, norm_offset, outer_bias, inner_bias)
    (*weights, small_all), (whole_in, whole_cotangent) = gather_all(
        [
            joint_weight[0],
            output_weight[0],
            expand_weight[0],
            contract_weight[0],
            pack_small(vectors_own),
        ],
        [hidden_in, cotangent],
        1,
    )
    vectors = unpack_small(small_all, [member.shape[1] for member in vectors_own], devices)
    results = run_blocks(lengths, whole_in, whole_cotangent, vectors, weights, 2)
    hidden_out, input_grad = results[:2]
    small = results[8:]
    small_packed = pack_small([member.reshape(devices, -1) for member in small])
    shapes = [weight.shape for weight in weights]
    joint_sum, output_sum, expand_sum, contract_sum, small_sum = [
        member.astype(jnp.float32) for member in reduce_all(results[2:8], small_packed, shapes, 3)
    ]
    gain_sum, offset_sum, outer_sum, inner_sum = unpack_small(
        small_sum, [member.shape[1] // devices for member in small], devices
    )
    return (
        hidden_out,
        input_grad,
        gain_sum[None],
        offset_sum[None],
        joint_sum[None],
        output_sum[None],
        expand_sum[None],
        inner_sum[None],
        contract_sum[None],
        outer_sum[None],
    )


def solution(mesh):
    return jax.shard_map(
        local,
        mesh=mesh,
        in_specs=(
            P("batch", "section"),
            P("batch", "section"),
            P("batch"),
            P("section", "batch"),
            P("section", "batch"),
            P("section", "batch", None),
            P("section", "batch", None),
            P("section", "batch", None),
            P("section", "batch"),
            P("section", "batch", None),
            P("section", "batch"),
        ),
        out_specs=(
            P("batch", "section"),
            P("batch", "section"),
            P("section", None),
            P("section", None),
            P("section", None, None),
            P("section", None, None),
            P("section", None, None),
            P("section", None),
            P("section", None, None),
            P("section", None),
        ),
        check_vma=False,
    )
```

```python
from functools import partial

import jax
import jax.numpy as jnp
import numpy as np
from jax import lax
from jax.experimental import pallas as pl
from jax.experimental.pallas import tpu as pltpu
from jax.sharding import PartitionSpec as P

HEADS = 16
HEAD_DIM = 64
ROT = 32
SLOT = 256
MICRO = 2
SMALL_ROWS = 16
LANES = 128
ROW_STEP = 256
FF_STEP = 4096
JOINT_STEP = 1024
GELU_SCALE = (2.0 / np.pi) ** 0.5
GELU_CUBE = 0.044715
norm_epsilon = 1e-05
rotary_base = 10000.0
masked_score = -1e30
MESH = pl.DeviceIdType.MESH
ANY = pl.BlockSpec(memory_space=pl.ANY)


class Place:
    def __init__(self):
        index = lax.axis_index("batch")
        self.levels = lax.axis_size("batch") // 4
        self.last = self.levels - 1
        self.z, self.y, self.c = index // 4, index // 2 % 2, index % 2

    def at(self, z=None, y=None, c=None):
        z = self.z if z is None else z
        y = self.y if y is None else y
        c = self.c if c is None else c
        return z * 4 + y * 2 + c


class Piece:
    def __init__(self, array, offset, rows, columns, direct):
        self.array, self.offset, self.rows, self.columns = array, offset, rows, columns
        self.direct = direct

    def sides(self, y):
        return (y,) if self.direct else (y, 1 - y)


def pieces_of(blocks):
    joint, output, expand, contract, small = blocks
    cut = contract[0] // 4
    return [
        Piece(1, 0, *output, False),
        Piece(3, 0, cut, contract[1], False),
        Piece(0, 0, *joint, True),
        Piece(2, 0, *expand, True),
        Piece(3, cut, contract[0] - cut, contract[1], True),
        Piece(4, 0, *small, True),
    ]


def remote(source, target, send, receive, index):
    return pltpu.make_async_remote_copy(
        source, target, send, receive, device_id={"batch": index}, device_id_type=MESH
    )


def greet(here, with_section):
    barrier = pltpu.get_barrier_semaphore()

    def signal(**who):
        pl.semaphore_signal(barrier, inc=1, device_id=who, device_id_type=MESH)

    signal(batch=here.at(y=1 - here.y))
    signal(batch=here.at(c=1 - here.c))
    pl.when(here.z > 0)(lambda: signal(batch=here.at(z=here.z - 1)))
    pl.when(here.z < here.last)(lambda: signal(batch=here.at(z=here.z + 1)))
    waits = 2
    if with_section:
        signal(section=1 - lax.axis_index("section"))
        waits = 3
    below = jnp.minimum(here.z, 1)
    above = jnp.minimum(here.last - here.z, 1)
    pl.semaphore_wait(barrier, waits + below + above)


def spread_semaphores(count, levels):
    dma = pltpu.SemaphoreType.DMA
    return [
        dma((count,)),
        dma((count, levels, 2, 2)),
        dma((count, levels, 2)),
        dma((count, levels)),
        dma((count, levels)),
        dma((count, levels, 2)),
        dma((count, levels, 2)),
    ]


class Spread:
    def __init__(self, here, pieces, owns, outs, semaphores):
        self.here, self.pieces, self.owns, self.outs = here, pieces, owns, outs
        (self.keep, self.zs, self.zr, self.ys, self.yr, self.cs, self.cr) = semaphores

    def block(self, p, z, y, c):
        piece = self.pieces[p]
        out = self.outs[piece.array]
        rows = out.shape[0] // (4 * self.here.levels)
        start = (z * 4 + y * 2 + c) * rows + piece.offset
        return out.at[pl.ds(pl.multiple_of(start, 8), piece.rows), :]

    def along(self, p, z, y, source, way):
        here = self.here
        return remote(
            source,
            self.block(p, z, y, here.c),
            self.zs.at[p, z, y, way],
            self.zr.at[p, z, y],
            here.at(z=here.z + (1 if way == 0 else -1)),
        )

    def across(self, p, z, source):
        here = self.here
        target = self.block(p, z, here.y, here.c)
        return remote(source, target, self.ys.at[p, z], self.yr.at[p, z], here.at(y=1 - here.y))

    def beside(self, p, z, y, source):
        here = self.here
        target = self.block(p, z, y, here.c)
        return remote(
            source, target, self.cs.at[p, z, y], self.cr.at[p, z, y], here.at(c=1 - here.c)
        )

    def both_ways(self, p, y, source):
        here = self.here
        pl.when(here.z < here.last)(lambda: self.along(p, here.z, y, source, 0).start())
        pl.when(here.z > 0)(lambda: self.along(p, here.z, y, source, 1).start())

    def begin(self, p, held=False):
        here, own = self.here, self.owns[p]
        self.across(p, here.z, own).start()
        if not held:
            self.both_ways(p, here.y, own)
        self.beside(p, here.z, here.y, own).start()
        target = self.block(p, here.z, here.y, here.c)
        pltpu.make_async_copy(own, target, self.keep.at[p]).start()

    def from_z(self, p, z, y, way):
        here = self.here
        block = self.block(p, z, y, here.c)
        self.along(p, z, y, block, way).wait_recv()
        more = here.z < here.last if way == 0 else here.z > 0
        pl.when(more)(lambda: self.along(p, z, y, block, way).start())
        if self.pieces[p].direct:
            self.across(p, z, block).start()
        self.beside(p, z, y, block).start()

    def from_y(self, p, z):
        here = self.here
        block = self.block(p, z, 1 - here.y, here.c)
        self.across(p, z, block).wait_recv()
        if not self.pieces[p].direct:
            self.both_ways(p, 1 - here.y, block)
        self.beside(p, z, 1 - here.y, block).start()

    def swap(self):
        for p, piece in enumerate(self.pieces):
            if not piece.direct:
                self.from_y(p, self.here.z)

    def z_events(self, z, way):
        here = self.here
        for p, piece in enumerate(self.pieces):
            if piece.direct:
                self.from_z(p, z, here.y, way)
        for side in range(2):
            for p, piece in enumerate(self.pieces):
                if not piece.direct:
                    self.from_z(p, z, piece.sides(here.y)[side], way)

    def y_events(self, z):
        for p, piece in enumerate(self.pieces):
            if piece.direct:
                self.from_y(p, z)

    def middle(self):
        here = self.here

        def y_pair(distance):
            pl.when(here.z - distance >= 0)(lambda: self.y_events(here.z - distance))
            pl.when((here.z + distance <= here.last) & (distance > 0))(
                lambda: self.y_events(here.z + distance)
            )

        def step(distance, carry):
            pl.when(here.z - distance >= 0)(lambda: self.z_events(here.z - distance, 0))
            pl.when(here.z + distance <= here.last)(lambda: self.z_events(here.z + distance, 1))
            y_pair(distance - 1)
            return carry

        lax.fori_loop(1, here.levels, step, 0)
        y_pair(here.last)

    def finish(self):
        here = self.here

        def level(z, carry):
            for p, piece in enumerate(self.pieces):
                own = self.block(p, z, here.y, here.c)
                for y in range(2):
                    self.beside(p, z, y, own).wait_send()
                    self.beside(p, z, y, own).wait_recv()
                crossed = z >= 0 if piece.direct else z == here.z
                pl.when(crossed)(lambda p=p, own=own: self.across(p, z, own).wait_send())
                for y in piece.sides(here.y):
                    pl.when((z <= here.z) & (here.z < here.last))(
                        lambda p=p, y=y, own=own: self.along(p, z, y, own, 0).wait_send()
                    )
                    pl.when((z >= here.z) & (here.z > 0))(
                        lambda p=p, y=y, own=own: self.along(p, z, y, own, 1).wait_send()
                    )
            return carry

        lax.fori_loop(0, here.levels, level, 0)
        for p in range(len(self.pieces)):
            block = self.block(p, here.z, here.y, here.c)
            pltpu.make_async_copy(block, block, self.keep.at[p]).wait()


def gather_kernel(pieces, *refs):
    sources, halves, outs, wholes = refs[:5], refs[5:7], refs[7:12], refs[12:14]
    half_send, half_receive, half_keep = refs[14:17]
    here = Place()
    section = lax.axis_index("section")
    greet(here, True)
    owns = [sources[piece.array].at[pl.ds(piece.offset, piece.rows), :] for piece in pieces]
    spread = Spread(here, pieces, owns, outs, refs[17:])
    turned = [p for p, piece in enumerate(pieces) if not piece.direct]
    for p, piece in enumerate(pieces):
        spread.begin(p, held=not piece.direct)
    for p in turned:
        spread.both_ways(p, here.y, owns[p])
    moves = []
    for i, (half, whole) in enumerate(zip(halves, wholes)):
        width = half.shape[1]
        mine = whole.at[:, pl.ds(pl.multiple_of(section * width, width), width)]
        send = pltpu.make_async_remote_copy(
            half,
            mine,
            half_send.at[i],
            half_receive.at[i],
            device_id={"section": 1 - section},
            device_id_type=MESH,
        )
        keep = pltpu.make_async_copy(half, mine, half_keep.at[i])
        send.start()
        keep.start()
        moves.append((send, keep))
    spread.swap()
    spread.middle()
    spread.finish()
    for send, keep in moves:
        send.wait()
        keep.wait()


def gather_all(owns, halves, number):
    levels = lax.axis_size("batch") // 4
    pieces = pieces_of([own.shape for own in owns])
    shapes = [
        jax.ShapeDtypeStruct((own.shape[0] * 4 * levels, own.shape[1]), own.dtype) for own in owns
    ] + [jax.ShapeDtypeStruct((half.shape[0], half.shape[1] * 2), half.dtype) for half in halves]
    dma = pltpu.SemaphoreType.DMA
    results = pl.pallas_call(
        partial(gather_kernel, pieces),
        out_shape=shapes,
        in_specs=[ANY] * 7,
        out_specs=[ANY] * 7,
        scratch_shapes=[dma((2,)), dma((2,)), dma((2,))] + spread_semaphores(len(pieces), levels),
        compiler_params=pltpu.CompilerParams(collective_id=number, has_side_effects=True),
        name="gather_weights",
    )(*owns, *halves)
    return results[:5], results[5:]


def add_rows(target, other):
    rows = target.shape[0]
    step = min(rows, 16)

    def body(i, carry):
        at = pl.ds(pl.multiple_of(i * step, step), step)
        total = target[at, :].astype(jnp.float32) + other[at, :].astype(jnp.float32)
        target[at, :] = total.astype(target.dtype)
        return carry

    lax.fori_loop(0, rows // step, body, 0)


FACTORS = ((0, 3), (1, 5), (0, 4), (2, 5))
MAKE_ORDER = (1, 3, 0, 2, 4)
COLUMN_STEP = 1024


class Reduce:
    def __init__(self, here, pieces, factors, small, product_rows, buffers, semaphores):
        self.here, self.pieces, self.factors, self.small = here, pieces, factors, small
        self.made = product_rows
        self.mine, self.sent, self.sib, self.yb, self.zb = buffers
        (self.load, self.cs, self.cr, self.ys, self.yr, self.zs, self.zr, self.credit) = semaphores

    def level(self, i):
        here = self.here
        above, below = here.last - here.z, here.z
        lead = jnp.maximum(above, below) - jnp.minimum(above, below)
        single = jnp.where(above > below, here.last - i, i)
        later = i - lead
        distance = jnp.minimum(above, below) - later // 2
        outer = jnp.where(above > below, here.z - distance, here.z + distance)
        paired = jnp.where(later % 2 == 0, outer, 2 * here.z - outer)
        return jnp.where(i < lead, single, paired)

    def to_core(self, p, slot, y):
        here = self.here
        return remote(
            self.sent[p].at[slot, y],
            self.sib[p].at[slot, y],
            self.cs.at[p, slot, y],
            self.cr.at[p, slot, y],
            here.at(c=1 - here.c),
        )

    def to_y(self, p, z):
        here = self.here
        return remote(
            self.mine[p].at[z, 1 - here.y],
            self.yb[p].at[z if self.pieces[p].direct else 0],
            self.ys.at[p, z],
            self.yr.at[p, z],
            here.at(y=1 - here.y),
        )

    def slot(self, z, at_z, way):
        if way == 0:
            return z
        return jnp.where(z == at_z, self.here.levels, z)

    def to_z(self, p, z, y, way):
        here = self.here
        step = 1 if way == 0 else -1
        slot = self.slot(z, here.z + step, way)
        side = 0 if self.pieces[p].direct else y
        return remote(
            self.mine[p].at[z, y],
            self.zb[p].at[slot, side],
            self.zs.at[p, z, side],
            self.zr.at[p, slot, side],
            here.at(z=here.z + step),
        )

    def arrive(self, p, z, y, way):
        here = self.here
        slot = self.slot(z, here.z, way)
        side = 0 if self.pieces[p].direct else y
        block = self.zb[p].at[slot, side]
        remote(
            block, block, self.zs.at[p, z, side], self.zr.at[p, slot, side], here.at(y=1 - here.y)
        ).wait_recv()
        add_rows(self.mine[p].at[z, y], block)

    def store(self, array, z, slot, y, own, value, column):
        at = pl.ds(column, value.shape[1])
        for p, piece in enumerate(self.pieces):
            if piece.array == array:
                target = self.mine[p].at[z, y] if own else self.sent[p].at[slot, y]
                rows = value[piece.offset : piece.offset + piece.rows]
                target[:, at] = rows.astype(jnp.bfloat16)

    def make(self, array, z, slot):
        here = self.here
        rows = sum(piece.rows for piece in self.pieces if piece.array == array)
        cores = ((False, 1 - here.c), (True, here.c))
        if array == 4:
            for own, c in cores:
                for y in range(2):
                    at = pl.multiple_of((z * 4 + y * 2 + c) * rows, 16)
                    self.store(array, z, slot, y, own, self.small[pl.ds(at, rows), :], 0)
            return
        left, right = (self.factors[i] for i in FACTORS[array])
        columns = right.shape[1]
        tiles = range(0, columns, COLUMN_STEP)
        if rows % 128 == 0:
            for own, c in cores:
                for y in range(2):
                    at = pl.multiple_of((z * 4 + y * 2 + c) * rows, 128)
                    turned = left[:, pl.ds(at, rows)].T
                    for tile in tiles:
                        value = product(turned, right[:, tile : tile + COLUMN_STEP])
                        self.store(array, z, slot, y, own, value, tile)
            return
        span = max(4 * rows, 128)
        start = z * 4 * rows // span * span
        turned = left[:, pl.ds(pl.multiple_of(start, 128), span)].T
        for tile in tiles:
            self.made[:span, :] = product(turned, right[:, tile : tile + COLUMN_STEP])
            for own, c in cores:
                for y in range(2):
                    at = pl.multiple_of((z * 4 + y * 2 + c) * rows - start, 8)
                    self.store(array, z, slot, y, own, self.made[pl.ds(at, rows), :], tile)

    def of(self, array):
        return [p for p, piece in enumerate(self.pieces) if piece.array == array]

    def build(self, i, waits):
        here = self.here
        z, slot = self.level(i), i % 2

        @pl.when(i >= 2)
        def _():
            for p in range(len(self.pieces)):
                for y in range(2):
                    self.to_core(p, slot, y).wait_send()
            pl.semaphore_wait(self.credit, 1)

        def add(array):
            for p in self.of(array):
                for y in range(2):
                    self.to_core(p, slot, y).wait_recv()
                    add_rows(self.mine[p].at[z, y], self.sib[p].at[slot, y])
                if self.pieces[p].direct:
                    self.to_y(p, z).start()
                else:
                    self.pass_on(z, [p])

        for step, array in enumerate(MAKE_ORDER):
            waits(i, array)
            self.make(array, z, slot)
            for p in self.of(array):
                for y in range(2):
                    self.to_core(p, slot, y).start()
            if step > 0:
                add(MAKE_ORDER[step - 1])
        add(MAKE_ORDER[-1])

        @pl.when(i < here.levels - 2)
        def _():
            other = {"batch": here.at(c=1 - here.c)}
            pl.semaphore_signal(self.credit, inc=1, device_id=other, device_id_type=MESH)

    def rows(self, p, z):
        self.to_y(p, z).wait_recv()
        source = self.yb[p].at[z if self.pieces[p].direct else 0]
        add_rows(self.mine[p].at[z, self.here.y], source)

    def pass_on(self, z, chosen):
        here = self.here

        def hop(way):
            further = here.z > 0 if way == 0 else here.z < here.last
            for p in chosen:
                if self.pieces[p].direct:
                    self.rows(p, z)
                for y in self.pieces[p].sides(here.y):
                    pl.when(further)(lambda p=p, y=y: self.arrive(p, z, y, way))
                    self.to_z(p, z, y, way).start()

        pl.when(z > here.z)(lambda: hop(0))
        pl.when(z < here.z)(lambda: hop(1))

    def run(self, waits):
        here = self.here
        made = [p for array in MAKE_ORDER for p in self.of(array)]
        direct = [p for p in made if self.pieces[p].direct]

        def step(i, carry):
            self.build(i, waits)
            pl.when(i > 0)(lambda: self.pass_on(self.level(i - 1), direct))
            return carry

        lax.fori_loop(0, here.levels, step, 0)

    def settle(self, p):
        here = self.here
        for y in self.pieces[p].sides(here.y):
            pl.when(here.z > 0)(lambda y=y: self.arrive(p, here.z, y, 0))
            pl.when(here.z < here.last)(lambda y=y: self.arrive(p, here.z, y, 1))

    def finish(self):
        here = self.here
        for slot in range(min(2, here.levels)):
            for p in range(len(self.pieces)):
                for y in range(2):
                    self.to_core(p, slot, y).wait_send()

        def level(z, carry):
            for p, piece in enumerate(self.pieces):
                crossed = z >= 0 if piece.direct else z == here.z
                pl.when(crossed)(lambda p=p: self.to_y(p, z).wait_send())
                for y in piece.sides(here.y):
                    pl.when(z > here.z)(lambda p=p, y=y: self.to_z(p, z, y, 0).wait_send())
                    pl.when(z < here.z)(lambda p=p, y=y: self.to_z(p, z, y, 1).wait_send())
            return carry

        lax.fori_loop(0, here.levels, level, 0)


def reduce_kernel(pieces, *refs):
    count = len(pieces)
    sources, outs, rest = refs[:7], refs[7:12], refs[12:]
    factors, small, made = rest[:6], rest[6], rest[7]
    rest = rest[8:]
    buffers = [rest[i * count : (i + 1) * count] for i in range(5)]
    rest = rest[5 * count :]
    here = Place()
    loads = [
        pltpu.make_async_copy(source, target, rest[0].at[i])
        for i, (source, target) in enumerate(zip(sources, [*factors, small]))
    ]
    order = (1, 5, 2, 0, 3, 4, 6)
    for i in order:
        loads[i].start()
    greet(here, False)
    reduce = Reduce(here, pieces, factors, small, made, buffers, rest[:8])
    needs = {1: (1, 5), 3: (2,), 0: (0, 3), 2: (4,), 4: (6,)}

    def waits(i, array):
        @pl.when(i == 0)
        def _():
            for k in needs[array]:
                loads[k].wait()

    reduce.run(waits)
    owns = [buffers[0][p].at[here.z, here.y] for p in range(count)]
    spread = Spread(here, pieces, owns, outs, rest[8:])
    turned = [p for p in range(count) if not pieces[p].direct]
    for p in turned:
        reduce.settle(p)
        reduce.to_y(p, here.z).start()
    for p in range(count):
        if pieces[p].direct:
            reduce.rows(p, here.z)
            reduce.settle(p)
            spread.begin(p)
    for p in turned:
        reduce.rows(p, here.z)
        spread.begin(p)
    spread.swap()
    spread.middle()
    reduce.finish()
    spread.finish()


def reduce_all(factors, small, shapes, number):
    levels = lax.axis_size("batch") // 4
    shapes = [*shapes, small.shape]
    pieces = pieces_of([(rows // (4 * levels), columns) for rows, columns in shapes])
    count = len(pieces)
    dma = pltpu.SemaphoreType.DMA
    low = jnp.bfloat16
    scratch = [pltpu.VMEM(factor.shape, low) for factor in factors]
    scratch += [pltpu.VMEM(small.shape, low), pltpu.VMEM((256, COLUMN_STEP), jnp.float32)]
    blocks = [(piece.rows, piece.columns) for piece in pieces]
    scratch += [pltpu.VMEM((levels, 2) + block, low) for block in blocks]
    scratch += [pltpu.VMEM((2, 2) + block, low) for block in blocks] * 2
    scratch += [
        pltpu.VMEM((levels if piece.direct else 1,) + block, low)
        for piece, block in zip(pieces, blocks)
    ]
    scratch += [
        pltpu.VMEM((levels + 1, 1 if piece.direct else 2) + block, low)
        for piece, block in zip(pieces, blocks)
    ]
    scratch += [
        dma((7,)),
        dma((count, 2, 2)),
        dma((count, 2, 2)),
        dma((count, levels)),
        dma((count, levels)),
        dma((count, levels, 2)),
        dma((count, levels + 1, 2)),
        pltpu.SemaphoreType.REGULAR,
    ] + spread_semaphores(count, levels)
    return pl.pallas_call(
        partial(reduce_kernel, pieces),
        out_shape=[jax.ShapeDtypeStruct(shape, low) for shape in shapes],
        in_specs=[ANY] * 7,
        out_specs=[ANY] * 5,
        scratch_shapes=scratch,
        compiler_params=pltpu.CompilerParams(
            collective_id=number, has_side_effects=True, vmem_limit_bytes=60 * 2**20
        ),
        name="reduce_gradients",
    )(*factors, small)


def rotary_rows():
    positions = np.arange(SLOT, dtype=np.float64)[:, None]
    lane = np.arange(2 * HEAD_DIM)[None, :] % HEAD_DIM
    angles = positions * rotary_base ** (-(lane // 2 * 2.0) / ROT)
    turned = lane < ROT
    cosine = np.where(turned, np.cos(angles), 1.0)
    sine = np.where(turned, np.sin(angles), 0.0)
    even = np.where(lane % 2 == 0, sine, 0.0)
    odd = np.where(lane % 2 == 1, sine, 0.0)
    return np.stack([cosine, even, odd]).astype(np.float32)


def turn(pair, tables, back):
    lanes = pair.shape[1]
    following = pltpu.roll(pair, lanes - 1, 1)
    preceding = pltpu.roll(pair, 1, 1)
    side = following * tables[1] - preceding * tables[2]
    return pair * tables[0] + (side if back else -side)


def product(left, right, left_axis=1, right_axis=0):
    return lax.dot_general(
        left, right, (((left_axis,), (right_axis,)), ((), ())), preferred_element_type=jnp.float32
    )


def statistics(rows):
    average = jnp.mean(rows, axis=-1, keepdims=True)
    centered = rows - average
    variance = jnp.mean(centered * centered, axis=-1, keepdims=True)
    inverse = lax.rsqrt(variance + norm_epsilon)
    return centered * inverse, inverse


def low_lanes(width):
    return lax.broadcasted_iota(jnp.int32, (1, width), 1) < HEAD_DIM


def pair_lanes(index):
    return pl.ds(pl.multiple_of(index * 2 * HEAD_DIM, 2 * HEAD_DIM), 2 * HEAD_DIM)


def rows_at(index, step):
    return pl.ds(pl.multiple_of(index * step, step), step)


def forward_block(m, length, loads, refs):
    (x, normed, qkv, attention, mixture, active, slope, total, result) = refs["state"]
    joint, output, expand, contract = refs["weights"]
    gain, offset, outer, inner = refs["vectors"]
    tables = refs["tables"]
    width = x.shape[2]

    def norm(i, carry):
        at = rows_at(i, ROW_STEP)
        standard, _ = statistics(x[m, at, :].astype(jnp.float32))
        normed[m, at, :] = (standard * gain[...] + offset[...]).astype(jnp.bfloat16)
        return carry

    lax.fori_loop(0, SLOT // ROW_STEP, norm, 0)
    loads(0)
    for part in range(3):
        scale = HEAD_DIM**-0.5 if part == 0 else 1.0
        total[...] = product(normed[m], joint[:, part * width : (part + 1) * width])
        if part == 2:
            qkv[m, :, 2 * width :] = total[...].astype(jnp.bfloat16)
        else:

            def rotary(i, carry, part=part, scale=scale):
                pair = turn(total[:, pair_lanes(i)], tables, False)
                at = pair_lanes(i + part * (width // (2 * HEAD_DIM)))
                qkv[m, :, at] = pair.astype(jnp.bfloat16) * jnp.bfloat16(scale)
                return carry

            lax.fori_loop(0, width // (2 * HEAD_DIM), rotary, 0)

    query = lax.broadcasted_iota(jnp.int32, (SLOT, SLOT), 0)
    key = lax.broadcasted_iota(jnp.int32, (SLOT, SLOT), 1)
    allowed = (key <= query) & (key < length)
    pairs = width // (2 * HEAD_DIM)
    low = low_lanes(2 * HEAD_DIM)

    def heads(i, carry):
        queries, keys = qkv[m, :, pair_lanes(i)], qkv[m, :, pair_lanes(i + pairs)]
        values = qkv[m, :, pair_lanes(i + 2 * pairs)]
        mixed = []
        for half in range(2):
            own = jnp.where(low == (half == 0), queries, jnp.zeros_like(queries))
            scores = jnp.where(allowed, product(own, keys, 1, 1), masked_score)
            raised = jnp.exp(scores - jnp.max(scores, axis=-1, keepdims=True))
            share = raised * (1.0 / jnp.sum(raised, axis=-1, keepdims=True))
            share = share.astype(jnp.bfloat16)
            attention[m, 2 * i + half] = share
            mixed.append(product(share, values))
        mixture[m, :, pair_lanes(i)] = jnp.where(low, mixed[0], mixed[1]).astype(jnp.bfloat16)
        return carry

    lax.fori_loop(0, pairs, heads, 0, unroll=8)
    loads(1)
    total[...] = x[m].astype(jnp.float32) + outer[...] + product(mixture[m], output[...])
    loads(2)
    loads(3)

    def hidden(i, carry):
        at = rows_at(i, FF_STEP)
        pre = product(normed[m], expand[:, at]) + inner[:, at]
        square = pre * pre
        bend = jnp.tanh(GELU_SCALE * (pre + GELU_CUBE * (square * pre)))
        lifted = 0.5 * (1.0 + bend)
        slant = (0.5 * GELU_SCALE) * (1.0 + (3.0 * GELU_CUBE) * square)
        slope[m, :, at] = (lifted + pre * (1.0 - bend * bend) * slant).astype(jnp.bfloat16)
        activated = (pre * lifted).astype(jnp.bfloat16)
        active[m, :, at] = activated
        total[...] += product(activated, contract[at, :])
        return carry

    lax.fori_loop(0, slope.shape[2] // FF_STEP, hidden, 0)
    result[m] = total[...].astype(jnp.bfloat16)


def backward_block(m, refs):
    (x, _, qkv, attention, _, _, slope, total, result) = refs["state"]
    joint, output, expand, contract = refs["weights"]
    gain, offset, outer, inner = refs["vectors"]
    upstream, mixture_grad = refs["gradients"]
    gain_sum, offset_sum, outer_sum, inner_sum = refs["sums"]
    tables = refs["tables"]
    width = x.shape[2]
    outer_sum[...] += jnp.sum(upstream[m].astype(jnp.float32), axis=0, keepdims=True)
    mixture_grad[...] = product(upstream[m], output[...], 1, 1).astype(jnp.bfloat16)
    total[...] = jnp.zeros_like(total)

    def hidden(i, carry):
        at = rows_at(i, FF_STEP)
        active_grad = product(upstream[m], contract[at, :], 1, 1)
        pre_grad = (active_grad * slope[m, :, at].astype(jnp.float32)).astype(jnp.bfloat16)
        slope[m, :, at] = pre_grad
        inner_sum[:, at] += jnp.sum(pre_grad.astype(jnp.float32), axis=0, keepdims=True)
        total[...] += product(pre_grad, expand[:, at], 1, 1)
        return carry

    lax.fori_loop(0, slope.shape[2] // FF_STEP, hidden, 0)
    pairs = width // (2 * HEAD_DIM)
    low = low_lanes(2 * HEAD_DIM)

    def heads(i, carry):
        queries, keys = qkv[m, :, pair_lanes(i)], qkv[m, :, pair_lanes(i + pairs)]
        values = qkv[m, :, pair_lanes(i + 2 * pairs)]
        mixed_grad = mixture_grad[:, pair_lanes(i)]
        query_grads, key_grads, value_grads = [], [], []
        for half in range(2):
            share = attention[m, 2 * i + half]
            own = jnp.where(low == (half == 0), mixed_grad, jnp.zeros_like(mixed_grad))
            value_grads.append(product(share, mixed_grad, 0, 0))
            share_grad = product(own, values, 1, 1)
            weight = share.astype(jnp.float32)
            weighted = weight * share_grad
            score_grad = weighted - weight * jnp.sum(weighted, axis=-1, keepdims=True)
            score_grad = score_grad.astype(jnp.bfloat16)
            query_grads.append(product(score_grad, keys))
            key_grads.append(product(score_grad, queries, 0, 0))
        query_grad = jnp.where(low, query_grads[0], query_grads[1]) * HEAD_DIM**-0.5
        key_grad = jnp.where(low, key_grads[0], key_grads[1])
        value_grad = jnp.where(low, value_grads[0], value_grads[1])
        qkv[m, :, pair_lanes(i)] = turn(query_grad, tables, True).astype(jnp.bfloat16)
        qkv[m, :, pair_lanes(i + pairs)] = turn(key_grad, tables, True).astype(jnp.bfloat16)
        qkv[m, :, pair_lanes(i + 2 * pairs)] = value_grad.astype(jnp.bfloat16)
        return carry

    lax.fori_loop(0, pairs, heads, 0, unroll=2)

    def project(i, carry):
        at = rows_at(i, JOINT_STEP)
        total[:, at] += product(qkv[m], joint[at, :], 1, 1)
        return carry

    lax.fori_loop(0, width // JOINT_STEP, project, 0)

    def norm(i, carry):
        at = rows_at(i, ROW_STEP)
        standard, inverse = statistics(x[m, at, :].astype(jnp.float32))
        normed_grad = total[at, :]
        gain_sum[...] += jnp.sum(normed_grad * standard, axis=0, keepdims=True)
        offset_sum[...] += jnp.sum(normed_grad, axis=0, keepdims=True)
        scaled = normed_grad * gain[...]
        inner_mean = jnp.mean(scaled, axis=-1, keepdims=True)
        along = jnp.mean(scaled * standard, axis=-1, keepdims=True)
        change = inverse * (scaled - inner_mean - standard * along)
        result[m, at, :] = (upstream[m, at, :].astype(jnp.float32) + change).astype(jnp.bfloat16)
        return carry

    lax.fori_loop(0, SLOT // ROW_STEP, norm, 0)


BLOCK_OUTPUTS = 12


def blocks_kernel(*refs):
    lengths, whole_in, cotangent, tables_in, gain, offset, outer, inner = refs[:8]
    weight_sources = refs[8:12]
    outs = refs[12:24]
    weights = refs[24:28]
    x, normed, qkv, attention, mixture, active, slope, total, result = refs[28:37]
    upstream, mixture_grad, tables = refs[37:40]
    weight_sem, in_sem, hand_send, hand_receive, half_send, half_receive, half_keep, out_sem = refs[
        40:48
    ]
    hidden_out, input_grad = outs[:2]
    factor_outs, sums = outs[2:8], outs[8:12]
    section = lax.axis_index("section")
    partner = {"section": 1 - section}
    barrier = pltpu.get_barrier_semaphore()
    pl.semaphore_signal(barrier, inc=1, device_id=partner, device_id_type=MESH)
    pl.semaphore_wait(barrier, 1)
    half = hidden_out.shape[1]

    def loading(i):
        return pltpu.make_async_copy(weight_sources[i], weights[i], weight_sem.at[i])

    def taking(source, target, m):
        return pltpu.make_async_copy(source.at[rows_at(m, SLOT), :], target.at[m], in_sem.at[m])

    def handing(target, m):
        return pltpu.make_async_remote_copy(
            result.at[m],
            target.at[m],
            hand_send.at[m],
            hand_receive.at[m],
            device_id=partner,
            device_id_type=MESH,
        )

    def away(target, start, m):
        return pltpu.make_async_remote_copy(
            result.at[m, :, pl.ds(start, half)],
            target.at[rows_at(m, SLOT), :],
            half_send.at[m],
            half_receive.at[m],
            device_id=partner,
            device_id_type=MESH,
        )

    def kept(target, start, m):
        return pltpu.make_async_copy(
            result.at[m, :, pl.ds(start, half)], target.at[rows_at(m, SLOT), :], half_keep.at[m]
        )

    def giving(i, source, m):
        return pltpu.make_async_copy(
            source.at[m], factor_outs[i].at[rows_at(m, SLOT), :], out_sem.at[i, m]
        )

    pltpu.make_async_copy(tables_in, tables, weight_sem.at[4]).start()
    for m in range(MICRO):
        pl.when(section == 0)(lambda m=m: taking(whole_in, x, m).start())
        pl.when(section == 1)(lambda m=m: taking(cotangent, upstream, m).start())
    for i in range(4):
        loading(i).start()
    for total_sum in sums:
        total_sum[...] = jnp.zeros_like(total_sum)
    pltpu.make_async_copy(tables_in, tables, weight_sem.at[4]).wait()
    shared = {
        "state": (x, normed, qkv, attention, mixture, active, slope, total, result),
        "weights": weights,
        "vectors": (gain, offset, outer, inner),
        "tables": tables,
        "gradients": (upstream, mixture_grad),
        "sums": sums,
    }

    def forward(m, carry):
        pl.when(section == 0)(lambda: taking(whole_in, x, m).wait())
        pl.when(section == 1)(lambda: handing(x, m).wait_recv())
        forward_block(
            m, lengths[m], lambda i: pl.when(m == 0)(lambda: loading(i).wait()), shared
        )

        @pl.when(section == 0)
        def _():
            handing(x, m).start()

        @pl.when(section == 1)
        def _():
            away(hidden_out, 0, m).start()
            kept(hidden_out, half, m).start()

        for i, source in enumerate((normed, mixture, active)):
            giving(i, source, m).start()
        return carry

    lax.fori_loop(0, MICRO, forward, 0)

    def backward(m, carry):
        @pl.when(section == 0)
        def _():
            handing(x, m).wait_send()
            handing(upstream, m).wait_recv()

        @pl.when(section == 1)
        def _():
            away(hidden_out, 0, m).wait_send()
            kept(hidden_out, half, m).wait()
            taking(cotangent, upstream, m).wait()
            row = lax.broadcasted_iota(jnp.int32, (SLOT, 1), 0)
            inside = (row < lengths[m]).astype(jnp.float32)
            masked = upstream[m].astype(jnp.float32) * inside
            upstream[m] = masked.astype(jnp.bfloat16)

        backward_block(m, shared)

        @pl.when(section == 1)
        def _():
            handing(upstream, m).start()

        @pl.when(section == 0)
        def _():
            away(input_grad, half, m).start()
            kept(input_grad, 0, m).start()

        for i, source in enumerate((qkv, slope, upstream)):
            giving(3 + i, source, m).start()
        return carry

    lax.fori_loop(0, MICRO, backward, 0)

    def last(m, carry):
        @pl.when(section == 0)
        def _():
            away(input_grad, half, m).wait_send()
            kept(input_grad, 0, m).wait()
            away(hidden_out, 0, m).wait_recv()

        @pl.when(section == 1)
        def _():
            handing(upstream, m).wait_send()
            away(input_grad, half, m).wait_recv()

        for i, source in enumerate((normed, mixture, active, qkv, slope, upstream)):
            giving(i, source, m).wait()
        return carry

    lax.fori_loop(0, MICRO, last, 0)


def run_blocks(lengths, whole_in, cotangent, vectors, weights, number):
    tokens, width = whole_in.shape
    wide = weights[2].shape[1]
    half = width // lax.axis_size("section")
    low, full = jnp.bfloat16, jnp.float32
    shape = jax.ShapeDtypeStruct
    vmem = pltpu.VMEM
    dma = pltpu.SemaphoreType.DMA
    inside = pl.BlockSpec(memory_space=vmem)
    outputs = [shape((tokens, half), low)] * 2
    outputs += [shape((tokens, n), low) for n in (width, width, wide, 3 * width, wide, width)]
    outputs += [shape((1, n), full) for n in (width, width, width, wide)]
    scratch = [vmem(weight.shape, low) for weight in weights]
    scratch += [
        vmem((MICRO, SLOT, width), low),
        vmem((MICRO, SLOT, width), low),
        vmem((MICRO, SLOT, 3 * width), low),
        vmem((MICRO, HEADS, SLOT, SLOT), low),
        vmem((MICRO, SLOT, width), low),
        vmem((MICRO, SLOT, wide), low),
        vmem((MICRO, SLOT, wide), low),
        vmem((SLOT, width), full),
        vmem((MICRO, SLOT, width), low),
        vmem((MICRO, SLOT, width), low),
        vmem((SLOT, width), low),
        vmem((3, SLOT, 2 * HEAD_DIM), full),
        dma((5,)),
        dma((MICRO,)),
        dma((MICRO,)),
        dma((MICRO,)),
        dma((MICRO,)),
        dma((MICRO,)),
        dma((MICRO,)),
        dma((6, MICRO)),
    ]
    vectors = [vector.astype(full).reshape(1, -1) for vector in vectors]
    return pl.pallas_call(
        blocks_kernel,
        out_shape=outputs,
        in_specs=[pl.BlockSpec(memory_space=pltpu.SMEM), ANY, ANY, ANY] + [inside] * 4 + [ANY] * 4,
        out_specs=[ANY] * 8 + [inside] * 4,
        scratch_shapes=scratch,
        compiler_params=pltpu.CompilerParams(
            collective_id=number, has_side_effects=True, vmem_limit_bytes=60 * 2**20
        ),
        name="two_blocks",
    )(lengths, whole_in, cotangent, jnp.asarray(rotary_rows()), *vectors, *weights)


def pack_small(members):
    flat = jnp.concatenate([member.astype(jnp.float32) for member in members], axis=1)
    flat = jnp.pad(flat, ((0, 0), (0, SMALL_ROWS * LANES - flat.shape[1])))
    return flat.reshape(-1, LANES).astype(jnp.bfloat16)


def unpack_small(packed, widths, devices):
    flat = packed.reshape(devices, -1)
    members, start = [], 0
    for width in widths:
        members.append(flat[:, start : start + width].reshape(-1))
        start += width
    return members


def local(
    hidden_in,
    cotangent,
    lengths,
    norm_gain,
    norm_offset,
    joint_weight,
    output_weight,
    expand_weight,
    inner_bias,
    contract_weight,
    outer_bias,
):
    devices = lax.axis_size("batch")
    vectors_own = (norm_gain, norm_offset, outer_bias, inner_bias)
    (*weights, small_all), (whole_in, whole_cotangent) = gather_all(
        [
            joint_weight[0],
            output_weight[0],
            expand_weight[0],
            contract_weight[0],
            pack_small(vectors_own),
        ],
        [hidden_in, cotangent],
        1,
    )
    vectors = unpack_small(small_all, [member.shape[1] for member in vectors_own], devices)
    results = run_blocks(lengths, whole_in, whole_cotangent, vectors, weights, 2)
    hidden_out, input_grad = results[:2]
    small = results[8:]
    small_packed = pack_small([member.reshape(devices, -1) for member in small])
    shapes = [weight.shape for weight in weights]
    joint_sum, output_sum, expand_sum, contract_sum, small_sum = [
        member.astype(jnp.float32) for member in reduce_all(results[2:8], small_packed, shapes, 3)
    ]
    gain_sum, offset_sum, outer_sum, inner_sum = unpack_small(
        small_sum, [member.shape[1] // devices for member in small], devices
    )
    return (
        hidden_out,
        input_grad,
        gain_sum[None],
        offset_sum[None],
        joint_sum[None],
        output_sum[None],
        expand_sum[None],
        inner_sum[None],
        contract_sum[None],
        outer_sum[None],
    )


def solution(mesh):
    return jax.shard_map(
        local,
        mesh=mesh,
        in_specs=(
            P("batch", "section"),
            P("batch", "section"),
            P("batch"),
            P("section", "batch"),
            P("section", "batch"),
            P("section", "batch", None),
            P("section", "batch", None),
            P("section", "batch", None),
            P("section", "batch"),
            P("section", "batch", None),
            P("section", "batch"),
        ),
        out_specs=(
            P("batch", "section"),
            P("batch", "section"),
            P("section", None),
            P("section", None),
            P("section", None, None),
            P("section", None, None),
            P("section", None, None),
            P("section", None),
            P("section", None, None),
            P("section", None),
        ),
        check_vma=False,
    )
```

```python
from functools import partial

import jax
import jax.numpy as jnp
import numpy as np
from jax import lax
from jax.experimental import pallas as pl
from jax.experimental.pallas import tpu as pltpu
from jax.sharding import PartitionSpec as P

HEADS = 16
HEAD_DIM = 64
ROT = 32
SLOT = 256
MICRO = 2
SMALL_ROWS = 16
LANES = 128
ROW_STEP = 256
FF_STEP = 4096
JOINT_STEP = 1024
GELU_SCALE = (2.0 / np.pi) ** 0.5
GELU_CUBE = 0.044715
norm_epsilon = 1e-05
rotary_base = 10000.0
masked_score = -1e30
MESH = pl.DeviceIdType.MESH
ANY = pl.BlockSpec(memory_space=pl.ANY)


class Place:
    def __init__(self):
        index = lax.axis_index("batch")
        self.levels = lax.axis_size("batch") // 4
        self.last = self.levels - 1
        self.z, self.y, self.c = index // 4, index // 2 % 2, index % 2

    def at(self, z=None, y=None, c=None):
        z = self.z if z is None else z
        y = self.y if y is None else y
        c = self.c if c is None else c
        return z * 4 + y * 2 + c


class Piece:
    def __init__(self, array, offset, rows, column, columns, direct):
        self.array, self.offset, self.rows = array, offset, rows
        self.column, self.columns, self.direct = column, columns, direct

    def sides(self, y):
        return (y,) if self.direct else (y, 1 - y)

    def of(self, block):
        return block.at[pl.ds(self.offset, self.rows), pl.ds(self.column, self.columns)]


def pieces_of(blocks):
    joint, output, expand, contract, small = blocks
    cut = contract[0] // 4
    pieces = [
        Piece(1, 0, output[0], 0, output[1], False),
        Piece(3, 0, cut, 0, contract[1], False),
    ]
    for array, offset, (rows, columns), parts in (
        (0, 0, joint, 1),
        (2, 0, expand, 1),
        (3, cut, contract, 1),
        (4, 0, small, 1),
    ):
        for i in range(parts):
            width = columns // parts
            pieces.append(Piece(array, offset, rows - offset, i * width, width, True))
    return pieces


def remote(source, target, send, receive, index):
    return pltpu.make_async_remote_copy(
        source, target, send, receive, device_id={"batch": index}, device_id_type=MESH
    )


def greet(here, with_section):
    barrier = pltpu.get_barrier_semaphore()

    def signal(**who):
        pl.semaphore_signal(barrier, inc=1, device_id=who, device_id_type=MESH)

    signal(batch=here.at(y=1 - here.y))
    signal(batch=here.at(c=1 - here.c))
    pl.when(here.z > 0)(lambda: signal(batch=here.at(z=here.z - 1)))
    pl.when(here.z < here.last)(lambda: signal(batch=here.at(z=here.z + 1)))
    waits = 2
    if with_section:
        signal(section=1 - lax.axis_index("section"))
        waits = 3
    below = jnp.minimum(here.z, 1)
    above = jnp.minimum(here.last - here.z, 1)
    pl.semaphore_wait(barrier, waits + below + above)


def spread_semaphores(count, levels):
    dma = pltpu.SemaphoreType.DMA
    return [
        dma((count,)),
        dma((count, levels, 2, 2)),
        dma((count, levels, 2)),
        dma((count, levels)),
        dma((count, levels)),
        dma((count, levels, 2)),
        dma((count, levels, 2)),
    ]


class Spread:
    def __init__(self, here, pieces, owns, outs, semaphores):
        self.here, self.pieces, self.owns, self.outs = here, pieces, owns, outs
        (self.keep, self.zs, self.zr, self.ys, self.yr, self.cs, self.cr) = semaphores

    def block(self, p, z, y, c):
        piece = self.pieces[p]
        out = self.outs[piece.array]
        rows = out.shape[0] // (4 * self.here.levels)
        start = (z * 4 + y * 2 + c) * rows + piece.offset
        return out.at[
            pl.ds(pl.multiple_of(start, 8), piece.rows), pl.ds(piece.column, piece.columns)
        ]

    def along(self, p, z, y, source, way):
        here = self.here
        return remote(
            source,
            self.block(p, z, y, here.c),
            self.zs.at[p, z, y, way],
            self.zr.at[p, z, y],
            here.at(z=here.z + (1 if way == 0 else -1)),
        )

    def across(self, p, z, source):
        here = self.here
        target = self.block(p, z, here.y, here.c)
        return remote(source, target, self.ys.at[p, z], self.yr.at[p, z], here.at(y=1 - here.y))

    def beside(self, p, z, y, source):
        here = self.here
        target = self.block(p, z, y, here.c)
        return remote(
            source, target, self.cs.at[p, z, y], self.cr.at[p, z, y], here.at(c=1 - here.c)
        )

    def both_ways(self, p, y, source):
        here = self.here
        pl.when(here.z < here.last)(lambda: self.along(p, here.z, y, source, 0).start())
        pl.when(here.z > 0)(lambda: self.along(p, here.z, y, source, 1).start())

    def begin(self, p, held=False):
        here, own = self.here, self.owns[p]
        self.across(p, here.z, own).start()
        if not held:
            self.both_ways(p, here.y, own)
        self.beside(p, here.z, here.y, own).start()
        target = self.block(p, here.z, here.y, here.c)
        pltpu.make_async_copy(own, target, self.keep.at[p]).start()

    def begin_all(self, chosen):
        order = sorted(chosen, key=lambda p: self.pieces[p].direct)
        for p in order:
            self.begin(p, held=not self.pieces[p].direct)
        for p in order:
            if not self.pieces[p].direct:
                self.both_ways(p, self.here.y, self.owns[p])

    def from_z(self, p, z, y, way):
        here = self.here
        block = self.block(p, z, y, here.c)
        self.along(p, z, y, block, way).wait_recv()
        more = here.z < here.last if way == 0 else here.z > 0
        pl.when(more)(lambda: self.along(p, z, y, block, way).start())
        if self.pieces[p].direct:
            self.across(p, z, block).start()
        self.beside(p, z, y, block).start()

    def from_y(self, p, z):
        here = self.here
        block = self.block(p, z, 1 - here.y, here.c)
        self.across(p, z, block).wait_recv()
        if not self.pieces[p].direct:
            self.both_ways(p, 1 - here.y, block)
        self.beside(p, z, 1 - here.y, block).start()

    def z_events(self, chosen, distance):
        here = self.here

        def pair(p, side):
            y = self.pieces[p].sides(here.y)[side]
            pl.when(here.z - distance >= 0)(lambda: self.from_z(p, here.z - distance, y, 0))
            pl.when(here.z + distance <= here.last)(
                lambda: self.from_z(p, here.z + distance, y, 1)
            )

        for p in chosen:
            if self.pieces[p].direct:
                pair(p, 0)
        for side in range(2):
            for p in chosen:
                if not self.pieces[p].direct:
                    pair(p, side)

    def y_events(self, chosen, z):
        for p in chosen:
            if self.pieces[p].direct:
                self.from_y(p, z)

    def middle(self, chosen, then=None):
        here = self.here
        for p in chosen:
            if not self.pieces[p].direct:
                self.from_y(p, here.z)

        def y_pair(distance):
            pl.when(here.z - distance >= 0)(lambda: self.y_events(chosen, here.z - distance))
            pl.when((here.z + distance <= here.last) & (distance > 0))(
                lambda: self.y_events(chosen, here.z + distance)
            )

        def step(distance, carry):
            self.z_events(chosen, distance)
            y_pair(distance - 1)
            return carry

        lax.fori_loop(1, here.levels, step, 0)
        if then is not None:
            then()
        y_pair(here.last)

    def received(self, chosen):
        here = self.here

        def level(z, carry):
            for p in chosen:
                own = self.block(p, z, here.y, here.c)
                for y in range(2):
                    self.beside(p, z, y, own).wait_recv()
            return carry

        lax.fori_loop(0, here.levels, level, 0)
        for p in chosen:
            block = self.block(p, here.z, here.y, here.c)
            pltpu.make_async_copy(block, block, self.keep.at[p]).wait()

    def sent(self):
        here = self.here

        def level(z, carry):
            for p, piece in enumerate(self.pieces):
                own = self.block(p, z, here.y, here.c)
                for y in range(2):
                    self.beside(p, z, y, own).wait_send()
                crossed = z >= 0 if piece.direct else z == here.z
                pl.when(crossed)(lambda p=p, own=own: self.across(p, z, own).wait_send())
                for y in piece.sides(here.y):
                    pl.when((z <= here.z) & (here.z < here.last))(
                        lambda p=p, y=y, own=own: self.along(p, z, y, own, 0).wait_send()
                    )
                    pl.when((z >= here.z) & (here.z > 0))(
                        lambda p=p, y=y, own=own: self.along(p, z, y, own, 1).wait_send()
                    )
            return carry

        lax.fori_loop(0, here.levels, level, 0)


def add_rows(target, other):
    rows = target.shape[0]
    step = min(rows, 16)

    def body(i, carry):
        at = pl.ds(pl.multiple_of(i * step, step), step)
        total = target[at, :].astype(jnp.float32) + other[at, :].astype(jnp.float32)
        target[at, :] = total.astype(target.dtype)
        return carry

    lax.fori_loop(0, rows // step, body, 0)


FACTORS = ((0, 3), (1, 5), (0, 4), (2, 5))
MAKE_ORDER = (1, 3, 0, 2, 4)
COLUMN_STEP = 1024


class Reduce:
    def __init__(self, here, pieces, factors, small, product_rows, buffers, semaphores):
        self.here, self.pieces, self.factors, self.small = here, pieces, factors, small
        self.made = product_rows
        self.mine, self.sent, self.sib, self.yb, self.zb = buffers
        (self.load, self.cs, self.cr, self.ys, self.yr, self.zs, self.zr, self.credit) = semaphores

    def level(self, i):
        here = self.here
        above, below = here.last - here.z, here.z
        lead = jnp.maximum(above, below) - jnp.minimum(above, below)
        single = jnp.where(above > below, here.last - i, i)
        later = i - lead
        distance = jnp.minimum(above, below) - later // 2
        outer = jnp.where(above > below, here.z - distance, here.z + distance)
        paired = jnp.where(later % 2 == 0, outer, 2 * here.z - outer)
        return jnp.where(i < lead, single, paired)

    def to_core(self, p, slot, y):
        here = self.here
        return remote(
            self.sent[p].at[slot, y],
            self.sib[p].at[slot, y],
            self.cs.at[p, slot, y],
            self.cr.at[p, slot, y],
            here.at(c=1 - here.c),
        )

    def to_y(self, p, z):
        here = self.here
        return remote(
            self.mine[p].at[z, 1 - here.y],
            self.yb[p].at[z if self.pieces[p].direct else 0],
            self.ys.at[p, z],
            self.yr.at[p, z],
            here.at(y=1 - here.y),
        )

    def slot(self, z, at_z, way):
        if way == 0:
            return z
        return jnp.where(z == at_z, self.here.levels, z)

    def to_z(self, p, z, y, way):
        here = self.here
        step = 1 if way == 0 else -1
        slot = self.slot(z, here.z + step, way)
        side = 0 if self.pieces[p].direct else y
        return remote(
            self.mine[p].at[z, y],
            self.zb[p].at[slot, side],
            self.zs.at[p, z, side],
            self.zr.at[p, slot, side],
            here.at(z=here.z + step),
        )

    def arrive(self, p, z, y, way):
        here = self.here
        slot = self.slot(z, here.z, way)
        side = 0 if self.pieces[p].direct else y
        block = self.zb[p].at[slot, side]
        remote(
            block, block, self.zs.at[p, z, side], self.zr.at[p, slot, side], here.at(y=1 - here.y)
        ).wait_recv()
        add_rows(self.mine[p].at[z, y], block)

    def store(self, array, z, slot, y, own, value, column):
        for p, piece in enumerate(self.pieces):
            first = max(column, piece.column)
            end = min(column + value.shape[1], piece.column + piece.columns)
            if piece.array == array and first < end:
                target = self.mine[p].at[z, y] if own else self.sent[p].at[slot, y]
                part = value[piece.offset : piece.offset + piece.rows, first - column : end - column]
                target[:, first - piece.column : end - piece.column] = part.astype(jnp.bfloat16)

    def make(self, array, z, slot):
        here = self.here
        rows = max(p.offset + p.rows for p in self.pieces if p.array == array)
        cores = ((False, 1 - here.c), (True, here.c))
        if array == 4:
            for own, c in cores:
                for y in range(2):
                    at = pl.multiple_of((z * 4 + y * 2 + c) * rows, 16)
                    self.store(array, z, slot, y, own, self.small[pl.ds(at, rows), :], 0)
            return
        left, right = (self.factors[i] for i in FACTORS[array])
        columns = right.shape[1]
        tiles = range(0, columns, COLUMN_STEP)
        if rows % 128 == 0:
            for own, c in cores:
                for y in range(2):
                    at = pl.multiple_of((z * 4 + y * 2 + c) * rows, 128)
                    turned = left[:, pl.ds(at, rows)].T
                    for tile in tiles:
                        value = product(turned, right[:, tile : tile + COLUMN_STEP])
                        self.store(array, z, slot, y, own, value, tile)
            return
        span = max(4 * rows, 128)
        start = z * 4 * rows // span * span
        turned = left[:, pl.ds(pl.multiple_of(start, 128), span)].T
        for tile in tiles:
            self.made[:span, :] = product(turned, right[:, tile : tile + COLUMN_STEP])
            for own, c in cores:
                for y in range(2):
                    at = pl.multiple_of((z * 4 + y * 2 + c) * rows - start, 8)
                    self.store(array, z, slot, y, own, self.made[pl.ds(at, rows), :], tile)

    def of(self, array):
        return [p for p, piece in enumerate(self.pieces) if piece.array == array]

    def build(self, i, waits):
        here = self.here
        z, slot = self.level(i), i % 2

        @pl.when(i >= 2)
        def _():
            for p in range(len(self.pieces)):
                for y in range(2):
                    self.to_core(p, slot, y).wait_send()
            pl.semaphore_wait(self.credit, 1)

        def add(array):
            for p in self.of(array):
                for y in range(2):
                    self.to_core(p, slot, y).wait_recv()
                    add_rows(self.mine[p].at[z, y], self.sib[p].at[slot, y])
                if self.pieces[p].direct:
                    self.to_y(p, z).start()
                else:
                    self.pass_on(z, [p])

        for step, array in enumerate(MAKE_ORDER):
            waits(i, array)
            self.make(array, z, slot)
            for p in self.of(array):
                for y in range(2):
                    self.to_core(p, slot, y).start()
            if step > 0:
                add(MAKE_ORDER[step - 1])
        add(MAKE_ORDER[-1])

        @pl.when(i < here.levels - 2)
        def _():
            other = {"batch": here.at(c=1 - here.c)}
            pl.semaphore_signal(self.credit, inc=1, device_id=other, device_id_type=MESH)

    def rows(self, p, z):
        self.to_y(p, z).wait_recv()
        source = self.yb[p].at[z if self.pieces[p].direct else 0]
        add_rows(self.mine[p].at[z, self.here.y], source)

    def pass_on(self, z, chosen):
        here = self.here

        def hop(way):
            further = here.z > 0 if way == 0 else here.z < here.last
            for p in chosen:
                if self.pieces[p].direct:
                    self.rows(p, z)
                for y in self.pieces[p].sides(here.y):
                    pl.when(further)(lambda p=p, y=y: self.arrive(p, z, y, way))
                    self.to_z(p, z, y, way).start()

        pl.when(z > here.z)(lambda: hop(0))
        pl.when(z < here.z)(lambda: hop(1))

    def run(self, waits):
        here = self.here
        made = [p for array in MAKE_ORDER for p in self.of(array)]
        direct = [p for p in made if self.pieces[p].direct]

        def step(i, carry):
            self.build(i, waits)
            pl.when(i > 0)(lambda: self.pass_on(self.level(i - 1), direct))
            return carry

        lax.fori_loop(0, here.levels, step, 0)

    def settle(self, p):
        here = self.here
        for y in self.pieces[p].sides(here.y):
            pl.when(here.z > 0)(lambda y=y: self.arrive(p, here.z, y, 0))
            pl.when(here.z < here.last)(lambda y=y: self.arrive(p, here.z, y, 1))

    def finish(self):
        here = self.here
        for slot in range(min(2, here.levels)):
            for p in range(len(self.pieces)):
                for y in range(2):
                    self.to_core(p, slot, y).wait_send()

        def level(z, carry):
            for p, piece in enumerate(self.pieces):
                crossed = z >= 0 if piece.direct else z == here.z
                pl.when(crossed)(lambda p=p: self.to_y(p, z).wait_send())
                for y in piece.sides(here.y):
                    pl.when(z > here.z)(lambda p=p, y=y: self.to_z(p, z, y, 0).wait_send())
                    pl.when(z < here.z)(lambda p=p, y=y: self.to_z(p, z, y, 1).wait_send())
            return carry

        lax.fori_loop(0, here.levels, level, 0)


def reduce_kernel(pieces, *refs):
    count = len(pieces)
    sources, outs, rest = refs[:7], refs[7:12], refs[12:]
    factors, small, made = rest[:6], rest[6], rest[7]
    rest = rest[8:]
    buffers = [rest[i * count : (i + 1) * count] for i in range(5)]
    rest = rest[5 * count :]
    here = Place()
    loads = [
        pltpu.make_async_copy(source, target, rest[0].at[i])
        for i, (source, target) in enumerate(zip(sources, [*factors, small]))
    ]
    order = (1, 5, 2, 0, 3, 4, 6)
    for i in order:
        loads[i].start()
    greet(here, False)
    reduce = Reduce(here, pieces, factors, small, made, buffers, rest[:8])
    needs = {1: (1, 5), 3: (2,), 0: (0, 3), 2: (4,), 4: (6,)}

    def waits(i, array):
        @pl.when(i == 0)
        def _():
            for k in needs[array]:
                loads[k].wait()

    reduce.run(waits)
    owns = [buffers[0][p].at[here.z, here.y] for p in range(count)]
    spread = Spread(here, pieces, owns, outs, rest[8:])
    turned = [p for p in range(count) if not pieces[p].direct]
    for p in turned:
        reduce.settle(p)
        reduce.to_y(p, here.z).start()
    for p in range(count):
        if pieces[p].direct:
            reduce.rows(p, here.z)
            reduce.settle(p)
            spread.begin(p)
    for p in turned:
        reduce.rows(p, here.z)
        spread.begin(p)
    spread.middle(range(count))
    reduce.finish()
    spread.received(range(count))
    spread.sent()


def reduce_all(factors, small, shapes, number):
    levels = lax.axis_size("batch") // 4
    shapes = [*shapes, small.shape]
    pieces = pieces_of([(rows // (4 * levels), columns) for rows, columns in shapes])
    count = len(pieces)
    dma = pltpu.SemaphoreType.DMA
    low = jnp.bfloat16
    scratch = [pltpu.VMEM(factor.shape, low) for factor in factors]
    scratch += [pltpu.VMEM(small.shape, low), pltpu.VMEM((256, COLUMN_STEP), jnp.float32)]
    blocks = [(piece.rows, piece.columns) for piece in pieces]
    scratch += [pltpu.VMEM((levels, 2) + block, low) for block in blocks]
    scratch += [pltpu.VMEM((2, 2) + block, low) for block in blocks] * 2
    scratch += [
        pltpu.VMEM((levels if piece.direct else 1,) + block, low)
        for piece, block in zip(pieces, blocks)
    ]
    scratch += [
        pltpu.VMEM((levels + 1, 1 if piece.direct else 2) + block, low)
        for piece, block in zip(pieces, blocks)
    ]
    scratch += [
        dma((7,)),
        dma((count, 2, 2)),
        dma((count, 2, 2)),
        dma((count, levels)),
        dma((count, levels)),
        dma((count, levels, 2)),
        dma((count, levels + 1, 2)),
        pltpu.SemaphoreType.REGULAR,
    ] + spread_semaphores(count, levels)
    return pl.pallas_call(
        partial(reduce_kernel, pieces),
        out_shape=[jax.ShapeDtypeStruct(shape, low) for shape in shapes],
        in_specs=[ANY] * 7,
        out_specs=[ANY] * 5,
        scratch_shapes=scratch,
        compiler_params=pltpu.CompilerParams(
            collective_id=number, has_side_effects=True, vmem_limit_bytes=60 * 2**20
        ),
        name="reduce_gradients",
    )(*factors, small)


def rotary_rows():
    positions = np.arange(SLOT, dtype=np.float64)[:, None]
    lane = np.arange(2 * HEAD_DIM)[None, :] % HEAD_DIM
    angles = positions * rotary_base ** (-(lane // 2 * 2.0) / ROT)
    turned = lane < ROT
    cosine = np.where(turned, np.cos(angles), 1.0)
    sine = np.where(turned, np.sin(angles), 0.0)
    even = np.where(lane % 2 == 0, sine, 0.0)
    odd = np.where(lane % 2 == 1, sine, 0.0)
    return np.stack([cosine, even, odd]).astype(np.float32)


def turn(pair, tables, back):
    lanes = pair.shape[1]
    following = pltpu.roll(pair, lanes - 1, 1)
    preceding = pltpu.roll(pair, 1, 1)
    side = following * tables[1] - preceding * tables[2]
    return pair * tables[0] + (side if back else -side)


def product(left, right, left_axis=1, right_axis=0):
    return lax.dot_general(
        left, right, (((left_axis,), (right_axis,)), ((), ())), preferred_element_type=jnp.float32
    )


def statistics(rows):
    average = jnp.mean(rows, axis=-1, keepdims=True)
    centered = rows - average
    variance = jnp.mean(centered * centered, axis=-1, keepdims=True)
    inverse = lax.rsqrt(variance + norm_epsilon)
    return centered * inverse, inverse


def low_lanes(width):
    return lax.broadcasted_iota(jnp.int32, (1, width), 1) < HEAD_DIM


def pair_lanes(index):
    return pl.ds(pl.multiple_of(index * 2 * HEAD_DIM, 2 * HEAD_DIM), 2 * HEAD_DIM)


def rows_at(index, step):
    return pl.ds(pl.multiple_of(index * step, step), step)


def attend(m, length, refs):
    (x, normed, qkv, attention, mixture, active, slope, total, result) = refs["state"]
    joint, output, expand, contract = refs["weights"]
    gain, offset, outer, inner = refs["vectors"]
    tables = refs["tables"]
    width = x.shape[2]

    def norm(i, carry):
        at = rows_at(i, ROW_STEP)
        standard, _ = statistics(x[m, at, :].astype(jnp.float32))
        normed[m, at, :] = (standard * gain[...] + offset[...]).astype(jnp.bfloat16)
        return carry

    lax.fori_loop(0, SLOT // ROW_STEP, norm, 0)
    for part in range(3):
        scale = HEAD_DIM**-0.5 if part == 0 else 1.0
        total[...] = product(normed[m], joint[:, part * width : (part + 1) * width])
        if part == 2:
            qkv[m, :, 2 * width :] = total[...].astype(jnp.bfloat16)
        else:

            def rotary(i, carry, part=part, scale=scale):
                pair = turn(total[:, pair_lanes(i)], tables, False)
                at = pair_lanes(i + part * (width // (2 * HEAD_DIM)))
                qkv[m, :, at] = pair.astype(jnp.bfloat16) * jnp.bfloat16(scale)
                return carry

            lax.fori_loop(0, width // (2 * HEAD_DIM), rotary, 0)

    query = lax.broadcasted_iota(jnp.int32, (SLOT, SLOT), 0)
    key = lax.broadcasted_iota(jnp.int32, (SLOT, SLOT), 1)
    allowed = (key <= query) & (key < length)
    pairs = width // (2 * HEAD_DIM)
    low = low_lanes(2 * HEAD_DIM)

    def heads(i, carry):
        queries, keys = qkv[m, :, pair_lanes(i)], qkv[m, :, pair_lanes(i + pairs)]
        values = qkv[m, :, pair_lanes(i + 2 * pairs)]
        mixed = []
        for half in range(2):
            own = jnp.where(low == (half == 0), queries, jnp.zeros_like(queries))
            scores = jnp.where(allowed, product(own, keys, 1, 1), masked_score)
            raised = jnp.exp(scores - jnp.max(scores, axis=-1, keepdims=True))
            share = raised * (1.0 / jnp.sum(raised, axis=-1, keepdims=True))
            share = share.astype(jnp.bfloat16)
            attention[m, 2 * i + half] = share
            mixed.append(product(share, values))
        mixture[m, :, pair_lanes(i)] = jnp.where(low, mixed[0], mixed[1]).astype(jnp.bfloat16)
        return carry

    lax.fori_loop(0, pairs, heads, 0, unroll=8)


def feed(m, refs):
    (x, normed, _, _, mixture, active, slope, total, result) = refs["state"]
    joint, output, expand, contract = refs["weights"]
    gain, offset, outer, inner = refs["vectors"]
    total[...] = x[m].astype(jnp.float32) + outer[...] + product(mixture[m], output[...])

    def hidden(i, carry):
        at = rows_at(i, FF_STEP)
        pre = product(normed[m], expand[:, at]) + inner[:, at]
        square = pre * pre
        bend = jnp.tanh(GELU_SCALE * (pre + GELU_CUBE * (square * pre)))
        lifted = 0.5 * (1.0 + bend)
        slant = (0.5 * GELU_SCALE) * (1.0 + (3.0 * GELU_CUBE) * square)
        slope[m, :, at] = (lifted + pre * (1.0 - bend * bend) * slant).astype(jnp.bfloat16)
        activated = (pre * lifted).astype(jnp.bfloat16)
        active[m, :, at] = activated
        total[...] += product(activated, contract[at, :])
        return carry

    lax.fori_loop(0, slope.shape[2] // FF_STEP, hidden, 0)
    result[m] = total[...].astype(jnp.bfloat16)


def backward_block(m, refs):
    (x, _, qkv, attention, _, _, slope, total, result) = refs["state"]
    joint, output, expand, contract = refs["weights"]
    gain, offset, outer, inner = refs["vectors"]
    upstream, mixture_grad = refs["gradients"]
    gain_sum, offset_sum, outer_sum, inner_sum = refs["sums"]
    tables = refs["tables"]
    width = x.shape[2]
    outer_sum[...] += jnp.sum(upstream[m].astype(jnp.float32), axis=0, keepdims=True)
    mixture_grad[...] = product(upstream[m], output[...], 1, 1).astype(jnp.bfloat16)
    total[...] = jnp.zeros_like(total)

    def hidden(i, carry):
        at = rows_at(i, FF_STEP)
        active_grad = product(upstream[m], contract[at, :], 1, 1)
        pre_grad = (active_grad * slope[m, :, at].astype(jnp.float32)).astype(jnp.bfloat16)
        slope[m, :, at] = pre_grad
        inner_sum[:, at] += jnp.sum(pre_grad.astype(jnp.float32), axis=0, keepdims=True)
        total[...] += product(pre_grad, expand[:, at], 1, 1)
        return carry

    lax.fori_loop(0, slope.shape[2] // FF_STEP, hidden, 0)
    pairs = width // (2 * HEAD_DIM)
    low = low_lanes(2 * HEAD_DIM)

    def heads(i, carry):
        queries, keys = qkv[m, :, pair_lanes(i)], qkv[m, :, pair_lanes(i + pairs)]
        values = qkv[m, :, pair_lanes(i + 2 * pairs)]
        mixed_grad = mixture_grad[:, pair_lanes(i)]
        query_grads, key_grads, value_grads = [], [], []
        for half in range(2):
            share = attention[m, 2 * i + half]
            own = jnp.where(low == (half == 0), mixed_grad, jnp.zeros_like(mixed_grad))
            value_grads.append(product(share, mixed_grad, 0, 0))
            share_grad = product(own, values, 1, 1)
            weight = share.astype(jnp.float32)
            weighted = weight * share_grad
            score_grad = weighted - weight * jnp.sum(weighted, axis=-1, keepdims=True)
            score_grad = score_grad.astype(jnp.bfloat16)
            query_grads.append(product(score_grad, keys))
            key_grads.append(product(score_grad, queries, 0, 0))
        query_grad = jnp.where(low, query_grads[0], query_grads[1]) * HEAD_DIM**-0.5
        key_grad = jnp.where(low, key_grads[0], key_grads[1])
        value_grad = jnp.where(low, value_grads[0], value_grads[1])
        qkv[m, :, pair_lanes(i)] = turn(query_grad, tables, True).astype(jnp.bfloat16)
        qkv[m, :, pair_lanes(i + pairs)] = turn(key_grad, tables, True).astype(jnp.bfloat16)
        qkv[m, :, pair_lanes(i + 2 * pairs)] = value_grad.astype(jnp.bfloat16)
        return carry

    lax.fori_loop(0, pairs, heads, 0, unroll=2)

    def project(i, carry):
        at = rows_at(i, JOINT_STEP)
        total[:, at] += product(qkv[m], joint[at, :], 1, 1)
        return carry

    lax.fori_loop(0, width // JOINT_STEP, project, 0)

    def norm(i, carry):
        at = rows_at(i, ROW_STEP)
        standard, inverse = statistics(x[m, at, :].astype(jnp.float32))
        normed_grad = total[at, :]
        gain_sum[...] += jnp.sum(normed_grad * standard, axis=0, keepdims=True)
        offset_sum[...] += jnp.sum(normed_grad, axis=0, keepdims=True)
        scaled = normed_grad * gain[...]
        inner_mean = jnp.mean(scaled, axis=-1, keepdims=True)
        along = jnp.mean(scaled * standard, axis=-1, keepdims=True)
        change = inverse * (scaled - inner_mean - standard * along)
        result[m, at, :] = (upstream[m, at, :].astype(jnp.float32) + change).astype(jnp.bfloat16)
        return carry

    lax.fori_loop(0, SLOT // ROW_STEP, norm, 0)


def vector_rows(width):
    return max(1, width // LANES), max(1, LANES // width)


def lane_range(device, width):
    lane = lax.broadcasted_iota(jnp.int32, (1, LANES), 1)
    start = device * width % LANES
    return (lane >= start) & (lane < start + width)


def unpack_vectors(small, devices, vectors):
    width = vectors[0].shape[1] // devices
    wide = vectors[3].shape[1] // devices

    def gathered(index, shared):
        rows = small[pl.ds(pl.multiple_of(index * shared * SMALL_ROWS, SMALL_ROWS), SMALL_ROWS), :]
        total = rows.astype(jnp.float32)
        for other in range(1, shared):
            at = pl.multiple_of((index * shared + other) * SMALL_ROWS, SMALL_ROWS)
            total += small[pl.ds(at, SMALL_ROWS), :].astype(jnp.float32)
        return total

    _, shared = vector_rows(width)

    def narrow(index, carry):
        total = gathered(index, shared)
        at = rows_at(index, LANES)
        for i in range(3):
            vectors[i][:, at] = total[i : i + 1]
        return carry

    lax.fori_loop(0, devices // shared, narrow, 0)
    count, shared_wide = vector_rows(wide)

    def broad(index, carry):
        total = gathered(index, shared_wide)
        for i in range(count):
            vectors[3][:, rows_at(index * count + i, LANES)] = total[3 + i : 4 + i]
        return carry

    lax.fori_loop(0, devices // shared_wide, broad, 0)


def pack_sums(sums, devices, packed):
    width = sums[0].shape[1] // devices
    wide = sums[3].shape[1] // devices
    count, _ = vector_rows(wide)
    row = lax.broadcasted_iota(jnp.int32, (SMALL_ROWS, LANES), 0)

    def device(index, carry):
        rows = []
        inside = lane_range(index, width)
        for i in range(3):
            rows.append(jnp.where(inside, sums[i][:, rows_at(index * width // LANES, LANES)], 0.0))
        for i in range(count):
            line = sums[3][:, rows_at(index * wide // LANES + i, LANES)]
            rows.append(line if wide >= LANES else jnp.where(lane_range(index, wide), line, 0.0))
        block = jnp.zeros((SMALL_ROWS, LANES), jnp.float32)
        for i, line in enumerate(rows):
            block = jnp.where(row == i, line, block)
        packed[rows_at(index, SMALL_ROWS), :] = block.astype(jnp.bfloat16)
        return carry

    lax.fori_loop(0, devices, device, 0)


def blocks_kernel(pieces, *refs):
    lengths, hidden_in, cotangent, tables_in = refs[:4]
    sources = refs[4:9]
    hidden_out, input_grad = refs[9:11]
    factor_outs, packed = refs[11:17], refs[17]
    weights, small = refs[18:22], refs[22]
    x, normed, qkv, attention, mixture, active, slope, total, result = refs[23:32]
    upstream, mixture_grad, tables = refs[32:35]
    vectors, sums = refs[35:39], refs[39:43]
    table_sem, in_keep, in_send, in_receive, hand_send, hand_receive = refs[43:49]
    half_send, half_receive, half_keep, out_sem = refs[49:53]
    here = Place()
    section = lax.axis_index("section")
    partner = {"section": 1 - section}
    half = hidden_out.shape[1]
    devices = 4 * here.levels

    def keeping(source, target, start, m):
        return pltpu.make_async_copy(
            source.at[rows_at(m, SLOT), :], target.at[m, :, pl.ds(start, half)], in_keep.at[m]
        )

    def halving(source, target, start, m):
        return pltpu.make_async_remote_copy(
            source.at[rows_at(m, SLOT), :],
            target.at[m, :, pl.ds(start, half)],
            in_send.at[m],
            in_receive.at[m],
            device_id=partner,
            device_id_type=MESH,
        )

    def handing(target, m):
        return pltpu.make_async_remote_copy(
            result.at[m],
            target.at[m],
            hand_send.at[m],
            hand_receive.at[m],
            device_id=partner,
            device_id_type=MESH,
        )

    def away(target, start, m):
        return pltpu.make_async_remote_copy(
            result.at[m, :, pl.ds(start, half)],
            target.at[rows_at(m, SLOT), :],
            half_send.at[m],
            half_receive.at[m],
            device_id=partner,
            device_id_type=MESH,
        )

    def kept(target, start, m):
        return pltpu.make_async_copy(
            result.at[m, :, pl.ds(start, half)], target.at[rows_at(m, SLOT), :], half_keep.at[m]
        )

    def giving(i, source, m):
        return pltpu.make_async_copy(
            source.at[m], factor_outs[i].at[rows_at(m, SLOT), :], out_sem.at[i, m]
        )

    reading = pltpu.make_async_copy(tables_in, tables, table_sem.at[0])
    reading.start()
    for m in range(MICRO):
        pl.when(section == 0)(lambda m=m: keeping(hidden_in, x, 0, m).start())
        pl.when(section == 1)(lambda m=m: keeping(cotangent, upstream, half, m).start())
    for total_sum in sums:
        total_sum[...] = jnp.zeros_like(total_sum)
    greet(here, True)
    owns = [piece.of(sources[piece.array]) for piece in pieces]
    spread = Spread(here, pieces, owns, [*weights, small], refs[53:])
    early = [p for p, piece in enumerate(pieces) if piece.array in (0, 1, 4)]
    late = [p for p, piece in enumerate(pieces) if piece.array in (2, 3)]
    spread.begin_all(early)
    for m in range(MICRO):
        pl.when(section == 1)(lambda m=m: halving(hidden_in, x, half, m).start())
        pl.when(section == 0)(lambda m=m: halving(cotangent, upstream, 0, m).start())
    shared = {
        "state": (x, normed, qkv, attention, mixture, active, slope, total, result),
        "weights": weights,
        "vectors": vectors,
        "tables": tables,
        "gradients": (upstream, mixture_grad),
        "sums": sums,
    }
    spread.middle(early, lambda: spread.begin_all(late))
    spread.received(early)
    unpack_vectors(small, devices, vectors)
    reading.wait()

    @pl.when(section == 0)
    def _():
        def ahead(m, carry):
            keeping(hidden_in, x, 0, m).wait()
            halving(hidden_in, x, half, m).wait_recv()
            attend(m, lengths[m], shared)
            return carry

        lax.fori_loop(0, MICRO, ahead, 0)

    spread.middle(late)
    spread.received(late)

    def forward(m, carry):
        @pl.when(section == 1)
        def _():
            handing(x, m).wait_recv()
            attend(m, lengths[m], shared)

        feed(m, shared)

        @pl.when(section == 0)
        def _():
            handing(x, m).start()

        @pl.when(section == 1)
        def _():
            away(hidden_out, 0, m).start()
            kept(hidden_out, half, m).start()

        for i, source in enumerate((normed, mixture, active)):
            giving(i, source, m).start()
        return carry

    lax.fori_loop(0, MICRO, forward, 0)

    def backward(m, carry):
        @pl.when(section == 0)
        def _():
            handing(x, m).wait_send()
            handing(upstream, m).wait_recv()

        @pl.when(section == 1)
        def _():
            away(hidden_out, 0, m).wait_send()
            kept(hidden_out, half, m).wait()
            keeping(cotangent, upstream, half, m).wait()
            halving(cotangent, upstream, 0, m).wait_recv()
            row = lax.broadcasted_iota(jnp.int32, (SLOT, 1), 0)
            inside = (row < lengths[m]).astype(jnp.float32)
            masked = upstream[m].astype(jnp.float32) * inside
            upstream[m] = masked.astype(jnp.bfloat16)

        backward_block(m, shared)

        @pl.when(section == 1)
        def _():
            handing(upstream, m).start()

        @pl.when(section == 0)
        def _():
            away(input_grad, half, m).start()
            kept(input_grad, 0, m).start()

        for i, source in enumerate((qkv, slope, upstream)):
            giving(3 + i, source, m).start()
        return carry

    lax.fori_loop(0, MICRO, backward, 0)
    pack_sums(sums, devices, packed)

    def last(m, carry):
        @pl.when(section == 0)
        def _():
            halving(cotangent, upstream, 0, m).wait_send()
            away(input_grad, half, m).wait_send()
            kept(input_grad, 0, m).wait()
            away(hidden_out, 0, m).wait_recv()

        @pl.when(section == 1)
        def _():
            halving(hidden_in, x, half, m).wait_send()
            handing(upstream, m).wait_send()
            away(input_grad, half, m).wait_recv()

        for i, source in enumerate((normed, mixture, active, qkv, slope, upstream)):
            giving(i, source, m).wait()
        return carry

    lax.fori_loop(0, MICRO, last, 0)
    spread.sent()


def run_blocks(lengths, hidden_in, cotangent, owns, number):
    levels = lax.axis_size("batch") // 4
    devices = 4 * levels
    tokens, half = hidden_in.shape
    width = half * lax.axis_size("section")
    wide = owns[2].shape[1]
    low, full = jnp.bfloat16, jnp.float32
    shape = jax.ShapeDtypeStruct
    vmem = pltpu.VMEM
    dma = pltpu.SemaphoreType.DMA
    pieces = pieces_of([own.shape for own in owns])
    outputs = [shape((tokens, half), low)] * 2
    outputs += [shape((tokens, n), low) for n in (width, width, wide, 3 * width, wide, width)]
    outputs += [shape((devices * SMALL_ROWS, LANES), low)]
    scratch = [vmem((devices * own.shape[0], own.shape[1]), low) for own in owns]
    scratch += [
        vmem((MICRO, SLOT, width), low),
        vmem((MICRO, SLOT, width), low),
        vmem((MICRO, SLOT, 3 * width), low),
        vmem((MICRO, HEADS, SLOT, SLOT), low),
        vmem((MICRO, SLOT, width), low),
        vmem((MICRO, SLOT, wide), low),
        vmem((MICRO, SLOT, wide), low),
        vmem((SLOT, width), full),
        vmem((MICRO, SLOT, width), low),
        vmem((MICRO, SLOT, width), low),
        vmem((SLOT, width), low),
        vmem((3, SLOT, 2 * HEAD_DIM), full),
    ]
    scratch += [vmem((1, n), full) for n in (width, width, width, wide)] * 2
    scratch += [dma((1,))] + [dma((MICRO,))] * 8 + [dma((6, MICRO))]
    scratch += spread_semaphores(len(pieces), levels)
    return pl.pallas_call(
        partial(blocks_kernel, pieces),
        out_shape=outputs,
        in_specs=[pl.BlockSpec(memory_space=pltpu.SMEM)] + [ANY] * 8,
        out_specs=[ANY] * 8 + [pl.BlockSpec(memory_space=vmem)],
        scratch_shapes=scratch,
        compiler_params=pltpu.CompilerParams(
            collective_id=number, has_side_effects=True, vmem_limit_bytes=60 * 2**20
        ),
        name="two_blocks",
    )(lengths, hidden_in, cotangent, jnp.asarray(rotary_rows()), *owns)


def pack_vectors(vectors):
    device = lax.axis_index("batch")
    rows = []
    for vector in vectors:
        width = vector.shape[1]
        if width >= LANES:
            rows.append(vector.reshape(-1, LANES))
            continue
        lines = jnp.tile(vector, (1, LANES // width))
        rows.append(jnp.where(lane_range(device, width), lines, jnp.zeros_like(lines)))
    rows = jnp.concatenate(rows)
    return jnp.pad(rows, ((0, SMALL_ROWS - rows.shape[0]), (0, 0)))


def unpack_sums(packed, width, wide, devices):
    rows = packed.astype(jnp.float32).reshape(devices, SMALL_ROWS, LANES)
    _, shared = vector_rows(width)
    narrow = rows.reshape(-1, shared, SMALL_ROWS, LANES).sum(axis=1)
    count, shared_wide = vector_rows(wide)
    broad = rows.reshape(-1, shared_wide, SMALL_ROWS, LANES).sum(axis=1)
    members = [narrow[:, i].reshape(1, -1) for i in range(3)]
    return members + [broad[:, 3 : 3 + count].reshape(1, -1)]


def local(
    hidden_in,
    cotangent,
    lengths,
    norm_gain,
    norm_offset,
    joint_weight,
    output_weight,
    expand_weight,
    inner_bias,
    contract_weight,
    outer_bias,
):
    devices = lax.axis_size("batch")
    owns = [
        joint_weight[0],
        output_weight[0],
        expand_weight[0],
        contract_weight[0],
        pack_vectors((norm_gain, norm_offset, outer_bias, inner_bias)),
    ]
    results = run_blocks(lengths, hidden_in, cotangent, owns, 1)
    hidden_out, input_grad = results[:2]
    shapes = [(own.shape[0] * devices, own.shape[1]) for own in owns[:4]]
    joint_sum, output_sum, expand_sum, contract_sum, small_sum = reduce_all(
        results[2:8], results[8], shapes, 2
    )
    gain_sum, offset_sum, outer_sum, inner_sum = unpack_sums(
        small_sum, norm_gain.shape[1], inner_bias.shape[1], devices
    )
    joint_sum, output_sum, expand_sum, contract_sum = [
        member.astype(jnp.float32)[None]
        for member in (joint_sum, output_sum, expand_sum, contract_sum)
    ]
    return (
        hidden_out,
        input_grad,
        gain_sum,
        offset_sum,
        joint_sum,
        output_sum,
        expand_sum,
        inner_sum,
        contract_sum,
        outer_sum,
    )


def solution(mesh):
    return jax.shard_map(
        local,
        mesh=mesh,
        in_specs=(
            P("batch", "section"),
            P("batch", "section"),
            P("batch"),
            P("section", "batch"),
            P("section", "batch"),
            P("section", "batch", None),
            P("section", "batch", None),
            P("section", "batch", None),
            P("section", "batch"),
            P("section", "batch", None),
            P("section", "batch"),
        ),
        out_specs=(
            P("batch", "section"),
            P("batch", "section"),
            P("section", None),
            P("section", None),
            P("section", None, None),
            P("section", None, None),
            P("section", None, None),
            P("section", None),
            P("section", None, None),
            P("section", None),
        ),
        check_vma=False,
    )
```

```python
from functools import partial

import jax
import jax.numpy as jnp
import numpy as np
from jax import lax
from jax.experimental import pallas as pl
from jax.experimental.pallas import tpu as pltpu
from jax.sharding import PartitionSpec as P

HEADS = 16
HEAD_DIM = 64
ROT = 32
SLOT = 256
MICRO = 2
SMALL_ROWS = 16
LANES = 128
ROW_STEP = 256
FF_STEP = 4096
JOINT_STEP = 1024
GELU_SCALE = (2.0 / np.pi) ** 0.5
GELU_CUBE = 0.044715
norm_epsilon = 1e-05
rotary_base = 10000.0
masked_score = -1e30
MESH = pl.DeviceIdType.MESH
ANY = pl.BlockSpec(memory_space=pl.ANY)


class Place:
    def __init__(self):
        index = lax.axis_index("batch")
        self.levels = lax.axis_size("batch") // 4
        self.last = self.levels - 1
        self.z, self.y, self.c = index // 4, index // 2 % 2, index % 2

    def at(self, z=None, y=None, c=None):
        z = self.z if z is None else z
        y = self.y if y is None else y
        c = self.c if c is None else c
        return z * 4 + y * 2 + c


class Piece:
    def __init__(self, array, offset, rows, column, columns, direct):
        self.array, self.offset, self.rows = array, offset, rows
        self.column, self.columns, self.direct = column, columns, direct

    def sides(self, y):
        return (y,) if self.direct else (y, 1 - y)

    def of(self, block):
        return block.at[pl.ds(self.offset, self.rows), pl.ds(self.column, self.columns)]


def pieces_of(blocks):
    joint, output, expand, contract, small = blocks
    cut = contract[0] // 4
    pieces = [
        Piece(1, 0, output[0], 0, output[1], False),
        Piece(3, 0, cut, 0, contract[1], False),
    ]
    for array, offset, (rows, columns), parts in (
        (0, 0, joint, 1),
        (2, 0, expand, 1),
        (3, cut, contract, 1),
        (4, 0, small, 1),
    ):
        for i in range(parts):
            width = columns // parts
            pieces.append(Piece(array, offset, rows - offset, i * width, width, True))
    return pieces


def remote(source, target, send, receive, index):
    return pltpu.make_async_remote_copy(
        source, target, send, receive, device_id={"batch": index}, device_id_type=MESH
    )


def greet(here, with_section):
    barrier = pltpu.get_barrier_semaphore()

    def signal(**who):
        pl.semaphore_signal(barrier, inc=1, device_id=who, device_id_type=MESH)

    signal(batch=here.at(y=1 - here.y))
    signal(batch=here.at(c=1 - here.c))
    pl.when(here.z > 0)(lambda: signal(batch=here.at(z=here.z - 1)))
    pl.when(here.z < here.last)(lambda: signal(batch=here.at(z=here.z + 1)))
    waits = 2
    if with_section:
        signal(section=1 - lax.axis_index("section"))
        waits = 3
    below = jnp.minimum(here.z, 1)
    above = jnp.minimum(here.last - here.z, 1)
    pl.semaphore_wait(barrier, waits + below + above)


def spread_semaphores(count, levels):
    dma = pltpu.SemaphoreType.DMA
    return [
        dma((count,)),
        dma((count, levels, 2, 2)),
        dma((count, levels, 2)),
        dma((count, levels)),
        dma((count, levels)),
        dma((count, levels, 2)),
        dma((count, levels, 2)),
    ]


class Spread:
    def __init__(self, here, pieces, owns, outs, semaphores):
        self.here, self.pieces, self.owns, self.outs = here, pieces, owns, outs
        (self.keep, self.zs, self.zr, self.ys, self.yr, self.cs, self.cr) = semaphores

    def block(self, p, z, y, c):
        piece = self.pieces[p]
        out = self.outs[piece.array]
        rows = out.shape[0] // (4 * self.here.levels)
        start = (z * 4 + y * 2 + c) * rows + piece.offset
        return out.at[
            pl.ds(pl.multiple_of(start, 8), piece.rows), pl.ds(piece.column, piece.columns)
        ]

    def along(self, p, z, y, source, way):
        here = self.here
        return remote(
            source,
            self.block(p, z, y, here.c),
            self.zs.at[p, z, y, way],
            self.zr.at[p, z, y],
            here.at(z=here.z + (1 if way == 0 else -1)),
        )

    def across(self, p, z, source):
        here = self.here
        target = self.block(p, z, here.y, here.c)
        return remote(source, target, self.ys.at[p, z], self.yr.at[p, z], here.at(y=1 - here.y))

    def beside(self, p, z, y, source):
        here = self.here
        target = self.block(p, z, y, here.c)
        return remote(
            source, target, self.cs.at[p, z, y], self.cr.at[p, z, y], here.at(c=1 - here.c)
        )

    def both_ways(self, p, y, source):
        here = self.here
        pl.when(here.z < here.last)(lambda: self.along(p, here.z, y, source, 0).start())
        pl.when(here.z > 0)(lambda: self.along(p, here.z, y, source, 1).start())

    def begin(self, p, held=False):
        here, own = self.here, self.owns[p]
        self.across(p, here.z, own).start()
        if not held:
            self.both_ways(p, here.y, own)
        self.beside(p, here.z, here.y, own).start()
        target = self.block(p, here.z, here.y, here.c)
        pltpu.make_async_copy(own, target, self.keep.at[p]).start()

    def begin_all(self, chosen):
        order = sorted(chosen, key=lambda p: self.pieces[p].direct)
        for p in order:
            self.begin(p, held=not self.pieces[p].direct)
        for p in order:
            if not self.pieces[p].direct:
                self.both_ways(p, self.here.y, self.owns[p])

    def from_z(self, p, z, y, way):
        here = self.here
        block = self.block(p, z, y, here.c)
        self.along(p, z, y, block, way).wait_recv()
        more = here.z < here.last if way == 0 else here.z > 0
        pl.when(more)(lambda: self.along(p, z, y, block, way).start())
        if self.pieces[p].direct:
            self.across(p, z, block).start()
        self.beside(p, z, y, block).start()

    def from_y(self, p, z):
        here = self.here
        block = self.block(p, z, 1 - here.y, here.c)
        self.across(p, z, block).wait_recv()
        if not self.pieces[p].direct:
            self.both_ways(p, 1 - here.y, block)
        self.beside(p, z, 1 - here.y, block).start()

    def z_events(self, chosen, distance):
        here = self.here

        def pair(p, side):
            y = self.pieces[p].sides(here.y)[side]
            pl.when(here.z - distance >= 0)(lambda: self.from_z(p, here.z - distance, y, 0))
            pl.when(here.z + distance <= here.last)(
                lambda: self.from_z(p, here.z + distance, y, 1)
            )

        for p in chosen:
            if self.pieces[p].direct:
                pair(p, 0)
        for side in range(2):
            for p in chosen:
                if not self.pieces[p].direct:
                    pair(p, side)

    def y_events(self, chosen, z):
        for p in chosen:
            if self.pieces[p].direct:
                self.from_y(p, z)

    def middle(self, chosen, then=None):
        here = self.here
        for p in chosen:
            if not self.pieces[p].direct:
                self.from_y(p, here.z)

        def y_pair(distance):
            pl.when(here.z - distance >= 0)(lambda: self.y_events(chosen, here.z - distance))
            pl.when((here.z + distance <= here.last) & (distance > 0))(
                lambda: self.y_events(chosen, here.z + distance)
            )

        def step(distance, carry):
            self.z_events(chosen, distance)
            y_pair(distance - 1)
            return carry

        lax.fori_loop(1, here.levels, step, 0)
        if then is not None:
            then()
        y_pair(here.last)

    def received(self, chosen):
        here = self.here

        def level(z, carry):
            for p in chosen:
                own = self.block(p, z, here.y, here.c)
                for y in range(2):
                    self.beside(p, z, y, own).wait_recv()
            return carry

        lax.fori_loop(0, here.levels, level, 0)
        for p in chosen:
            block = self.block(p, here.z, here.y, here.c)
            pltpu.make_async_copy(block, block, self.keep.at[p]).wait()

    def sent(self):
        here = self.here

        def level(z, carry):
            for p, piece in enumerate(self.pieces):
                own = self.block(p, z, here.y, here.c)
                for y in range(2):
                    self.beside(p, z, y, own).wait_send()
                crossed = z >= 0 if piece.direct else z == here.z
                pl.when(crossed)(lambda p=p, own=own: self.across(p, z, own).wait_send())
                for y in piece.sides(here.y):
                    pl.when((z <= here.z) & (here.z < here.last))(
                        lambda p=p, y=y, own=own: self.along(p, z, y, own, 0).wait_send()
                    )
                    pl.when((z >= here.z) & (here.z > 0))(
                        lambda p=p, y=y, own=own: self.along(p, z, y, own, 1).wait_send()
                    )
            return carry

        lax.fori_loop(0, here.levels, level, 0)


def add_rows(target, other):
    rows = target.shape[0]
    step = min(rows, 16)

    def body(i, carry):
        at = pl.ds(pl.multiple_of(i * step, step), step)
        total = target[at, :].astype(jnp.float32) + other[at, :].astype(jnp.float32)
        target[at, :] = total.astype(target.dtype)
        return carry

    lax.fori_loop(0, rows // step, body, 0)


FACTORS = ((0, 3), (1, 5), (0, 4), (2, 5))
MAKE_ORDER = (1, 3, 0, 2, 4)
COLUMN_STEP = 1024


class Reduce:
    def __init__(self, here, pieces, factors, small, product_rows, buffers, semaphores):
        self.here, self.pieces, self.factors, self.small = here, pieces, factors, small
        self.made = product_rows
        self.mine, self.sent, self.sib, self.yb, self.zb = buffers
        (self.load, self.cs, self.cr, self.ys, self.yr, self.zs, self.zr, self.credit) = semaphores

    def level(self, i):
        here = self.here
        above, below = here.last - here.z, here.z
        lead = jnp.maximum(above, below) - jnp.minimum(above, below)
        single = jnp.where(above > below, here.last - i, i)
        later = i - lead
        distance = jnp.minimum(above, below) - later // 2
        outer = jnp.where(above > below, here.z - distance, here.z + distance)
        paired = jnp.where(later % 2 == 0, outer, 2 * here.z - outer)
        return jnp.where(i < lead, single, paired)

    def to_core(self, p, slot, y):
        here = self.here
        return remote(
            self.sent[p].at[slot, y],
            self.sib[p].at[slot, y],
            self.cs.at[p, slot, y],
            self.cr.at[p, slot, y],
            here.at(c=1 - here.c),
        )

    def to_y(self, p, z):
        here = self.here
        return remote(
            self.mine[p].at[z, 1 - here.y],
            self.yb[p].at[z if self.pieces[p].direct else 0],
            self.ys.at[p, z],
            self.yr.at[p, z],
            here.at(y=1 - here.y),
        )

    def slot(self, z, at_z, way):
        if way == 0:
            return z
        return jnp.where(z == at_z, self.here.levels, z)

    def to_z(self, p, z, y, way):
        here = self.here
        step = 1 if way == 0 else -1
        slot = self.slot(z, here.z + step, way)
        side = 0 if self.pieces[p].direct else y
        return remote(
            self.mine[p].at[z, y],
            self.zb[p].at[slot, side],
            self.zs.at[p, z, side],
            self.zr.at[p, slot, side],
            here.at(z=here.z + step),
        )

    def arrive(self, p, z, y, way):
        here = self.here
        slot = self.slot(z, here.z, way)
        side = 0 if self.pieces[p].direct else y
        block = self.zb[p].at[slot, side]
        remote(
            block, block, self.zs.at[p, z, side], self.zr.at[p, slot, side], here.at(y=1 - here.y)
        ).wait_recv()
        add_rows(self.mine[p].at[z, y], block)

    def store(self, array, z, slot, y, own, value, column):
        for p, piece in enumerate(self.pieces):
            first = max(column, piece.column)
            end = min(column + value.shape[1], piece.column + piece.columns)
            if piece.array == array and first < end:
                target = self.mine[p].at[z, y] if own else self.sent[p].at[slot, y]
                part = value[piece.offset : piece.offset + piece.rows, first - column : end - column]
                target[:, first - piece.column : end - piece.column] = part.astype(jnp.bfloat16)

    def make(self, array, z, slot):
        here = self.here
        rows = max(p.offset + p.rows for p in self.pieces if p.array == array)
        cores = ((False, 1 - here.c), (True, here.c))
        if array == 4:
            for own, c in cores:
                for y in range(2):
                    at = pl.multiple_of((z * 4 + y * 2 + c) * rows, 16)
                    self.store(array, z, slot, y, own, self.small[pl.ds(at, rows), :], 0)
            return
        left, right = (self.factors[i] for i in FACTORS[array])
        columns = right.shape[1]
        tiles = range(0, columns, COLUMN_STEP)
        if rows % 128 == 0:
            for own, c in cores:
                for y in range(2):
                    at = pl.multiple_of((z * 4 + y * 2 + c) * rows, 128)
                    turned = left[:, pl.ds(at, rows)].T
                    for tile in tiles:
                        value = product(turned, right[:, tile : tile + COLUMN_STEP])
                        self.store(array, z, slot, y, own, value, tile)
            return
        span = max(4 * rows, 128)
        start = z * 4 * rows // span * span
        turned = left[:, pl.ds(pl.multiple_of(start, 128), span)].T
        for tile in tiles:
            self.made[:span, :] = product(turned, right[:, tile : tile + COLUMN_STEP])
            for own, c in cores:
                for y in range(2):
                    at = pl.multiple_of((z * 4 + y * 2 + c) * rows - start, 8)
                    self.store(array, z, slot, y, own, self.made[pl.ds(at, rows), :], tile)

    def of(self, array):
        return [p for p, piece in enumerate(self.pieces) if piece.array == array]

    def build(self, i, waits):
        here = self.here
        z, slot = self.level(i), i % 2

        @pl.when(i >= 2)
        def _():
            for p in range(len(self.pieces)):
                for y in range(2):
                    self.to_core(p, slot, y).wait_send()
            pl.semaphore_wait(self.credit, 1)

        def add(array):
            for p in self.of(array):
                for y in range(2):
                    self.to_core(p, slot, y).wait_recv()
                    add_rows(self.mine[p].at[z, y], self.sib[p].at[slot, y])
                if self.pieces[p].direct:
                    self.to_y(p, z).start()
                else:
                    self.pass_on(z, [p])

        for step, array in enumerate(MAKE_ORDER):
            waits(i, array)
            self.make(array, z, slot)
            for p in self.of(array):
                for y in range(2):
                    self.to_core(p, slot, y).start()
            if step > 0:
                add(MAKE_ORDER[step - 1])
        add(MAKE_ORDER[-1])

        @pl.when(i < here.levels - 2)
        def _():
            other = {"batch": here.at(c=1 - here.c)}
            pl.semaphore_signal(self.credit, inc=1, device_id=other, device_id_type=MESH)

    def rows(self, p, z):
        self.to_y(p, z).wait_recv()
        source = self.yb[p].at[z if self.pieces[p].direct else 0]
        add_rows(self.mine[p].at[z, self.here.y], source)

    def pass_on(self, z, chosen):
        here = self.here

        def hop(way):
            further = here.z > 0 if way == 0 else here.z < here.last
            for p in chosen:
                if self.pieces[p].direct:
                    self.rows(p, z)
                for y in self.pieces[p].sides(here.y):
                    pl.when(further)(lambda p=p, y=y: self.arrive(p, z, y, way))
                    self.to_z(p, z, y, way).start()

        pl.when(z > here.z)(lambda: hop(0))
        pl.when(z < here.z)(lambda: hop(1))

    def run(self, waits):
        here = self.here
        made = [p for array in MAKE_ORDER for p in self.of(array)]
        direct = [p for p in made if self.pieces[p].direct]

        def step(i, carry):
            self.build(i, waits)
            pl.when(i > 0)(lambda: self.pass_on(self.level(i - 1), direct))
            return carry

        lax.fori_loop(0, here.levels, step, 0)

    def settle(self, p):
        here = self.here
        for y in self.pieces[p].sides(here.y):
            pl.when(here.z > 0)(lambda y=y: self.arrive(p, here.z, y, 0))
            pl.when(here.z < here.last)(lambda y=y: self.arrive(p, here.z, y, 1))

    def finish(self):
        here = self.here
        for slot in range(min(2, here.levels)):
            for p in range(len(self.pieces)):
                for y in range(2):
                    self.to_core(p, slot, y).wait_send()

        def level(z, carry):
            for p, piece in enumerate(self.pieces):
                crossed = z >= 0 if piece.direct else z == here.z
                pl.when(crossed)(lambda p=p: self.to_y(p, z).wait_send())
                for y in piece.sides(here.y):
                    pl.when(z > here.z)(lambda p=p, y=y: self.to_z(p, z, y, 0).wait_send())
                    pl.when(z < here.z)(lambda p=p, y=y: self.to_z(p, z, y, 1).wait_send())
            return carry

        lax.fori_loop(0, here.levels, level, 0)


def reduce_kernel(pieces, *refs):
    count = len(pieces)
    sources, outs, rest = refs[:7], refs[7:12], refs[12:]
    factors, small, made = rest[:6], rest[6], rest[7]
    rest = rest[8:]
    buffers = [rest[i * count : (i + 1) * count] for i in range(5)]
    rest = rest[5 * count :]
    here = Place()
    loads = [
        pltpu.make_async_copy(source, target, rest[0].at[i])
        for i, (source, target) in enumerate(zip(sources, [*factors, small]))
    ]
    order = (1, 5, 2, 0, 3, 4, 6)
    for i in order:
        loads[i].start()
    greet(here, False)
    reduce = Reduce(here, pieces, factors, small, made, buffers, rest[:8])
    needs = {1: (1, 5), 3: (2,), 0: (0, 3), 2: (4,), 4: (6,)}

    def waits(i, array):
        @pl.when(i == 0)
        def _():
            for k in needs[array]:
                loads[k].wait()

    reduce.run(waits)
    owns = [buffers[0][p].at[here.z, here.y] for p in range(count)]
    spread = Spread(here, pieces, owns, outs, rest[8:])
    turned = [p for p in range(count) if not pieces[p].direct]
    for p in turned:
        reduce.settle(p)
        reduce.to_y(p, here.z).start()
    for p in range(count):
        if pieces[p].direct:
            reduce.rows(p, here.z)
            reduce.settle(p)
            spread.begin(p)
    for p in turned:
        reduce.rows(p, here.z)
        spread.begin(p)
    spread.middle(range(count))
    reduce.finish()
    spread.received(range(count))
    spread.sent()


def reduce_all(factors, small, shapes, number):
    levels = lax.axis_size("batch") // 4
    shapes = [*shapes, small.shape]
    pieces = pieces_of([(rows // (4 * levels), columns) for rows, columns in shapes])
    count = len(pieces)
    dma = pltpu.SemaphoreType.DMA
    low = jnp.bfloat16
    scratch = [pltpu.VMEM(factor.shape, low) for factor in factors]
    scratch += [pltpu.VMEM(small.shape, low), pltpu.VMEM((256, COLUMN_STEP), jnp.float32)]
    blocks = [(piece.rows, piece.columns) for piece in pieces]
    scratch += [pltpu.VMEM((levels, 2) + block, low) for block in blocks]
    scratch += [pltpu.VMEM((2, 2) + block, low) for block in blocks] * 2
    scratch += [
        pltpu.VMEM((levels if piece.direct else 1,) + block, low)
        for piece, block in zip(pieces, blocks)
    ]
    scratch += [
        pltpu.VMEM((levels + 1, 1 if piece.direct else 2) + block, low)
        for piece, block in zip(pieces, blocks)
    ]
    scratch += [
        dma((7,)),
        dma((count, 2, 2)),
        dma((count, 2, 2)),
        dma((count, levels)),
        dma((count, levels)),
        dma((count, levels, 2)),
        dma((count, levels + 1, 2)),
        pltpu.SemaphoreType.REGULAR,
    ] + spread_semaphores(count, levels)
    return pl.pallas_call(
        partial(reduce_kernel, pieces),
        out_shape=[jax.ShapeDtypeStruct(shape, low) for shape in shapes],
        in_specs=[ANY] * 7,
        out_specs=[ANY] * 5,
        scratch_shapes=scratch,
        compiler_params=pltpu.CompilerParams(
            collective_id=number, has_side_effects=True, vmem_limit_bytes=60 * 2**20
        ),
        name="reduce_gradients",
    )(*factors, small)


def rotary_rows():
    positions = np.arange(SLOT, dtype=np.float64)[:, None]
    lane = np.arange(2 * HEAD_DIM)[None, :] % HEAD_DIM
    angles = positions * rotary_base ** (-(lane // 2 * 2.0) / ROT)
    turned = lane < ROT
    cosine = np.where(turned, np.cos(angles), 1.0)
    sine = np.where(turned, np.sin(angles), 0.0)
    even = np.where(lane % 2 == 0, sine, 0.0)
    odd = np.where(lane % 2 == 1, sine, 0.0)
    return np.stack([cosine, even, odd]).astype(np.float32)


def turn(pair, tables, back):
    lanes = pair.shape[1]
    following = pltpu.roll(pair, lanes - 1, 1)
    preceding = pltpu.roll(pair, 1, 1)
    side = following * tables[1] - preceding * tables[2]
    return pair * tables[0] + (side if back else -side)


def product(left, right, left_axis=1, right_axis=0):
    return lax.dot_general(
        left, right, (((left_axis,), (right_axis,)), ((), ())), preferred_element_type=jnp.float32
    )


def statistics(rows):
    average = jnp.mean(rows, axis=-1, keepdims=True)
    centered = rows - average
    variance = jnp.mean(centered * centered, axis=-1, keepdims=True)
    inverse = lax.rsqrt(variance + norm_epsilon)
    return centered * inverse, inverse


def low_lanes(width):
    return lax.broadcasted_iota(jnp.int32, (1, width), 1) < HEAD_DIM


def pair_lanes(index):
    return pl.ds(pl.multiple_of(index * 2 * HEAD_DIM, 2 * HEAD_DIM), 2 * HEAD_DIM)


def rows_at(index, step):
    return pl.ds(pl.multiple_of(index * step, step), step)


def attend(m, length, refs):
    (x, normed, qkv, attention, mixture, active, slope, total, result) = refs["state"]
    joint, output, expand, contract = refs["weights"]
    gain, offset, outer, inner = refs["vectors"]
    tables = refs["tables"]
    width = x.shape[2]

    def norm(i, carry):
        at = rows_at(i, ROW_STEP)
        standard, _ = statistics(x[m, at, :].astype(jnp.float32))
        normed[m, at, :] = (standard * gain[...] + offset[...]).astype(jnp.bfloat16)
        return carry

    lax.fori_loop(0, SLOT // ROW_STEP, norm, 0)
    for part in range(3):
        scale = HEAD_DIM**-0.5 if part == 0 else 1.0
        total[...] = product(normed[m], joint[:, part * width : (part + 1) * width])
        if part == 2:
            qkv[m, :, 2 * width :] = total[...].astype(jnp.bfloat16)
        else:

            def rotary(i, carry, part=part, scale=scale):
                pair = turn(total[:, pair_lanes(i)], tables, False)
                at = pair_lanes(i + part * (width // (2 * HEAD_DIM)))
                qkv[m, :, at] = pair.astype(jnp.bfloat16) * jnp.bfloat16(scale)
                return carry

            lax.fori_loop(0, width // (2 * HEAD_DIM), rotary, 0)

    query = lax.broadcasted_iota(jnp.int32, (SLOT, SLOT), 0)
    key = lax.broadcasted_iota(jnp.int32, (SLOT, SLOT), 1)
    allowed = (key <= query) & (key < length)
    pairs = width // (2 * HEAD_DIM)
    low = low_lanes(2 * HEAD_DIM)

    def heads(i, carry):
        queries, keys = qkv[m, :, pair_lanes(i)], qkv[m, :, pair_lanes(i + pairs)]
        values = qkv[m, :, pair_lanes(i + 2 * pairs)]
        mixed = []
        for half in range(2):
            own = jnp.where(low == (half == 0), queries, jnp.zeros_like(queries))
            scores = jnp.where(allowed, product(own, keys, 1, 1), masked_score)
            raised = jnp.exp(scores - jnp.max(scores, axis=-1, keepdims=True))
            share = raised * (1.0 / jnp.sum(raised, axis=-1, keepdims=True))
            share = share.astype(jnp.bfloat16)
            attention[m, 2 * i + half] = share
            mixed.append(product(share, values))
        mixture[m, :, pair_lanes(i)] = jnp.where(low, mixed[0], mixed[1]).astype(jnp.bfloat16)
        return carry

    lax.fori_loop(0, pairs, heads, 0, unroll=8)


def feed(m, refs):
    (x, normed, _, _, mixture, active, slope, total, result) = refs["state"]
    joint, output, expand, contract = refs["weights"]
    gain, offset, outer, inner = refs["vectors"]
    total[...] = x[m].astype(jnp.float32) + outer[...] + product(mixture[m], output[...])

    def hidden(i, carry):
        at = rows_at(i, FF_STEP)
        pre = product(normed[m], expand[:, at]) + inner[:, at]
        square = pre * pre
        bend = jnp.tanh(GELU_SCALE * (pre + GELU_CUBE * (square * pre)))
        lifted = 0.5 * (1.0 + bend)
        slant = (0.5 * GELU_SCALE) * (1.0 + (3.0 * GELU_CUBE) * square)
        slope[m, :, at] = (lifted + pre * (1.0 - bend * bend) * slant).astype(jnp.bfloat16)
        activated = (pre * lifted).astype(jnp.bfloat16)
        active[m, :, at] = activated
        total[...] += product(activated, contract[at, :])
        return carry

    lax.fori_loop(0, slope.shape[2] // FF_STEP, hidden, 0)
    result[m] = total[...].astype(jnp.bfloat16)


def backward_block(m, refs):
    (x, _, qkv, attention, _, _, slope, total, result) = refs["state"]
    joint, output, expand, contract = refs["weights"]
    gain, offset, outer, inner = refs["vectors"]
    upstream, mixture_grad = refs["gradients"]
    gain_sum, offset_sum, outer_sum, inner_sum = refs["sums"]
    tables = refs["tables"]
    width = x.shape[2]
    outer_sum[...] += jnp.sum(upstream[m].astype(jnp.float32), axis=0, keepdims=True)
    mixture_grad[...] = product(upstream[m], output[...], 1, 1).astype(jnp.bfloat16)
    total[...] = jnp.zeros_like(total)

    def hidden(i, carry):
        at = rows_at(i, FF_STEP)
        active_grad = product(upstream[m], contract[at, :], 1, 1)
        pre_grad = (active_grad * slope[m, :, at].astype(jnp.float32)).astype(jnp.bfloat16)
        slope[m, :, at] = pre_grad
        inner_sum[:, at] += jnp.sum(pre_grad.astype(jnp.float32), axis=0, keepdims=True)
        total[...] += product(pre_grad, expand[:, at], 1, 1)
        return carry

    lax.fori_loop(0, slope.shape[2] // FF_STEP, hidden, 0)
    pairs = width // (2 * HEAD_DIM)
    low = low_lanes(2 * HEAD_DIM)

    def heads(i, carry):
        queries, keys = qkv[m, :, pair_lanes(i)], qkv[m, :, pair_lanes(i + pairs)]
        values = qkv[m, :, pair_lanes(i + 2 * pairs)]
        mixed_grad = mixture_grad[:, pair_lanes(i)]
        query_grads, key_grads, value_grads = [], [], []
        for half in range(2):
            share = attention[m, 2 * i + half]
            own = jnp.where(low == (half == 0), mixed_grad, jnp.zeros_like(mixed_grad))
            value_grads.append(product(share, mixed_grad, 0, 0))
            share_grad = product(own, values, 1, 1)
            weight = share.astype(jnp.float32)
            weighted = weight * share_grad
            score_grad = weighted - weight * jnp.sum(weighted, axis=-1, keepdims=True)
            score_grad = score_grad.astype(jnp.bfloat16)
            query_grads.append(product(score_grad, keys))
            key_grads.append(product(score_grad, queries, 0, 0))
        query_grad = jnp.where(low, query_grads[0], query_grads[1]) * HEAD_DIM**-0.5
        key_grad = jnp.where(low, key_grads[0], key_grads[1])
        value_grad = jnp.where(low, value_grads[0], value_grads[1])
        qkv[m, :, pair_lanes(i)] = turn(query_grad, tables, True).astype(jnp.bfloat16)
        qkv[m, :, pair_lanes(i + pairs)] = turn(key_grad, tables, True).astype(jnp.bfloat16)
        qkv[m, :, pair_lanes(i + 2 * pairs)] = value_grad.astype(jnp.bfloat16)
        return carry

    lax.fori_loop(0, pairs, heads, 0, unroll=2)

    def project(i, carry):
        at = rows_at(i, JOINT_STEP)
        total[:, at] += product(qkv[m], joint[at, :], 1, 1)
        return carry

    lax.fori_loop(0, width // JOINT_STEP, project, 0)

    def norm(i, carry):
        at = rows_at(i, ROW_STEP)
        standard, inverse = statistics(x[m, at, :].astype(jnp.float32))
        normed_grad = total[at, :]
        gain_sum[...] += jnp.sum(normed_grad * standard, axis=0, keepdims=True)
        offset_sum[...] += jnp.sum(normed_grad, axis=0, keepdims=True)
        scaled = normed_grad * gain[...]
        inner_mean = jnp.mean(scaled, axis=-1, keepdims=True)
        along = jnp.mean(scaled * standard, axis=-1, keepdims=True)
        change = inverse * (scaled - inner_mean - standard * along)
        result[m, at, :] = (upstream[m, at, :].astype(jnp.float32) + change).astype(jnp.bfloat16)
        return carry

    lax.fori_loop(0, SLOT // ROW_STEP, norm, 0)


def vector_rows(width):
    return max(1, width // LANES), max(1, LANES // width)


def lane_range(device, width):
    lane = lax.broadcasted_iota(jnp.int32, (1, LANES), 1)
    start = device * width % LANES
    return (lane >= start) & (lane < start + width)


def unpack_vectors(small, devices, vectors):
    width = vectors[0].shape[1] // devices
    wide = vectors[3].shape[1] // devices

    def gathered(index, shared):
        rows = small[pl.ds(pl.multiple_of(index * shared * SMALL_ROWS, SMALL_ROWS), SMALL_ROWS), :]
        total = rows.astype(jnp.float32)
        for other in range(1, shared):
            at = pl.multiple_of((index * shared + other) * SMALL_ROWS, SMALL_ROWS)
            total += small[pl.ds(at, SMALL_ROWS), :].astype(jnp.float32)
        return total

    _, shared = vector_rows(width)

    def narrow(index, carry):
        total = gathered(index, shared)
        at = rows_at(index, LANES)
        for i in range(3):
            vectors[i][:, at] = total[i : i + 1]
        return carry

    lax.fori_loop(0, devices // shared, narrow, 0)
    count, shared_wide = vector_rows(wide)

    def broad(index, carry):
        total = gathered(index, shared_wide)
        for i in range(count):
            vectors[3][:, rows_at(index * count + i, LANES)] = total[3 + i : 4 + i]
        return carry

    lax.fori_loop(0, devices // shared_wide, broad, 0)


def pack_sums(sums, devices, packed):
    width = sums[0].shape[1] // devices
    wide = sums[3].shape[1] // devices
    count, _ = vector_rows(wide)
    row = lax.broadcasted_iota(jnp.int32, (SMALL_ROWS, LANES), 0)

    def device(index, carry):
        rows = []
        inside = lane_range(index, width)
        for i in range(3):
            rows.append(jnp.where(inside, sums[i][:, rows_at(index * width // LANES, LANES)], 0.0))
        for i in range(count):
            line = sums[3][:, rows_at(index * wide // LANES + i, LANES)]
            rows.append(line if wide >= LANES else jnp.where(lane_range(index, wide), line, 0.0))
        block = jnp.zeros((SMALL_ROWS, LANES), jnp.float32)
        for i, line in enumerate(rows):
            block = jnp.where(row == i, line, block)
        packed[rows_at(index, SMALL_ROWS), :] = block.astype(jnp.bfloat16)
        return carry

    lax.fori_loop(0, devices, device, 0)


def blocks_kernel(pieces, *refs):
    lengths, hidden_in, cotangent, tables_in = refs[:4]
    sources = refs[4:9]
    hidden_out, input_grad = refs[9:11]
    factor_outs, packed = refs[11:17], refs[17]
    weights, small = refs[18:22], refs[22]
    x, normed, qkv, attention, mixture, active, slope, total, result = refs[23:32]
    upstream, mixture_grad, tables = refs[32:35]
    vectors, sums = refs[35:39], refs[39:43]
    table_sem, in_keep, in_send, in_receive, hand_send, hand_receive = refs[43:49]
    half_send, half_receive, half_keep, out_sem = refs[49:53]
    here = Place()
    section = lax.axis_index("section")
    partner = {"section": 1 - section}
    half = hidden_out.shape[1]
    devices = 4 * here.levels

    def keeping(source, target, start, m):
        return pltpu.make_async_copy(
            source.at[rows_at(m, SLOT), :], target.at[m, :, pl.ds(start, half)], in_keep.at[m]
        )

    def halving(source, target, start, m):
        return pltpu.make_async_remote_copy(
            source.at[rows_at(m, SLOT), :],
            target.at[m, :, pl.ds(start, half)],
            in_send.at[m],
            in_receive.at[m],
            device_id=partner,
            device_id_type=MESH,
        )

    def handing(target, m):
        return pltpu.make_async_remote_copy(
            result.at[m],
            target.at[m],
            hand_send.at[m],
            hand_receive.at[m],
            device_id=partner,
            device_id_type=MESH,
        )

    def away(target, start, m):
        return pltpu.make_async_remote_copy(
            result.at[m, :, pl.ds(start, half)],
            target.at[rows_at(m, SLOT), :],
            half_send.at[m],
            half_receive.at[m],
            device_id=partner,
            device_id_type=MESH,
        )

    def kept(target, start, m):
        return pltpu.make_async_copy(
            result.at[m, :, pl.ds(start, half)], target.at[rows_at(m, SLOT), :], half_keep.at[m]
        )

    def giving(i, source, m):
        return pltpu.make_async_copy(
            source.at[m], factor_outs[i].at[rows_at(m, SLOT), :], out_sem.at[i, m]
        )

    reading = pltpu.make_async_copy(tables_in, tables, table_sem.at[0])
    reading.start()
    for m in range(MICRO):
        pl.when(section == 0)(lambda m=m: keeping(hidden_in, x, 0, m).start())
        pl.when(section == 1)(lambda m=m: keeping(cotangent, upstream, half, m).start())
    for total_sum in sums:
        total_sum[...] = jnp.zeros_like(total_sum)
    greet(here, True)
    owns = [piece.of(sources[piece.array]) for piece in pieces]
    spread = Spread(here, pieces, owns, [*weights, small], refs[53:])
    early = [p for p, piece in enumerate(pieces) if piece.array in (0, 1, 4)]
    late = [p for p, piece in enumerate(pieces) if piece.array in (2, 3)]
    spread.begin_all(early)
    for m in range(MICRO):
        pl.when(section == 1)(lambda m=m: halving(hidden_in, x, half, m).start())
        pl.when(section == 0)(lambda m=m: halving(cotangent, upstream, 0, m).start())
    shared = {
        "state": (x, normed, qkv, attention, mixture, active, slope, total, result),
        "weights": weights,
        "vectors": vectors,
        "tables": tables,
        "gradients": (upstream, mixture_grad),
        "sums": sums,
    }
    spread.middle(early, lambda: spread.begin_all(late))
    spread.received(early)
    unpack_vectors(small, devices, vectors)
    reading.wait()

    @pl.when(section == 0)
    def _():
        def ahead(m, carry):
            keeping(hidden_in, x, 0, m).wait()
            halving(hidden_in, x, half, m).wait_recv()
            attend(m, lengths[m], shared)
            return carry

        lax.fori_loop(0, MICRO, ahead, 0)

    spread.middle(late)
    spread.received(late)

    def forward(m, carry):
        @pl.when(section == 1)
        def _():
            handing(x, m).wait_recv()
            attend(m, lengths[m], shared)

        feed(m, shared)

        @pl.when(section == 0)
        def _():
            handing(x, m).start()

        @pl.when(section == 1)
        def _():
            away(hidden_out, 0, m).start()
            kept(hidden_out, half, m).start()

        for i, source in enumerate((normed, mixture, active)):
            giving(i, source, m).start()
        return carry

    lax.fori_loop(0, MICRO, forward, 0)

    def backward(m, carry):
        @pl.when(section == 0)
        def _():
            handing(x, m).wait_send()
            handing(upstream, m).wait_recv()

        @pl.when(section == 1)
        def _():
            away(hidden_out, 0, m).wait_send()
            kept(hidden_out, half, m).wait()
            keeping(cotangent, upstream, half, m).wait()
            halving(cotangent, upstream, 0, m).wait_recv()
            row = lax.broadcasted_iota(jnp.int32, (SLOT, 1), 0)
            inside = (row < lengths[m]).astype(jnp.float32)
            masked = upstream[m].astype(jnp.float32) * inside
            upstream[m] = masked.astype(jnp.bfloat16)

        backward_block(m, shared)

        @pl.when(section == 1)
        def _():
            handing(upstream, m).start()

        @pl.when(section == 0)
        def _():
            away(input_grad, half, m).start()
            kept(input_grad, 0, m).start()

        for i, source in enumerate((qkv, slope, upstream)):
            giving(3 + i, source, m).start()
        return carry

    lax.fori_loop(0, MICRO, backward, 0)
    pack_sums(sums, devices, packed)

    def last(m, carry):
        @pl.when(section == 0)
        def _():
            halving(cotangent, upstream, 0, m).wait_send()
            away(input_grad, half, m).wait_send()
            kept(input_grad, 0, m).wait()
            away(hidden_out, 0, m).wait_recv()

        @pl.when(section == 1)
        def _():
            halving(hidden_in, x, half, m).wait_send()
            handing(upstream, m).wait_send()
            away(input_grad, half, m).wait_recv()

        for i, source in enumerate((normed, mixture, active, qkv, slope, upstream)):
            giving(i, source, m).wait()
        return carry

    lax.fori_loop(0, MICRO, last, 0)
    spread.sent()


def run_blocks(lengths, hidden_in, cotangent, owns, number):
    levels = lax.axis_size("batch") // 4
    devices = 4 * levels
    tokens, half = hidden_in.shape
    width = half * lax.axis_size("section")
    wide = owns[2].shape[1]
    low, full = jnp.bfloat16, jnp.float32
    shape = jax.ShapeDtypeStruct
    vmem = pltpu.VMEM
    dma = pltpu.SemaphoreType.DMA
    pieces = pieces_of([own.shape for own in owns])
    outputs = [shape((tokens, half), low)] * 2
    outputs += [shape((tokens, n), low) for n in (width, width, wide, 3 * width, wide, width)]
    outputs += [shape((devices * SMALL_ROWS, LANES), low)]
    scratch = [vmem((devices * own.shape[0], own.shape[1]), low) for own in owns]
    scratch += [
        vmem((MICRO, SLOT, width), low),
        vmem((MICRO, SLOT, width), low),
        vmem((MICRO, SLOT, 3 * width), low),
        vmem((MICRO, HEADS, SLOT, SLOT), low),
        vmem((MICRO, SLOT, width), low),
        vmem((MICRO, SLOT, wide), low),
        vmem((MICRO, SLOT, wide), low),
        vmem((SLOT, width), full),
        vmem((MICRO, SLOT, width), low),
        vmem((MICRO, SLOT, width), low),
        vmem((SLOT, width), low),
        vmem((3, SLOT, 2 * HEAD_DIM), full),
    ]
    scratch += [vmem((1, n), full) for n in (width, width, width, wide)] * 2
    scratch += [dma((1,))] + [dma((MICRO,))] * 8 + [dma((6, MICRO))]
    scratch += spread_semaphores(len(pieces), levels)
    return pl.pallas_call(
        partial(blocks_kernel, pieces),
        out_shape=outputs,
        in_specs=[pl.BlockSpec(memory_space=pltpu.SMEM)] + [ANY] * 8,
        out_specs=[ANY] * 8 + [pl.BlockSpec(memory_space=vmem)],
        scratch_shapes=scratch,
        compiler_params=pltpu.CompilerParams(
            collective_id=number, has_side_effects=True, vmem_limit_bytes=60 * 2**20
        ),
        name="two_blocks",
    )(lengths, hidden_in, cotangent, jnp.asarray(rotary_rows()), *owns)


def pack_vectors(vectors):
    device = lax.axis_index("batch")
    size = SMALL_ROWS * LANES
    total = jnp.zeros((1, size), jnp.float32)
    row = 0
    for vector in vectors:
        width = vector.shape[1]
        used = min(width, LANES)
        slot = device * width % LANES // used
        for i in range(LANES // used):
            start = row * LANES + i * used
            moved = jnp.pad(vector.astype(jnp.float32), ((0, 0), (start, size - start - width)))
            total = total + jnp.where(slot == i, moved, 0.0)
        row += max(1, width // LANES)
    return total.reshape(SMALL_ROWS, LANES).astype(jnp.bfloat16)


def widen_kernel(devices, *refs):
    small, sources = refs[0], refs[1 : (len(refs) - 5) // 2 + 1]
    targets, vectors = refs[len(sources) + 1 : -4], refs[-4:]
    pl.when(pl.program_id(0) == 0)(lambda: unpack_vectors(small, devices, vectors))
    for source, target in zip(sources, targets):
        target[...] = source[...].astype(target.dtype).reshape(target.shape)


def widen(small, sums, kept, widths, devices):
    steps = 8
    arrays = [*sums, *kept]
    whole = lambda i: (0, 0)
    in_specs = [
        pl.BlockSpec((array.shape[0] // steps, array.shape[1]), lambda i: (i, 0))
        for array in arrays
    ]
    out_specs = [
        pl.BlockSpec((1, array.shape[0] // steps, array.shape[1]), lambda i: (0, i, 0))
        for array in sums
    ] + in_specs[len(sums) :]
    out_specs += [pl.BlockSpec((1, width), whole) for width in widths]
    shapes = [jax.ShapeDtypeStruct((1, *array.shape), jnp.float32) for array in sums]
    shapes += [jax.ShapeDtypeStruct(array.shape, array.dtype) for array in kept]
    shapes += [jax.ShapeDtypeStruct((1, width), jnp.float32) for width in widths]
    return pl.pallas_call(
        partial(widen_kernel, devices),
        out_shape=shapes,
        grid=(steps,),
        in_specs=[pl.BlockSpec(small.shape, whole)] + in_specs,
        out_specs=out_specs,
        compiler_params=pltpu.CompilerParams(vmem_limit_bytes=60 * 2**20),
        name="widen",
    )(small, *arrays)


def local(
    hidden_in,
    cotangent,
    lengths,
    norm_gain,
    norm_offset,
    joint_weight,
    output_weight,
    expand_weight,
    inner_bias,
    contract_weight,
    outer_bias,
):
    devices = lax.axis_size("batch")
    owns = [
        joint_weight[0],
        output_weight[0],
        expand_weight[0],
        contract_weight[0],
        pack_vectors((norm_gain, norm_offset, outer_bias, inner_bias)),
    ]
    results = run_blocks(lengths, hidden_in, cotangent, owns, 1)
    shapes = [(own.shape[0] * devices, own.shape[1]) for own in owns[:4]]
    *sums, small_sum = reduce_all(results[2:8], results[8], shapes, 2)
    width, wide = norm_gain.shape[1] * devices, inner_bias.shape[1] * devices
    (
        joint_sum,
        output_sum,
        expand_sum,
        contract_sum,
        hidden_out,
        input_grad,
        gain_sum,
        offset_sum,
        outer_sum,
        inner_sum,
    ) = widen(small_sum, sums, results[:2], (width, width, width, wide), devices)
    return (
        hidden_out,
        input_grad,
        gain_sum,
        offset_sum,
        joint_sum,
        output_sum,
        expand_sum,
        inner_sum,
        contract_sum,
        outer_sum,
    )


def solution(mesh):
    return jax.shard_map(
        local,
        mesh=mesh,
        in_specs=(
            P("batch", "section"),
            P("batch", "section"),
            P("batch"),
            P("section", "batch"),
            P("section", "batch"),
            P("section", "batch", None),
            P("section", "batch", None),
            P("section", "batch", None),
            P("section", "batch"),
            P("section", "batch", None),
            P("section", "batch"),
        ),
        out_specs=(
            P("batch", "section"),
            P("batch", "section"),
            P("section", None),
            P("section", None),
            P("section", None, None),
            P("section", None, None),
            P("section", None, None),
            P("section", None),
            P("section", None, None),
            P("section", None),
        ),
        check_vma=False,
    )
```

```python
from functools import partial

import jax
import jax.numpy as jnp
import numpy as np
from jax import lax
from jax.experimental import pallas as pl
from jax.experimental.pallas import tpu as pltpu
from jax.sharding import PartitionSpec as P

HEADS = 16
HEAD_DIM = 64
ROT = 32
SLOT = 256
MICRO = 2
SMALL_ROWS = 16
LANES = 128
ROW_STEP = 256
FF_STEP = 4096
JOINT_STEP = 1024
GELU_SCALE = (2.0 / np.pi) ** 0.5
GELU_CUBE = 0.044715
norm_epsilon = 1e-05
rotary_base = 10000.0
masked_score = -1e30
MESH = pl.DeviceIdType.MESH
ANY = pl.BlockSpec(memory_space=pl.ANY)


class Place:
    def __init__(self):
        index = lax.axis_index("batch")
        self.levels = lax.axis_size("batch") // 4
        self.last = self.levels - 1
        self.z, self.y, self.c = index // 4, index // 2 % 2, index % 2

    def at(self, z=None, y=None, c=None):
        z = self.z if z is None else z
        y = self.y if y is None else y
        c = self.c if c is None else c
        return z * 4 + y * 2 + c


class Piece:
    def __init__(self, array, offset, rows, column, columns, direct):
        self.array, self.offset, self.rows = array, offset, rows
        self.column, self.columns, self.direct = column, columns, direct

    def sides(self, y):
        return (y,) if self.direct else (y, 1 - y)

    def of(self, block):
        return block.at[pl.ds(self.offset, self.rows), pl.ds(self.column, self.columns)]


def pieces_of(blocks):
    joint, output, expand, contract, small = blocks
    cut = contract[0] // 4
    pieces = [
        Piece(1, 0, output[0], 0, output[1], False),
        Piece(3, 0, cut, 0, contract[1], False),
    ]
    for array, offset, (rows, columns), parts in (
        (0, 0, joint, 1),
        (2, 0, expand, 1),
        (3, cut, contract, 1),
        (4, 0, small, 1),
    ):
        for i in range(parts):
            width = columns // parts
            pieces.append(Piece(array, offset, rows - offset, i * width, width, True))
    return pieces


def remote(source, target, send, receive, index):
    return pltpu.make_async_remote_copy(
        source, target, send, receive, device_id={"batch": index}, device_id_type=MESH
    )


def greet(here, with_section):
    barrier = pltpu.get_barrier_semaphore()

    def signal(**who):
        pl.semaphore_signal(barrier, inc=1, device_id=who, device_id_type=MESH)

    signal(batch=here.at(y=1 - here.y))
    signal(batch=here.at(c=1 - here.c))
    pl.when(here.z > 0)(lambda: signal(batch=here.at(z=here.z - 1)))
    pl.when(here.z < here.last)(lambda: signal(batch=here.at(z=here.z + 1)))
    waits = 2
    if with_section:
        signal(section=1 - lax.axis_index("section"))
        waits = 3
    below = jnp.minimum(here.z, 1)
    above = jnp.minimum(here.last - here.z, 1)
    pl.semaphore_wait(barrier, waits + below + above)


def spread_semaphores(count, levels):
    dma = pltpu.SemaphoreType.DMA
    return [
        dma((count,)),
        dma((count, levels, 2, 2)),
        dma((count, levels, 2)),
        dma((count, levels)),
        dma((count, levels)),
        dma((count, levels, 2)),
        dma((count, levels, 2)),
    ]


class Spread:
    def __init__(self, here, pieces, owns, outs, semaphores):
        self.here, self.pieces, self.owns, self.outs = here, pieces, owns, outs
        (self.keep, self.zs, self.zr, self.ys, self.yr, self.cs, self.cr) = semaphores

    def block(self, p, z, y, c):
        piece = self.pieces[p]
        out = self.outs[piece.array]
        rows = out.shape[0] // (4 * self.here.levels)
        start = (z * 4 + y * 2 + c) * rows + piece.offset
        return out.at[
            pl.ds(pl.multiple_of(start, 8), piece.rows), pl.ds(piece.column, piece.columns)
        ]

    def along(self, p, z, y, source, way):
        here = self.here
        return remote(
            source,
            self.block(p, z, y, here.c),
            self.zs.at[p, z, y, way],
            self.zr.at[p, z, y],
            here.at(z=here.z + (1 if way == 0 else -1)),
        )

    def across(self, p, z, source):
        here = self.here
        target = self.block(p, z, here.y, here.c)
        return remote(source, target, self.ys.at[p, z], self.yr.at[p, z], here.at(y=1 - here.y))

    def beside(self, p, z, y, source):
        here = self.here
        target = self.block(p, z, y, here.c)
        return remote(
            source, target, self.cs.at[p, z, y], self.cr.at[p, z, y], here.at(c=1 - here.c)
        )

    def both_ways(self, p, y, source):
        here = self.here
        pl.when(here.z < here.last)(lambda: self.along(p, here.z, y, source, 0).start())
        pl.when(here.z > 0)(lambda: self.along(p, here.z, y, source, 1).start())

    def begin(self, p, held=False):
        here, own = self.here, self.owns[p]
        self.across(p, here.z, own).start()
        if not held:
            self.both_ways(p, here.y, own)
        self.beside(p, here.z, here.y, own).start()
        target = self.block(p, here.z, here.y, here.c)
        pltpu.make_async_copy(own, target, self.keep.at[p]).start()

    def begin_all(self, chosen):
        order = sorted(chosen, key=lambda p: self.pieces[p].direct)
        for p in order:
            self.begin(p, held=not self.pieces[p].direct)
        for p in order:
            if not self.pieces[p].direct:
                self.both_ways(p, self.here.y, self.owns[p])

    def from_z(self, p, z, y, way):
        here = self.here
        block = self.block(p, z, y, here.c)
        self.along(p, z, y, block, way).wait_recv()
        more = here.z < here.last if way == 0 else here.z > 0
        pl.when(more)(lambda: self.along(p, z, y, block, way).start())
        if self.pieces[p].direct:
            self.across(p, z, block).start()
        self.beside(p, z, y, block).start()

    def from_y(self, p, z):
        here = self.here
        block = self.block(p, z, 1 - here.y, here.c)
        self.across(p, z, block).wait_recv()
        if not self.pieces[p].direct:
            self.both_ways(p, 1 - here.y, block)
        self.beside(p, z, 1 - here.y, block).start()

    def z_events(self, chosen, distance):
        here = self.here

        def pair(p, side):
            y = self.pieces[p].sides(here.y)[side]
            pl.when(here.z - distance >= 0)(lambda: self.from_z(p, here.z - distance, y, 0))
            pl.when(here.z + distance <= here.last)(
                lambda: self.from_z(p, here.z + distance, y, 1)
            )

        for p in chosen:
            if self.pieces[p].direct:
                pair(p, 0)
        for side in range(2):
            for p in chosen:
                if not self.pieces[p].direct:
                    pair(p, side)

    def y_events(self, chosen, z):
        for p in chosen:
            if self.pieces[p].direct:
                self.from_y(p, z)

    def middle(self, chosen, then=None):
        here = self.here
        for p in chosen:
            if not self.pieces[p].direct:
                self.from_y(p, here.z)

        def y_pair(distance):
            pl.when(here.z - distance >= 0)(lambda: self.y_events(chosen, here.z - distance))
            pl.when((here.z + distance <= here.last) & (distance > 0))(
                lambda: self.y_events(chosen, here.z + distance)
            )

        def step(distance, carry):
            self.z_events(chosen, distance)
            y_pair(distance - 1)
            return carry

        lax.fori_loop(1, here.levels, step, 0)
        if then is not None:
            then()
        y_pair(here.last)

    def received(self, chosen):
        here = self.here

        def level(z, carry):
            for p in chosen:
                own = self.block(p, z, here.y, here.c)
                for y in range(2):
                    self.beside(p, z, y, own).wait_recv()
            return carry

        lax.fori_loop(0, here.levels, level, 0)
        for p in chosen:
            block = self.block(p, here.z, here.y, here.c)
            pltpu.make_async_copy(block, block, self.keep.at[p]).wait()

    def sent(self):
        here = self.here

        def level(z, carry):
            for p, piece in enumerate(self.pieces):
                own = self.block(p, z, here.y, here.c)
                for y in range(2):
                    self.beside(p, z, y, own).wait_send()
                crossed = z >= 0 if piece.direct else z == here.z
                pl.when(crossed)(lambda p=p, own=own: self.across(p, z, own).wait_send())
                for y in piece.sides(here.y):
                    pl.when((z <= here.z) & (here.z < here.last))(
                        lambda p=p, y=y, own=own: self.along(p, z, y, own, 0).wait_send()
                    )
                    pl.when((z >= here.z) & (here.z > 0))(
                        lambda p=p, y=y, own=own: self.along(p, z, y, own, 1).wait_send()
                    )
            return carry

        lax.fori_loop(0, here.levels, level, 0)


def add_rows(target, other):
    rows = target.shape[0]
    step = min(rows, 16)

    def body(i, carry):
        at = pl.ds(pl.multiple_of(i * step, step), step)
        total = target[at, :].astype(jnp.float32) + other[at, :].astype(jnp.float32)
        target[at, :] = total.astype(target.dtype)
        return carry

    lax.fori_loop(0, rows // step, body, 0)


FACTORS = ((0, 3), (1, 5), (0, 4), (2, 5))
MAKE_ORDER = (1, 3, 0, 2, 4)
COLUMN_STEP = 1024


class Reduce:
    def __init__(self, here, pieces, factors, small, product_rows, buffers, semaphores):
        self.here, self.pieces, self.factors, self.small = here, pieces, factors, small
        self.made = product_rows
        self.mine, self.sent, self.sib, self.yb, self.zb = buffers
        (self.load, self.cs, self.cr, self.ys, self.yr, self.zs, self.zr, self.credit) = semaphores

    def level(self, i):
        here = self.here
        above, below = here.last - here.z, here.z
        lead = jnp.maximum(above, below) - jnp.minimum(above, below)
        single = jnp.where(above > below, here.last - i, i)
        later = i - lead
        distance = jnp.minimum(above, below) - later // 2
        outer = jnp.where(above > below, here.z - distance, here.z + distance)
        paired = jnp.where(later % 2 == 0, outer, 2 * here.z - outer)
        return jnp.where(i < lead, single, paired)

    def to_core(self, p, slot, y):
        here = self.here
        return remote(
            self.sent[p].at[slot, y],
            self.sib[p].at[slot, y],
            self.cs.at[p, slot, y],
            self.cr.at[p, slot, y],
            here.at(c=1 - here.c),
        )

    def to_y(self, p, z):
        here = self.here
        return remote(
            self.mine[p].at[z, 1 - here.y],
            self.yb[p].at[z if self.pieces[p].direct else 0],
            self.ys.at[p, z],
            self.yr.at[p, z],
            here.at(y=1 - here.y),
        )

    def slot(self, z, at_z, way):
        if way == 0:
            return z
        return jnp.where(z == at_z, self.here.levels, z)

    def to_z(self, p, z, y, way):
        here = self.here
        step = 1 if way == 0 else -1
        slot = self.slot(z, here.z + step, way)
        side = 0 if self.pieces[p].direct else y
        return remote(
            self.mine[p].at[z, y],
            self.zb[p].at[slot, side],
            self.zs.at[p, z, side],
            self.zr.at[p, slot, side],
            here.at(z=here.z + step),
        )

    def arrive(self, p, z, y, way):
        here = self.here
        slot = self.slot(z, here.z, way)
        side = 0 if self.pieces[p].direct else y
        block = self.zb[p].at[slot, side]
        remote(
            block, block, self.zs.at[p, z, side], self.zr.at[p, slot, side], here.at(y=1 - here.y)
        ).wait_recv()
        add_rows(self.mine[p].at[z, y], block)

    def store(self, array, z, slot, y, own, value, column):
        for p, piece in enumerate(self.pieces):
            first = max(column, piece.column)
            end = min(column + value.shape[1], piece.column + piece.columns)
            if piece.array == array and first < end:
                target = self.mine[p].at[z, y] if own else self.sent[p].at[slot, y]
                part = value[piece.offset : piece.offset + piece.rows, first - column : end - column]
                target[:, first - piece.column : end - piece.column] = part.astype(jnp.bfloat16)

    def make(self, array, z, slot):
        here = self.here
        rows = max(p.offset + p.rows for p in self.pieces if p.array == array)
        cores = ((False, 1 - here.c), (True, here.c))
        if array == 4:
            for own, c in cores:
                for y in range(2):
                    at = pl.multiple_of((z * 4 + y * 2 + c) * rows, 16)
                    self.store(array, z, slot, y, own, self.small[pl.ds(at, rows), :], 0)
            return
        left, right = (self.factors[i] for i in FACTORS[array])
        columns = right.shape[1]
        tiles = range(0, columns, COLUMN_STEP)
        if rows % 128 == 0:
            for own, c in cores:
                for y in range(2):
                    at = pl.multiple_of((z * 4 + y * 2 + c) * rows, 128)
                    turned = left[:, pl.ds(at, rows)].T
                    for tile in tiles:
                        value = product(turned, right[:, tile : tile + COLUMN_STEP])
                        self.store(array, z, slot, y, own, value, tile)
            return
        span = max(4 * rows, 128)
        start = z * 4 * rows // span * span
        turned = left[:, pl.ds(pl.multiple_of(start, 128), span)].T
        for tile in tiles:
            self.made[:span, :] = product(turned, right[:, tile : tile + COLUMN_STEP])
            for own, c in cores:
                for y in range(2):
                    at = pl.multiple_of((z * 4 + y * 2 + c) * rows - start, 8)
                    self.store(array, z, slot, y, own, self.made[pl.ds(at, rows), :], tile)

    def of(self, array):
        return [p for p, piece in enumerate(self.pieces) if piece.array == array]

    def build(self, i, waits):
        here = self.here
        z, slot = self.level(i), i % 2

        @pl.when(i >= 2)
        def _():
            for p in range(len(self.pieces)):
                for y in range(2):
                    self.to_core(p, slot, y).wait_send()
            pl.semaphore_wait(self.credit, 1)

        def add(array):
            for p in self.of(array):
                for y in range(2):
                    self.to_core(p, slot, y).wait_recv()
                    add_rows(self.mine[p].at[z, y], self.sib[p].at[slot, y])
                if self.pieces[p].direct:
                    self.to_y(p, z).start()
                else:
                    self.pass_on(z, [p])

        for step, array in enumerate(MAKE_ORDER):
            waits(i, array)
            self.make(array, z, slot)
            for p in self.of(array):
                for y in range(2):
                    self.to_core(p, slot, y).start()
            if step > 0:
                add(MAKE_ORDER[step - 1])
        add(MAKE_ORDER[-1])

        @pl.when(i < here.levels - 2)
        def _():
            other = {"batch": here.at(c=1 - here.c)}
            pl.semaphore_signal(self.credit, inc=1, device_id=other, device_id_type=MESH)

    def rows(self, p, z):
        self.to_y(p, z).wait_recv()
        source = self.yb[p].at[z if self.pieces[p].direct else 0]
        add_rows(self.mine[p].at[z, self.here.y], source)

    def pass_on(self, z, chosen):
        here = self.here

        def hop(way):
            further = here.z > 0 if way == 0 else here.z < here.last
            for p in chosen:
                if self.pieces[p].direct:
                    self.rows(p, z)
                for y in self.pieces[p].sides(here.y):
                    pl.when(further)(lambda p=p, y=y: self.arrive(p, z, y, way))
                    self.to_z(p, z, y, way).start()

        pl.when(z > here.z)(lambda: hop(0))
        pl.when(z < here.z)(lambda: hop(1))

    def run(self, waits):
        here = self.here
        made = [p for array in MAKE_ORDER for p in self.of(array)]
        direct = [p for p in made if self.pieces[p].direct]

        def step(i, carry):
            self.build(i, waits)
            pl.when(i > 0)(lambda: self.pass_on(self.level(i - 1), direct))
            return carry

        lax.fori_loop(0, here.levels, step, 0)

    def settle(self, p):
        here = self.here
        for y in self.pieces[p].sides(here.y):
            pl.when(here.z > 0)(lambda y=y: self.arrive(p, here.z, y, 0))
            pl.when(here.z < here.last)(lambda y=y: self.arrive(p, here.z, y, 1))

    def finish(self):
        here = self.here
        for slot in range(min(2, here.levels)):
            for p in range(len(self.pieces)):
                for y in range(2):
                    self.to_core(p, slot, y).wait_send()

        def level(z, carry):
            for p, piece in enumerate(self.pieces):
                crossed = z >= 0 if piece.direct else z == here.z
                pl.when(crossed)(lambda p=p: self.to_y(p, z).wait_send())
                for y in piece.sides(here.y):
                    pl.when(z > here.z)(lambda p=p, y=y: self.to_z(p, z, y, 0).wait_send())
                    pl.when(z < here.z)(lambda p=p, y=y: self.to_z(p, z, y, 1).wait_send())
            return carry

        lax.fori_loop(0, here.levels, level, 0)


def reduce_kernel(pieces, *refs):
    count = len(pieces)
    sources, change, outs, input_grad, rest = refs[:7], refs[7], refs[8:13], refs[13], refs[14:]
    factors, small, made = rest[:6], rest[6], rest[7]
    rest = rest[8:]
    buffers = [rest[i * count : (i + 1) * count] for i in range(5)]
    rest = rest[5 * count :]
    here = Place()
    loads = [
        pltpu.make_async_copy(source, target, rest[0].at[i])
        for i, (source, target) in enumerate(zip(sources, [*factors, small]))
    ]
    order = (1, 5, 2, 0, 3, 4, 6)
    for i in order:
        loads[i].start()
    greet(here, True)
    section = lax.axis_index("section")
    half = input_grad.shape[1]
    over = pltpu.make_async_remote_copy(
        change.at[:, pl.ds(half, half)],
        input_grad,
        rest[-1].at[0],
        rest[-1].at[1],
        device_id={"section": 1 - section},
        device_id_type=MESH,
    )
    keep = pltpu.make_async_copy(change.at[:, pl.ds(0, half)], input_grad, rest[-1].at[2])

    @pl.when(section == 0)
    def _():
        over.start()
        keep.start()

    reduce = Reduce(here, pieces, factors, small, made, buffers, rest[:8])
    needs = {1: (1, 5), 3: (2,), 0: (0, 3), 2: (4,), 4: (6,)}

    def waits(i, array):
        @pl.when(i == 0)
        def _():
            for k in needs[array]:
                loads[k].wait()

    reduce.run(waits)
    owns = [buffers[0][p].at[here.z, here.y] for p in range(count)]
    spread = Spread(here, pieces, owns, outs, rest[8:-1])
    turned = [p for p in range(count) if not pieces[p].direct]
    for p in turned:
        reduce.settle(p)
        reduce.to_y(p, here.z).start()
    for p in range(count):
        if pieces[p].direct:
            reduce.rows(p, here.z)
            reduce.settle(p)
            spread.begin(p)
    for p in turned:
        reduce.rows(p, here.z)
        spread.begin(p)
    spread.middle(range(count))
    reduce.finish()
    spread.received(range(count))
    spread.sent()

    @pl.when(section == 0)
    def _():
        over.wait_send()
        keep.wait()

    pl.when(section == 1)(over.wait_recv)


def reduce_all(factors, small, change, shapes, number):
    levels = lax.axis_size("batch") // 4
    shapes = [*shapes, small.shape]
    pieces = pieces_of([(rows // (4 * levels), columns) for rows, columns in shapes])
    count = len(pieces)
    dma = pltpu.SemaphoreType.DMA
    low = jnp.bfloat16
    scratch = [pltpu.VMEM(factor.shape, low) for factor in factors]
    scratch += [pltpu.VMEM(small.shape, low), pltpu.VMEM((256, COLUMN_STEP), jnp.float32)]
    blocks = [(piece.rows, piece.columns) for piece in pieces]
    scratch += [pltpu.VMEM((levels, 2) + block, low) for block in blocks]
    scratch += [pltpu.VMEM((2, 2) + block, low) for block in blocks] * 2
    scratch += [
        pltpu.VMEM((levels if piece.direct else 1,) + block, low)
        for piece, block in zip(pieces, blocks)
    ]
    scratch += [
        pltpu.VMEM((levels + 1, 1 if piece.direct else 2) + block, low)
        for piece, block in zip(pieces, blocks)
    ]
    scratch += [
        dma((7,)),
        dma((count, 2, 2)),
        dma((count, 2, 2)),
        dma((count, levels)),
        dma((count, levels)),
        dma((count, levels, 2)),
        dma((count, levels + 1, 2)),
        pltpu.SemaphoreType.REGULAR,
    ]
    scratch += spread_semaphores(count, levels) + [dma((3,))]
    results = [*shapes, (change.shape[0], change.shape[1] // 2)]
    return pl.pallas_call(
        partial(reduce_kernel, pieces),
        out_shape=[jax.ShapeDtypeStruct(shape, low) for shape in results],
        in_specs=[ANY] * 8,
        out_specs=[ANY] * 6,
        scratch_shapes=scratch,
        compiler_params=pltpu.CompilerParams(
            collective_id=number, has_side_effects=True, vmem_limit_bytes=60 * 2**20
        ),
        name="reduce_gradients",
    )(*factors, small, change)


def rotary_rows():
    positions = np.arange(SLOT, dtype=np.float64)[:, None]
    lane = np.arange(2 * HEAD_DIM)[None, :] % HEAD_DIM
    angles = positions * rotary_base ** (-(lane // 2 * 2.0) / ROT)
    turned = lane < ROT
    cosine = np.where(turned, np.cos(angles), 1.0)
    sine = np.where(turned, np.sin(angles), 0.0)
    even = np.where(lane % 2 == 0, sine, 0.0)
    odd = np.where(lane % 2 == 1, sine, 0.0)
    return np.stack([cosine, even, odd]).astype(np.float32)


def turn(pair, tables, back):
    lanes = pair.shape[1]
    following = pltpu.roll(pair, lanes - 1, 1)
    preceding = pltpu.roll(pair, 1, 1)
    side = following * tables[1] - preceding * tables[2]
    return pair * tables[0] + (side if back else -side)


def product(left, right, left_axis=1, right_axis=0):
    return lax.dot_general(
        left, right, (((left_axis,), (right_axis,)), ((), ())), preferred_element_type=jnp.float32
    )


def statistics(rows):
    average = jnp.mean(rows, axis=-1, keepdims=True)
    centered = rows - average
    variance = jnp.mean(centered * centered, axis=-1, keepdims=True)
    inverse = lax.rsqrt(variance + norm_epsilon)
    return centered * inverse, inverse


def low_lanes(width):
    return lax.broadcasted_iota(jnp.int32, (1, width), 1) < HEAD_DIM


def pair_lanes(index):
    return pl.ds(pl.multiple_of(index * 2 * HEAD_DIM, 2 * HEAD_DIM), 2 * HEAD_DIM)


def rows_at(index, step):
    return pl.ds(pl.multiple_of(index * step, step), step)


def attend(m, length, refs):
    (x, normed, qkv, attention, mixture, active, slope, total, result) = refs["state"]
    joint, output, expand, contract = refs["weights"]
    gain, offset, outer, inner = refs["vectors"]
    tables = refs["tables"]
    width = x.shape[2]

    def norm(i, carry):
        at = rows_at(i, ROW_STEP)
        standard, _ = statistics(x[m, at, :].astype(jnp.float32))
        normed[m, at, :] = (standard * gain[...] + offset[...]).astype(jnp.bfloat16)
        return carry

    lax.fori_loop(0, SLOT // ROW_STEP, norm, 0)
    for part in range(3):
        scale = HEAD_DIM**-0.5 if part == 0 else 1.0
        total[...] = product(normed[m], joint[:, part * width : (part + 1) * width])
        if part == 2:
            qkv[m, :, 2 * width :] = total[...].astype(jnp.bfloat16)
        else:

            def rotary(i, carry, part=part, scale=scale):
                pair = turn(total[:, pair_lanes(i)], tables, False)
                at = pair_lanes(i + part * (width // (2 * HEAD_DIM)))
                qkv[m, :, at] = pair.astype(jnp.bfloat16) * jnp.bfloat16(scale)
                return carry

            lax.fori_loop(0, width // (2 * HEAD_DIM), rotary, 0)

    key = lax.broadcasted_iota(jnp.int32, (SLOT, SLOT), 0)
    query = lax.broadcasted_iota(jnp.int32, (SLOT, SLOT), 1)
    allowed = (key <= query) & (key < length)
    pairs = width // (2 * HEAD_DIM)
    low = low_lanes(2 * HEAD_DIM)

    def heads(i, carry):
        queries, keys = qkv[m, :, pair_lanes(i)], qkv[m, :, pair_lanes(i + pairs)]
        values = qkv[m, :, pair_lanes(i + 2 * pairs)]
        mixed = []
        for half in range(2):
            own = jnp.where(low == (half == 0), queries, jnp.zeros_like(queries))
            scores = jnp.where(allowed, product(keys, own, 1, 1), masked_score)
            raised = jnp.exp(scores - jnp.max(scores, axis=0, keepdims=True))
            share = raised * (1.0 / jnp.sum(raised, axis=0, keepdims=True))
            share = share.astype(jnp.bfloat16)
            attention[m, 2 * i + half] = share
            mixed.append(product(share, values, 0, 0))
        mixture[m, :, pair_lanes(i)] = jnp.where(low, mixed[0], mixed[1]).astype(jnp.bfloat16)
        return carry

    lax.fori_loop(0, pairs, heads, 0, unroll=8)


def feed(m, refs):
    (x, normed, _, _, mixture, active, slope, total, result) = refs["state"]
    joint, output, expand, contract = refs["weights"]
    gain, offset, outer, inner = refs["vectors"]
    total[...] = x[m].astype(jnp.float32) + outer[...] + product(mixture[m], output[...])

    def hidden(i, carry):
        at = rows_at(i, FF_STEP)
        pre = product(normed[m], expand[:, at]) + inner[:, at]
        square = pre * pre
        bend = jnp.tanh(GELU_SCALE * (pre + GELU_CUBE * (square * pre)))
        lifted = 0.5 * (1.0 + bend)
        slant = (0.5 * GELU_SCALE) * (1.0 + (3.0 * GELU_CUBE) * square)
        slope[m, :, at] = (lifted + pre * (1.0 - bend * bend) * slant).astype(jnp.bfloat16)
        activated = (pre * lifted).astype(jnp.bfloat16)
        active[m, :, at] = activated
        total[...] += product(activated, contract[at, :])
        return carry

    lax.fori_loop(0, slope.shape[2] // FF_STEP, hidden, 0)
    result[m] = total[...].astype(jnp.bfloat16)


def backward_block(m, refs):
    (x, _, qkv, attention, _, _, slope, total, result) = refs["state"]
    joint, output, expand, contract = refs["weights"]
    gain, offset, outer, inner = refs["vectors"]
    upstream, mixture_grad = refs["gradients"]
    gain_sum, offset_sum, outer_sum, inner_sum = refs["sums"]
    tables = refs["tables"]
    width = x.shape[2]
    outer_sum[...] += jnp.sum(upstream[m].astype(jnp.float32), axis=0, keepdims=True)
    mixture_grad[...] = product(upstream[m], output[...], 1, 1).astype(jnp.bfloat16)
    total[...] = jnp.zeros_like(total)

    def hidden(i, carry):
        at = rows_at(i, FF_STEP)
        active_grad = product(upstream[m], contract[at, :], 1, 1)
        pre_grad = (active_grad * slope[m, :, at].astype(jnp.float32)).astype(jnp.bfloat16)
        slope[m, :, at] = pre_grad
        inner_sum[:, at] += jnp.sum(pre_grad.astype(jnp.float32), axis=0, keepdims=True)
        total[...] += product(pre_grad, expand[:, at], 1, 1)
        return carry

    lax.fori_loop(0, slope.shape[2] // FF_STEP, hidden, 0)
    pairs = width // (2 * HEAD_DIM)
    low = low_lanes(2 * HEAD_DIM)

    def heads(i, carry):
        queries, keys = qkv[m, :, pair_lanes(i)], qkv[m, :, pair_lanes(i + pairs)]
        values = qkv[m, :, pair_lanes(i + 2 * pairs)]
        mixed_grad = mixture_grad[:, pair_lanes(i)]
        query_grads, key_grads, value_grads = [], [], []
        for half in range(2):
            share = attention[m, 2 * i + half]
            own = jnp.where(low == (half == 0), mixed_grad, jnp.zeros_like(mixed_grad))
            value_grads.append(product(share, mixed_grad))
            share_grad = product(values, own, 1, 1)
            weight = share.astype(jnp.float32)
            weighted = weight * share_grad
            score_grad = weighted - weight * jnp.sum(weighted, axis=0, keepdims=True)
            score_grad = score_grad.astype(jnp.bfloat16)
            query_grads.append(product(score_grad, keys, 0, 0))
            key_grads.append(product(score_grad, queries))
        query_grad = jnp.where(low, query_grads[0], query_grads[1]) * HEAD_DIM**-0.5
        key_grad = jnp.where(low, key_grads[0], key_grads[1])
        value_grad = jnp.where(low, value_grads[0], value_grads[1])
        qkv[m, :, pair_lanes(i)] = turn(query_grad, tables, True).astype(jnp.bfloat16)
        qkv[m, :, pair_lanes(i + pairs)] = turn(key_grad, tables, True).astype(jnp.bfloat16)
        qkv[m, :, pair_lanes(i + 2 * pairs)] = value_grad.astype(jnp.bfloat16)
        return carry

    lax.fori_loop(0, pairs, heads, 0, unroll=8)

    def project(i, carry):
        at = rows_at(i, JOINT_STEP)
        total[:, at] += product(qkv[m], joint[at, :], 1, 1)
        return carry

    lax.fori_loop(0, width // JOINT_STEP, project, 0)

    def norm(i, carry):
        at = rows_at(i, ROW_STEP)
        standard, inverse = statistics(x[m, at, :].astype(jnp.float32))
        normed_grad = total[at, :]
        gain_sum[...] += jnp.sum(normed_grad * standard, axis=0, keepdims=True)
        offset_sum[...] += jnp.sum(normed_grad, axis=0, keepdims=True)
        scaled = normed_grad * gain[...]
        inner_mean = jnp.mean(scaled, axis=-1, keepdims=True)
        along = jnp.mean(scaled * standard, axis=-1, keepdims=True)
        change = inverse * (scaled - inner_mean - standard * along)
        result[m, at, :] = (upstream[m, at, :].astype(jnp.float32) + change).astype(jnp.bfloat16)
        return carry

    lax.fori_loop(0, SLOT // ROW_STEP, norm, 0)


def vector_rows(width):
    return max(1, width // LANES), max(1, LANES // width)


def lane_range(device, width):
    lane = lax.broadcasted_iota(jnp.int32, (1, LANES), 1)
    start = device * width % LANES
    return (lane >= start) & (lane < start + width)


def unpack_vectors(small, devices, vectors):
    width = vectors[0].shape[1] // devices
    wide = vectors[3].shape[1] // devices

    def gathered(index, shared):
        rows = small[pl.ds(pl.multiple_of(index * shared * SMALL_ROWS, SMALL_ROWS), SMALL_ROWS), :]
        total = rows.astype(jnp.float32)
        for other in range(1, shared):
            at = pl.multiple_of((index * shared + other) * SMALL_ROWS, SMALL_ROWS)
            total += small[pl.ds(at, SMALL_ROWS), :].astype(jnp.float32)
        return total

    _, shared = vector_rows(width)

    def narrow(index, carry):
        total = gathered(index, shared)
        at = rows_at(index, LANES)
        for i in range(3):
            vectors[i][:, at] = total[i : i + 1]
        return carry

    lax.fori_loop(0, devices // shared, narrow, 0)
    count, shared_wide = vector_rows(wide)

    def broad(index, carry):
        total = gathered(index, shared_wide)
        for i in range(count):
            vectors[3][:, rows_at(index * count + i, LANES)] = total[3 + i : 4 + i]
        return carry

    lax.fori_loop(0, devices // shared_wide, broad, 0)


def pack_sums(sums, devices, packed):
    width = sums[0].shape[1] // devices
    wide = sums[3].shape[1] // devices
    count, _ = vector_rows(wide)
    row = lax.broadcasted_iota(jnp.int32, (SMALL_ROWS, LANES), 0)

    def device(index, carry):
        rows = []
        inside = lane_range(index, width)
        for i in range(3):
            rows.append(jnp.where(inside, sums[i][:, rows_at(index * width // LANES, LANES)], 0.0))
        for i in range(count):
            line = sums[3][:, rows_at(index * wide // LANES + i, LANES)]
            rows.append(line if wide >= LANES else jnp.where(lane_range(index, wide), line, 0.0))
        block = jnp.zeros((SMALL_ROWS, LANES), jnp.float32)
        for i, line in enumerate(rows):
            block = jnp.where(row == i, line, block)
        packed[rows_at(index, SMALL_ROWS), :] = block.astype(jnp.bfloat16)
        return carry

    lax.fori_loop(0, devices, device, 0)


def blocks_kernel(pieces, *refs):
    lengths, hidden_in, cotangent, tables_in = refs[:4]
    sources = refs[4:9]
    hidden_out, input_grad = refs[9:11]
    factor_outs, packed = refs[11:17], refs[17]
    weights, small = refs[18:22], refs[22]
    x, normed, qkv, attention, mixture, active, slope, total, result = refs[23:32]
    upstream, mixture_grad, tables = refs[32:35]
    vectors, sums = refs[35:39], refs[39:43]
    table_sem, in_keep, in_send, in_receive, hand_send, hand_receive = refs[43:49]
    half_send, half_receive, half_keep, out_sem = refs[49:53]
    here = Place()
    section = lax.axis_index("section")
    partner = {"section": 1 - section}
    half = hidden_out.shape[1]
    devices = 4 * here.levels

    def keeping(source, target, start, m):
        return pltpu.make_async_copy(
            source.at[rows_at(m, SLOT), :], target.at[m, :, pl.ds(start, half)], in_keep.at[m]
        )

    def halving(source, target, start, m):
        return pltpu.make_async_remote_copy(
            source.at[rows_at(m, SLOT), :],
            target.at[m, :, pl.ds(start, half)],
            in_send.at[m],
            in_receive.at[m],
            device_id=partner,
            device_id_type=MESH,
        )

    def handing(target, m):
        return pltpu.make_async_remote_copy(
            result.at[m],
            target.at[m],
            hand_send.at[m],
            hand_receive.at[m],
            device_id=partner,
            device_id_type=MESH,
        )

    def away(target, start, m):
        return pltpu.make_async_remote_copy(
            result.at[m, :, pl.ds(start, half)],
            target.at[rows_at(m, SLOT), :],
            half_send.at[m],
            half_receive.at[m],
            device_id=partner,
            device_id_type=MESH,
        )

    def kept(target, start, m):
        return pltpu.make_async_copy(
            result.at[m, :, pl.ds(start, half)], target.at[rows_at(m, SLOT), :], half_keep.at[m]
        )

    def stored(m):
        return pltpu.make_async_copy(
            result.at[m], input_grad.at[rows_at(m, SLOT), :], half_keep.at[m]
        )

    def giving(i, source, m):
        return pltpu.make_async_copy(
            source.at[m], factor_outs[i].at[rows_at(m, SLOT), :], out_sem.at[i, m]
        )

    reading = pltpu.make_async_copy(tables_in, tables, table_sem.at[0])
    reading.start()
    for m in range(MICRO):
        pl.when(section == 0)(lambda m=m: keeping(hidden_in, x, 0, m).start())
        pl.when(section == 1)(lambda m=m: keeping(cotangent, upstream, half, m).start())
    for total_sum in sums:
        total_sum[...] = jnp.zeros_like(total_sum)
    greet(here, True)
    owns = [piece.of(sources[piece.array]) for piece in pieces]
    spread = Spread(here, pieces, owns, [*weights, small], refs[53:])
    early = [p for p, piece in enumerate(pieces) if piece.array in (0, 1, 4)]
    late = [p for p, piece in enumerate(pieces) if piece.array in (2, 3)]
    spread.begin_all(early)
    for m in range(MICRO):
        pl.when(section == 1)(lambda m=m: halving(hidden_in, x, half, m).start())
        pl.when(section == 0)(lambda m=m: halving(cotangent, upstream, 0, m).start())
    shared = {
        "state": (x, normed, qkv, attention, mixture, active, slope, total, result),
        "weights": weights,
        "vectors": vectors,
        "tables": tables,
        "gradients": (upstream, mixture_grad),
        "sums": sums,
    }
    spread.middle(early, lambda: spread.begin_all(late))
    spread.received(early)
    unpack_vectors(small, devices, vectors)
    reading.wait()

    @pl.when(section == 0)
    def _():
        def ahead(m, carry):
            keeping(hidden_in, x, 0, m).wait()
            halving(hidden_in, x, half, m).wait_recv()
            attend(m, lengths[m], shared)
            return carry

        lax.fori_loop(0, MICRO, ahead, 0)

    spread.middle(late)
    spread.received(late)

    def forward(m, carry):
        @pl.when(section == 1)
        def _():
            handing(x, m).wait_recv()
            attend(m, lengths[m], shared)

        feed(m, shared)

        @pl.when(section == 0)
        def _():
            pl.when(m > 0)(lambda: handing(x, m - 1).wait_send())
            handing(x, m).start()

        @pl.when(section == 1)
        def _():
            away(hidden_out, 0, m).start()
            kept(hidden_out, half, m).start()

        for i, source in enumerate((normed, mixture, active)):
            giving(i, source, m).start()
        return carry

    lax.fori_loop(0, MICRO, forward, 0)

    def backward(m, carry):
        @pl.when(section == 0)
        def _():
            pl.when(m == 0)(lambda: handing(x, MICRO - 1).wait_send())
            handing(upstream, m).wait_recv()

        @pl.when(section == 1)
        def _():
            away(hidden_out, 0, m).wait_send()
            kept(hidden_out, half, m).wait()
            keeping(cotangent, upstream, half, m).wait()
            halving(cotangent, upstream, 0, m).wait_recv()
            row = lax.broadcasted_iota(jnp.int32, (SLOT, 1), 0)
            inside = (row < lengths[m]).astype(jnp.float32)
            masked = upstream[m].astype(jnp.float32) * inside
            upstream[m] = masked.astype(jnp.bfloat16)

        backward_block(m, shared)

        @pl.when(section == 1)
        def _():
            handing(upstream, m).start()

        pl.when(section == 0)(lambda: stored(m).start())
        for i, source in enumerate((qkv, slope, upstream)):
            giving(3 + i, source, m).start()
        return carry

    lax.fori_loop(0, MICRO, backward, 0)
    pack_sums(sums, devices, packed)

    def last(m, carry):
        @pl.when(section == 0)
        def _():
            halving(cotangent, upstream, 0, m).wait_send()
            stored(m).wait()
            away(hidden_out, 0, m).wait_recv()

        @pl.when(section == 1)
        def _():
            halving(hidden_in, x, half, m).wait_send()
            handing(upstream, m).wait_send()

        for i, source in enumerate((normed, mixture, active, qkv, slope, upstream)):
            giving(i, source, m).wait()
        return carry

    lax.fori_loop(0, MICRO, last, 0)
    spread.sent()


def run_blocks(lengths, hidden_in, cotangent, owns, number):
    levels = lax.axis_size("batch") // 4
    devices = 4 * levels
    tokens, half = hidden_in.shape
    width = half * lax.axis_size("section")
    wide = owns[2].shape[1]
    low, full = jnp.bfloat16, jnp.float32
    shape = jax.ShapeDtypeStruct
    vmem = pltpu.VMEM
    dma = pltpu.SemaphoreType.DMA
    pieces = pieces_of([own.shape for own in owns])
    outputs = [shape((tokens, half), low), shape((tokens, width), low)]
    outputs += [shape((tokens, n), low) for n in (width, width, wide, 3 * width, wide, width)]
    outputs += [shape((devices * SMALL_ROWS, LANES), low)]
    scratch = [vmem((devices * own.shape[0], own.shape[1]), low) for own in owns]
    scratch += [
        vmem((MICRO, SLOT, width), low),
        vmem((MICRO, SLOT, width), low),
        vmem((MICRO, SLOT, 3 * width), low),
        vmem((MICRO, HEADS, SLOT, SLOT), low),
        vmem((MICRO, SLOT, width), low),
        vmem((MICRO, SLOT, wide), low),
        vmem((MICRO, SLOT, wide), low),
        vmem((SLOT, width), full),
        vmem((MICRO, SLOT, width), low),
        vmem((MICRO, SLOT, width), low),
        vmem((SLOT, width), low),
        vmem((3, SLOT, 2 * HEAD_DIM), full),
    ]
    scratch += [vmem((1, n), full) for n in (width, width, width, wide)] * 2
    scratch += [dma((1,))] + [dma((MICRO,))] * 8 + [dma((6, MICRO))]
    scratch += spread_semaphores(len(pieces), levels)
    return pl.pallas_call(
        partial(blocks_kernel, pieces),
        out_shape=outputs,
        in_specs=[pl.BlockSpec(memory_space=pltpu.SMEM)] + [ANY] * 8,
        out_specs=[ANY] * 8 + [pl.BlockSpec(memory_space=vmem)],
        scratch_shapes=scratch,
        compiler_params=pltpu.CompilerParams(
            collective_id=number, has_side_effects=True, vmem_limit_bytes=60 * 2**20
        ),
        name="two_blocks",
    )(lengths, hidden_in, cotangent, jnp.asarray(rotary_rows()), *owns)


def pack_vectors(vectors):
    device = lax.axis_index("batch")
    size = SMALL_ROWS * LANES
    total = jnp.zeros((1, size), jnp.float32)
    row = 0
    for vector in vectors:
        width = vector.shape[1]
        used = min(width, LANES)
        slot = device * width % LANES // used
        for i in range(LANES // used):
            start = row * LANES + i * used
            moved = jnp.pad(vector.astype(jnp.float32), ((0, 0), (start, size - start - width)))
            total = total + jnp.where(slot == i, moved, 0.0)
        row += max(1, width // LANES)
    return total.reshape(SMALL_ROWS, LANES).astype(jnp.bfloat16)


def widen_kernel(devices, *refs):
    small, sources = refs[0], refs[1 : (len(refs) - 5) // 2 + 1]
    targets, vectors = refs[len(sources) + 1 : -4], refs[-4:]
    pl.when(pl.program_id(0) == 0)(lambda: unpack_vectors(small, devices, vectors))
    for source, target in zip(sources, targets):
        target[...] = source[...].astype(target.dtype).reshape(target.shape)


def widen(small, sums, kept, widths, devices):
    steps = 8
    arrays = [*sums, *kept]
    whole = lambda i: (0, 0)
    in_specs = [
        pl.BlockSpec((array.shape[0] // steps, array.shape[1]), lambda i: (i, 0))
        for array in arrays
    ]
    out_specs = [
        pl.BlockSpec((1, array.shape[0] // steps, array.shape[1]), lambda i: (0, i, 0))
        for array in sums
    ] + in_specs[len(sums) :]
    out_specs += [pl.BlockSpec((1, width), whole) for width in widths]
    shapes = [jax.ShapeDtypeStruct((1, *array.shape), jnp.float32) for array in sums]
    shapes += [jax.ShapeDtypeStruct(array.shape, array.dtype) for array in kept]
    shapes += [jax.ShapeDtypeStruct((1, width), jnp.float32) for width in widths]
    return pl.pallas_call(
        partial(widen_kernel, devices),
        out_shape=shapes,
        grid=(steps,),
        in_specs=[pl.BlockSpec(small.shape, whole)] + in_specs,
        out_specs=out_specs,
        compiler_params=pltpu.CompilerParams(vmem_limit_bytes=60 * 2**20),
        name="widen",
    )(small, *arrays)


def local(
    hidden_in,
    cotangent,
    lengths,
    norm_gain,
    norm_offset,
    joint_weight,
    output_weight,
    expand_weight,
    inner_bias,
    contract_weight,
    outer_bias,
):
    devices = lax.axis_size("batch")
    owns = [
        joint_weight[0],
        output_weight[0],
        expand_weight[0],
        contract_weight[0],
        pack_vectors((norm_gain, norm_offset, outer_bias, inner_bias)),
    ]
    results = run_blocks(lengths, hidden_in, cotangent, owns, 1)
    shapes = [(own.shape[0] * devices, own.shape[1]) for own in owns[:4]]
    *sums, small_sum, own_grad = reduce_all(results[2:8], results[8], results[1], shapes, 2)
    width, wide = norm_gain.shape[1] * devices, inner_bias.shape[1] * devices
    (
        joint_sum,
        output_sum,
        expand_sum,
        contract_sum,
        hidden_out,
        input_grad,
        gain_sum,
        offset_sum,
        outer_sum,
        inner_sum,
    ) = widen(small_sum, sums, [results[0], own_grad], (width, width, width, wide), devices)
    return (
        hidden_out,
        input_grad,
        gain_sum,
        offset_sum,
        joint_sum,
        output_sum,
        expand_sum,
        inner_sum,
        contract_sum,
        outer_sum,
    )


def solution(mesh):
    return jax.shard_map(
        local,
        mesh=mesh,
        in_specs=(
            P("batch", "section"),
            P("batch", "section"),
            P("batch"),
            P("section", "batch"),
            P("section", "batch"),
            P("section", "batch", None),
            P("section", "batch", None),
            P("section", "batch", None),
            P("section", "batch"),
            P("section", "batch", None),
            P("section", "batch"),
        ),
        out_specs=(
            P("batch", "section"),
            P("batch", "section"),
            P("section", None),
            P("section", None),
            P("section", None, None),
            P("section", None, None),
            P("section", None, None),
            P("section", None),
            P("section", None, None),
            P("section", None),
        ),
        check_vma=False,
    )
```

```python
from functools import partial

import jax
import jax.numpy as jnp
import numpy as np
from jax import lax
from jax.experimental import pallas as pl
from jax.experimental.pallas import tpu as pltpu
from jax.sharding import PartitionSpec as P

HEADS = 16
HEAD_DIM = 64
ROT = 32
SLOT = 256
MICRO = 2
SMALL_ROWS = 16
LANES = 128
ROW_STEP = 256
FF_STEP = 4096
JOINT_STEP = 1024
GELU_SCALE = (2.0 / np.pi) ** 0.5
GELU_CUBE = 0.044715
norm_epsilon = 1e-05
rotary_base = 10000.0
masked_score = -1e30
MESH = pl.DeviceIdType.MESH
ANY = pl.BlockSpec(memory_space=pl.ANY)


class Place:
    def __init__(self):
        index = lax.axis_index("batch")
        self.levels = lax.axis_size("batch") // 4
        self.last = self.levels - 1
        self.z, self.y, self.c = index // 4, index // 2 % 2, index % 2

    def at(self, z=None, y=None, c=None):
        z = self.z if z is None else z
        y = self.y if y is None else y
        c = self.c if c is None else c
        return z * 4 + y * 2 + c


class Piece:
    def __init__(self, array, offset, rows, column, columns, direct):
        self.array, self.offset, self.rows = array, offset, rows
        self.column, self.columns, self.direct = column, columns, direct

    def sides(self, y):
        return (y,) if self.direct else (y, 1 - y)

    def of(self, block):
        return block.at[pl.ds(self.offset, self.rows), pl.ds(self.column, self.columns)]


def pieces_of(blocks):
    joint, output, expand, contract, small = blocks
    cut = contract[0] // 4
    pieces = [
        Piece(1, 0, output[0], 0, output[1], False),
        Piece(3, 0, cut, 0, contract[1], False),
    ]
    for array, offset, (rows, columns), parts in (
        (0, 0, joint, 1),
        (2, 0, expand, 1),
        (3, cut, contract, 1),
        (4, 0, small, 1),
    ):
        for i in range(parts):
            width = columns // parts
            pieces.append(Piece(array, offset, rows - offset, i * width, width, True))
    return pieces


def remote(source, target, send, receive, index):
    return pltpu.make_async_remote_copy(
        source, target, send, receive, device_id={"batch": index}, device_id_type=MESH
    )


def greet(here, with_section):
    barrier = pltpu.get_barrier_semaphore()

    def signal(**who):
        pl.semaphore_signal(barrier, inc=1, device_id=who, device_id_type=MESH)

    signal(batch=here.at(y=1 - here.y))
    signal(batch=here.at(c=1 - here.c))
    pl.when(here.z > 0)(lambda: signal(batch=here.at(z=here.z - 1)))
    pl.when(here.z < here.last)(lambda: signal(batch=here.at(z=here.z + 1)))
    waits = 2
    if with_section:
        signal(section=1 - lax.axis_index("section"))
        waits = 3
    below = jnp.minimum(here.z, 1)
    above = jnp.minimum(here.last - here.z, 1)
    pl.semaphore_wait(barrier, waits + below + above)


def spread_semaphores(count, levels):
    dma = pltpu.SemaphoreType.DMA
    return [
        dma((count,)),
        dma((count, levels, 2, 2)),
        dma((count, levels, 2)),
        dma((count, levels)),
        dma((count, levels)),
        dma((count, levels, 2)),
        dma((count, levels, 2)),
    ]


class Spread:
    def __init__(self, here, pieces, owns, outs, semaphores):
        self.here, self.pieces, self.owns, self.outs = here, pieces, owns, outs
        (self.keep, self.zs, self.zr, self.ys, self.yr, self.cs, self.cr) = semaphores

    def block(self, p, z, y, c):
        piece = self.pieces[p]
        out = self.outs[piece.array]
        rows = out.shape[0] // (4 * self.here.levels)
        start = (z * 4 + y * 2 + c) * rows + piece.offset
        return out.at[
            pl.ds(pl.multiple_of(start, 8), piece.rows), pl.ds(piece.column, piece.columns)
        ]

    def along(self, p, z, y, source, way):
        here = self.here
        return remote(
            source,
            self.block(p, z, y, here.c),
            self.zs.at[p, z, y, way],
            self.zr.at[p, z, y],
            here.at(z=here.z + (1 if way == 0 else -1)),
        )

    def across(self, p, z, source):
        here = self.here
        target = self.block(p, z, here.y, here.c)
        return remote(source, target, self.ys.at[p, z], self.yr.at[p, z], here.at(y=1 - here.y))

    def beside(self, p, z, y, source):
        here = self.here
        target = self.block(p, z, y, here.c)
        return remote(
            source, target, self.cs.at[p, z, y], self.cr.at[p, z, y], here.at(c=1 - here.c)
        )

    def both_ways(self, p, y, source):
        here = self.here
        pl.when(here.z < here.last)(lambda: self.along(p, here.z, y, source, 0).start())
        pl.when(here.z > 0)(lambda: self.along(p, here.z, y, source, 1).start())

    def begin(self, p, held=False):
        here, own = self.here, self.owns[p]
        self.across(p, here.z, own).start()
        if not held:
            self.both_ways(p, here.y, own)
        self.beside(p, here.z, here.y, own).start()
        target = self.block(p, here.z, here.y, here.c)
        pltpu.make_async_copy(own, target, self.keep.at[p]).start()

    def begin_all(self, chosen):
        order = sorted(chosen, key=lambda p: self.pieces[p].direct)
        for p in order:
            self.begin(p, held=not self.pieces[p].direct)
        for p in order:
            if not self.pieces[p].direct:
                self.both_ways(p, self.here.y, self.owns[p])

    def from_z(self, p, z, y, way):
        here = self.here
        block = self.block(p, z, y, here.c)
        self.along(p, z, y, block, way).wait_recv()
        more = here.z < here.last if way == 0 else here.z > 0
        pl.when(more)(lambda: self.along(p, z, y, block, way).start())
        if self.pieces[p].direct:
            self.across(p, z, block).start()
        self.beside(p, z, y, block).start()

    def from_y(self, p, z):
        here = self.here
        block = self.block(p, z, 1 - here.y, here.c)
        self.across(p, z, block).wait_recv()
        if not self.pieces[p].direct:
            self.both_ways(p, 1 - here.y, block)
        self.beside(p, z, 1 - here.y, block).start()

    def z_events(self, chosen, distance):
        here = self.here

        def pair(p, side):
            y = self.pieces[p].sides(here.y)[side]
            pl.when(here.z - distance >= 0)(lambda: self.from_z(p, here.z - distance, y, 0))
            pl.when(here.z + distance <= here.last)(
                lambda: self.from_z(p, here.z + distance, y, 1)
            )

        for p in chosen:
            if self.pieces[p].direct:
                pair(p, 0)
        for side in range(2):
            for p in chosen:
                if not self.pieces[p].direct:
                    pair(p, side)

    def y_events(self, chosen, z):
        for p in chosen:
            if self.pieces[p].direct:
                self.from_y(p, z)

    def middle(self, chosen, then=None):
        here = self.here
        for p in chosen:
            if not self.pieces[p].direct:
                self.from_y(p, here.z)

        def y_pair(distance):
            pl.when(here.z - distance >= 0)(lambda: self.y_events(chosen, here.z - distance))
            pl.when((here.z + distance <= here.last) & (distance > 0))(
                lambda: self.y_events(chosen, here.z + distance)
            )

        def step(distance, carry):
            self.z_events(chosen, distance)
            y_pair(distance - 1)
            return carry

        lax.fori_loop(1, here.levels, step, 0)
        if then is not None:
            then()
        y_pair(here.last)

    def received(self, chosen):
        here = self.here

        def level(z, carry):
            for p in chosen:
                own = self.block(p, z, here.y, here.c)
                for y in range(2):
                    self.beside(p, z, y, own).wait_recv()
            return carry

        lax.fori_loop(0, here.levels, level, 0)
        for p in chosen:
            block = self.block(p, here.z, here.y, here.c)
            pltpu.make_async_copy(block, block, self.keep.at[p]).wait()

    def sent(self):
        here = self.here

        def level(z, carry):
            for p, piece in enumerate(self.pieces):
                own = self.block(p, z, here.y, here.c)
                for y in range(2):
                    self.beside(p, z, y, own).wait_send()
                crossed = z >= 0 if piece.direct else z == here.z
                pl.when(crossed)(lambda p=p, own=own: self.across(p, z, own).wait_send())
                for y in piece.sides(here.y):
                    pl.when((z <= here.z) & (here.z < here.last))(
                        lambda p=p, y=y, own=own: self.along(p, z, y, own, 0).wait_send()
                    )
                    pl.when((z >= here.z) & (here.z > 0))(
                        lambda p=p, y=y, own=own: self.along(p, z, y, own, 1).wait_send()
                    )
            return carry

        lax.fori_loop(0, here.levels, level, 0)


def add_rows(target, other):
    rows = target.shape[0]
    step = min(rows, 16)

    def body(i, carry):
        at = pl.ds(pl.multiple_of(i * step, step), step)
        total = target[at, :].astype(jnp.float32) + other[at, :].astype(jnp.float32)
        target[at, :] = total.astype(target.dtype)
        return carry

    lax.fori_loop(0, rows // step, body, 0)


FACTORS = ((0, 3), (1, 5), (0, 4), (2, 5))
MAKE_ORDER = (3, 1, 2, 0, 4)
COLUMN_STEP = 1024


class Reduce:
    def __init__(self, here, pieces, factors, small, product_rows, buffers, semaphores):
        self.here, self.pieces, self.factors, self.small = here, pieces, factors, small
        self.made = product_rows
        self.mine, self.sent, self.sib, self.yb, self.zb = buffers
        (self.load, self.cs, self.cr, self.ys, self.yr, self.zs, self.zr, self.credit) = semaphores

    def level(self, i):
        here = self.here
        above, below = here.last - here.z, here.z
        lead = jnp.maximum(above, below) - jnp.minimum(above, below)
        single = jnp.where(above > below, here.last - i, i)
        later = i - lead
        distance = jnp.minimum(above, below) - later // 2
        outer = jnp.where(above > below, here.z - distance, here.z + distance)
        paired = jnp.where(later % 2 == 0, outer, 2 * here.z - outer)
        return jnp.where(i < lead, single, paired)

    def to_core(self, p, slot, y):
        here = self.here
        return remote(
            self.sent[p].at[slot, y],
            self.sib[p].at[slot, y],
            self.cs.at[p, slot, y],
            self.cr.at[p, slot, y],
            here.at(c=1 - here.c),
        )

    def to_y(self, p, z):
        here = self.here
        return remote(
            self.mine[p].at[z, 1 - here.y],
            self.yb[p].at[z if self.pieces[p].direct else 0],
            self.ys.at[p, z],
            self.yr.at[p, z],
            here.at(y=1 - here.y),
        )

    def slot(self, z, at_z, way):
        if way == 0:
            return z
        return jnp.where(z == at_z, self.here.levels, z)

    def to_z(self, p, z, y, way):
        here = self.here
        step = 1 if way == 0 else -1
        slot = self.slot(z, here.z + step, way)
        side = 0 if self.pieces[p].direct else y
        return remote(
            self.mine[p].at[z, y],
            self.zb[p].at[slot, side],
            self.zs.at[p, z, side],
            self.zr.at[p, slot, side],
            here.at(z=here.z + step),
        )

    def arrive(self, p, z, y, way):
        here = self.here
        slot = self.slot(z, here.z, way)
        side = 0 if self.pieces[p].direct else y
        block = self.zb[p].at[slot, side]
        remote(
            block, block, self.zs.at[p, z, side], self.zr.at[p, slot, side], here.at(y=1 - here.y)
        ).wait_recv()
        add_rows(self.mine[p].at[z, y], block)

    def store(self, array, z, slot, y, own, value, column):
        for p, piece in enumerate(self.pieces):
            first = max(column, piece.column)
            end = min(column + value.shape[1], piece.column + piece.columns)
            if piece.array == array and first < end:
                target = self.mine[p].at[z, y] if own else self.sent[p].at[slot, y]
                part = value[piece.offset : piece.offset + piece.rows, first - column : end - column]
                target[:, first - piece.column : end - piece.column] = part.astype(jnp.bfloat16)

    def make(self, array, z, slot):
        here = self.here
        rows = max(p.offset + p.rows for p in self.pieces if p.array == array)
        cores = ((False, 1 - here.c), (True, here.c))
        if array == 4:
            for own, c in cores:
                for y in range(2):
                    at = pl.multiple_of((z * 4 + y * 2 + c) * rows, 16)
                    self.store(array, z, slot, y, own, self.small[pl.ds(at, rows), :], 0)
            return
        left, right = (self.factors[i] for i in FACTORS[array])
        columns = right.shape[1]
        tiles = range(0, columns, COLUMN_STEP)
        if rows % 128 == 0:
            for own, c in cores:
                for y in range(2):
                    at = pl.multiple_of((z * 4 + y * 2 + c) * rows, 128)
                    turned = left[:, pl.ds(at, rows)].T
                    for tile in tiles:
                        value = product(turned, right[:, tile : tile + COLUMN_STEP])
                        self.store(array, z, slot, y, own, value, tile)
            return
        span = max(4 * rows, 128)
        start = z * 4 * rows // span * span
        turned = left[:, pl.ds(pl.multiple_of(start, 128), span)].T
        for tile in tiles:
            self.made[:span, :] = product(turned, right[:, tile : tile + COLUMN_STEP])
            for own, c in cores:
                for y in range(2):
                    at = pl.multiple_of((z * 4 + y * 2 + c) * rows - start, 8)
                    self.store(array, z, slot, y, own, self.made[pl.ds(at, rows), :], tile)

    def of(self, array):
        return [p for p, piece in enumerate(self.pieces) if piece.array == array]

    def build(self, i, waits):
        here = self.here
        z, slot = self.level(i), i % 2

        @pl.when(i >= 2)
        def _():
            for p in range(len(self.pieces)):
                for y in range(2):
                    self.to_core(p, slot, y).wait_send()
            pl.semaphore_wait(self.credit, 1)

        def add(array):
            for p in self.of(array):
                for y in range(2):
                    self.to_core(p, slot, y).wait_recv()
                    add_rows(self.mine[p].at[z, y], self.sib[p].at[slot, y])
                if self.pieces[p].direct:
                    self.to_y(p, z).start()
                else:
                    self.pass_on(z, [p])

        for step, array in enumerate(MAKE_ORDER):
            waits(i, array)
            self.make(array, z, slot)
            for p in self.of(array):
                for y in range(2):
                    self.to_core(p, slot, y).start()
            if step > 0:
                add(MAKE_ORDER[step - 1])
        add(MAKE_ORDER[-1])

        @pl.when(i < here.levels - 2)
        def _():
            other = {"batch": here.at(c=1 - here.c)}
            pl.semaphore_signal(self.credit, inc=1, device_id=other, device_id_type=MESH)

    def rows(self, p, z):
        self.to_y(p, z).wait_recv()
        source = self.yb[p].at[z if self.pieces[p].direct else 0]
        add_rows(self.mine[p].at[z, self.here.y], source)

    def pass_on(self, z, chosen):
        here = self.here

        def hop(way):
            further = here.z > 0 if way == 0 else here.z < here.last
            for p in chosen:
                if self.pieces[p].direct:
                    self.rows(p, z)
                for y in self.pieces[p].sides(here.y):
                    pl.when(further)(lambda p=p, y=y: self.arrive(p, z, y, way))
                    self.to_z(p, z, y, way).start()

        pl.when(z > here.z)(lambda: hop(0))
        pl.when(z < here.z)(lambda: hop(1))

    def run(self, waits):
        here = self.here
        made = [p for array in MAKE_ORDER for p in self.of(array)]
        direct = [p for p in made if self.pieces[p].direct]

        def step(i, carry):
            self.build(i, waits)
            pl.when(i > 0)(lambda: self.pass_on(self.level(i - 1), direct))
            return carry

        lax.fori_loop(0, here.levels, step, 0)

    def settle(self, p):
        here = self.here
        for y in self.pieces[p].sides(here.y):
            pl.when(here.z > 0)(lambda y=y: self.arrive(p, here.z, y, 0))
            pl.when(here.z < here.last)(lambda y=y: self.arrive(p, here.z, y, 1))

    def finish(self):
        here = self.here
        for slot in range(min(2, here.levels)):
            for p in range(len(self.pieces)):
                for y in range(2):
                    self.to_core(p, slot, y).wait_send()

        def level(z, carry):
            for p, piece in enumerate(self.pieces):
                crossed = z >= 0 if piece.direct else z == here.z
                pl.when(crossed)(lambda p=p: self.to_y(p, z).wait_send())
                for y in piece.sides(here.y):
                    pl.when(z > here.z)(lambda p=p, y=y: self.to_z(p, z, y, 0).wait_send())
                    pl.when(z < here.z)(lambda p=p, y=y: self.to_z(p, z, y, 1).wait_send())
            return carry

        lax.fori_loop(0, here.levels, level, 0)


def reduce_kernel(pieces, *refs):
    count = len(pieces)
    sources, change, outs, input_grad, rest = refs[:7], refs[7], refs[8:13], refs[13], refs[14:]
    factors, small, made = rest[:6], rest[6], rest[7]
    rest = rest[8:]
    buffers = [rest[i * count : (i + 1) * count] for i in range(5)]
    rest = rest[5 * count :]
    here = Place()
    loads = [
        pltpu.make_async_copy(source, target, rest[0].at[i])
        for i, (source, target) in enumerate(zip(sources, [*factors, small]))
    ]
    order = (2, 5, 1, 0, 4, 3, 6)
    for i in order:
        loads[i].start()
    greet(here, True)
    section = lax.axis_index("section")
    half = input_grad.shape[1]
    over = pltpu.make_async_remote_copy(
        change.at[:, pl.ds(half, half)],
        input_grad,
        rest[-1].at[0],
        rest[-1].at[1],
        device_id={"section": 1 - section},
        device_id_type=MESH,
    )
    keep = pltpu.make_async_copy(change.at[:, pl.ds(0, half)], input_grad, rest[-1].at[2])

    @pl.when(section == 0)
    def _():
        over.start()
        keep.start()

    reduce = Reduce(here, pieces, factors, small, made, buffers, rest[:8])
    needs = {3: (2, 5), 1: (1,), 2: (0, 4), 0: (3,), 4: (6,)}

    def waits(i, array):
        @pl.when(i == 0)
        def _():
            for k in needs[array]:
                loads[k].wait()

    reduce.run(waits)
    owns = [buffers[0][p].at[here.z, here.y] for p in range(count)]
    spread = Spread(here, pieces, owns, outs, rest[8:-1])
    turned = [p for p in range(count) if not pieces[p].direct]
    for p in turned:
        reduce.settle(p)
        reduce.to_y(p, here.z).start()
    for p in range(count):
        if pieces[p].direct:
            reduce.rows(p, here.z)
            reduce.settle(p)
            spread.begin(p)
    for p in turned:
        reduce.rows(p, here.z)
        spread.begin(p)
    spread.middle(range(count))
    reduce.finish()
    spread.received(range(count))
    spread.sent()

    @pl.when(section == 0)
    def _():
        over.wait_send()
        keep.wait()

    pl.when(section == 1)(over.wait_recv)


def reduce_all(factors, small, change, shapes, number):
    levels = lax.axis_size("batch") // 4
    shapes = [*shapes, small.shape]
    pieces = pieces_of([(rows // (4 * levels), columns) for rows, columns in shapes])
    count = len(pieces)
    dma = pltpu.SemaphoreType.DMA
    low = jnp.bfloat16
    scratch = [pltpu.VMEM(factor.shape, low) for factor in factors]
    scratch += [pltpu.VMEM(small.shape, low), pltpu.VMEM((256, COLUMN_STEP), jnp.float32)]
    blocks = [(piece.rows, piece.columns) for piece in pieces]
    scratch += [pltpu.VMEM((levels, 2) + block, low) for block in blocks]
    scratch += [pltpu.VMEM((2, 2) + block, low) for block in blocks] * 2
    scratch += [
        pltpu.VMEM((levels if piece.direct else 1,) + block, low)
        for piece, block in zip(pieces, blocks)
    ]
    scratch += [
        pltpu.VMEM((levels + 1, 1 if piece.direct else 2) + block, low)
        for piece, block in zip(pieces, blocks)
    ]
    scratch += [
        dma((7,)),
        dma((count, 2, 2)),
        dma((count, 2, 2)),
        dma((count, levels)),
        dma((count, levels)),
        dma((count, levels, 2)),
        dma((count, levels + 1, 2)),
        pltpu.SemaphoreType.REGULAR,
    ]
    scratch += spread_semaphores(count, levels) + [dma((3,))]
    results = [*shapes, (change.shape[0], change.shape[1] // 2)]
    return pl.pallas_call(
        partial(reduce_kernel, pieces),
        out_shape=[jax.ShapeDtypeStruct(shape, low) for shape in results],
        in_specs=[ANY] * 8,
        out_specs=[ANY] * 6,
        scratch_shapes=scratch,
        compiler_params=pltpu.CompilerParams(
            collective_id=number, has_side_effects=True, vmem_limit_bytes=60 * 2**20
        ),
        name="reduce_gradients",
    )(*factors, small, change)


def rotary_rows():
    positions = np.arange(SLOT, dtype=np.float64)[:, None]
    lane = np.arange(2 * HEAD_DIM)[None, :] % HEAD_DIM
    angles = positions * rotary_base ** (-(lane // 2 * 2.0) / ROT)
    turned = lane < ROT
    cosine = np.where(turned, np.cos(angles), 1.0)
    sine = np.where(turned, np.sin(angles), 0.0)
    even = np.where(lane % 2 == 0, sine, 0.0)
    odd = np.where(lane % 2 == 1, sine, 0.0)
    return np.stack([cosine, even, odd]).astype(np.float32)


def turn(pair, tables, back):
    lanes = pair.shape[1]
    following = pltpu.roll(pair, lanes - 1, 1)
    preceding = pltpu.roll(pair, 1, 1)
    side = following * tables[1] - preceding * tables[2]
    return pair * tables[0] + (side if back else -side)


def product(left, right, left_axis=1, right_axis=0):
    return lax.dot_general(
        left, right, (((left_axis,), (right_axis,)), ((), ())), preferred_element_type=jnp.float32
    )


def statistics(rows):
    average = jnp.mean(rows, axis=-1, keepdims=True)
    centered = rows - average
    variance = jnp.mean(centered * centered, axis=-1, keepdims=True)
    inverse = lax.rsqrt(variance + norm_epsilon)
    return centered * inverse, inverse


def low_lanes(width):
    return lax.broadcasted_iota(jnp.int32, (1, width), 1) < HEAD_DIM


def pair_lanes(index):
    return pl.ds(pl.multiple_of(index * 2 * HEAD_DIM, 2 * HEAD_DIM), 2 * HEAD_DIM)


def rows_at(index, step):
    return pl.ds(pl.multiple_of(index * step, step), step)


def attend(m, length, refs):
    (x, normed, qkv, attention, mixture, active, slope, total, result) = refs["state"]
    joint, output, expand, contract = refs["weights"]
    gain, offset, outer, inner = refs["vectors"]
    tables = refs["tables"]
    width = x.shape[2]

    def norm(i, carry):
        at = rows_at(i, ROW_STEP)
        standard, _ = statistics(x[m, at, :].astype(jnp.float32))
        normed[m, at, :] = (standard * gain[...] + offset[...]).astype(jnp.bfloat16)
        return carry

    lax.fori_loop(0, SLOT // ROW_STEP, norm, 0)
    for part in range(3):
        scale = HEAD_DIM**-0.5 if part == 0 else 1.0
        total[...] = product(normed[m], joint[:, part * width : (part + 1) * width])
        if part == 2:
            qkv[m, :, 2 * width :] = total[...].astype(jnp.bfloat16)
        else:

            def rotary(i, carry, part=part, scale=scale):
                pair = turn(total[:, pair_lanes(i)], tables, False)
                at = pair_lanes(i + part * (width // (2 * HEAD_DIM)))
                qkv[m, :, at] = pair.astype(jnp.bfloat16) * jnp.bfloat16(scale)
                return carry

            lax.fori_loop(0, width // (2 * HEAD_DIM), rotary, 0, unroll=8)

    key = lax.broadcasted_iota(jnp.int32, (SLOT, SLOT), 0)
    query = lax.broadcasted_iota(jnp.int32, (SLOT, SLOT), 1)
    allowed = (key <= query) & (key < length)
    pairs = width // (2 * HEAD_DIM)
    low = low_lanes(2 * HEAD_DIM)

    def heads(i, carry):
        queries, keys = qkv[m, :, pair_lanes(i)], qkv[m, :, pair_lanes(i + pairs)]
        values = qkv[m, :, pair_lanes(i + 2 * pairs)]
        mixed = []
        for half in range(2):
            own = jnp.where(low == (half == 0), queries, jnp.zeros_like(queries))
            scores = jnp.where(allowed, product(keys, own, 1, 1), masked_score)
            raised = jnp.exp(scores - jnp.max(scores, axis=0, keepdims=True))
            share = raised * (1.0 / jnp.sum(raised, axis=0, keepdims=True))
            share = share.astype(jnp.bfloat16)
            attention[m, 2 * i + half] = share
            mixed.append(product(share, values, 0, 0))
        mixture[m, :, pair_lanes(i)] = jnp.where(low, mixed[0], mixed[1]).astype(jnp.bfloat16)
        return carry

    lax.fori_loop(0, pairs, heads, 0, unroll=8)


def feed(m, refs):
    (x, normed, _, _, mixture, active, slope, total, result) = refs["state"]
    joint, output, expand, contract = refs["weights"]
    gain, offset, outer, inner = refs["vectors"]
    total[...] = x[m].astype(jnp.float32) + outer[...] + product(mixture[m], output[...])

    def hidden(i, carry):
        at = rows_at(i, FF_STEP)
        pre = product(normed[m], expand[:, at]) + inner[:, at]
        square = pre * pre
        bend = jnp.tanh(GELU_SCALE * (pre + GELU_CUBE * (square * pre)))
        lifted = 0.5 * (1.0 + bend)
        slant = (0.5 * GELU_SCALE) * (1.0 + (3.0 * GELU_CUBE) * square)
        slope[m, :, at] = (lifted + pre * (1.0 - bend * bend) * slant).astype(jnp.bfloat16)
        activated = (pre * lifted).astype(jnp.bfloat16)
        active[m, :, at] = activated
        total[...] += product(activated, contract[at, :])
        return carry

    lax.fori_loop(0, slope.shape[2] // FF_STEP, hidden, 0)
    result[m] = total[...].astype(jnp.bfloat16)


def backward_block(m, refs):
    (x, _, qkv, attention, _, _, slope, total, result) = refs["state"]
    joint, output, expand, contract = refs["weights"]
    gain, offset, outer, inner = refs["vectors"]
    upstream, mixture_grad = refs["gradients"]
    gain_sum, offset_sum, outer_sum, inner_sum = refs["sums"]
    tables = refs["tables"]
    width = x.shape[2]
    outer_sum[...] += jnp.sum(upstream[m].astype(jnp.float32), axis=0, keepdims=True)
    mixture_grad[...] = product(upstream[m], output[...], 1, 1).astype(jnp.bfloat16)
    total[...] = jnp.zeros_like(total)

    def hidden(i, carry):
        at = rows_at(i, FF_STEP)
        active_grad = product(upstream[m], contract[at, :], 1, 1)
        pre_grad = (active_grad * slope[m, :, at].astype(jnp.float32)).astype(jnp.bfloat16)
        slope[m, :, at] = pre_grad
        inner_sum[:, at] += jnp.sum(pre_grad.astype(jnp.float32), axis=0, keepdims=True)
        total[...] += product(pre_grad, expand[:, at], 1, 1)
        return carry

    lax.fori_loop(0, slope.shape[2] // FF_STEP, hidden, 0)
    pairs = width // (2 * HEAD_DIM)
    low = low_lanes(2 * HEAD_DIM)

    def heads(i, carry):
        queries, keys = qkv[m, :, pair_lanes(i)], qkv[m, :, pair_lanes(i + pairs)]
        values = qkv[m, :, pair_lanes(i + 2 * pairs)]
        mixed_grad = mixture_grad[:, pair_lanes(i)]
        query_grads, key_grads, value_grads = [], [], []
        for half in range(2):
            share = attention[m, 2 * i + half]
            own = jnp.where(low == (half == 0), mixed_grad, jnp.zeros_like(mixed_grad))
            value_grads.append(product(share, mixed_grad))
            share_grad = product(values, own, 1, 1)
            weight = share.astype(jnp.float32)
            weighted = weight * share_grad
            score_grad = weighted - weight * jnp.sum(weighted, axis=0, keepdims=True)
            score_grad = score_grad.astype(jnp.bfloat16)
            query_grads.append(product(score_grad, keys, 0, 0))
            key_grads.append(product(score_grad, queries))
        query_grad = jnp.where(low, query_grads[0], query_grads[1]) * HEAD_DIM**-0.5
        key_grad = jnp.where(low, key_grads[0], key_grads[1])
        value_grad = jnp.where(low, value_grads[0], value_grads[1])
        qkv[m, :, pair_lanes(i)] = turn(query_grad, tables, True).astype(jnp.bfloat16)
        qkv[m, :, pair_lanes(i + pairs)] = turn(key_grad, tables, True).astype(jnp.bfloat16)
        qkv[m, :, pair_lanes(i + 2 * pairs)] = value_grad.astype(jnp.bfloat16)
        return carry

    lax.fori_loop(0, pairs, heads, 0, unroll=8)

    def project(i, carry):
        at = rows_at(i, JOINT_STEP)
        total[:, at] += product(qkv[m], joint[at, :], 1, 1)
        return carry

    lax.fori_loop(0, width // JOINT_STEP, project, 0)

    def norm(i, carry):
        at = rows_at(i, ROW_STEP)
        standard, inverse = statistics(x[m, at, :].astype(jnp.float32))
        normed_grad = total[at, :]
        gain_sum[...] += jnp.sum(normed_grad * standard, axis=0, keepdims=True)
        offset_sum[...] += jnp.sum(normed_grad, axis=0, keepdims=True)
        scaled = normed_grad * gain[...]
        inner_mean = jnp.mean(scaled, axis=-1, keepdims=True)
        along = jnp.mean(scaled * standard, axis=-1, keepdims=True)
        change = inverse * (scaled - inner_mean - standard * along)
        result[m, at, :] = (upstream[m, at, :].astype(jnp.float32) + change).astype(jnp.bfloat16)
        return carry

    lax.fori_loop(0, SLOT // ROW_STEP, norm, 0)


def vector_rows(width):
    return max(1, width // LANES), max(1, LANES // width)


def lane_range(device, width):
    lane = lax.broadcasted_iota(jnp.int32, (1, LANES), 1)
    start = device * width % LANES
    return (lane >= start) & (lane < start + width)


def unpack_vectors(small, devices, vectors):
    width = vectors[0].shape[1] // devices
    wide = vectors[3].shape[1] // devices

    def gathered(index, shared):
        rows = small[pl.ds(pl.multiple_of(index * shared * SMALL_ROWS, SMALL_ROWS), SMALL_ROWS), :]
        total = rows.astype(jnp.float32)
        for other in range(1, shared):
            at = pl.multiple_of((index * shared + other) * SMALL_ROWS, SMALL_ROWS)
            total += small[pl.ds(at, SMALL_ROWS), :].astype(jnp.float32)
        return total

    _, shared = vector_rows(width)

    def narrow(index, carry):
        total = gathered(index, shared)
        at = rows_at(index, LANES)
        for i in range(3):
            vectors[i][:, at] = total[i : i + 1]
        return carry

    lax.fori_loop(0, devices // shared, narrow, 0)
    count, shared_wide = vector_rows(wide)

    def broad(index, carry):
        total = gathered(index, shared_wide)
        for i in range(count):
            vectors[3][:, rows_at(index * count + i, LANES)] = total[3 + i : 4 + i]
        return carry

    lax.fori_loop(0, devices // shared_wide, broad, 0)


def pack_sums(sums, devices, packed):
    width = sums[0].shape[1] // devices
    wide = sums[3].shape[1] // devices
    count, _ = vector_rows(wide)
    row = lax.broadcasted_iota(jnp.int32, (SMALL_ROWS, LANES), 0)

    def device(index, carry):
        rows = []
        inside = lane_range(index, width)
        for i in range(3):
            rows.append(jnp.where(inside, sums[i][:, rows_at(index * width // LANES, LANES)], 0.0))
        for i in range(count):
            line = sums[3][:, rows_at(index * wide // LANES + i, LANES)]
            rows.append(line if wide >= LANES else jnp.where(lane_range(index, wide), line, 0.0))
        block = jnp.zeros((SMALL_ROWS, LANES), jnp.float32)
        for i, line in enumerate(rows):
            block = jnp.where(row == i, line, block)
        packed[rows_at(index, SMALL_ROWS), :] = block.astype(jnp.bfloat16)
        return carry

    lax.fori_loop(0, devices, device, 0)


def blocks_kernel(pieces, *refs):
    lengths, hidden_in, cotangent, tables_in = refs[:4]
    sources = refs[4:9]
    hidden_out, input_grad = refs[9:11]
    factor_outs, packed = refs[11:17], refs[17]
    weights, small = refs[18:22], refs[22]
    x, normed, qkv, attention, mixture, active, slope, total, result = refs[23:32]
    upstream, mixture_grad, tables = refs[32:35]
    vectors, sums = refs[35:39], refs[39:43]
    table_sem, in_keep, in_send, in_receive, hand_send, hand_receive = refs[43:49]
    half_send, half_receive, half_keep, out_sem = refs[49:53]
    here = Place()
    section = lax.axis_index("section")
    partner = {"section": 1 - section}
    half = hidden_out.shape[1]
    devices = 4 * here.levels

    def keeping(source, target, start, m):
        return pltpu.make_async_copy(
            source.at[rows_at(m, SLOT), :], target.at[m, :, pl.ds(start, half)], in_keep.at[m]
        )

    def halving(source, target, start, m):
        return pltpu.make_async_remote_copy(
            source.at[rows_at(m, SLOT), :],
            target.at[m, :, pl.ds(start, half)],
            in_send.at[m],
            in_receive.at[m],
            device_id=partner,
            device_id_type=MESH,
        )

    def handing(target, m):
        return pltpu.make_async_remote_copy(
            result.at[m],
            target.at[m],
            hand_send.at[m],
            hand_receive.at[m],
            device_id=partner,
            device_id_type=MESH,
        )

    def away(target, start, m):
        return pltpu.make_async_remote_copy(
            result.at[m, :, pl.ds(start, half)],
            target.at[rows_at(m, SLOT), :],
            half_send.at[m],
            half_receive.at[m],
            device_id=partner,
            device_id_type=MESH,
        )

    def kept(target, start, m):
        return pltpu.make_async_copy(
            result.at[m, :, pl.ds(start, half)], target.at[rows_at(m, SLOT), :], half_keep.at[m]
        )

    def stored(m):
        return pltpu.make_async_copy(
            result.at[m], input_grad.at[rows_at(m, SLOT), :], half_keep.at[m]
        )

    def giving(i, source, m):
        return pltpu.make_async_copy(
            source.at[m], factor_outs[i].at[rows_at(m, SLOT), :], out_sem.at[i, m]
        )

    reading = pltpu.make_async_copy(tables_in, tables, table_sem.at[0])
    reading.start()
    for m in range(MICRO):
        pl.when(section == 0)(lambda m=m: keeping(hidden_in, x, 0, m).start())
        pl.when(section == 1)(lambda m=m: keeping(cotangent, upstream, half, m).start())
    for total_sum in sums:
        total_sum[...] = jnp.zeros_like(total_sum)
    greet(here, True)
    owns = [piece.of(sources[piece.array]) for piece in pieces]
    spread = Spread(here, pieces, owns, [*weights, small], refs[53:])
    early = [p for p, piece in enumerate(pieces) if piece.array in (0, 1, 4)]
    late = [p for p, piece in enumerate(pieces) if piece.array in (2, 3)]
    spread.begin_all(early)
    for m in range(MICRO):
        pl.when(section == 1)(lambda m=m: halving(hidden_in, x, half, m).start())
        pl.when(section == 0)(lambda m=m: halving(cotangent, upstream, 0, m).start())
    shared = {
        "state": (x, normed, qkv, attention, mixture, active, slope, total, result),
        "weights": weights,
        "vectors": vectors,
        "tables": tables,
        "gradients": (upstream, mixture_grad),
        "sums": sums,
    }
    spread.middle(early, lambda: spread.begin_all(late))
    spread.received(early)
    unpack_vectors(small, devices, vectors)
    reading.wait()

    @pl.when(section == 0)
    def _():
        def ahead(m, carry):
            keeping(hidden_in, x, 0, m).wait()
            halving(hidden_in, x, half, m).wait_recv()
            attend(m, lengths[m], shared)
            return carry

        lax.fori_loop(0, MICRO, ahead, 0)

    spread.middle(late)
    spread.received(late)

    def forward(m, carry):
        @pl.when(section == 1)
        def _():
            handing(x, m).wait_recv()
            attend(m, lengths[m], shared)

        feed(m, shared)

        @pl.when(section == 0)
        def _():
            pl.when(m > 0)(lambda: handing(x, m - 1).wait_send())
            handing(x, m).start()

        @pl.when(section == 1)
        def _():
            away(hidden_out, 0, m).start()
            kept(hidden_out, half, m).start()

        for i, source in enumerate((normed, mixture, active)):
            giving(i, source, m).start()
        return carry

    lax.fori_loop(0, MICRO, forward, 0)

    def backward(m, carry):
        @pl.when(section == 0)
        def _():
            pl.when(m == 0)(lambda: handing(x, MICRO - 1).wait_send())
            handing(upstream, m).wait_recv()

        @pl.when(section == 1)
        def _():
            away(hidden_out, 0, m).wait_send()
            kept(hidden_out, half, m).wait()
            keeping(cotangent, upstream, half, m).wait()
            halving(cotangent, upstream, 0, m).wait_recv()
            row = lax.broadcasted_iota(jnp.int32, (SLOT, 1), 0)
            inside = (row < lengths[m]).astype(jnp.float32)
            masked = upstream[m].astype(jnp.float32) * inside
            upstream[m] = masked.astype(jnp.bfloat16)

        backward_block(m, shared)

        @pl.when(section == 1)
        def _():
            handing(upstream, m).start()

        pl.when(section == 0)(lambda: stored(m).start())
        for i, source in enumerate((qkv, slope, upstream)):
            giving(3 + i, source, m).start()
        return carry

    lax.fori_loop(0, MICRO, backward, 0)
    pack_sums(sums, devices, packed)

    def last(m, carry):
        @pl.when(section == 0)
        def _():
            halving(cotangent, upstream, 0, m).wait_send()
            stored(m).wait()
            away(hidden_out, 0, m).wait_recv()

        @pl.when(section == 1)
        def _():
            halving(hidden_in, x, half, m).wait_send()
            handing(upstream, m).wait_send()

        for i, source in enumerate((normed, mixture, active, qkv, slope, upstream)):
            giving(i, source, m).wait()
        return carry

    lax.fori_loop(0, MICRO, last, 0)
    spread.sent()


def run_blocks(lengths, hidden_in, cotangent, owns, number):
    levels = lax.axis_size("batch") // 4
    devices = 4 * levels
    tokens, half = hidden_in.shape
    width = half * lax.axis_size("section")
    wide = owns[2].shape[1]
    low, full = jnp.bfloat16, jnp.float32
    shape = jax.ShapeDtypeStruct
    vmem = pltpu.VMEM
    dma = pltpu.SemaphoreType.DMA
    pieces = pieces_of([own.shape for own in owns])
    outputs = [shape((tokens, half), low), shape((tokens, width), low)]
    outputs += [shape((tokens, n), low) for n in (width, width, wide, 3 * width, wide, width)]
    outputs += [shape((devices * SMALL_ROWS, LANES), low)]
    scratch = [vmem((devices * own.shape[0], own.shape[1]), low) for own in owns]
    scratch += [
        vmem((MICRO, SLOT, width), low),
        vmem((MICRO, SLOT, width), low),
        vmem((MICRO, SLOT, 3 * width), low),
        vmem((MICRO, HEADS, SLOT, SLOT), low),
        vmem((MICRO, SLOT, width), low),
        vmem((MICRO, SLOT, wide), low),
        vmem((MICRO, SLOT, wide), low),
        vmem((SLOT, width), full),
        vmem((MICRO, SLOT, width), low),
        vmem((MICRO, SLOT, width), low),
        vmem((SLOT, width), low),
        vmem((3, SLOT, 2 * HEAD_DIM), full),
    ]
    scratch += [vmem((1, n), full) for n in (width, width, width, wide)] * 2
    scratch += [dma((1,))] + [dma((MICRO,))] * 8 + [dma((6, MICRO))]
    scratch += spread_semaphores(len(pieces), levels)
    return pl.pallas_call(
        partial(blocks_kernel, pieces),
        out_shape=outputs,
        in_specs=[pl.BlockSpec(memory_space=pltpu.SMEM)] + [ANY] * 8,
        out_specs=[ANY] * 8 + [pl.BlockSpec(memory_space=vmem)],
        scratch_shapes=scratch,
        compiler_params=pltpu.CompilerParams(
            collective_id=number, has_side_effects=True, vmem_limit_bytes=60 * 2**20
        ),
        name="two_blocks",
    )(lengths, hidden_in, cotangent, jnp.asarray(rotary_rows()), *owns)


def pack_vectors(vectors):
    device = lax.axis_index("batch")
    size = SMALL_ROWS * LANES
    total = jnp.zeros((1, size), jnp.bfloat16)
    row = 0
    for vector in vectors:
        width = vector.shape[1]
        used = min(width, LANES)
        slot = device * width % LANES // used
        for i in range(LANES // used):
            start = row * LANES + i * used
            moved = jnp.pad(vector, ((0, 0), (start, size - start - width)))
            total = total + jnp.where(slot == i, moved, jnp.zeros_like(moved))
        row += max(1, width // LANES)
    return total.reshape(SMALL_ROWS, LANES)


def widen_kernel(devices, *refs):
    small, sources = refs[0], refs[1 : (len(refs) - 5) // 2 + 1]
    targets, vectors = refs[len(sources) + 1 : -4], refs[-4:]
    pl.when(pl.program_id(0) == 0)(lambda: unpack_vectors(small, devices, vectors))
    for source, target in zip(sources, targets):
        target[...] = source[...].astype(target.dtype).reshape(target.shape)


def widen(small, sums, kept, widths, devices):
    steps = 8
    arrays = [*sums, *kept]
    whole = lambda i: (0, 0)
    in_specs = [
        pl.BlockSpec((array.shape[0] // steps, array.shape[1]), lambda i: (i, 0))
        for array in arrays
    ]
    out_specs = [
        pl.BlockSpec((1, array.shape[0] // steps, array.shape[1]), lambda i: (0, i, 0))
        for array in sums
    ] + in_specs[len(sums) :]
    out_specs += [pl.BlockSpec((1, width), whole) for width in widths]
    shapes = [jax.ShapeDtypeStruct((1, *array.shape), jnp.float32) for array in sums]
    shapes += [jax.ShapeDtypeStruct(array.shape, array.dtype) for array in kept]
    shapes += [jax.ShapeDtypeStruct((1, width), jnp.float32) for width in widths]
    return pl.pallas_call(
        partial(widen_kernel, devices),
        out_shape=shapes,
        grid=(steps,),
        in_specs=[pl.BlockSpec(small.shape, whole)] + in_specs,
        out_specs=out_specs,
        compiler_params=pltpu.CompilerParams(vmem_limit_bytes=60 * 2**20),
        name="widen",
    )(small, *arrays)


def local(
    hidden_in,
    cotangent,
    lengths,
    norm_gain,
    norm_offset,
    joint_weight,
    output_weight,
    expand_weight,
    inner_bias,
    contract_weight,
    outer_bias,
):
    devices = lax.axis_size("batch")
    owns = [
        joint_weight[0],
        output_weight[0],
        expand_weight[0],
        contract_weight[0],
        pack_vectors((norm_gain, norm_offset, outer_bias, inner_bias)),
    ]
    results = run_blocks(lengths, hidden_in, cotangent, owns, 1)
    shapes = [(own.shape[0] * devices, own.shape[1]) for own in owns[:4]]
    *sums, small_sum, own_grad = reduce_all(results[2:8], results[8], results[1], shapes, 2)
    width, wide = norm_gain.shape[1] * devices, inner_bias.shape[1] * devices
    (
        joint_sum,
        output_sum,
        expand_sum,
        contract_sum,
        hidden_out,
        input_grad,
        gain_sum,
        offset_sum,
        outer_sum,
        inner_sum,
    ) = widen(small_sum, sums, [results[0], own_grad], (width, width, width, wide), devices)
    return (
        hidden_out,
        input_grad,
        gain_sum,
        offset_sum,
        joint_sum,
        output_sum,
        expand_sum,
        inner_sum,
        contract_sum,
        outer_sum,
    )


def solution(mesh):
    return jax.shard_map(
        local,
        mesh=mesh,
        in_specs=(
            P("batch", "section"),
            P("batch", "section"),
            P("batch"),
            P("section", "batch"),
            P("section", "batch"),
            P("section", "batch", None),
            P("section", "batch", None),
            P("section", "batch", None),
            P("section", "batch"),
            P("section", "batch", None),
            P("section", "batch"),
        ),
        out_specs=(
            P("batch", "section"),
            P("batch", "section"),
            P("section", None),
            P("section", None),
            P("section", None, None),
            P("section", None, None),
            P("section", None, None),
            P("section", None),
            P("section", None, None),
            P("section", None),
        ),
        check_vma=False,
    )
```

```python
from functools import partial

import jax
import jax.numpy as jnp
import numpy as np
from jax import lax
from jax.experimental import pallas as pl
from jax.experimental.pallas import tpu as pltpu
from jax.sharding import PartitionSpec as P

HEADS = 16
HEAD_DIM = 64
ROT = 32
SLOT = 256
MICRO = 2
SMALL_ROWS = 16
LANES = 128
ROW_STEP = 256
FF_STEP = 4096
JOINT_STEP = 1024
GELU_SCALE = (2.0 / np.pi) ** 0.5
GELU_CUBE = 0.044715
norm_epsilon = 1e-05
rotary_base = 10000.0
masked_score = -1e30
MESH = pl.DeviceIdType.MESH
ANY = pl.BlockSpec(memory_space=pl.ANY)


class Place:
    def __init__(self):
        index = lax.axis_index("batch")
        self.levels = lax.axis_size("batch") // 4
        self.last = self.levels - 1
        self.z, self.y, self.c = index // 4, index // 2 % 2, index % 2

    def at(self, z=None, y=None, c=None):
        z = self.z if z is None else z
        y = self.y if y is None else y
        c = self.c if c is None else c
        return z * 4 + y * 2 + c


class Piece:
    def __init__(self, array, offset, rows, column, columns, direct):
        self.array, self.offset, self.rows = array, offset, rows
        self.column, self.columns, self.direct = column, columns, direct

    def sides(self, y):
        return (y,) if self.direct else (y, 1 - y)

    def of(self, block):
        return block.at[pl.ds(self.offset, self.rows), pl.ds(self.column, self.columns)]


def pieces_of(blocks):
    joint, output, expand, contract, small = blocks
    cut = contract[0] // 4
    pieces = [
        Piece(1, 0, output[0], 0, output[1], False),
        Piece(3, 0, cut, 0, contract[1], False),
    ]
    for array, offset, (rows, columns), parts in (
        (0, 0, joint, 1),
        (2, 0, expand, 1),
        (3, cut, contract, 1),
        (4, 0, small, 1),
    ):
        for i in range(parts):
            width = columns // parts
            pieces.append(Piece(array, offset, rows - offset, i * width, width, True))
    return pieces


def remote(source, target, send, receive, index):
    return pltpu.make_async_remote_copy(
        source, target, send, receive, device_id={"batch": index}, device_id_type=MESH
    )


def greet(here, with_section):
    barrier = pltpu.get_barrier_semaphore()

    def signal(**who):
        pl.semaphore_signal(barrier, inc=1, device_id=who, device_id_type=MESH)

    signal(batch=here.at(y=1 - here.y))
    signal(batch=here.at(c=1 - here.c))
    pl.when(here.z > 0)(lambda: signal(batch=here.at(z=here.z - 1)))
    pl.when(here.z < here.last)(lambda: signal(batch=here.at(z=here.z + 1)))
    waits = 2
    if with_section:
        signal(section=1 - lax.axis_index("section"))
        waits = 3
    below = jnp.minimum(here.z, 1)
    above = jnp.minimum(here.last - here.z, 1)
    pl.semaphore_wait(barrier, waits + below + above)


def spread_semaphores(count, levels):
    dma = pltpu.SemaphoreType.DMA
    return [
        dma((count,)),
        dma((count, levels, 2, 2)),
        dma((count, levels, 2)),
        dma((count, levels)),
        dma((count, levels)),
        dma((count, levels, 2)),
        dma((count, levels, 2)),
    ]


class Spread:
    def __init__(self, here, pieces, owns, outs, semaphores):
        self.here, self.pieces, self.owns, self.outs = here, pieces, owns, outs
        (self.keep, self.zs, self.zr, self.ys, self.yr, self.cs, self.cr) = semaphores

    def block(self, p, z, y, c):
        piece = self.pieces[p]
        out = self.outs[piece.array]
        rows = out.shape[0] // (4 * self.here.levels)
        start = (z * 4 + y * 2 + c) * rows + piece.offset
        return out.at[
            pl.ds(pl.multiple_of(start, 8), piece.rows), pl.ds(piece.column, piece.columns)
        ]

    def along(self, p, z, y, source, way):
        here = self.here
        if way == 0:
            target = jnp.minimum(here.z + 1, here.last)
        else:
            target = jnp.maximum(here.z - 1, 0)
        return remote(
            source,
            self.block(p, z, y, here.c),
            self.zs.at[p, z, y, way],
            self.zr.at[p, z, y],
            here.at(z=target),
        )

    def across(self, p, z, source):
        here = self.here
        target = self.block(p, z, here.y, here.c)
        return remote(source, target, self.ys.at[p, z], self.yr.at[p, z], here.at(y=1 - here.y))

    def beside(self, p, z, y, source):
        here = self.here
        target = self.block(p, z, y, here.c)
        return remote(
            source, target, self.cs.at[p, z, y], self.cr.at[p, z, y], here.at(c=1 - here.c)
        )

    def both_ways(self, p, y, source):
        here = self.here
        pl.when(here.z < here.last)(lambda: self.along(p, here.z, y, source, 0).start())
        pl.when(here.z > 0)(lambda: self.along(p, here.z, y, source, 1).start())

    def begin(self, p, held=False):
        here, own = self.here, self.owns[p]
        self.across(p, here.z, own).start()
        if not held:
            self.both_ways(p, here.y, own)
        self.beside(p, here.z, here.y, own).start()
        target = self.block(p, here.z, here.y, here.c)
        pltpu.make_async_copy(own, target, self.keep.at[p]).start()

    def begin_all(self, chosen):
        order = sorted(chosen, key=lambda p: self.pieces[p].direct)
        for p in order:
            self.begin(p, held=not self.pieces[p].direct)
        for p in order:
            if not self.pieces[p].direct:
                self.both_ways(p, self.here.y, self.owns[p])

    def from_z(self, p, z, y, way):
        here = self.here
        block = self.block(p, z, y, here.c)
        self.along(p, z, y, block, way).wait_recv()
        more = here.z < here.last if way == 0 else here.z > 0
        pl.when(more)(lambda: self.along(p, z, y, block, way).start())
        if self.pieces[p].direct:
            self.across(p, z, block).start()
        self.beside(p, z, y, block).start()

    def from_y(self, p, z):
        here = self.here
        block = self.block(p, z, 1 - here.y, here.c)
        self.across(p, z, block).wait_recv()
        if not self.pieces[p].direct:
            self.both_ways(p, 1 - here.y, block)
        self.beside(p, z, 1 - here.y, block).start()

    def z_events(self, chosen, distance):
        here = self.here

        def pair(p, side):
            y = self.pieces[p].sides(here.y)[side]
            pl.when(here.z - distance >= 0)(lambda: self.from_z(p, here.z - distance, y, 0))
            pl.when(here.z + distance <= here.last)(
                lambda: self.from_z(p, here.z + distance, y, 1)
            )

        for p in chosen:
            if self.pieces[p].direct:
                pair(p, 0)
        for side in range(2):
            for p in chosen:
                if not self.pieces[p].direct:
                    pair(p, side)

    def y_events(self, chosen, z):
        for p in chosen:
            if self.pieces[p].direct:
                self.from_y(p, z)

    def middle(self, chosen, then=None):
        here = self.here
        for p in chosen:
            if not self.pieces[p].direct:
                self.from_y(p, here.z)

        def y_pair(distance):
            pl.when(here.z - distance >= 0)(lambda: self.y_events(chosen, here.z - distance))
            pl.when((here.z + distance <= here.last) & (distance > 0))(
                lambda: self.y_events(chosen, here.z + distance)
            )

        def step(distance, carry):
            self.z_events(chosen, distance)
            y_pair(distance - 1)
            return carry

        lax.fori_loop(1, here.levels, step, 0)
        if then is not None:
            then()
        y_pair(here.last)

    def received(self, chosen):
        here = self.here

        def level(z, carry):
            for p in chosen:
                own = self.block(p, z, here.y, here.c)
                for y in range(2):
                    self.beside(p, z, y, own).wait_recv()
            return carry

        lax.fori_loop(0, here.levels, level, 0)
        for p in chosen:
            block = self.block(p, here.z, here.y, here.c)
            pltpu.make_async_copy(block, block, self.keep.at[p]).wait()

    def sent(self):
        here = self.here

        def level(z, carry):
            for p, piece in enumerate(self.pieces):
                own = self.block(p, z, here.y, here.c)
                for y in range(2):
                    self.beside(p, z, y, own).wait_send()
                crossed = z >= 0 if piece.direct else z == here.z
                pl.when(crossed)(lambda p=p, own=own: self.across(p, z, own).wait_send())
                for y in piece.sides(here.y):
                    pl.when((z <= here.z) & (here.z < here.last))(
                        lambda p=p, y=y, own=own: self.along(p, z, y, own, 0).wait_send()
                    )
                    pl.when((z >= here.z) & (here.z > 0))(
                        lambda p=p, y=y, own=own: self.along(p, z, y, own, 1).wait_send()
                    )
            return carry

        lax.fori_loop(0, here.levels, level, 0)


def add_rows(target, other):
    rows = target.shape[0]
    step = min(rows, 16)

    def body(i, carry):
        at = pl.ds(pl.multiple_of(i * step, step), step)
        total = target[at, :].astype(jnp.float32) + other[at, :].astype(jnp.float32)
        target[at, :] = total.astype(target.dtype)
        return carry

    lax.fori_loop(0, rows // step, body, 0)


FACTORS = ((0, 3), (1, 5), (0, 4), (2, 5))
MAKE_ORDER = (3, 1, 2, 0, 4)
COLUMN_STEP = 1024


class Reduce:
    def __init__(self, here, pieces, factors, small, product_rows, buffers, semaphores):
        self.here, self.pieces, self.factors, self.small = here, pieces, factors, small
        self.made = product_rows
        self.mine, self.sent, self.sib, self.yb, self.zb = buffers
        (self.load, self.cs, self.cr, self.ys, self.yr, self.zs, self.zr, self.credit) = semaphores

    def level(self, i):
        here = self.here
        above, below = here.last - here.z, here.z
        lead = jnp.maximum(above, below) - jnp.minimum(above, below)
        single = jnp.where(above > below, here.last - i, i)
        later = i - lead
        distance = jnp.minimum(above, below) - later // 2
        outer = jnp.where(above > below, here.z - distance, here.z + distance)
        paired = jnp.where(later % 2 == 0, outer, 2 * here.z - outer)
        return jnp.where(i < lead, single, paired)

    def to_core(self, p, slot, y):
        here = self.here
        return remote(
            self.sent[p].at[slot, y],
            self.sib[p].at[slot, y],
            self.cs.at[p, slot, y],
            self.cr.at[p, slot, y],
            here.at(c=1 - here.c),
        )

    def to_y(self, p, z):
        here = self.here
        return remote(
            self.mine[p].at[z, 1 - here.y],
            self.yb[p].at[z if self.pieces[p].direct else 0],
            self.ys.at[p, z],
            self.yr.at[p, z],
            here.at(y=1 - here.y),
        )

    def slot(self, z, at_z, way):
        if way == 0:
            return z
        return jnp.where(z == at_z, self.here.levels, z)

    def to_z(self, p, z, y, way):
        here = self.here
        step = 1 if way == 0 else -1
        slot = self.slot(z, here.z + step, way)
        side = 0 if self.pieces[p].direct else y
        return remote(
            self.mine[p].at[z, y],
            self.zb[p].at[slot, side],
            self.zs.at[p, z, side],
            self.zr.at[p, slot, side],
            here.at(z=here.z + step),
        )

    def arrive(self, p, z, y, way):
        here = self.here
        slot = self.slot(z, here.z, way)
        side = 0 if self.pieces[p].direct else y
        block = self.zb[p].at[slot, side]
        remote(
            block, block, self.zs.at[p, z, side], self.zr.at[p, slot, side], here.at(y=1 - here.y)
        ).wait_recv()
        add_rows(self.mine[p].at[z, y], block)

    def store(self, array, z, slot, y, own, value, column):
        for p, piece in enumerate(self.pieces):
            first = max(column, piece.column)
            end = min(column + value.shape[1], piece.column + piece.columns)
            if piece.array == array and first < end:
                target = self.mine[p].at[z, y] if own else self.sent[p].at[slot, y]
                part = value[piece.offset : piece.offset + piece.rows, first - column : end - column]
                target[:, first - piece.column : end - piece.column] = part.astype(jnp.bfloat16)

    def make(self, array, z, slot):
        here = self.here
        rows = max(p.offset + p.rows for p in self.pieces if p.array == array)
        cores = ((False, 1 - here.c), (True, here.c))
        if array == 4:
            for own, c in cores:
                for y in range(2):
                    at = pl.multiple_of((z * 4 + y * 2 + c) * rows, 16)
                    self.store(array, z, slot, y, own, self.small[pl.ds(at, rows), :], 0)
            return
        left, right = (self.factors[i] for i in FACTORS[array])
        columns = right.shape[1]
        tiles = range(0, columns, COLUMN_STEP)
        if rows % 128 == 0:
            for own, c in cores:
                for y in range(2):
                    at = pl.multiple_of((z * 4 + y * 2 + c) * rows, 128)
                    turned = left[:, pl.ds(at, rows)].T
                    for tile in tiles:
                        value = product(turned, right[:, tile : tile + COLUMN_STEP])
                        self.store(array, z, slot, y, own, value, tile)
            return
        span = max(4 * rows, 128)
        start = z * 4 * rows // span * span
        turned = left[:, pl.ds(pl.multiple_of(start, 128), span)].T
        for tile in tiles:
            self.made[:span, :] = product(turned, right[:, tile : tile + COLUMN_STEP])
            for own, c in cores:
                for y in range(2):
                    at = pl.multiple_of((z * 4 + y * 2 + c) * rows - start, 8)
                    self.store(array, z, slot, y, own, self.made[pl.ds(at, rows), :], tile)

    def of(self, array):
        return [p for p, piece in enumerate(self.pieces) if piece.array == array]

    def build(self, i, waits):
        here = self.here
        z, slot = self.level(i), i % 2

        @pl.when(i >= 2)
        def _():
            for p in range(len(self.pieces)):
                for y in range(2):
                    self.to_core(p, slot, y).wait_send()
            pl.semaphore_wait(self.credit, 1)

        def add(array):
            for p in self.of(array):
                for y in range(2):
                    self.to_core(p, slot, y).wait_recv()
                    add_rows(self.mine[p].at[z, y], self.sib[p].at[slot, y])
                if self.pieces[p].direct:
                    self.to_y(p, z).start()
                else:
                    self.pass_on(z, [p])

        for step, array in enumerate(MAKE_ORDER):
            waits(i, array)
            self.make(array, z, slot)
            for p in self.of(array):
                for y in range(2):
                    self.to_core(p, slot, y).start()
            if step > 0:
                add(MAKE_ORDER[step - 1])
        add(MAKE_ORDER[-1])

        @pl.when(i < here.levels - 2)
        def _():
            other = {"batch": here.at(c=1 - here.c)}
            pl.semaphore_signal(self.credit, inc=1, device_id=other, device_id_type=MESH)

    def rows(self, p, z):
        self.to_y(p, z).wait_recv()
        source = self.yb[p].at[z if self.pieces[p].direct else 0]
        add_rows(self.mine[p].at[z, self.here.y], source)

    def pass_on(self, z, chosen):
        here = self.here

        def hop(way):
            further = here.z > 0 if way == 0 else here.z < here.last
            for p in chosen:
                if self.pieces[p].direct:
                    self.rows(p, z)
                for y in self.pieces[p].sides(here.y):
                    pl.when(further)(lambda p=p, y=y: self.arrive(p, z, y, way))
                    self.to_z(p, z, y, way).start()

        pl.when(z > here.z)(lambda: hop(0))
        pl.when(z < here.z)(lambda: hop(1))

    def run(self, waits):
        here = self.here
        made = [p for array in MAKE_ORDER for p in self.of(array)]
        direct = [p for p in made if self.pieces[p].direct]

        def step(i, carry):
            self.build(i, waits)
            pl.when(i > 0)(lambda: self.pass_on(self.level(i - 1), direct))
            return carry

        lax.fori_loop(0, here.levels, step, 0)

    def settle(self, p):
        here = self.here
        for y in self.pieces[p].sides(here.y):
            pl.when(here.z > 0)(lambda y=y: self.arrive(p, here.z, y, 0))
            pl.when(here.z < here.last)(lambda y=y: self.arrive(p, here.z, y, 1))

    def finish(self):
        here = self.here
        for slot in range(min(2, here.levels)):
            for p in range(len(self.pieces)):
                for y in range(2):
                    self.to_core(p, slot, y).wait_send()

        def level(z, carry):
            for p, piece in enumerate(self.pieces):
                crossed = z >= 0 if piece.direct else z == here.z
                pl.when(crossed)(lambda p=p: self.to_y(p, z).wait_send())
                for y in piece.sides(here.y):
                    pl.when(z > here.z)(lambda p=p, y=y: self.to_z(p, z, y, 0).wait_send())
                    pl.when(z < here.z)(lambda p=p, y=y: self.to_z(p, z, y, 1).wait_send())
            return carry

        lax.fori_loop(0, here.levels, level, 0)


def reduce_kernel(pieces, *refs):
    count = len(pieces)
    sources, change, outs, input_grad, rest = refs[:7], refs[7], refs[8:13], refs[13], refs[14:]
    factors, small, made = rest[:6], rest[6], rest[7]
    rest = rest[8:]
    buffers = [rest[i * count : (i + 1) * count] for i in range(5)]
    rest = rest[5 * count :]
    here = Place()
    loads = [
        pltpu.make_async_copy(source, target, rest[0].at[i])
        for i, (source, target) in enumerate(zip(sources, [*factors, small]))
    ]
    order = (2, 5, 1, 0, 4, 3, 6)
    for i in order:
        loads[i].start()
    greet(here, True)
    section = lax.axis_index("section")
    half = input_grad.shape[1]
    over = pltpu.make_async_remote_copy(
        change.at[:, pl.ds(half, half)],
        input_grad,
        rest[-1].at[0],
        rest[-1].at[1],
        device_id={"section": 1 - section},
        device_id_type=MESH,
    )
    keep = pltpu.make_async_copy(change.at[:, pl.ds(0, half)], input_grad, rest[-1].at[2])

    @pl.when(section == 0)
    def _():
        over.start()
        keep.start()

    reduce = Reduce(here, pieces, factors, small, made, buffers, rest[:8])
    needs = {3: (2, 5), 1: (1,), 2: (0, 4), 0: (3,), 4: (6,)}

    def waits(i, array):
        @pl.when(i == 0)
        def _():
            for k in needs[array]:
                loads[k].wait()

    reduce.run(waits)
    owns = [buffers[0][p].at[here.z, here.y] for p in range(count)]
    spread = Spread(here, pieces, owns, outs, rest[8:-1])
    turned = [p for p in range(count) if not pieces[p].direct]
    for p in turned:
        reduce.settle(p)
        reduce.to_y(p, here.z).start()
    for p in range(count):
        if pieces[p].direct:
            reduce.rows(p, here.z)
            reduce.settle(p)
            spread.begin(p)
    for p in turned:
        reduce.rows(p, here.z)
        spread.begin(p)
    spread.middle(range(count))
    reduce.finish()
    spread.received(range(count))
    spread.sent()

    @pl.when(section == 0)
    def _():
        over.wait_send()
        keep.wait()

    pl.when(section == 1)(over.wait_recv)


def reduce_all(factors, small, change, shapes, number):
    levels = lax.axis_size("batch") // 4
    shapes = [*shapes, small.shape]
    pieces = pieces_of([(rows // (4 * levels), columns) for rows, columns in shapes])
    count = len(pieces)
    dma = pltpu.SemaphoreType.DMA
    low = jnp.bfloat16
    scratch = [pltpu.VMEM(factor.shape, low) for factor in factors]
    scratch += [pltpu.VMEM(small.shape, low), pltpu.VMEM((256, COLUMN_STEP), jnp.float32)]
    blocks = [(piece.rows, piece.columns) for piece in pieces]
    scratch += [pltpu.VMEM((levels, 2) + block, low) for block in blocks]
    scratch += [pltpu.VMEM((2, 2) + block, low) for block in blocks] * 2
    scratch += [
        pltpu.VMEM((levels if piece.direct else 1,) + block, low)
        for piece, block in zip(pieces, blocks)
    ]
    scratch += [
        pltpu.VMEM((levels + 1, 1 if piece.direct else 2) + block, low)
        for piece, block in zip(pieces, blocks)
    ]
    scratch += [
        dma((7,)),
        dma((count, 2, 2)),
        dma((count, 2, 2)),
        dma((count, levels)),
        dma((count, levels)),
        dma((count, levels, 2)),
        dma((count, levels + 1, 2)),
        pltpu.SemaphoreType.REGULAR,
    ]
    scratch += spread_semaphores(count, levels) + [dma((3,))]
    results = [*shapes, (change.shape[0], change.shape[1] // 2)]
    return pl.pallas_call(
        partial(reduce_kernel, pieces),
        out_shape=[jax.ShapeDtypeStruct(shape, low) for shape in results],
        in_specs=[ANY] * 8,
        out_specs=[ANY] * 6,
        scratch_shapes=scratch,
        compiler_params=pltpu.CompilerParams(
            collective_id=number, has_side_effects=True, vmem_limit_bytes=60 * 2**20
        ),
        name="reduce_gradients",
    )(*factors, small, change)


def rotary_rows():
    positions = np.arange(SLOT, dtype=np.float64)[:, None]
    lane = np.arange(2 * HEAD_DIM)[None, :] % HEAD_DIM
    angles = positions * rotary_base ** (-(lane // 2 * 2.0) / ROT)
    turned = lane < ROT
    cosine = np.where(turned, np.cos(angles), 1.0)
    sine = np.where(turned, np.sin(angles), 0.0)
    even = np.where(lane % 2 == 0, sine, 0.0)
    odd = np.where(lane % 2 == 1, sine, 0.0)
    return np.stack([cosine, even, odd]).astype(np.float32)


def turn(pair, tables, back):
    lanes = pair.shape[1]
    following = pltpu.roll(pair, lanes - 1, 1)
    preceding = pltpu.roll(pair, 1, 1)
    side = following * tables[1] - preceding * tables[2]
    return pair * tables[0] + (side if back else -side)


def product(left, right, left_axis=1, right_axis=0):
    return lax.dot_general(
        left, right, (((left_axis,), (right_axis,)), ((), ())), preferred_element_type=jnp.float32
    )


def statistics(rows):
    average = jnp.mean(rows, axis=-1, keepdims=True)
    centered = rows - average
    variance = jnp.mean(centered * centered, axis=-1, keepdims=True)
    inverse = lax.rsqrt(variance + norm_epsilon)
    return centered * inverse, inverse


def low_lanes(width):
    return lax.broadcasted_iota(jnp.int32, (1, width), 1) < HEAD_DIM


def pair_lanes(index):
    return pl.ds(pl.multiple_of(index * 2 * HEAD_DIM, 2 * HEAD_DIM), 2 * HEAD_DIM)


def rows_at(index, step):
    return pl.ds(pl.multiple_of(index * step, step), step)


def attend(m, length, refs):
    (x, normed, qkv, attention, mixture, active, slope, total, result) = refs["state"]
    joint, output, expand, contract = refs["weights"]
    gain, offset, outer, inner = refs["vectors"]
    tables = refs["tables"]
    width = x.shape[2]

    def norm(i, carry):
        at = rows_at(i, ROW_STEP)
        standard, _ = statistics(x[m, at, :].astype(jnp.float32))
        normed[m, at, :] = (standard * gain[...] + offset[...]).astype(jnp.bfloat16)
        return carry

    lax.fori_loop(0, SLOT // ROW_STEP, norm, 0)
    for part in range(3):
        scale = HEAD_DIM**-0.5 if part == 0 else 1.0
        total[...] = product(normed[m], joint[:, part * width : (part + 1) * width])
        if part == 2:
            qkv[m, :, 2 * width :] = total[...].astype(jnp.bfloat16)
        else:

            def rotary(i, carry, part=part, scale=scale):
                pair = turn(total[:, pair_lanes(i)], tables, False)
                at = pair_lanes(i + part * (width // (2 * HEAD_DIM)))
                qkv[m, :, at] = pair.astype(jnp.bfloat16) * jnp.bfloat16(scale)
                return carry

            lax.fori_loop(0, width // (2 * HEAD_DIM), rotary, 0, unroll=8)

    key = lax.broadcasted_iota(jnp.int32, (SLOT, SLOT), 0)
    query = lax.broadcasted_iota(jnp.int32, (SLOT, SLOT), 1)
    allowed = (key <= query) & (key < length)
    pairs = width // (2 * HEAD_DIM)
    low = low_lanes(2 * HEAD_DIM)

    def heads(i, carry):
        queries, keys = qkv[m, :, pair_lanes(i)], qkv[m, :, pair_lanes(i + pairs)]
        values = qkv[m, :, pair_lanes(i + 2 * pairs)]
        mixed = []
        for half in range(2):
            own = jnp.where(low == (half == 0), queries, jnp.zeros_like(queries))
            scores = jnp.where(allowed, product(keys, own, 1, 1), masked_score)
            raised = jnp.exp(scores - jnp.max(scores, axis=0, keepdims=True))
            share = raised * (1.0 / jnp.sum(raised, axis=0, keepdims=True))
            share = share.astype(jnp.bfloat16)
            attention[m, 2 * i + half] = share
            mixed.append(product(share, values, 0, 0))
        mixture[m, :, pair_lanes(i)] = jnp.where(low, mixed[0], mixed[1]).astype(jnp.bfloat16)
        return carry

    lax.fori_loop(0, pairs, heads, 0, unroll=8)


def feed(m, refs):
    (x, normed, _, _, mixture, active, slope, total, result) = refs["state"]
    joint, output, expand, contract = refs["weights"]
    gain, offset, outer, inner = refs["vectors"]
    total[...] = x[m].astype(jnp.float32) + outer[...] + product(mixture[m], output[...])

    def hidden(i, carry):
        at = rows_at(i, FF_STEP)
        pre = product(normed[m], expand[:, at]) + inner[:, at]
        square = pre * pre
        bend = jnp.tanh(GELU_SCALE * (pre + GELU_CUBE * (square * pre)))
        lifted = 0.5 * (1.0 + bend)
        slant = (0.5 * GELU_SCALE) * (1.0 + (3.0 * GELU_CUBE) * square)
        slope[m, :, at] = (lifted + pre * (1.0 - bend * bend) * slant).astype(jnp.bfloat16)
        activated = (pre * lifted).astype(jnp.bfloat16)
        active[m, :, at] = activated
        total[...] += product(activated, contract[at, :])
        return carry

    lax.fori_loop(0, slope.shape[2] // FF_STEP, hidden, 0)
    result[m] = total[...].astype(jnp.bfloat16)


def backward_block(m, refs):
    (x, _, qkv, attention, _, _, slope, total, result) = refs["state"]
    joint, output, expand, contract = refs["weights"]
    gain, offset, outer, inner = refs["vectors"]
    upstream, mixture_grad = refs["gradients"]
    gain_sum, offset_sum, outer_sum, inner_sum = refs["sums"]
    tables = refs["tables"]
    width = x.shape[2]
    outer_sum[...] += jnp.sum(upstream[m].astype(jnp.float32), axis=0, keepdims=True)
    mixture_grad[...] = product(upstream[m], output[...], 1, 1).astype(jnp.bfloat16)
    total[...] = jnp.zeros_like(total)

    def hidden(i, carry):
        at = rows_at(i, FF_STEP)
        active_grad = product(upstream[m], contract[at, :], 1, 1)
        pre_grad = (active_grad * slope[m, :, at].astype(jnp.float32)).astype(jnp.bfloat16)
        slope[m, :, at] = pre_grad
        inner_sum[:, at] += jnp.sum(pre_grad.astype(jnp.float32), axis=0, keepdims=True)
        total[...] += product(pre_grad, expand[:, at], 1, 1)
        return carry

    lax.fori_loop(0, slope.shape[2] // FF_STEP, hidden, 0)
    pairs = width // (2 * HEAD_DIM)
    low = low_lanes(2 * HEAD_DIM)

    def heads(i, carry):
        queries, keys = qkv[m, :, pair_lanes(i)], qkv[m, :, pair_lanes(i + pairs)]
        values = qkv[m, :, pair_lanes(i + 2 * pairs)]
        mixed_grad = mixture_grad[:, pair_lanes(i)]
        query_grads, key_grads, value_grads = [], [], []
        for half in range(2):
            share = attention[m, 2 * i + half]
            own = jnp.where(low == (half == 0), mixed_grad, jnp.zeros_like(mixed_grad))
            value_grads.append(product(share, mixed_grad))
            share_grad = product(values, own, 1, 1)
            weight = share.astype(jnp.float32)
            weighted = weight * share_grad
            score_grad = weighted - weight * jnp.sum(weighted, axis=0, keepdims=True)
            score_grad = score_grad.astype(jnp.bfloat16)
            query_grads.append(product(score_grad, keys, 0, 0))
            key_grads.append(product(score_grad, queries))
        query_grad = jnp.where(low, query_grads[0], query_grads[1]) * HEAD_DIM**-0.5
        key_grad = jnp.where(low, key_grads[0], key_grads[1])
        value_grad = jnp.where(low, value_grads[0], value_grads[1])
        qkv[m, :, pair_lanes(i)] = turn(query_grad, tables, True).astype(jnp.bfloat16)
        qkv[m, :, pair_lanes(i + pairs)] = turn(key_grad, tables, True).astype(jnp.bfloat16)
        qkv[m, :, pair_lanes(i + 2 * pairs)] = value_grad.astype(jnp.bfloat16)
        return carry

    lax.fori_loop(0, pairs, heads, 0, unroll=8)

    def project(i, carry):
        at = rows_at(i, JOINT_STEP)
        total[:, at] += product(qkv[m], joint[at, :], 1, 1)
        return carry

    lax.fori_loop(0, width // JOINT_STEP, project, 0)

    def norm(i, carry):
        at = rows_at(i, ROW_STEP)
        standard, inverse = statistics(x[m, at, :].astype(jnp.float32))
        normed_grad = total[at, :]
        gain_sum[...] += jnp.sum(normed_grad * standard, axis=0, keepdims=True)
        offset_sum[...] += jnp.sum(normed_grad, axis=0, keepdims=True)
        scaled = normed_grad * gain[...]
        inner_mean = jnp.mean(scaled, axis=-1, keepdims=True)
        along = jnp.mean(scaled * standard, axis=-1, keepdims=True)
        change = inverse * (scaled - inner_mean - standard * along)
        result[m, at, :] = (upstream[m, at, :].astype(jnp.float32) + change).astype(jnp.bfloat16)
        return carry

    lax.fori_loop(0, SLOT // ROW_STEP, norm, 0)


def vector_rows(width):
    return max(1, width // LANES), max(1, LANES // width)


def lane_range(device, width):
    lane = lax.broadcasted_iota(jnp.int32, (1, LANES), 1)
    start = device * width % LANES
    return (lane >= start) & (lane < start + width)


def unpack_vectors(small, devices, vectors):
    width = vectors[0].shape[1] // devices
    wide = vectors[3].shape[1] // devices

    def gathered(index, shared):
        rows = small[pl.ds(pl.multiple_of(index * shared * SMALL_ROWS, SMALL_ROWS), SMALL_ROWS), :]
        total = rows.astype(jnp.float32)
        for other in range(1, shared):
            at = pl.multiple_of((index * shared + other) * SMALL_ROWS, SMALL_ROWS)
            total += small[pl.ds(at, SMALL_ROWS), :].astype(jnp.float32)
        return total

    _, shared = vector_rows(width)

    def narrow(index, carry):
        total = gathered(index, shared)
        at = rows_at(index, LANES)
        for i in range(3):
            vectors[i][:, at] = total[i : i + 1]
        return carry

    lax.fori_loop(0, devices // shared, narrow, 0)
    count, shared_wide = vector_rows(wide)

    def broad(index, carry):
        total = gathered(index, shared_wide)
        for i in range(count):
            vectors[3][:, rows_at(index * count + i, LANES)] = total[3 + i : 4 + i]
        return carry

    lax.fori_loop(0, devices // shared_wide, broad, 0)


def pack_sums(sums, devices, packed):
    width = sums[0].shape[1] // devices
    wide = sums[3].shape[1] // devices
    count, _ = vector_rows(wide)
    row = lax.broadcasted_iota(jnp.int32, (SMALL_ROWS, LANES), 0)

    def device(index, carry):
        rows = []
        inside = lane_range(index, width)
        for i in range(3):
            rows.append(jnp.where(inside, sums[i][:, rows_at(index * width // LANES, LANES)], 0.0))
        for i in range(count):
            line = sums[3][:, rows_at(index * wide // LANES + i, LANES)]
            rows.append(line if wide >= LANES else jnp.where(lane_range(index, wide), line, 0.0))
        block = jnp.zeros((SMALL_ROWS, LANES), jnp.float32)
        for i, line in enumerate(rows):
            block = jnp.where(row == i, line, block)
        packed[rows_at(index, SMALL_ROWS), :] = block.astype(jnp.bfloat16)
        return carry

    lax.fori_loop(0, devices, device, 0)


def blocks_kernel(pieces, *refs):
    lengths, hidden_in, cotangent, tables_in = refs[:4]
    sources = refs[4:9]
    hidden_out, input_grad = refs[9:11]
    factor_outs, packed = refs[11:17], refs[17]
    weights, small = refs[18:22], refs[22]
    x, normed, qkv, attention, mixture, active, slope, total, result = refs[23:32]
    upstream, mixture_grad, tables = refs[32:35]
    vectors, sums = refs[35:39], refs[39:43]
    table_sem, in_keep, in_send, in_receive, hand_send, hand_receive = refs[43:49]
    half_send, half_receive, half_keep, out_sem = refs[49:53]
    here = Place()
    section = lax.axis_index("section")
    partner = {"section": 1 - section}
    half = hidden_out.shape[1]
    devices = 4 * here.levels

    def keeping(source, target, start, m):
        return pltpu.make_async_copy(
            source.at[rows_at(m, SLOT), :], target.at[m, :, pl.ds(start, half)], in_keep.at[m]
        )

    def halving(source, target, start, m):
        return pltpu.make_async_remote_copy(
            source.at[rows_at(m, SLOT), :],
            target.at[m, :, pl.ds(start, half)],
            in_send.at[m],
            in_receive.at[m],
            device_id=partner,
            device_id_type=MESH,
        )

    def handing(target, m):
        return pltpu.make_async_remote_copy(
            result.at[m],
            target.at[m],
            hand_send.at[m],
            hand_receive.at[m],
            device_id=partner,
            device_id_type=MESH,
        )

    def away(target, start, m):
        return pltpu.make_async_remote_copy(
            result.at[m, :, pl.ds(start, half)],
            target.at[rows_at(m, SLOT), :],
            half_send.at[m],
            half_receive.at[m],
            device_id=partner,
            device_id_type=MESH,
        )

    def kept(target, start, m):
        return pltpu.make_async_copy(
            result.at[m, :, pl.ds(start, half)], target.at[rows_at(m, SLOT), :], half_keep.at[m]
        )

    def stored(m):
        return pltpu.make_async_copy(
            result.at[m], input_grad.at[rows_at(m, SLOT), :], half_keep.at[m]
        )

    def giving(i, source, m):
        return pltpu.make_async_copy(
            source.at[m], factor_outs[i].at[rows_at(m, SLOT), :], out_sem.at[i, m]
        )

    reading = pltpu.make_async_copy(tables_in, tables, table_sem.at[0])
    reading.start()
    for m in range(MICRO):
        pl.when(section == 0)(lambda m=m: keeping(hidden_in, x, 0, m).start())
        pl.when(section == 1)(lambda m=m: keeping(cotangent, upstream, half, m).start())
    for total_sum in sums:
        total_sum[...] = jnp.zeros_like(total_sum)
    greet(here, True)
    owns = [piece.of(sources[piece.array]) for piece in pieces]
    spread = Spread(here, pieces, owns, [*weights, small], refs[53:])
    early = [p for p, piece in enumerate(pieces) if piece.array in (0, 1, 4)]
    late = [p for p, piece in enumerate(pieces) if piece.array in (2, 3)]
    spread.begin_all(early)
    for m in range(MICRO):
        pl.when(section == 1)(lambda m=m: halving(hidden_in, x, half, m).start())
        pl.when(section == 0)(lambda m=m: halving(cotangent, upstream, 0, m).start())
    shared = {
        "state": (x, normed, qkv, attention, mixture, active, slope, total, result),
        "weights": weights,
        "vectors": vectors,
        "tables": tables,
        "gradients": (upstream, mixture_grad),
        "sums": sums,
    }
    spread.middle(early, lambda: spread.begin_all(late))
    spread.received(early)
    unpack_vectors(small, devices, vectors)
    reading.wait()

    @pl.when(section == 0)
    def _():
        def ahead(m, carry):
            keeping(hidden_in, x, 0, m).wait()
            halving(hidden_in, x, half, m).wait_recv()
            attend(m, lengths[m], shared)
            return carry

        lax.fori_loop(0, MICRO, ahead, 0)

    spread.middle(late)
    spread.received(late)

    def forward(m, carry):
        @pl.when(section == 1)
        def _():
            handing(x, m).wait_recv()
            attend(m, lengths[m], shared)

        feed(m, shared)

        @pl.when(section == 0)
        def _():
            pl.when(m > 0)(lambda: handing(x, m - 1).wait_send())
            handing(x, m).start()

        @pl.when(section == 1)
        def _():
            away(hidden_out, 0, m).start()
            kept(hidden_out, half, m).start()

        for i, source in enumerate((normed, mixture, active)):
            giving(i, source, m).start()
        return carry

    lax.fori_loop(0, MICRO, forward, 0)

    def backward(m, carry):
        @pl.when(section == 0)
        def _():
            pl.when(m == 0)(lambda: handing(x, MICRO - 1).wait_send())
            handing(upstream, m).wait_recv()

        @pl.when(section == 1)
        def _():
            away(hidden_out, 0, m).wait_send()
            kept(hidden_out, half, m).wait()
            keeping(cotangent, upstream, half, m).wait()
            halving(cotangent, upstream, 0, m).wait_recv()
            row = lax.broadcasted_iota(jnp.int32, (SLOT, 1), 0)
            inside = (row < lengths[m]).astype(jnp.float32)
            masked = upstream[m].astype(jnp.float32) * inside
            upstream[m] = masked.astype(jnp.bfloat16)

        backward_block(m, shared)

        @pl.when(section == 1)
        def _():
            handing(upstream, m).start()

        pl.when(section == 0)(lambda: stored(m).start())
        for i, source in enumerate((qkv, slope, upstream)):
            giving(3 + i, source, m).start()
        return carry

    lax.fori_loop(0, MICRO, backward, 0)
    pack_sums(sums, devices, packed)

    def last(m, carry):
        @pl.when(section == 0)
        def _():
            halving(cotangent, upstream, 0, m).wait_send()
            stored(m).wait()
            away(hidden_out, 0, m).wait_recv()

        @pl.when(section == 1)
        def _():
            halving(hidden_in, x, half, m).wait_send()
            handing(upstream, m).wait_send()

        for i, source in enumerate((normed, mixture, active, qkv, slope, upstream)):
            giving(i, source, m).wait()
        return carry

    lax.fori_loop(0, MICRO, last, 0)
    spread.sent()


def run_blocks(lengths, hidden_in, cotangent, owns, number):
    levels = lax.axis_size("batch") // 4
    devices = 4 * levels
    tokens, half = hidden_in.shape
    width = half * lax.axis_size("section")
    wide = owns[2].shape[1]
    low, full = jnp.bfloat16, jnp.float32
    shape = jax.ShapeDtypeStruct
    vmem = pltpu.VMEM
    dma = pltpu.SemaphoreType.DMA
    pieces = pieces_of([own.shape for own in owns])
    outputs = [shape((tokens, half), low), shape((tokens, width), low)]
    outputs += [shape((tokens, n), low) for n in (width, width, wide, 3 * width, wide, width)]
    outputs += [shape((devices * SMALL_ROWS, LANES), low)]
    scratch = [vmem((devices * own.shape[0], own.shape[1]), low) for own in owns]
    scratch += [
        vmem((MICRO, SLOT, width), low),
        vmem((MICRO, SLOT, width), low),
        vmem((MICRO, SLOT, 3 * width), low),
        vmem((MICRO, HEADS, SLOT, SLOT), low),
        vmem((MICRO, SLOT, width), low),
        vmem((MICRO, SLOT, wide), low),
        vmem((MICRO, SLOT, wide), low),
        vmem((SLOT, width), full),
        vmem((MICRO, SLOT, width), low),
        vmem((MICRO, SLOT, width), low),
        vmem((SLOT, width), low),
        vmem((3, SLOT, 2 * HEAD_DIM), full),
    ]
    scratch += [vmem((1, n), full) for n in (width, width, width, wide)] * 2
    scratch += [dma((1,))] + [dma((MICRO,))] * 8 + [dma((6, MICRO))]
    scratch += spread_semaphores(len(pieces), levels)
    return pl.pallas_call(
        partial(blocks_kernel, pieces),
        out_shape=outputs,
        in_specs=[pl.BlockSpec(memory_space=pltpu.SMEM)] + [ANY] * 8,
        out_specs=[ANY] * 8 + [pl.BlockSpec(memory_space=vmem)],
        scratch_shapes=scratch,
        compiler_params=pltpu.CompilerParams(
            collective_id=number, has_side_effects=True, vmem_limit_bytes=60 * 2**20
        ),
        name="two_blocks",
    )(lengths, hidden_in, cotangent, jnp.asarray(rotary_rows()), *owns)


def pack_vectors(vectors):
    device = lax.axis_index("batch")
    size = SMALL_ROWS * LANES
    total = jnp.zeros((1, size), jnp.bfloat16)
    row = 0
    for vector in vectors:
        width = vector.shape[1]
        used = min(width, LANES)
        slot = device * width % LANES // used
        for i in range(LANES // used):
            start = row * LANES + i * used
            moved = jnp.pad(vector, ((0, 0), (start, size - start - width)))
            total = total + jnp.where(slot == i, moved, jnp.zeros_like(moved))
        row += max(1, width // LANES)
    return total.reshape(SMALL_ROWS, LANES)


def widen_kernel(devices, *refs):
    small, sources = refs[0], refs[1 : (len(refs) - 5) // 2 + 1]
    targets, vectors = refs[len(sources) + 1 : -4], refs[-4:]
    pl.when(pl.program_id(0) == 0)(lambda: unpack_vectors(small, devices, vectors))
    for source, target in zip(sources, targets):
        target[...] = source[...].astype(target.dtype).reshape(target.shape)


def widen(small, sums, kept, widths, devices):
    steps = 4
    arrays = [*sums, *kept]
    whole = lambda i: (0, 0)
    in_specs = [
        pl.BlockSpec((array.shape[0] // steps, array.shape[1]), lambda i: (i, 0))
        for array in arrays
    ]
    out_specs = [
        pl.BlockSpec((1, array.shape[0] // steps, array.shape[1]), lambda i: (0, i, 0))
        for array in sums
    ] + in_specs[len(sums) :]
    out_specs += [pl.BlockSpec((1, width), whole) for width in widths]
    shapes = [jax.ShapeDtypeStruct((1, *array.shape), jnp.float32) for array in sums]
    shapes += [jax.ShapeDtypeStruct(array.shape, array.dtype) for array in kept]
    shapes += [jax.ShapeDtypeStruct((1, width), jnp.float32) for width in widths]
    return pl.pallas_call(
        partial(widen_kernel, devices),
        out_shape=shapes,
        grid=(steps,),
        in_specs=[pl.BlockSpec(small.shape, whole)] + in_specs,
        out_specs=out_specs,
        compiler_params=pltpu.CompilerParams(vmem_limit_bytes=60 * 2**20),
        name="widen",
    )(small, *arrays)


def local(
    hidden_in,
    cotangent,
    lengths,
    norm_gain,
    norm_offset,
    joint_weight,
    output_weight,
    expand_weight,
    inner_bias,
    contract_weight,
    outer_bias,
):
    devices = lax.axis_size("batch")
    owns = [
        joint_weight[0],
        output_weight[0],
        expand_weight[0],
        contract_weight[0],
        pack_vectors((norm_gain, norm_offset, outer_bias, inner_bias)),
    ]
    results = run_blocks(lengths, hidden_in, cotangent, owns, 1)
    shapes = [(own.shape[0] * devices, own.shape[1]) for own in owns[:4]]
    *sums, small_sum, own_grad = reduce_all(results[2:8], results[8], results[1], shapes, 2)
    width, wide = norm_gain.shape[1] * devices, inner_bias.shape[1] * devices
    (
        joint_sum,
        output_sum,
        expand_sum,
        contract_sum,
        hidden_out,
        input_grad,
        gain_sum,
        offset_sum,
        outer_sum,
        inner_sum,
    ) = widen(small_sum, sums, [results[0], own_grad], (width, width, width, wide), devices)
    return (
        hidden_out,
        input_grad,
        gain_sum,
        offset_sum,
        joint_sum,
        output_sum,
        expand_sum,
        inner_sum,
        contract_sum,
        outer_sum,
    )


def solution(mesh):
    return jax.shard_map(
        local,
        mesh=mesh,
        in_specs=(
            P("batch", "section"),
            P("batch", "section"),
            P("batch"),
            P("section", "batch"),
            P("section", "batch"),
            P("section", "batch", None),
            P("section", "batch", None),
            P("section", "batch", None),
            P("section", "batch"),
            P("section", "batch", None),
            P("section", "batch"),
        ),
        out_specs=(
            P("batch", "section"),
            P("batch", "section"),
            P("section", None),
            P("section", None),
            P("section", None, None),
            P("section", None, None),
            P("section", None, None),
            P("section", None),
            P("section", None, None),
            P("section", None),
        ),
        check_vma=False,
    )
```

```python
from functools import partial

import jax
import jax.numpy as jnp
import numpy as np
from jax import lax
from jax.experimental import pallas as pl
from jax.experimental.pallas import tpu as pltpu
from jax.sharding import PartitionSpec as P

HEADS = 16
HEAD_DIM = 64
ROT = 32
SLOT = 256
MICRO = 2
SMALL_ROWS = 16
LANES = 128
ROW_STEP = 256
FF_STEP = 4096
JOINT_STEP = 1024
GELU_SCALE = (2.0 / np.pi) ** 0.5
GELU_CUBE = 0.044715
norm_epsilon = 1e-05
rotary_base = 10000.0
masked_score = -1e30
MESH = pl.DeviceIdType.MESH
ANY = pl.BlockSpec(memory_space=pl.ANY)


class Place:
    def __init__(self):
        index = lax.axis_index("batch")
        self.levels = lax.axis_size("batch") // 4
        self.last = self.levels - 1
        self.z, self.y, self.c = index // 4, index // 2 % 2, index % 2

    def at(self, z=None, y=None, c=None):
        z = self.z if z is None else z
        y = self.y if y is None else y
        c = self.c if c is None else c
        return z * 4 + y * 2 + c


class Piece:
    def __init__(self, array, offset, rows, column, columns, direct):
        self.array, self.offset, self.rows = array, offset, rows
        self.column, self.columns, self.direct = column, columns, direct

    def sides(self, y):
        return (y,) if self.direct else (y, 1 - y)

    def of(self, block):
        return block.at[pl.ds(self.offset, self.rows), pl.ds(self.column, self.columns)]


def pieces_of(blocks):
    joint, output, expand, contract, small = blocks
    cut = contract[0] // 4
    pieces = [
        Piece(1, 0, output[0], 0, output[1], False),
        Piece(3, 0, cut, 0, contract[1], False),
    ]
    for array, offset, (rows, columns), parts in (
        (0, 0, joint, 1),
        (2, 0, expand, 1),
        (3, cut, contract, 1),
        (4, 0, small, 1),
    ):
        for i in range(parts):
            width = columns // parts
            pieces.append(Piece(array, offset, rows - offset, i * width, width, True))
    return pieces


def remote(source, target, send, receive, index):
    return pltpu.make_async_remote_copy(
        source, target, send, receive, device_id={"batch": index}, device_id_type=MESH
    )


def greet(here, with_section):
    barrier = pltpu.get_barrier_semaphore()

    def signal(**who):
        pl.semaphore_signal(barrier, inc=1, device_id=who, device_id_type=MESH)

    signal(batch=here.at(y=1 - here.y))
    signal(batch=here.at(c=1 - here.c))
    pl.when(here.z > 0)(lambda: signal(batch=here.at(z=here.z - 1)))
    pl.when(here.z < here.last)(lambda: signal(batch=here.at(z=here.z + 1)))
    waits = 2
    if with_section:
        signal(section=1 - lax.axis_index("section"))
        waits = 3
    below = jnp.minimum(here.z, 1)
    above = jnp.minimum(here.last - here.z, 1)
    pl.semaphore_wait(barrier, waits + below + above)


def spread_semaphores(count, levels):
    dma = pltpu.SemaphoreType.DMA
    return [
        dma((count,)),
        dma((count, levels, 2, 2)),
        dma((count, levels, 2)),
        dma((count, levels)),
        dma((count, levels)),
        dma((count, levels, 2)),
        dma((count, levels, 2)),
    ]


class Spread:
    def __init__(self, here, pieces, owns, outs, semaphores):
        self.here, self.pieces, self.owns, self.outs = here, pieces, owns, outs
        (self.keep, self.zs, self.zr, self.ys, self.yr, self.cs, self.cr) = semaphores

    def block(self, p, z, y, c):
        piece = self.pieces[p]
        out = self.outs[piece.array]
        rows = out.shape[0] // (4 * self.here.levels)
        start = (z * 4 + y * 2 + c) * rows + piece.offset
        return out.at[
            pl.ds(pl.multiple_of(start, 8), piece.rows), pl.ds(piece.column, piece.columns)
        ]

    def along(self, p, z, y, source, way):
        here = self.here
        if way == 0:
            target = jnp.minimum(here.z + 1, here.last)
        else:
            target = jnp.maximum(here.z - 1, 0)
        return remote(
            source,
            self.block(p, z, y, here.c),
            self.zs.at[p, z, y, way],
            self.zr.at[p, z, y],
            here.at(z=target),
        )

    def across(self, p, z, source):
        here = self.here
        target = self.block(p, z, here.y, here.c)
        return remote(source, target, self.ys.at[p, z], self.yr.at[p, z], here.at(y=1 - here.y))

    def beside(self, p, z, y, source):
        here = self.here
        target = self.block(p, z, y, here.c)
        return remote(
            source, target, self.cs.at[p, z, y], self.cr.at[p, z, y], here.at(c=1 - here.c)
        )

    def both_ways(self, p, y, source):
        here = self.here
        pl.when(here.z < here.last)(lambda: self.along(p, here.z, y, source, 0).start())
        pl.when(here.z > 0)(lambda: self.along(p, here.z, y, source, 1).start())

    def begin(self, p, held=False):
        here, own = self.here, self.owns[p]
        self.across(p, here.z, own).start()
        if not held:
            self.both_ways(p, here.y, own)
        self.beside(p, here.z, here.y, own).start()
        target = self.block(p, here.z, here.y, here.c)
        pltpu.make_async_copy(own, target, self.keep.at[p]).start()

    def begin_all(self, chosen):
        order = sorted(chosen, key=lambda p: self.pieces[p].direct)
        for p in order:
            self.begin(p, held=not self.pieces[p].direct)
        for p in order:
            if not self.pieces[p].direct:
                self.both_ways(p, self.here.y, self.owns[p])

    def from_z(self, p, z, y, way):
        here = self.here
        block = self.block(p, z, y, here.c)
        self.along(p, z, y, block, way).wait_recv()
        more = here.z < here.last if way == 0 else here.z > 0
        pl.when(more)(lambda: self.along(p, z, y, block, way).start())
        if self.pieces[p].direct:
            self.across(p, z, block).start()
        self.beside(p, z, y, block).start()

    def from_y(self, p, z):
        here = self.here
        block = self.block(p, z, 1 - here.y, here.c)
        self.across(p, z, block).wait_recv()
        if not self.pieces[p].direct:
            self.both_ways(p, 1 - here.y, block)
        self.beside(p, z, 1 - here.y, block).start()

    def z_events(self, chosen, distance):
        here = self.here

        def pair(p, side):
            y = self.pieces[p].sides(here.y)[side]
            pl.when(here.z - distance >= 0)(lambda: self.from_z(p, here.z - distance, y, 0))
            pl.when(here.z + distance <= here.last)(
                lambda: self.from_z(p, here.z + distance, y, 1)
            )

        for p in chosen:
            if self.pieces[p].direct:
                pair(p, 0)
        for side in range(2):
            for p in chosen:
                if not self.pieces[p].direct:
                    pair(p, side)

    def y_events(self, chosen, z):
        for p in chosen:
            if self.pieces[p].direct:
                self.from_y(p, z)

    def middle(self, chosen, then=None):
        here = self.here
        for p in chosen:
            if not self.pieces[p].direct:
                self.from_y(p, here.z)

        def y_pair(distance):
            pl.when(here.z - distance >= 0)(lambda: self.y_events(chosen, here.z - distance))
            pl.when((here.z + distance <= here.last) & (distance > 0))(
                lambda: self.y_events(chosen, here.z + distance)
            )

        def step(distance, carry):
            self.z_events(chosen, distance)
            y_pair(distance - 1)
            return carry

        lax.fori_loop(1, here.levels, step, 0)
        if then is not None:
            then()
        y_pair(here.last)

    def received(self, chosen):
        here = self.here

        def level(z, carry):
            for p in chosen:
                own = self.block(p, z, here.y, here.c)
                for y in range(2):
                    self.beside(p, z, y, own).wait_recv()
            return carry

        lax.fori_loop(0, here.levels, level, 0)
        for p in chosen:
            block = self.block(p, here.z, here.y, here.c)
            pltpu.make_async_copy(block, block, self.keep.at[p]).wait()

    def sent(self):
        here = self.here

        def level(z, carry):
            for p, piece in enumerate(self.pieces):
                own = self.block(p, z, here.y, here.c)
                for y in range(2):
                    self.beside(p, z, y, own).wait_send()
                crossed = z >= 0 if piece.direct else z == here.z
                pl.when(crossed)(lambda p=p, own=own: self.across(p, z, own).wait_send())
                for y in piece.sides(here.y):
                    pl.when((z <= here.z) & (here.z < here.last))(
                        lambda p=p, y=y, own=own: self.along(p, z, y, own, 0).wait_send()
                    )
                    pl.when((z >= here.z) & (here.z > 0))(
                        lambda p=p, y=y, own=own: self.along(p, z, y, own, 1).wait_send()
                    )
            return carry

        lax.fori_loop(0, here.levels, level, 0)


def add_rows(target, other):
    rows = target.shape[0]
    step = min(rows, 64)

    def body(i, carry):
        at = pl.ds(pl.multiple_of(i * step, step), step)
        total = target[at, :].astype(jnp.float32) + other[at, :].astype(jnp.float32)
        target[at, :] = total.astype(target.dtype)
        return carry

    lax.fori_loop(0, rows // step, body, 0)


FACTORS = ((0, 3), (1, 5), (0, 4), (2, 5))
MAKE_ORDER = (3, 1, 2, 0, 4)
COLUMN_STEP = 1024


class Reduce:
    def __init__(self, here, pieces, factors, small, product_rows, buffers, semaphores):
        self.here, self.pieces, self.factors, self.small = here, pieces, factors, small
        self.made = product_rows
        self.mine, self.sent, self.sib, self.yb, self.zb = buffers
        (self.load, self.cs, self.cr, self.ys, self.yr, self.zs, self.zr, self.credit) = semaphores

    def level(self, i):
        here = self.here
        above, below = here.last - here.z, here.z
        lead = jnp.maximum(above, below) - jnp.minimum(above, below)
        single = jnp.where(above > below, here.last - i, i)
        later = i - lead
        distance = jnp.minimum(above, below) - later // 2
        outer = jnp.where(above > below, here.z - distance, here.z + distance)
        paired = jnp.where(later % 2 == 0, outer, 2 * here.z - outer)
        return jnp.where(i < lead, single, paired)

    def to_core(self, p, slot, y):
        here = self.here
        return remote(
            self.sent[p].at[slot, y],
            self.sib[p].at[slot, y],
            self.cs.at[p, slot, y],
            self.cr.at[p, slot, y],
            here.at(c=1 - here.c),
        )

    def to_y(self, p, z):
        here = self.here
        return remote(
            self.mine[p].at[z, 1 - here.y],
            self.yb[p].at[z if self.pieces[p].direct else 0],
            self.ys.at[p, z],
            self.yr.at[p, z],
            here.at(y=1 - here.y),
        )

    def slot(self, z, at_z, way):
        if way == 0:
            return z
        return jnp.where(z == at_z, self.here.levels, z)

    def to_z(self, p, z, y, way):
        here = self.here
        step = 1 if way == 0 else -1
        slot = self.slot(z, here.z + step, way)
        side = 0 if self.pieces[p].direct else y
        return remote(
            self.mine[p].at[z, y],
            self.zb[p].at[slot, side],
            self.zs.at[p, z, side],
            self.zr.at[p, slot, side],
            here.at(z=here.z + step),
        )

    def arrive(self, p, z, y, way):
        here = self.here
        slot = self.slot(z, here.z, way)
        side = 0 if self.pieces[p].direct else y
        block = self.zb[p].at[slot, side]
        remote(
            block, block, self.zs.at[p, z, side], self.zr.at[p, slot, side], here.at(y=1 - here.y)
        ).wait_recv()
        add_rows(self.mine[p].at[z, y], block)

    def store(self, array, z, slot, y, own, value, column):
        for p, piece in enumerate(self.pieces):
            first = max(column, piece.column)
            end = min(column + value.shape[1], piece.column + piece.columns)
            if piece.array == array and first < end:
                target = self.mine[p].at[z, y] if own else self.sent[p].at[slot, y]
                part = value[piece.offset : piece.offset + piece.rows, first - column : end - column]
                target[:, first - piece.column : end - piece.column] = part.astype(jnp.bfloat16)

    def make(self, array, z, slot):
        here = self.here
        rows = max(p.offset + p.rows for p in self.pieces if p.array == array)
        cores = ((False, 1 - here.c), (True, here.c))
        if array == 4:
            for own, c in cores:
                for y in range(2):
                    at = pl.multiple_of((z * 4 + y * 2 + c) * rows, 16)
                    self.store(array, z, slot, y, own, self.small[pl.ds(at, rows), :], 0)
            return
        left, right = (self.factors[i] for i in FACTORS[array])
        columns = right.shape[1]
        tiles = range(0, columns, COLUMN_STEP)
        if rows % 128 == 0:
            for own, c in cores:
                for y in range(2):
                    at = pl.multiple_of((z * 4 + y * 2 + c) * rows, 128)
                    turned = left[:, pl.ds(at, rows)].T
                    for tile in tiles:
                        value = product(turned, right[:, tile : tile + COLUMN_STEP])
                        self.store(array, z, slot, y, own, value, tile)
            return
        span = max(4 * rows, 128)
        start = z * 4 * rows // span * span
        turned = left[:, pl.ds(pl.multiple_of(start, 128), span)].T
        for tile in tiles:
            self.made[:span, :] = product(turned, right[:, tile : tile + COLUMN_STEP])
            for own, c in cores:
                for y in range(2):
                    at = pl.multiple_of((z * 4 + y * 2 + c) * rows - start, 8)
                    self.store(array, z, slot, y, own, self.made[pl.ds(at, rows), :], tile)

    def of(self, array):
        return [p for p, piece in enumerate(self.pieces) if piece.array == array]

    def build(self, i, waits):
        here = self.here
        z, slot = self.level(i), i % 2

        @pl.when(i >= 2)
        def _():
            for p in range(len(self.pieces)):
                for y in range(2):
                    self.to_core(p, slot, y).wait_send()
            pl.semaphore_wait(self.credit, 1)

        def add(array):
            for p in self.of(array):
                for y in range(2):
                    self.to_core(p, slot, y).wait_recv()
                    add_rows(self.mine[p].at[z, y], self.sib[p].at[slot, y])
                if self.pieces[p].direct:
                    self.to_y(p, z).start()
                else:
                    self.pass_on(z, [p])

        for step, array in enumerate(MAKE_ORDER):
            waits(i, array)
            self.make(array, z, slot)
            for p in self.of(array):
                for y in range(2):
                    self.to_core(p, slot, y).start()
            if step > 0:
                add(MAKE_ORDER[step - 1])
        add(MAKE_ORDER[-1])

        @pl.when(i < here.levels - 2)
        def _():
            other = {"batch": here.at(c=1 - here.c)}
            pl.semaphore_signal(self.credit, inc=1, device_id=other, device_id_type=MESH)

    def rows(self, p, z):
        self.to_y(p, z).wait_recv()
        source = self.yb[p].at[z if self.pieces[p].direct else 0]
        add_rows(self.mine[p].at[z, self.here.y], source)

    def pass_on(self, z, chosen):
        here = self.here

        def hop(way):
            further = here.z > 0 if way == 0 else here.z < here.last
            for p in chosen:
                if self.pieces[p].direct:
                    self.rows(p, z)
                for y in self.pieces[p].sides(here.y):
                    pl.when(further)(lambda p=p, y=y: self.arrive(p, z, y, way))
                    self.to_z(p, z, y, way).start()

        pl.when(z > here.z)(lambda: hop(0))
        pl.when(z < here.z)(lambda: hop(1))

    def run(self, waits):
        here = self.here
        made = [p for array in MAKE_ORDER for p in self.of(array)]
        direct = [p for p in made if self.pieces[p].direct]

        def step(i, carry):
            self.build(i, waits)
            pl.when(i > 0)(lambda: self.pass_on(self.level(i - 1), direct))
            return carry

        lax.fori_loop(0, here.levels, step, 0)

    def settle(self, p):
        here = self.here
        for y in self.pieces[p].sides(here.y):
            pl.when(here.z > 0)(lambda y=y: self.arrive(p, here.z, y, 0))
            pl.when(here.z < here.last)(lambda y=y: self.arrive(p, here.z, y, 1))

    def finish(self):
        here = self.here
        for slot in range(min(2, here.levels)):
            for p in range(len(self.pieces)):
                for y in range(2):
                    self.to_core(p, slot, y).wait_send()

        def level(z, carry):
            for p, piece in enumerate(self.pieces):
                crossed = z >= 0 if piece.direct else z == here.z
                pl.when(crossed)(lambda p=p: self.to_y(p, z).wait_send())
                for y in piece.sides(here.y):
                    pl.when(z > here.z)(lambda p=p, y=y: self.to_z(p, z, y, 0).wait_send())
                    pl.when(z < here.z)(lambda p=p, y=y: self.to_z(p, z, y, 1).wait_send())
            return carry

        lax.fori_loop(0, here.levels, level, 0)


def reduce_kernel(pieces, *refs):
    count = len(pieces)
    sources, change, outs, input_grad, rest = refs[:7], refs[7], refs[8:13], refs[13], refs[14:]
    factors, small, made = rest[:6], rest[6], rest[7]
    rest = rest[8:]
    buffers = [rest[i * count : (i + 1) * count] for i in range(5)]
    rest = rest[5 * count :]
    here = Place()
    loads = [
        pltpu.make_async_copy(source, target, rest[0].at[i])
        for i, (source, target) in enumerate(zip(sources, [*factors, small]))
    ]
    order = (2, 5, 1, 0, 4, 3, 6)
    for i in order:
        loads[i].start()
    greet(here, True)
    section = lax.axis_index("section")
    half = input_grad.shape[1]
    over = pltpu.make_async_remote_copy(
        change.at[:, pl.ds(half, half)],
        input_grad,
        rest[-1].at[0],
        rest[-1].at[1],
        device_id={"section": 1 - section},
        device_id_type=MESH,
    )
    keep = pltpu.make_async_copy(change.at[:, pl.ds(0, half)], input_grad, rest[-1].at[2])

    @pl.when(section == 0)
    def _():
        over.start()
        keep.start()

    reduce = Reduce(here, pieces, factors, small, made, buffers, rest[:8])
    needs = {3: (2, 5), 1: (1,), 2: (0, 4), 0: (3,), 4: (6,)}

    def waits(i, array):
        @pl.when(i == 0)
        def _():
            for k in needs[array]:
                loads[k].wait()

    reduce.run(waits)
    owns = [buffers[0][p].at[here.z, here.y] for p in range(count)]
    spread = Spread(here, pieces, owns, outs, rest[8:-1])
    turned = [p for p in range(count) if not pieces[p].direct]
    for p in turned:
        reduce.settle(p)
        reduce.to_y(p, here.z).start()
    for p in range(count):
        if pieces[p].direct:
            reduce.rows(p, here.z)
            reduce.settle(p)
            spread.begin(p)
    for p in turned:
        reduce.rows(p, here.z)
        spread.begin(p)
    spread.middle(range(count))
    reduce.finish()
    spread.received(range(count))
    spread.sent()

    @pl.when(section == 0)
    def _():
        over.wait_send()
        keep.wait()

    pl.when(section == 1)(over.wait_recv)


def reduce_all(factors, small, change, shapes, number):
    levels = lax.axis_size("batch") // 4
    shapes = [*shapes, small.shape]
    pieces = pieces_of([(rows // (4 * levels), columns) for rows, columns in shapes])
    count = len(pieces)
    dma = pltpu.SemaphoreType.DMA
    low = jnp.bfloat16
    scratch = [pltpu.VMEM(factor.shape, low) for factor in factors]
    scratch += [pltpu.VMEM(small.shape, low), pltpu.VMEM((256, COLUMN_STEP), jnp.float32)]
    blocks = [(piece.rows, piece.columns) for piece in pieces]
    scratch += [pltpu.VMEM((levels, 2) + block, low) for block in blocks]
    scratch += [pltpu.VMEM((2, 2) + block, low) for block in blocks] * 2
    scratch += [
        pltpu.VMEM((levels if piece.direct else 1,) + block, low)
        for piece, block in zip(pieces, blocks)
    ]
    scratch += [
        pltpu.VMEM((levels + 1, 1 if piece.direct else 2) + block, low)
        for piece, block in zip(pieces, blocks)
    ]
    scratch += [
        dma((7,)),
        dma((count, 2, 2)),
        dma((count, 2, 2)),
        dma((count, levels)),
        dma((count, levels)),
        dma((count, levels, 2)),
        dma((count, levels + 1, 2)),
        pltpu.SemaphoreType.REGULAR,
    ]
    scratch += spread_semaphores(count, levels) + [dma((3,))]
    results = [*shapes, (change.shape[0], change.shape[1] // 2)]
    return pl.pallas_call(
        partial(reduce_kernel, pieces),
        out_shape=[jax.ShapeDtypeStruct(shape, low) for shape in results],
        in_specs=[ANY] * 8,
        out_specs=[ANY] * 6,
        scratch_shapes=scratch,
        compiler_params=pltpu.CompilerParams(
            collective_id=number, has_side_effects=True, vmem_limit_bytes=60 * 2**20
        ),
        name="reduce_gradients",
    )(*factors, small, change)


def rotary_rows():
    positions = np.arange(SLOT, dtype=np.float64)[:, None]
    lane = np.arange(2 * HEAD_DIM)[None, :] % HEAD_DIM
    angles = positions * rotary_base ** (-(lane // 2 * 2.0) / ROT)
    turned = lane < ROT
    cosine = np.where(turned, np.cos(angles), 1.0)
    sine = np.where(turned, np.sin(angles), 0.0)
    even = np.where(lane % 2 == 0, sine, 0.0)
    odd = np.where(lane % 2 == 1, sine, 0.0)
    return np.stack([cosine, even, odd]).astype(np.float32)


def turn(pair, tables, back):
    lanes = pair.shape[1]
    following = pltpu.roll(pair, lanes - 1, 1)
    preceding = pltpu.roll(pair, 1, 1)
    side = following * tables[1] - preceding * tables[2]
    return pair * tables[0] + (side if back else -side)


def product(left, right, left_axis=1, right_axis=0):
    return lax.dot_general(
        left, right, (((left_axis,), (right_axis,)), ((), ())), preferred_element_type=jnp.float32
    )


def statistics(rows):
    average = jnp.mean(rows, axis=-1, keepdims=True)
    centered = rows - average
    variance = jnp.mean(centered * centered, axis=-1, keepdims=True)
    inverse = lax.rsqrt(variance + norm_epsilon)
    return centered * inverse, inverse


def low_lanes(width):
    return lax.broadcasted_iota(jnp.int32, (1, width), 1) < HEAD_DIM


def pair_lanes(index):
    return pl.ds(pl.multiple_of(index * 2 * HEAD_DIM, 2 * HEAD_DIM), 2 * HEAD_DIM)


def rows_at(index, step):
    return pl.ds(pl.multiple_of(index * step, step), step)


def attend(m, length, refs):
    (x, normed, qkv, attention, mixture, active, slope, total, result) = refs["state"]
    joint, output, expand, contract = refs["weights"]
    gain, offset, outer, inner = refs["vectors"]
    tables = refs["tables"]
    width = x.shape[2]

    def norm(i, carry):
        at = rows_at(i, ROW_STEP)
        standard, _ = statistics(x[m, at, :].astype(jnp.float32))
        normed[m, at, :] = (standard * gain[...] + offset[...]).astype(jnp.bfloat16)
        return carry

    lax.fori_loop(0, SLOT // ROW_STEP, norm, 0)
    for part in range(3):
        scale = HEAD_DIM**-0.5 if part == 0 else 1.0
        total[...] = product(normed[m], joint[:, part * width : (part + 1) * width])
        if part == 2:
            qkv[m, :, 2 * width :] = total[...].astype(jnp.bfloat16)
        else:

            def rotary(i, carry, part=part, scale=scale):
                pair = turn(total[:, pair_lanes(i)], tables, False)
                at = pair_lanes(i + part * (width // (2 * HEAD_DIM)))
                qkv[m, :, at] = pair.astype(jnp.bfloat16) * jnp.bfloat16(scale)
                return carry

            lax.fori_loop(0, width // (2 * HEAD_DIM), rotary, 0, unroll=8)

    key = lax.broadcasted_iota(jnp.int32, (SLOT, SLOT), 0)
    query = lax.broadcasted_iota(jnp.int32, (SLOT, SLOT), 1)
    allowed = (key <= query) & (key < length)
    pairs = width // (2 * HEAD_DIM)
    low = low_lanes(2 * HEAD_DIM)

    def heads(i, carry):
        queries, keys = qkv[m, :, pair_lanes(i)], qkv[m, :, pair_lanes(i + pairs)]
        values = qkv[m, :, pair_lanes(i + 2 * pairs)]
        mixed = []
        for half in range(2):
            own = jnp.where(low == (half == 0), queries, jnp.zeros_like(queries))
            scores = jnp.where(allowed, product(keys, own, 1, 1), masked_score)
            raised = jnp.exp(scores - jnp.max(scores, axis=0, keepdims=True))
            share = raised * (1.0 / jnp.sum(raised, axis=0, keepdims=True))
            share = share.astype(jnp.bfloat16)
            attention[m, 2 * i + half] = share
            mixed.append(product(share, values, 0, 0))
        mixture[m, :, pair_lanes(i)] = jnp.where(low, mixed[0], mixed[1]).astype(jnp.bfloat16)
        return carry

    lax.fori_loop(0, pairs, heads, 0, unroll=8)


def feed(m, refs):
    (x, normed, _, _, mixture, active, slope, total, result) = refs["state"]
    joint, output, expand, contract = refs["weights"]
    gain, offset, outer, inner = refs["vectors"]
    total[...] = x[m].astype(jnp.float32) + outer[...] + product(mixture[m], output[...])

    def hidden(i, carry):
        at = rows_at(i, FF_STEP)
        pre = product(normed[m], expand[:, at]) + inner[:, at]
        square = pre * pre
        bend = jnp.tanh(GELU_SCALE * (pre + GELU_CUBE * (square * pre)))
        lifted = 0.5 * (1.0 + bend)
        slant = (0.5 * GELU_SCALE) * (1.0 + (3.0 * GELU_CUBE) * square)
        slope[m, :, at] = (lifted + pre * (1.0 - bend * bend) * slant).astype(jnp.bfloat16)
        activated = (pre * lifted).astype(jnp.bfloat16)
        active[m, :, at] = activated
        total[...] += product(activated, contract[at, :])
        return carry

    lax.fori_loop(0, slope.shape[2] // FF_STEP, hidden, 0)
    result[m] = total[...].astype(jnp.bfloat16)


def backward_block(m, refs):
    (x, _, qkv, attention, _, _, slope, total, result) = refs["state"]
    joint, output, expand, contract = refs["weights"]
    gain, offset, outer, inner = refs["vectors"]
    upstream, mixture_grad = refs["gradients"]
    gain_sum, offset_sum, outer_sum, inner_sum = refs["sums"]
    tables = refs["tables"]
    width = x.shape[2]
    outer_sum[...] += jnp.sum(upstream[m].astype(jnp.float32), axis=0, keepdims=True)
    mixture_grad[...] = product(upstream[m], output[...], 1, 1).astype(jnp.bfloat16)
    total[...] = jnp.zeros_like(total)

    def hidden(i, carry):
        at = rows_at(i, FF_STEP)
        active_grad = product(upstream[m], contract[at, :], 1, 1)
        pre_grad = (active_grad * slope[m, :, at].astype(jnp.float32)).astype(jnp.bfloat16)
        slope[m, :, at] = pre_grad
        inner_sum[:, at] += jnp.sum(pre_grad.astype(jnp.float32), axis=0, keepdims=True)
        total[...] += product(pre_grad, expand[:, at], 1, 1)
        return carry

    lax.fori_loop(0, slope.shape[2] // FF_STEP, hidden, 0)
    pairs = width // (2 * HEAD_DIM)
    low = low_lanes(2 * HEAD_DIM)

    def heads(i, carry):
        queries, keys = qkv[m, :, pair_lanes(i)], qkv[m, :, pair_lanes(i + pairs)]
        values = qkv[m, :, pair_lanes(i + 2 * pairs)]
        mixed_grad = mixture_grad[:, pair_lanes(i)]
        query_grads, key_grads, value_grads = [], [], []
        for half in range(2):
            share = attention[m, 2 * i + half]
            own = jnp.where(low == (half == 0), mixed_grad, jnp.zeros_like(mixed_grad))
            value_grads.append(product(share, mixed_grad))
            share_grad = product(values, own, 1, 1)
            weight = share.astype(jnp.float32)
            weighted = weight * share_grad
            score_grad = weighted - weight * jnp.sum(weighted, axis=0, keepdims=True)
            score_grad = score_grad.astype(jnp.bfloat16)
            query_grads.append(product(score_grad, keys, 0, 0))
            key_grads.append(product(score_grad, queries))
        query_grad = jnp.where(low, query_grads[0], query_grads[1]) * HEAD_DIM**-0.5
        key_grad = jnp.where(low, key_grads[0], key_grads[1])
        value_grad = jnp.where(low, value_grads[0], value_grads[1])
        qkv[m, :, pair_lanes(i)] = turn(query_grad, tables, True).astype(jnp.bfloat16)
        qkv[m, :, pair_lanes(i + pairs)] = turn(key_grad, tables, True).astype(jnp.bfloat16)
        qkv[m, :, pair_lanes(i + 2 * pairs)] = value_grad.astype(jnp.bfloat16)
        return carry

    lax.fori_loop(0, pairs, heads, 0, unroll=8)

    def project(i, carry):
        at = rows_at(i, JOINT_STEP)
        total[:, at] += product(qkv[m], joint[at, :], 1, 1)
        return carry

    lax.fori_loop(0, width // JOINT_STEP, project, 0)

    def norm(i, carry):
        at = rows_at(i, ROW_STEP)
        standard, inverse = statistics(x[m, at, :].astype(jnp.float32))
        normed_grad = total[at, :]
        gain_sum[...] += jnp.sum(normed_grad * standard, axis=0, keepdims=True)
        offset_sum[...] += jnp.sum(normed_grad, axis=0, keepdims=True)
        scaled = normed_grad * gain[...]
        inner_mean = jnp.mean(scaled, axis=-1, keepdims=True)
        along = jnp.mean(scaled * standard, axis=-1, keepdims=True)
        change = inverse * (scaled - inner_mean - standard * along)
        result[m, at, :] = (upstream[m, at, :].astype(jnp.float32) + change).astype(jnp.bfloat16)
        return carry

    lax.fori_loop(0, SLOT // ROW_STEP, norm, 0)


def vector_rows(width):
    return max(1, width // LANES), max(1, LANES // width)


def lane_range(device, width):
    lane = lax.broadcasted_iota(jnp.int32, (1, LANES), 1)
    start = device * width % LANES
    return (lane >= start) & (lane < start + width)


def unpack_vectors(small, devices, vectors):
    width = vectors[0].shape[1] // devices
    wide = vectors[3].shape[1] // devices

    def gathered(index, shared):
        rows = small[pl.ds(pl.multiple_of(index * shared * SMALL_ROWS, SMALL_ROWS), SMALL_ROWS), :]
        total = rows.astype(jnp.float32)
        for other in range(1, shared):
            at = pl.multiple_of((index * shared + other) * SMALL_ROWS, SMALL_ROWS)
            total += small[pl.ds(at, SMALL_ROWS), :].astype(jnp.float32)
        return total

    _, shared = vector_rows(width)

    def narrow(index, carry):
        total = gathered(index, shared)
        at = rows_at(index, LANES)
        for i in range(3):
            vectors[i][:, at] = total[i : i + 1]
        return carry

    lax.fori_loop(0, devices // shared, narrow, 0)
    count, shared_wide = vector_rows(wide)

    def broad(index, carry):
        total = gathered(index, shared_wide)
        for i in range(count):
            vectors[3][:, rows_at(index * count + i, LANES)] = total[3 + i : 4 + i]
        return carry

    lax.fori_loop(0, devices // shared_wide, broad, 0)


def pack_sums(sums, devices, packed):
    width = sums[0].shape[1] // devices
    wide = sums[3].shape[1] // devices
    count, _ = vector_rows(wide)
    row = lax.broadcasted_iota(jnp.int32, (SMALL_ROWS, LANES), 0)

    def device(index, carry):
        rows = []
        inside = lane_range(index, width)
        for i in range(3):
            rows.append(jnp.where(inside, sums[i][:, rows_at(index * width // LANES, LANES)], 0.0))
        for i in range(count):
            line = sums[3][:, rows_at(index * wide // LANES + i, LANES)]
            rows.append(line if wide >= LANES else jnp.where(lane_range(index, wide), line, 0.0))
        block = jnp.zeros((SMALL_ROWS, LANES), jnp.float32)
        for i, line in enumerate(rows):
            block = jnp.where(row == i, line, block)
        packed[rows_at(index, SMALL_ROWS), :] = block.astype(jnp.bfloat16)
        return carry

    lax.fori_loop(0, devices, device, 0)


def blocks_kernel(pieces, *refs):
    lengths, hidden_in, cotangent, tables_in = refs[:4]
    sources = refs[4:9]
    hidden_out, input_grad = refs[9:11]
    factor_outs, packed = refs[11:17], refs[17]
    weights, small = refs[18:22], refs[22]
    x, normed, qkv, attention, mixture, active, slope, total, result = refs[23:32]
    upstream, mixture_grad, tables = refs[32:35]
    vectors, sums = refs[35:39], refs[39:43]
    table_sem, in_keep, in_send, in_receive, hand_send, hand_receive = refs[43:49]
    half_send, half_receive, half_keep, out_sem = refs[49:53]
    here = Place()
    section = lax.axis_index("section")
    partner = {"section": 1 - section}
    half = hidden_out.shape[1]
    devices = 4 * here.levels

    def keeping(source, target, start, m):
        return pltpu.make_async_copy(
            source.at[rows_at(m, SLOT), :], target.at[m, :, pl.ds(start, half)], in_keep.at[m]
        )

    def halving(source, target, start, m):
        return pltpu.make_async_remote_copy(
            source.at[rows_at(m, SLOT), :],
            target.at[m, :, pl.ds(start, half)],
            in_send.at[m],
            in_receive.at[m],
            device_id=partner,
            device_id_type=MESH,
        )

    def handing(target, m):
        return pltpu.make_async_remote_copy(
            result.at[m],
            target.at[m],
            hand_send.at[m],
            hand_receive.at[m],
            device_id=partner,
            device_id_type=MESH,
        )

    def away(target, start, m):
        return pltpu.make_async_remote_copy(
            result.at[m, :, pl.ds(start, half)],
            target.at[rows_at(m, SLOT), :],
            half_send.at[m],
            half_receive.at[m],
            device_id=partner,
            device_id_type=MESH,
        )

    def kept(target, start, m):
        return pltpu.make_async_copy(
            result.at[m, :, pl.ds(start, half)], target.at[rows_at(m, SLOT), :], half_keep.at[m]
        )

    def stored(m):
        return pltpu.make_async_copy(
            result.at[m], input_grad.at[rows_at(m, SLOT), :], half_keep.at[m]
        )

    def giving(i, source, m):
        return pltpu.make_async_copy(
            source.at[m], factor_outs[i].at[rows_at(m, SLOT), :], out_sem.at[i, m]
        )

    reading = pltpu.make_async_copy(tables_in, tables, table_sem.at[0])
    reading.start()
    for m in range(MICRO):
        pl.when(section == 0)(lambda m=m: keeping(hidden_in, x, 0, m).start())
        pl.when(section == 1)(lambda m=m: keeping(cotangent, upstream, half, m).start())
    for total_sum in sums:
        total_sum[...] = jnp.zeros_like(total_sum)
    greet(here, True)
    owns = [piece.of(sources[piece.array]) for piece in pieces]
    spread = Spread(here, pieces, owns, [*weights, small], refs[53:])
    early = [p for p, piece in enumerate(pieces) if piece.array in (0, 1, 4)]
    late = [p for p, piece in enumerate(pieces) if piece.array in (2, 3)]
    spread.begin_all(early)
    for m in range(MICRO):
        pl.when(section == 1)(lambda m=m: halving(hidden_in, x, half, m).start())
        pl.when(section == 0)(lambda m=m: halving(cotangent, upstream, 0, m).start())
    shared = {
        "state": (x, normed, qkv, attention, mixture, active, slope, total, result),
        "weights": weights,
        "vectors": vectors,
        "tables": tables,
        "gradients": (upstream, mixture_grad),
        "sums": sums,
    }
    spread.middle(early, lambda: spread.begin_all(late))
    spread.received(early)
    unpack_vectors(small, devices, vectors)
    reading.wait()

    @pl.when(section == 0)
    def _():
        def ahead(m, carry):
            keeping(hidden_in, x, 0, m).wait()
            halving(hidden_in, x, half, m).wait_recv()
            attend(m, lengths[m], shared)
            return carry

        lax.fori_loop(0, MICRO, ahead, 0)

    spread.middle(late)
    spread.received(late)

    def forward(m, carry):
        @pl.when(section == 1)
        def _():
            handing(x, m).wait_recv()
            attend(m, lengths[m], shared)

        feed(m, shared)

        @pl.when(section == 0)
        def _():
            pl.when(m > 0)(lambda: handing(x, m - 1).wait_send())
            handing(x, m).start()

        @pl.when(section == 1)
        def _():
            away(hidden_out, 0, m).start()
            kept(hidden_out, half, m).start()

        for i, source in enumerate((normed, mixture, active)):
            giving(i, source, m).start()
        return carry

    lax.fori_loop(0, MICRO, forward, 0)

    def backward(m, carry):
        @pl.when(section == 0)
        def _():
            pl.when(m == 0)(lambda: handing(x, MICRO - 1).wait_send())
            handing(upstream, m).wait_recv()

        @pl.when(section == 1)
        def _():
            away(hidden_out, 0, m).wait_send()
            kept(hidden_out, half, m).wait()
            keeping(cotangent, upstream, half, m).wait()
            halving(cotangent, upstream, 0, m).wait_recv()
            row = lax.broadcasted_iota(jnp.int32, (SLOT, 1), 0)
            inside = (row < lengths[m]).astype(jnp.float32)
            masked = upstream[m].astype(jnp.float32) * inside
            upstream[m] = masked.astype(jnp.bfloat16)

        backward_block(m, shared)

        @pl.when(section == 1)
        def _():
            handing(upstream, m).start()

        pl.when(section == 0)(lambda: stored(m).start())
        for i, source in enumerate((qkv, slope, upstream)):
            giving(3 + i, source, m).start()
        return carry

    lax.fori_loop(0, MICRO, backward, 0)
    pack_sums(sums, devices, packed)

    def last(m, carry):
        @pl.when(section == 0)
        def _():
            halving(cotangent, upstream, 0, m).wait_send()
            stored(m).wait()
            away(hidden_out, 0, m).wait_recv()

        @pl.when(section == 1)
        def _():
            halving(hidden_in, x, half, m).wait_send()
            handing(upstream, m).wait_send()

        for i, source in enumerate((normed, mixture, active, qkv, slope, upstream)):
            giving(i, source, m).wait()
        return carry

    lax.fori_loop(0, MICRO, last, 0)
    spread.sent()


def run_blocks(lengths, hidden_in, cotangent, owns, number):
    levels = lax.axis_size("batch") // 4
    devices = 4 * levels
    tokens, half = hidden_in.shape
    width = half * lax.axis_size("section")
    wide = owns[2].shape[1]
    low, full = jnp.bfloat16, jnp.float32
    shape = jax.ShapeDtypeStruct
    vmem = pltpu.VMEM
    dma = pltpu.SemaphoreType.DMA
    pieces = pieces_of([own.shape for own in owns])
    outputs = [shape((tokens, half), low), shape((tokens, width), low)]
    outputs += [shape((tokens, n), low) for n in (width, width, wide, 3 * width, wide, width)]
    outputs += [shape((devices * SMALL_ROWS, LANES), low)]
    scratch = [vmem((devices * own.shape[0], own.shape[1]), low) for own in owns]
    scratch += [
        vmem((MICRO, SLOT, width), low),
        vmem((MICRO, SLOT, width), low),
        vmem((MICRO, SLOT, 3 * width), low),
        vmem((MICRO, HEADS, SLOT, SLOT), low),
        vmem((MICRO, SLOT, width), low),
        vmem((MICRO, SLOT, wide), low),
        vmem((MICRO, SLOT, wide), low),
        vmem((SLOT, width), full),
        vmem((MICRO, SLOT, width), low),
        vmem((MICRO, SLOT, width), low),
        vmem((SLOT, width), low),
        vmem((3, SLOT, 2 * HEAD_DIM), full),
    ]
    scratch += [vmem((1, n), full) for n in (width, width, width, wide)] * 2
    scratch += [dma((1,))] + [dma((MICRO,))] * 8 + [dma((6, MICRO))]
    scratch += spread_semaphores(len(pieces), levels)
    return pl.pallas_call(
        partial(blocks_kernel, pieces),
        out_shape=outputs,
        in_specs=[pl.BlockSpec(memory_space=pltpu.SMEM)] + [ANY] * 8,
        out_specs=[ANY] * 8 + [pl.BlockSpec(memory_space=vmem)],
        scratch_shapes=scratch,
        compiler_params=pltpu.CompilerParams(
            collective_id=number, has_side_effects=True, vmem_limit_bytes=60 * 2**20
        ),
        name="two_blocks",
    )(lengths, hidden_in, cotangent, jnp.asarray(rotary_rows()), *owns)


def pack_vectors(vectors):
    device = lax.axis_index("batch")
    size = SMALL_ROWS * LANES
    total = jnp.zeros((1, size), jnp.bfloat16)
    row = 0
    for vector in vectors:
        width = vector.shape[1]
        used = min(width, LANES)
        slot = device * width % LANES // used
        for i in range(LANES // used):
            start = row * LANES + i * used
            moved = jnp.pad(vector, ((0, 0), (start, size - start - width)))
            total = total + jnp.where(slot == i, moved, jnp.zeros_like(moved))
        row += max(1, width // LANES)
    return total.reshape(SMALL_ROWS, LANES)


def widen_kernel(devices, *refs):
    small, sources = refs[0], refs[1 : (len(refs) - 5) // 2 + 1]
    targets, vectors = refs[len(sources) + 1 : -4], refs[-4:]
    pl.when(pl.program_id(0) == 0)(lambda: unpack_vectors(small, devices, vectors))
    for source, target in zip(sources, targets):
        target[...] = source[...].astype(target.dtype).reshape(target.shape)


def widen(small, sums, kept, widths, devices):
    steps = 4
    arrays = [*sums, *kept]
    whole = lambda i: (0, 0)
    in_specs = [
        pl.BlockSpec((array.shape[0] // steps, array.shape[1]), lambda i: (i, 0))
        for array in arrays
    ]
    out_specs = [
        pl.BlockSpec((1, array.shape[0] // steps, array.shape[1]), lambda i: (0, i, 0))
        for array in sums
    ] + in_specs[len(sums) :]
    out_specs += [pl.BlockSpec((1, width), whole) for width in widths]
    shapes = [jax.ShapeDtypeStruct((1, *array.shape), jnp.float32) for array in sums]
    shapes += [jax.ShapeDtypeStruct(array.shape, array.dtype) for array in kept]
    shapes += [jax.ShapeDtypeStruct((1, width), jnp.float32) for width in widths]
    return pl.pallas_call(
        partial(widen_kernel, devices),
        out_shape=shapes,
        grid=(steps,),
        in_specs=[pl.BlockSpec(small.shape, whole)] + in_specs,
        out_specs=out_specs,
        compiler_params=pltpu.CompilerParams(vmem_limit_bytes=60 * 2**20),
        name="widen",
    )(small, *arrays)


def local(
    hidden_in,
    cotangent,
    lengths,
    norm_gain,
    norm_offset,
    joint_weight,
    output_weight,
    expand_weight,
    inner_bias,
    contract_weight,
    outer_bias,
):
    devices = lax.axis_size("batch")
    owns = [
        joint_weight[0],
        output_weight[0],
        expand_weight[0],
        contract_weight[0],
        pack_vectors((norm_gain, norm_offset, outer_bias, inner_bias)),
    ]
    results = run_blocks(lengths, hidden_in, cotangent, owns, 1)
    shapes = [(own.shape[0] * devices, own.shape[1]) for own in owns[:4]]
    *sums, small_sum, own_grad = reduce_all(results[2:8], results[8], results[1], shapes, 2)
    width, wide = norm_gain.shape[1] * devices, inner_bias.shape[1] * devices
    (
        joint_sum,
        output_sum,
        expand_sum,
        contract_sum,
        hidden_out,
        input_grad,
        gain_sum,
        offset_sum,
        outer_sum,
        inner_sum,
    ) = widen(small_sum, sums, [results[0], own_grad], (width, width, width, wide), devices)
    return (
        hidden_out,
        input_grad,
        gain_sum,
        offset_sum,
        joint_sum,
        output_sum,
        expand_sum,
        inner_sum,
        contract_sum,
        outer_sum,
    )


def solution(mesh):
    return jax.shard_map(
        local,
        mesh=mesh,
        in_specs=(
            P("batch", "section"),
            P("batch", "section"),
            P("batch"),
            P("section", "batch"),
            P("section", "batch"),
            P("section", "batch", None),
            P("section", "batch", None),
            P("section", "batch", None),
            P("section", "batch"),
            P("section", "batch", None),
            P("section", "batch"),
        ),
        out_specs=(
            P("batch", "section"),
            P("batch", "section"),
            P("section", None),
            P("section", None),
            P("section", None, None),
            P("section", None, None),
            P("section", None, None),
            P("section", None),
            P("section", None, None),
            P("section", None),
        ),
        check_vma=False,
    )
```
